32 devices in a mesh: dp: 16 (over z, y, core), seq: 2 (over x).
Axes of the slice: x: 2, y: 2, z: 4, core: 2. Of those that a mesh axis runs over, the one named last changes fastest.
Arguments:
- tokens: bfloat16 [64, 128, 1536], P(('dp', 'seq')), may hold values from -6 to 6
- cotangent: bfloat16 [64, 128, 1536], P(('dp', 'seq')), may hold values from -6 to 6
- w_query: bfloat16 [1536, 1536], P('dp'), may hold values from -0.15625 to 0.15625
- w_key: bfloat16 [1536, 768], P('dp'), may hold values from -0.15625 to 0.15625
- w_value: bfloat16 [1536, 768], P('dp'), may hold values from -0.15625 to 0.15625
- w_out: bfloat16 [1536, 1536], P('dp'), may hold values from -0.625 to 0.625
- w_gate: bfloat16 [1536, 4096], P('dp'), may hold values from -0.15625 to 0.15625
- w_up: bfloat16 [1536, 4096], P('dp'), may hold values from -0.15625 to 0.15625
- w_down: bfloat16 [4096, 1536], P('dp'), may hold values from -0.09375 to 0.09375
- gain_attn: bfloat16 [1536], P('dp'), may hold values from 0.5 to 1.5
- gain_mlp: bfloat16 [1536], P('dp'), may hold values from 0.5 to 1.5
Outputs:
- block_out: bfloat16 [64, 128, 1536], P(('dp', 'seq'))
- grad_tokens: bfloat16 [64, 128, 1536], P(('dp', 'seq'))
- grad_query: float32 [1536, 1536], P('dp')
- grad_key: float32 [1536, 768], P('dp')
- grad_value: float32 [1536, 768], P('dp')
- grad_out: float32 [1536, 1536], P('dp')
- grad_gate: float32 [1536, 4096], P('dp')
- grad_up: float32 [1536, 4096], P('dp')
- grad_down: float32 [4096, 1536], P('dp')
- grad_gain_attn: float32 [1536], P('dp')
- grad_gain_mlp: float32 [1536], P('dp')
The draws below stay inside these ranges and needn't reach their ends.
All inputs are finite; a program needn't handle non-finite values.
Results may differ from the reference program's by a relative error of at most 0.015.
Values may be sent and summed in bfloat16 or wider, within the bound.
A program may use at most 256 MiB of HBM per device.

```python
import jax
import jax.numpy as jnp
from jax import lax

D = 1536
HEADS = 16
KV_HEADS = 8
HD = 96
FF = 4096
LEN = 128
MB = 2
B = 64


def spiked(result, key, source, target, blocks, factor):
    def block_of(position):
        return (jnp.arange(result.shape[position]) // (result.shape[position] // blocks)).reshape((-1,) + (1,) * (result.ndim - 1 - position))

    near = jax.random.permutation(key, blocks)[block_of(target)]
    far = (block_of(target) + blocks // 2) % blocks
    return jnp.where((block_of(source) == near) | (block_of(source) == far), factor * result, result)


def block_scale(key, dims, split, low, largest):
    gain, own = 1.0, jax.random.fold_in(key, 6)
    for dim, shards_of in split:
        heights = jnp.exp(jax.random.uniform(jax.random.fold_in(own, dim), (shards_of,), jnp.float32, low / len(split), largest / len(split)))
        gain = gain * jnp.repeat(heights, dims[dim] // shards_of).reshape([-1 if axis == dim else 1 for axis in range(len(dims))])
    return gain


def normal_values(rng, shape, scale, reach, split=(), held_as=jnp.bfloat16):
    level = block_scale(rng, shape, split, -0.22, 0.18) if split else 1.0
    values = jax.random.normal(rng, shape, jnp.float32) * scale * level
    return jnp.minimum(jnp.maximum(values, -reach), reach).astype(held_as)


def gaussian_with(key, dims, scale, reach, cuts, heavy, kind=jnp.bfloat16):
    drawn = scale * jax.random.normal(key, dims, jnp.float32)
    if cuts:
        drawn = drawn * block_scale(key, dims, cuts, -0.22, 0.18)
    return jnp.clip(spiked(drawn, jax.random.fold_in(key, 3), *heavy), -reach, reach).astype(kind)


def setup_inputs(seed: int = 0) -> dict:
    seeds = jax.random.split(jax.random.key(seed), 12)
    tokens = gaussian_with(seeds[0], (B, LEN, D), 1.0, 6.0, ((0, 32),), (0, 2, 32, 2.75))
    cotangent = normal_values(seeds[1], (B, LEN, D), 1.0, 6.0, ((0, 32),))
    w_query = normal_values(seeds[2], (D, HEADS * HD), D ** -0.5, 0.15625, ((0, 16),))
    w_key = normal_values(seeds[3], (D, KV_HEADS * HD), D ** -0.5, 0.15625, ((0, 16),))
    w_value = normal_values(seeds[4], (D, KV_HEADS * HD), D ** -0.5, 0.15625, ((0, 16),))
    w_out = normal_values(seeds[5], (HEADS * HD, D), (HEADS * HD // 16) ** -0.5, 0.625, ((0, 16),))
    w_gate = normal_values(seeds[6], (D, FF), D ** -0.5, 0.15625, ((0, 16),))
    w_up = normal_values(seeds[7], (D, FF), D ** -0.5, 0.15625, ((0, 16),))
    w_down = normal_values(seeds[8], (FF, D), FF ** -0.5, 0.09375, ((0, 16),))
    gain_attn = jnp.clip(1.0 + 0.1 * jax.random.normal(seeds[9], (D,), jnp.float32), 0.5, 1.5).astype(jnp.bfloat16)
    gain_mlp = jnp.clip(1.0 + 0.1 * jax.random.normal(seeds[10], (D,), jnp.float32), 0.5, 1.5).astype(jnp.bfloat16)
    return {"tokens": tokens, "cotangent": cotangent, "w_query": w_query, "w_key": w_key, "w_value": w_value, "w_out": w_out, "w_gate": w_gate, "w_up": w_up, "w_down": w_down, "gain_attn": gain_attn, "gain_mlp": gain_mlp}


EPS = 1e-05
THETA = 100000.0

@jax.custom_vjp
def low(v):
    return lax.optimization_barrier(v.astype(jnp.bfloat16)).astype(jnp.float32)

@jax.custom_vjp
def low_back(v):
    return v

def low_keep(v):
    return (low(v), None)

def low_pass(kept, grad):
    return (grad,)

def back_keep(v):
    return (v, None)

def back_low(kept, grad):
    return (low(grad),)
low.defvjp(low_keep, low_pass)
low_back.defvjp(back_keep, back_low)

def rotary(positions, width):
    steps_half = jnp.arange(width // 2, dtype=jnp.float32)
    frequency = jnp.power(THETA, -2.0 * steps_half / width)
    angles = positions[:, None] * frequency[None, :]
    cosine = jnp.cos(angles)
    sine = jnp.sin(angles)
    return (jnp.concatenate([cosine, cosine], -1), jnp.concatenate([sine, sine], -1))

def rotate(values, cosine, sine):
    half_width = values.shape[-1] // 2
    first_half = values[..., :half_width]
    second_half = values[..., half_width:]
    turned = jnp.concatenate([-second_half, first_half], -1)
    return values * cosine[:, None, :] + turned * sine[:, None, :]

def matmul_high(left, right):
    return jnp.einsum('...d,de->...e', left, right, precision=lax.Precision.HIGHEST)

def rms_scaled(values, gain_vec):
    return values * lax.rsqrt(lax.optimization_barrier(jnp.mean(values * values, axis=-1, keepdims=True)) + EPS) * gain_vec

def attend(queries, keys, values):
    length = queries.shape[0]
    grouped = queries.reshape(length, KV_HEADS, HEADS // KV_HEADS, HD)
    scores = low_back(HD ** (-0.5) * jnp.einsum('qkgd,ckd->kgqc', grouped, keys, precision=lax.Precision.HIGHEST))
    causal = jnp.arange(length)[:, None] >= jnp.arange(length)[None, :]
    scores = jnp.where(causal, scores, -jnp.inf)
    top_score = lax.optimization_barrier(jnp.max(scores, -1, keepdims=True))
    exps = jnp.exp(scores - top_score)
    probs = exps / lax.optimization_barrier(jnp.sum(exps, -1, keepdims=True))
    mixed = jnp.einsum('kgqc,ckd->qkgd', low(probs), values, precision=lax.Precision.HIGHEST)
    return mixed.reshape(length, HEADS * HD)

def block_forward(inputs, w_query, w_key, w_value, w_out, w_gate, w_up, w_down, gain_attn, gain_mlp):
    micro = inputs.shape[0]
    cosine, sine = rotary(jnp.arange(LEN, dtype=jnp.float32), HD)
    normed = low(rms_scaled(inputs, gain_attn))
    queries = low(rotate(low_back(matmul_high(normed, w_query)).reshape(micro, LEN, HEADS, HD), cosine, sine))
    keys = low(rotate(low_back(matmul_high(normed, w_key)).reshape(micro, LEN, KV_HEADS, HD), cosine, sine))
    values = low(low_back(matmul_high(normed, w_value))).reshape(micro, LEN, KV_HEADS, HD)
    mixed = lax.map(lambda pieces: jax.checkpoint(attend)(pieces[0], pieces[1], pieces[2]), (queries, keys, values))
    mixed = low(low_back(mixed))
    hidden_one = inputs + low_back(matmul_high(mixed, w_out))
    normed_two = low(rms_scaled(hidden_one, gain_mlp))
    gate_act = low_back(matmul_high(normed_two, w_gate))
    up_act = low_back(matmul_high(normed_two, w_up))
    product = low(jax.nn.silu(gate_act) * up_act)
    return hidden_one + matmul_high(product, w_down)

def reference(tokens, cotangent, w_query, w_key, w_value, w_out, w_gate, w_up, w_down, gain_attn, gain_mlp):
    weights = (w_query.astype(jnp.float32), w_key.astype(jnp.float32), w_value.astype(jnp.float32), w_out.astype(jnp.float32), w_gate.astype(jnp.float32), w_up.astype(jnp.float32), w_down.astype(jnp.float32), gain_attn.astype(jnp.float32), gain_mlp.astype(jnp.float32))
    inputs_all = tokens.astype(jnp.float32).reshape(B // MB, MB, LEN, D)
    cots_all = cotangent.astype(jnp.float32).reshape(B // MB, MB, LEN, D)

    def group_step(totals, pieces):
        outputs, pullback = jax.vjp(block_forward, pieces[0], *weights)
        grads = pullback(pieces[1])
        totals = tuple((total + grad for total, grad in zip(totals, grads[1:])))
        return (totals, (outputs.astype(jnp.bfloat16), grads[0].astype(jnp.bfloat16)))
    start = tuple((jnp.zeros(weight.shape, jnp.float32) for weight in weights))
    totals, (outs_block, outs_grad) = lax.scan(group_step, start, (inputs_all, cots_all))
    return (outs_block.reshape(B, LEN, D), outs_grad.reshape(B, LEN, D), totals[0], totals[1], totals[2], totals[3], totals[4], totals[5], totals[6], totals[7], totals[8])
```

```python
import jax
import jax.numpy as jnp
from jax import lax
from jax.sharding import PartitionSpec as P

HD = 96
EPS = 1e-05
THETA = 100000.0


def rotary(positions, width):
    steps_half = jnp.arange(width // 2, dtype=jnp.float32)
    frequency = jnp.power(THETA, -2.0 * steps_half / width)
    angles = positions[:, None] * frequency[None, :]
    cosine = jnp.cos(angles)
    sine = jnp.sin(angles)
    return (jnp.concatenate([cosine, cosine], -1), jnp.concatenate([sine, sine], -1))


def rotate(values, cosine, sine):
    half = values.shape[-1] // 2
    turned = jnp.concatenate([-values[..., half:], values[..., :half]], -1)
    return values * cosine[:, None, :] + turned * sine[:, None, :]


def rotate_back(grads, cosine, sine):
    half = grads.shape[-1] // 2
    sined = grads * sine[:, None, :]
    turned = jnp.concatenate([sined[..., half:], -sined[..., :half]], -1)
    return grads * cosine[:, None, :] + turned


def dot32(left, right):
    return jnp.dot(left, right, preferred_element_type=jnp.float32)


def dot_t(left, right):
    return lax.dot_general(left, right, (((1,), (1,)), ((), ())), preferred_element_type=jnp.float32)


def dot_l(left, right):
    return lax.dot_general(left, right, (((0,), (0,)), ((), ())), preferred_element_type=jnp.float32)


def inv_rms(values):
    return lax.rsqrt(jnp.mean(values * values, axis=-1, keepdims=True) + EPS)


def low(values):
    return values.astype(jnp.bfloat16)


def attend(queries, keys, values):
    rows = queries.shape[1]
    ids = jnp.arange(rows, dtype=jnp.int32)
    visible = ids[:, None] >= ids[None, :]
    scores = HD ** (-0.5) * jnp.einsum("bqkgd,bckd->bkgqc", queries, keys, preferred_element_type=jnp.float32)
    scores = jnp.where(visible, scores, -jnp.inf)
    top = jnp.max(scores, -1, keepdims=True)
    exps = jnp.exp(scores - top)
    probs = exps / jnp.sum(exps, -1, keepdims=True)
    mixed = jnp.einsum("bkgqc,bckd->bqkgd", low(probs), values, preferred_element_type=jnp.float32)
    return probs, low(mixed)


def attend_back(queries, keys, values, probs, grad_mixed):
    grad_values = jnp.einsum("bkgqc,bqkgd->bckd", low(probs), grad_mixed, preferred_element_type=jnp.float32)
    grad_probs = jnp.einsum("bqkgd,bckd->bkgqc", grad_mixed, values, preferred_element_type=jnp.float32)
    grad_scores = low(probs * (grad_probs - jnp.sum(probs * grad_probs, -1, keepdims=True)))
    scale = HD ** (-0.5)
    grad_queries = scale * jnp.einsum("bkgqc,bckd->bqkgd", grad_scores, keys, preferred_element_type=jnp.float32)
    grad_keys = scale * jnp.einsum("bkgqc,bqkgd->bckd", grad_scores, queries, preferred_element_type=jnp.float32)
    return grad_queries, grad_keys, grad_values


def mlp_grads(gate, up, grad_hidden):
    sigma = jax.nn.sigmoid(gate)
    silu = gate * sigma
    hidden = low(silu * up)
    grad_gate = low(grad_hidden * up * sigma * (1.0 + gate * (1.0 - sigma)))
    grad_up = low(grad_hidden * silu)
    return hidden, grad_gate, grad_up


def shards_plain(tokens, cotangent, w_query, w_key, w_value, w_out, w_gate, w_up, w_down, gain_attn, gain_mlp):
    seqs, length, width = tokens.shape
    rows = seqs * length
    kv_heads = w_key.shape[1] // HD
    groups = w_query.shape[1] // w_key.shape[1]
    gather = lambda w: lax.all_gather(w, "dp", axis=0, tiled=True)
    full_query, full_key, full_value, full_out = map(gather, (w_query, w_key, w_value, w_out))
    gains = gather(jnp.stack([gain_attn, gain_mlp], 1)).astype(jnp.float32)
    gain_one, gain_two = gains[:, 0], gains[:, 1]
    full_gate, full_up, full_down = map(gather, (w_gate, w_up, w_down))
    cosine, sine = rotary(jnp.arange(length, dtype=jnp.float32), HD)
    cosine, sine = jnp.tile(cosine, (seqs, 1)), jnp.tile(sine, (seqs, 1))

    inputs = tokens.reshape(rows, width).astype(jnp.float32)
    grad_in = cotangent.reshape(rows, width)
    scale_one = inv_rms(inputs)
    normed = low(inputs * scale_one * gain_one)
    queries = low(rotate(dot32(normed, full_query).reshape(rows, -1, HD), cosine, sine))
    keys = low(rotate(dot32(normed, full_key).reshape(rows, -1, HD), cosine, sine))
    values = low(dot32(normed, full_value))
    queries = queries.reshape(seqs, length, kv_heads, groups, HD)
    keys = keys.reshape(seqs, length, kv_heads, HD)
    values = values.reshape(seqs, length, kv_heads, HD)
    probs, mixed = attend(queries, keys, values)
    mixed = mixed.reshape(rows, -1)
    hidden_one = inputs + dot32(mixed, full_out)
    scale_two = inv_rms(hidden_one)
    normed_two = low(hidden_one * scale_two * gain_two)
    gate, up = dot32(normed_two, full_gate), dot32(normed_two, full_up)
    hidden, grad_gate, grad_up = mlp_grads(gate, up, dot_t(grad_in, full_down))
    block_out = low(hidden_one + dot32(hidden, full_down))

    acc_down = dot_l(hidden, grad_in)
    acc_gate = dot_l(normed_two, grad_gate)
    acc_up = dot_l(normed_two, grad_up)
    grad_normed_two = dot_t(grad_gate, full_gate) + dot_t(grad_up, full_up)
    acc_gain_two = jnp.sum(grad_normed_two * hidden_one * scale_two, 0)
    weighted = grad_normed_two * gain_two
    grad_one = grad_in.astype(jnp.float32) + scale_two * (
        weighted - hidden_one * scale_two * scale_two * jnp.mean(weighted * hidden_one, -1, keepdims=True)
    )
    grad_branch = low(grad_one)
    acc_out = dot_l(mixed, grad_branch)
    grad_mixed = low(dot_t(grad_branch, full_out)).reshape(queries.shape)
    grad_queries, grad_keys, grad_values = attend_back(queries, keys, values, probs, grad_mixed)
    grad_queries = low(rotate_back(grad_queries.reshape(rows, -1, HD), cosine, sine)).reshape(rows, -1)
    grad_keys = low(rotate_back(grad_keys.reshape(rows, -1, HD), cosine, sine)).reshape(rows, -1)
    grad_values = low(grad_values).reshape(rows, -1)
    acc_query = dot_l(normed, grad_queries)
    acc_key = dot_l(normed, grad_keys)
    acc_value = dot_l(normed, grad_values)
    grad_normed = dot_t(grad_queries, full_query) + dot_t(grad_keys, full_key) + dot_t(grad_values, full_value)
    acc_gain_one = jnp.sum(grad_normed * inputs * scale_one, 0)
    weighted = grad_normed * gain_one
    grad_tokens = grad_one + scale_one * (
        weighted - inputs * scale_one * scale_one * jnp.mean(weighted * inputs, -1, keepdims=True)
    )

    def share(acc):
        owned = lax.psum_scatter(low(acc), "dp", scatter_dimension=0, tiled=True)
        return lax.psum(owned, "seq").astype(jnp.float32)

    grads = [share(a) for a in (acc_down, acc_gate, acc_up, acc_out, acc_query, acc_key, acc_value)]
    gain_grads = lax.psum(
        lax.psum_scatter(jnp.stack([acc_gain_one, acc_gain_two], 1), "dp", scatter_dimension=0, tiled=True), "seq"
    )
    down, gate, up, out, query, key, value = grads
    return (
        block_out.reshape(tokens.shape),
        low(grad_tokens).reshape(tokens.shape),
        query, key, value, out, gate, up, down,
        gain_grads[:, 0], gain_grads[:, 1],
    )


ROWS = P(("dp", "seq"), None, None)
SPLIT = P("dp", None)
IN_SPECS = (ROWS, ROWS) + (SPLIT,) * 7 + (P("dp"), P("dp"))
OUT_SPECS = (ROWS, ROWS) + (SPLIT,) * 7 + (P("dp"), P("dp"))


def solution(mesh):
    return jax.shard_map(shards_plain, mesh=mesh, in_specs=IN_SPECS, out_specs=OUT_SPECS, check_vma=False)
```

```python
import jax
import jax.numpy as jnp
from jax import lax
from jax.experimental import pallas as pl
from jax.experimental.pallas import tpu as pltpu
from jax.sharding import PartitionSpec as P

HD = 96
EPS = 1e-05
THETA = 100000.0


def rotary(positions, width):
    steps_half = jnp.arange(width // 2, dtype=jnp.float32)
    frequency = jnp.power(THETA, -2.0 * steps_half / width)
    angles = positions[:, None] * frequency[None, :]
    cosine = jnp.cos(angles)
    sine = jnp.sin(angles)
    return (jnp.concatenate([cosine, cosine], -1), jnp.concatenate([sine, sine], -1))


def rotate(values, cosine, sine):
    half = values.shape[-1] // 2
    turned = jnp.concatenate([-values[..., half:], values[..., :half]], -1)
    return values * cosine[:, None, :] + turned * sine[:, None, :]


def rotate_back(grads, cosine, sine):
    half = grads.shape[-1] // 2
    sined = grads * sine[:, None, :]
    turned = jnp.concatenate([sined[..., half:], -sined[..., :half]], -1)
    return grads * cosine[:, None, :] + turned


def dot32(left, right):
    return jnp.dot(left, right, preferred_element_type=jnp.float32)


def dot_t(left, right):
    return lax.dot_general(left, right, (((1,), (1,)), ((), ())), preferred_element_type=jnp.float32)


def dot_l(left, right):
    return lax.dot_general(left, right, (((0,), (0,)), ((), ())), preferred_element_type=jnp.float32)


def inv_rms(values):
    return lax.rsqrt(jnp.mean(values * values, axis=-1, keepdims=True) + EPS)


def low(values):
    return values.astype(jnp.bfloat16)


def attend(queries, keys, values):
    rows = queries.shape[1]
    ids = jnp.arange(rows, dtype=jnp.int32)
    visible = ids[:, None] >= ids[None, :]
    scores = HD ** (-0.5) * jnp.einsum("bqkgd,bckd->bkgqc", queries, keys, preferred_element_type=jnp.float32)
    scores = jnp.where(visible, scores, -jnp.inf)
    top = jnp.max(scores, -1, keepdims=True)
    exps = jnp.exp(scores - top)
    probs = exps / jnp.sum(exps, -1, keepdims=True)
    mixed = jnp.einsum("bkgqc,bckd->bqkgd", low(probs), values, preferred_element_type=jnp.float32)
    return probs, low(mixed)


def attend_back(queries, keys, values, probs, grad_mixed):
    grad_values = jnp.einsum("bkgqc,bqkgd->bckd", low(probs), grad_mixed, preferred_element_type=jnp.float32)
    grad_probs = jnp.einsum("bqkgd,bckd->bkgqc", grad_mixed, values, preferred_element_type=jnp.float32)
    grad_scores = low(probs * (grad_probs - jnp.sum(probs * grad_probs, -1, keepdims=True)))
    scale = HD ** (-0.5)
    grad_queries = scale * jnp.einsum("bkgqc,bckd->bqkgd", grad_scores, keys, preferred_element_type=jnp.float32)
    grad_keys = scale * jnp.einsum("bkgqc,bqkgd->bckd", grad_scores, queries, preferred_element_type=jnp.float32)
    return grad_queries, grad_keys, grad_values


def mlp_grads(gate, up, grad_hidden):
    sigma = jax.nn.sigmoid(gate)
    silu = gate * sigma
    hidden = low(silu * up)
    grad_gate = low(grad_hidden * up * sigma * (1.0 + gate * (1.0 - sigma)))
    grad_up = low(grad_hidden * silu)
    return hidden, grad_gate, grad_up


def shards_plain(tokens, cotangent, w_query, w_key, w_value, w_out, w_gate, w_up, w_down, gain_attn, gain_mlp):
    seqs, length, width = tokens.shape
    rows = seqs * length
    kv_heads = w_key.shape[1] // HD
    groups = w_query.shape[1] // w_key.shape[1]
    gather = lambda w: lax.all_gather(w, "dp", axis=0, tiled=True)
    full_query, full_key, full_value, full_out = map(gather, (w_query, w_key, w_value, w_out))
    gains = gather(jnp.stack([gain_attn, gain_mlp], 1)).astype(jnp.float32)
    gain_one, gain_two = gains[:, 0], gains[:, 1]
    full_gate, full_up, full_down = map(gather, (w_gate, w_up, w_down))
    cosine, sine = rotary(jnp.arange(length, dtype=jnp.float32), HD)
    cosine, sine = jnp.tile(cosine, (seqs, 1)), jnp.tile(sine, (seqs, 1))

    inputs = tokens.reshape(rows, width).astype(jnp.float32)
    grad_in = cotangent.reshape(rows, width)
    scale_one = inv_rms(inputs)
    normed = low(inputs * scale_one * gain_one)
    queries = low(rotate(dot32(normed, full_query).reshape(rows, -1, HD), cosine, sine))
    keys = low(rotate(dot32(normed, full_key).reshape(rows, -1, HD), cosine, sine))
    values = low(dot32(normed, full_value))
    queries = queries.reshape(seqs, length, kv_heads, groups, HD)
    keys = keys.reshape(seqs, length, kv_heads, HD)
    values = values.reshape(seqs, length, kv_heads, HD)
    probs, mixed = attend(queries, keys, values)
    mixed = mixed.reshape(rows, -1)
    hidden_one = inputs + dot32(mixed, full_out)
    scale_two = inv_rms(hidden_one)
    normed_two = low(hidden_one * scale_two * gain_two)
    gate, up = dot32(normed_two, full_gate), dot32(normed_two, full_up)
    hidden, grad_gate, grad_up = mlp_grads(gate, up, dot_t(grad_in, full_down))
    block_out = low(hidden_one + dot32(hidden, full_down))

    acc_down = dot_l(hidden, grad_in)
    acc_gate = dot_l(normed_two, grad_gate)
    acc_up = dot_l(normed_two, grad_up)
    grad_normed_two = dot_t(grad_gate, full_gate) + dot_t(grad_up, full_up)
    acc_gain_two = jnp.sum(grad_normed_two * hidden_one * scale_two, 0)
    weighted = grad_normed_two * gain_two
    grad_one = grad_in.astype(jnp.float32) + scale_two * (
        weighted - hidden_one * scale_two * scale_two * jnp.mean(weighted * hidden_one, -1, keepdims=True)
    )
    grad_branch = low(grad_one)
    acc_out = dot_l(mixed, grad_branch)
    grad_mixed = low(dot_t(grad_branch, full_out)).reshape(queries.shape)
    grad_queries, grad_keys, grad_values = attend_back(queries, keys, values, probs, grad_mixed)
    grad_queries = low(rotate_back(grad_queries.reshape(rows, -1, HD), cosine, sine)).reshape(rows, -1)
    grad_keys = low(rotate_back(grad_keys.reshape(rows, -1, HD), cosine, sine)).reshape(rows, -1)
    grad_values = low(grad_values).reshape(rows, -1)
    acc_query = dot_l(normed, grad_queries)
    acc_key = dot_l(normed, grad_keys)
    acc_value = dot_l(normed, grad_values)
    grad_normed = dot_t(grad_queries, full_query) + dot_t(grad_keys, full_key) + dot_t(grad_values, full_value)
    acc_gain_one = jnp.sum(grad_normed * inputs * scale_one, 0)
    weighted = grad_normed * gain_one
    grad_tokens = grad_one + scale_one * (
        weighted - inputs * scale_one * scale_one * jnp.mean(weighted * inputs, -1, keepdims=True)
    )

    def share(acc):
        owned = lax.psum_scatter(low(acc), "dp", scatter_dimension=0, tiled=True)
        return lax.psum(owned, "seq").astype(jnp.float32)

    grads = [share(a) for a in (acc_down, acc_gate, acc_up, acc_out, acc_query, acc_key, acc_value)]
    gain_grads = lax.psum(
        lax.psum_scatter(jnp.stack([acc_gain_one, acc_gain_two], 1), "dp", scatter_dimension=0, tiled=True), "seq"
    )
    down, gate, up, out, query, key, value = grads
    return (
        block_out.reshape(tokens.shape),
        low(grad_tokens).reshape(tokens.shape),
        query, key, value, out, gate, up, down,
        gain_grads[:, 0], gain_grads[:, 1],
    )


ROWS = P(("dp", "seq"), None, None)
SPLIT = P("dp", None)
IN_SPECS = (ROWS, ROWS) + (SPLIT,) * 7 + (P("dp"), P("dp"))
OUT_SPECS = (ROWS, ROWS) + (SPLIT,) * 7 + (P("dp"), P("dp"))


MESH = pl.DeviceIdType.MESH
VMEM = pl.BlockSpec(memory_space=pltpu.VMEM)
ANY = pl.BlockSpec(memory_space=pl.ANY)
BF = jnp.bfloat16
F32 = jnp.float32
STRIP = 16


class Place:
    def __init__(self, planes):
        self.planes = planes
        d = lax.axis_index("dp")
        self.d, self.s = d, lax.axis_index("seq")
        self.c, self.y, self.z = d % 2, (d // 2) % 2, d // 4
        self.p = d // 2
        self.rank = 2 * self.s + self.c
        self.core = (d + 1 - 2 * self.c, self.s)
        self.across = (d, 1 - self.s)
        self.corner = (d + 1 - 2 * self.c, 1 - self.s)
        self.side = (d + 2 - 4 * self.y, self.s)
        self.right = (lax.rem(d + 4, 4 * planes), self.s)
        self.left = (lax.rem(d + 4 * planes - 4, 4 * planes), self.s)
        self.has_right, self.has_left = self.z < planes - 1, self.z > 0


def greet(me):
    barrier = pltpu.get_barrier_semaphore()
    for peer in (me.core, me.across, me.corner, me.side, me.right, me.left):
        pl.semaphore_signal(barrier, inc=1, device_id=peer, device_id_type=MESH)
    pl.semaphore_wait(barrier, 6)


def push(src, dst, send, recv, peer):
    return pltpu.make_async_remote_copy(
        src_ref=src, dst_ref=dst, send_sem=send, recv_sem=recv, device_id=peer, device_id_type=MESH
    )


def arrived(dst, recv, peer):
    push(dst, dst, recv, recv, peer).wait_recv()


def left_over(src, send, peer):
    push(src, src, send, send, peer).wait_send()


def group_start(me, src, dst, local, send, recv):
    keep = pltpu.make_async_copy(src, dst.at[me.rank], local)
    keep.start()
    push(src, dst.at[me.rank], send.at[0], recv.at[0], me.core).start()
    push(src, dst.at[me.rank], send.at[1], recv.at[1], me.across).start()


def group_relay(me, dst, send, recv):
    slot = dst.at[2 * (1 - me.s) + me.c]
    arrived(slot, recv.at[1], me.across)
    push(slot, slot, send.at[2], recv.at[2], me.core).start()


def group_finish(me, src, dst, local, send, recv):
    pltpu.make_async_copy(src, dst.at[me.rank], local).wait()
    arrived(dst.at[2 * me.s + 1 - me.c], recv.at[0], me.core)
    arrived(dst.at[2 * (1 - me.s) + 1 - me.c], recv.at[2], me.core)
    left_over(src, send.at[0], me.core)
    left_over(src, send.at[1], me.across)
    slot = dst.at[2 * (1 - me.s) + me.c]
    left_over(slot, send.at[2], me.core)


def group_sems():
    return [pltpu.SemaphoreType.DMA, pltpu.SemaphoreType.DMA((3,)), pltpu.SemaphoreType.DMA((3,))]


def line_start(me, dst, sems):
    to_right, to_left, line, to_side, side = sems
    slot = dst.at[me.p]
    push(slot, slot, to_side.at[me.z], side.at[me.z], me.side).start()

    @pl.when(me.has_right)
    def _():
        push(slot, slot, to_right.at[me.z], line.at[me.z], me.right).start()

    @pl.when(me.has_left)
    def _():
        push(slot, slot, to_left.at[me.z], line.at[me.z], me.left).start()


def line_hop(me, dst, sems, hop):
    to_right, to_left, line, to_side, side = sems

    def pass_on(item, back, forth, may, sends):
        slot = dst.at[2 * item + me.y]
        arrived(slot, line.at[item], back)

        @pl.when(may)
        def _():
            push(slot, slot, sends.at[item], line.at[item], forth).start()

        push(slot, slot, to_side.at[item], side.at[item], me.side).start()

    @pl.when(me.z >= hop)
    def _():
        pass_on(me.z - hop, me.left, me.right, me.has_right, to_right)

    @pl.when(me.z + hop < me.planes)
    def _():
        pass_on(me.z + hop, me.right, me.left, me.has_left, to_left)


def line_finish(me, dst, sems):
    to_right, to_left, line, to_side, side = sems
    for item in range(me.planes):
        arrived(dst.at[2 * item + 1 - me.y], side.at[item], me.side)
        mine = dst.at[2 * item + me.y]
        left_over(mine, to_side.at[item], me.side)

        @pl.when(jnp.logical_and(me.has_right, item <= me.z))
        def _():
            left_over(mine, to_right.at[item], me.right)

        @pl.when(jnp.logical_and(me.has_left, item >= me.z))
        def _():
            left_over(mine, to_left.at[item], me.left)


def line_sems(planes):
    return [pltpu.SemaphoreType.DMA((planes,))] * 5


def pick(table, index):
    value = jnp.int32(table[0])
    for i in range(1, len(table)):
        value = jnp.where(index == i, table[i], value)
    return value


def far_first(planes):
    return [sorted(range(planes), key=lambda i, z=z: (-abs(i - z), i)) for z in range(planes)]


def add_into(dst, *others):
    rows = dst.shape[0]

    def body(i, carry):
        strip = pl.ds(pl.multiple_of(i * STRIP, STRIP), STRIP)
        total = dst[strip, :].astype(F32)
        for other in others:
            total = total + other[strip, :].astype(F32)
        dst[strip, :] = total.astype(dst.dtype)
        return carry

    lax.fori_loop(0, rows // STRIP, body, 0)


def reduce_start(me, own, half, sems):
    to_side, side = sems[0], sems[1]
    orders = far_first(me.planes)
    for i in range(me.planes):
        item = pick([o[i] for o in orders], me.z)
        push(own.at[2 * item + 1 - me.y], half.at[item], to_side.at[item], side.at[item], me.side).start()


def reduce_step(me, own, half, from_left, from_right, sems, i):
    to_side, side, to_right, to_left, left, right = sems
    item = pick([o[i] for o in far_first(me.planes)], me.z)
    mine = half.at[item]
    arrived(mine, side.at[item], me.side)
    add_into(mine, own.at[2 * item + me.y])

    @pl.when(jnp.logical_and(me.has_left, item >= me.z))
    def _():
        arrived(from_left.at[item], left.at[item], me.left)
        add_into(mine, from_left.at[item])

    @pl.when(jnp.logical_and(me.has_right, item <= me.z))
    def _():
        arrived(from_right.at[item], right.at[item], me.right)
        add_into(mine, from_right.at[item])

    @pl.when(item > me.z)
    def _():
        push(mine, from_left.at[item], to_right.at[item], left.at[item], me.right).start()

    @pl.when(item < me.z)
    def _():
        push(mine, from_right.at[item], to_left.at[item], right.at[item], me.left).start()


def reduce_finish(me, own, half, sems):
    to_side, side, to_right, to_left, left, right = sems
    for item in range(me.planes):
        left_over(own.at[2 * item + 1 - me.y], to_side.at[item], me.side)

        @pl.when(item > me.z)
        def _():
            left_over(half.at[item], to_right.at[item], me.right)

        @pl.when(item < me.z)
        def _():
            left_over(half.at[item], to_left.at[item], me.left)


def reduce_sems(planes):
    return [pltpu.SemaphoreType.DMA((planes,))] * 6


def reduce_buffers(planes, rows, columns):
    return [pltpu.VMEM((planes, rows, columns), BF)] * 3


def deal_start(me, final, rows, out, local, send, recv):
    mine = out.at[me.rank]
    part = lambda core: final.at[pl.ds(pl.multiple_of(core * rows, rows), rows)]
    pltpu.make_async_copy(part(me.c), mine, local).start()
    push(part(1 - me.c), mine, send.at[0], recv.at[0], me.core).start()
    push(part(me.c), mine, send.at[1], recv.at[1], me.across).start()
    push(part(1 - me.c), mine, send.at[2], recv.at[2], me.corner).start()


def deal_finish(me, final, rows, out, local, send, recv):
    part = lambda core: final.at[pl.ds(pl.multiple_of(core * rows, rows), rows)]
    pltpu.make_async_copy(part(me.c), out.at[me.rank], local).wait()
    left_over(part(1 - me.c), send.at[0], me.core)
    left_over(part(me.c), send.at[1], me.across)
    left_over(part(1 - me.c), send.at[2], me.corner)
    arrived(out.at[2 * me.s + 1 - me.c], recv.at[0], me.core)
    arrived(out.at[2 * (1 - me.s) + me.c], recv.at[1], me.across)
    arrived(out.at[2 * (1 - me.s) + 1 - me.c], recv.at[2], me.corner)


def blocks_start(me, part, got, send, recv):
    for i, seq in enumerate((1 - me.s, me.s)):
        push(part.at[2 * seq + 1 - me.c], got.at[seq], send.at[i], recv.at[i], me.core).start()


def blocks_cross(me, part, got, last, send, recv):
    away = 1 - me.s
    arrived(got.at[away], recv.at[0], me.core)
    add_into(got.at[away], part.at[2 * away + me.c])
    push(got.at[away], last, send.at[2], recv.at[2], me.across).start()


def blocks_finish(me, part, got, last, send, recv):
    arrived(got.at[me.s], recv.at[1], me.core)
    arrived(last, recv.at[2], me.across)
    for i, seq in enumerate((1 - me.s, me.s)):
        left_over(part.at[2 * seq + 1 - me.c], send.at[i], me.core)
    left_over(got.at[1 - me.s], send.at[2], me.across)


def blocks_sems():
    return [pltpu.SemaphoreType.DMA((3,))] * 2


def blocks_buffers(rows, width):
    return [pltpu.VMEM((2, rows, width), BF), pltpu.VMEM((rows, width), BF)]


def strips(rows, body):
    def step(i, carry):
        body(pl.ds(pl.multiple_of(i * STRIP, STRIP), STRIP))
        return carry

    lax.fori_loop(0, rows // STRIP, step, 0)


def comm_call(kernel, ident, outs, out_specs, ins, scratch, name):
    return pl.pallas_call(
        kernel,
        out_shape=outs,
        in_specs=[spec for spec, _ in ins],
        out_specs=out_specs,
        scratch_shapes=scratch,
        name=name,
        compiler_params=pltpu.CompilerParams(
            collective_id=ident, has_side_effects=True, vmem_limit_bytes=60 * 1024 * 1024
        ),
    )(*[value for _, value in ins])


def shape(dims, dtype=BF):
    return jax.ShapeDtypeStruct(dims, dtype)


def split_start(me, local_part, dst, keep, send, recv):
    pltpu.make_async_copy(local_part.at[me.c], dst.at[me.p, me.c], keep).start()
    push(local_part.at[1 - me.c], dst.at[me.p, me.c], send, recv, me.core).start()


def split_finish(me, local_part, dst, keep, send, recv):
    pltpu.make_async_copy(local_part.at[me.c], dst.at[me.p, me.c], keep).wait()
    arrived(dst.at[me.p, 1 - me.c], recv, me.core)
    left_over(local_part.at[1 - me.c], send, me.core)


def gather_attention(planes, normed, cot, w_qkv, w_out):
    rows, width = normed.shape
    head = w_out.shape[0]

    def kernel(n_ref, g_ref, qkv_ref, out_ref, n_all, g_all, qkv_all, out_all, *scr):
        it = iter(scr)
        take = lambda k: [next(it) for _ in range(k)]
        n_sems, g_sems, split, line, edge = take(3), take(3), take(3), take(5), take(6)
        me = Place(planes)
        greet(me)
        split_start(me, qkv_ref, qkv_all, *split)
        group_start(me, n_ref, n_all, *n_sems)
        group_start(me, g_ref, g_all, *g_sems)
        keep, send, recv, to_right, to_left, sides = edge
        here = me.s == me.z // 2
        owner = me.z == me.rank
        spot = out_all.at[me.y, pl.ds(pl.multiple_of(me.c * head, head), head)]
        other = out_all.at[me.y, pl.ds(pl.multiple_of((1 - me.c) * head, head), head)]
        mine = out_all.at[me.y]

        @pl.when(owner)
        def _():
            pltpu.make_async_copy(out_ref, spot, keep).start()

        @pl.when(jnp.logical_and(here, jnp.logical_not(owner)))
        def _():
            push(out_ref, spot, send, recv.at[0], me.core).start()

        split_finish(me, qkv_ref, qkv_all, *split)
        line_start(me, qkv_all, line)

        @pl.when(owner)
        def _():
            pltpu.make_async_copy(out_ref, spot, keep).wait()
            arrived(other, recv.at[0], me.core)

        @pl.when(jnp.logical_and(here, jnp.logical_not(owner)))
        def _():
            left_over(out_ref, send, me.core)

        @pl.when(me.z > me.rank)
        def _():
            arrived(mine, recv.at[1], me.left)

        @pl.when(me.z < me.rank)
        def _():
            arrived(mine, recv.at[1], me.right)

        go_right = jnp.logical_and(me.z >= me.rank, me.has_right)
        go_left = jnp.logical_and(me.z <= me.rank, me.has_left)

        @pl.when(go_right)
        def _():
            push(mine, mine, to_right, recv.at[1], me.right).start()

        @pl.when(go_left)
        def _():
            push(mine, mine, to_left, recv.at[1], me.left).start()

        push(mine, mine, sides.at[0], sides.at[1], me.side).start()
        group_relay(me, n_all, *n_sems[1:])
        for hop in range(1, planes):
            line_hop(me, qkv_all, line, hop)
        group_relay(me, g_all, *g_sems[1:])
        line_finish(me, qkv_all, line)
        arrived(out_all.at[1 - me.y], sides.at[1], me.side)
        left_over(mine, sides.at[0], me.side)

        @pl.when(go_right)
        def _():
            left_over(mine, to_right, me.right)

        @pl.when(go_left)
        def _():
            left_over(mine, to_left, me.left)

        group_finish(me, n_ref, n_all, *n_sems)
        group_finish(me, g_ref, g_all, *g_sems)

    one, two = pltpu.SemaphoreType.DMA, pltpu.SemaphoreType.DMA((2,))
    return comm_call(
        kernel, 0,
        [shape((4, rows, width)), shape((4, rows, width)),
         shape((2 * planes, 2) + w_qkv.shape[1:]), shape((2, 2 * head, width))],
        [ANY] * 4,
        [(VMEM, normed), (VMEM, cot), (VMEM, w_qkv), (VMEM, w_out)],
        group_sems() + group_sems() + [one] * 3 + line_sems(planes) + [one, one, two, one, one, two],
        "gather_attention",
    )


def gather_mlp(planes, part, tokens, w_gu, w_down):
    rows, width = tokens.shape

    def kernel(part_ref, x_ref, gu_ref, down_ref, x1_ref, n_all, gu_all, down_all, *scr):
        it = iter(scr)
        take = lambda k: [next(it) for _ in range(k)]
        (got, last, normed), b_sems = take(3), take(2)
        n_sems, split, line, down_keep, down_line = take(3), take(3), take(5), take(1)[0], take(5)
        me = Place(planes)
        greet(me)
        split_start(me, gu_ref, gu_all, *split)
        blocks_start(me, part_ref, got, *b_sems)
        keep = pltpu.make_async_copy(down_ref, down_all.at[me.p], down_keep)
        keep.start()
        split_finish(me, gu_ref, gu_all, *split)
        line_start(me, gu_all, line)
        keep.wait()
        line_start(me, down_all, down_line)
        blocks_cross(me, part_ref, got, last, *b_sems)
        line_hop(me, gu_all, line, 1)
        blocks_finish(me, part_ref, got, last, *b_sems)

        def body(strip):
            total = x_ref[strip, :].astype(F32) + (
                part_ref[me.rank, strip, :].astype(F32)
                + got[me.s, strip, :].astype(F32)
                + last[strip, :].astype(F32)
            )
            x1_ref[strip, :] = total
            normed[strip, :] = low(total * inv_rms(total))

        strips(rows, body)
        group_start(me, normed, n_all, *n_sems)
        line_hop(me, down_all, down_line, 1)
        group_relay(me, n_all, *n_sems[1:])
        for hop in range(2, planes):
            line_hop(me, gu_all, line, hop)
            line_hop(me, down_all, down_line, hop)
        line_finish(me, gu_all, line)
        line_finish(me, down_all, down_line)
        group_finish(me, normed, n_all, *n_sems)

    one = pltpu.SemaphoreType.DMA
    return comm_call(
        kernel, 1,
        [shape((rows, width), F32), shape((4, rows, width)),
         shape((2 * planes, 2) + w_gu.shape[1:]), shape((2 * planes,) + w_down.shape)],
        [VMEM, ANY, ANY, ANY],
        [(VMEM, part), (VMEM, tokens), (VMEM, w_gu), (VMEM, w_down)],
        blocks_buffers(rows, width) + [pltpu.VMEM((rows, width), BF)] + blocks_sems()
        + group_sems() + [one] * 3 + line_sems(planes) + [one] + line_sems(planes),
        "gather_mlp",
    )


def norm_back(values, weighted, base):
    scale = inv_rms(values)
    return base + scale * (
        weighted - values * scale * scale * jnp.mean(weighted * values, -1, keepdims=True)
    )


def reduce_mlp(planes, part_back, part_out, x1, cot, g_gu, g_down):
    rows, width = x1.shape
    gu_rows, gu_cols = g_gu.shape[1:]
    dn_rows = g_down.shape[1]

    def kernel(back_ref, fwd_ref, x1_ref, g_ref, gu_ref, dn_ref,
               bo_ref, dx_ref, dx_all, gu_out, dn_out, *scr):
        it = iter(scr)
        take = lambda k: [next(it) for _ in range(k)]
        (got_b, last_b), (got_f, last_f), branch = take(2), take(2), take(1)[0]
        gu_buf, dn_buf = take(3), take(3)
        b_sems, f_sems, n_sems = take(2), take(2), take(3)
        gu_sems, dn_sems, deal, dn_deal = take(6), take(6), take(3), take(3)
        me = Place(planes)
        greet(me)
        blocks_start(me, back_ref, got_b, *b_sems)
        reduce_start(me, gu_ref, gu_buf[0], gu_sems)
        blocks_start(me, fwd_ref, got_f, *f_sems)
        reduce_start(me, dn_ref, dn_buf[0], dn_sems)
        blocks_cross(me, back_ref, got_b, last_b, *b_sems)
        blocks_finish(me, back_ref, got_b, last_b, *b_sems)

        def back(strip):
            weighted = (
                back_ref[me.rank, strip, :].astype(F32)
                + got_b[me.s, strip, :].astype(F32)
                + last_b[strip, :].astype(F32)
            )
            grad = norm_back(x1_ref[strip, :], weighted, g_ref[strip, :].astype(F32))
            dx_ref[strip, :] = grad
            branch[strip, :] = low(grad)

        strips(rows, back)
        group_start(me, branch, dx_all, *n_sems)
        blocks_cross(me, fwd_ref, got_f, last_f, *f_sems)
        reduce_step(me, gu_ref, *gu_buf, gu_sems, 0)
        group_relay(me, dx_all, *n_sems[1:])
        reduce_step(me, gu_ref, *gu_buf, gu_sems, 1)
        blocks_finish(me, fwd_ref, got_f, last_f, *f_sems)

        def forth(strip):
            total = (
                fwd_ref[me.rank, strip, :].astype(F32)
                + got_f[me.s, strip, :].astype(F32)
                + last_f[strip, :].astype(F32)
            )
            bo_ref[strip, :] = low(x1_ref[strip, :] + total)

        strips(rows, forth)
        for i in range(2, planes):
            reduce_step(me, gu_ref, *gu_buf, gu_sems, i)
        final = gu_buf[0].at[me.z]
        deal_start(me, final, gu_rows // 2, gu_out, *deal)
        for i in range(planes):
            reduce_step(me, dn_ref, *dn_buf, dn_sems, i)
        final_dn = dn_buf[0].at[me.z]
        keep, send, recv = dn_deal
        pltpu.make_async_copy(final_dn, dn_out.at[me.s], keep).start()
        push(final_dn, dn_out.at[me.s], send, recv, me.across).start()
        reduce_finish(me, gu_ref, gu_buf[0], gu_sems)
        reduce_finish(me, dn_ref, dn_buf[0], dn_sems)
        group_finish(me, branch, dx_all, *n_sems)
        deal_finish(me, final, gu_rows // 2, gu_out, *deal)
        pltpu.make_async_copy(final_dn, dn_out.at[me.s], keep).wait()
        left_over(final_dn, send, me.across)
        arrived(dn_out.at[1 - me.s], recv, me.across)

    one, three = pltpu.SemaphoreType.DMA, pltpu.SemaphoreType.DMA((3,))
    return comm_call(
        kernel, 2,
        [shape((rows, width)), shape((rows, width), F32), shape((4, rows, width)),
         shape((4, gu_rows // 2, gu_cols)), shape((2, dn_rows, width))],
        [VMEM, VMEM, ANY, ANY, ANY],
        [(VMEM, part_back), (VMEM, part_out), (VMEM, x1), (VMEM, cot), (VMEM, g_gu), (VMEM, g_down)],
        blocks_buffers(rows, width) * 2 + [pltpu.VMEM((rows, width), BF)]
        + reduce_buffers(planes, gu_rows, gu_cols) + reduce_buffers(planes, dn_rows, width)
        + blocks_sems() * 2 + group_sems() + reduce_sems(planes) * 2 + [one, three, three] + [one] * 3,
        "reduce_mlp",
    )


def reduce_attention(planes, part, x, dx, g_qkv, g_out):
    rows, width = dx.shape
    q_rows, q_cols = g_qkv.shape[1:]
    o_rows = g_out.shape[1]

    def kernel(part_ref, x_ref, dx_ref, qkv_ref, out_ref, gx_ref, qkv_out, out_out, *scr):
        it = iter(scr)
        take = lambda k: [next(it) for _ in range(k)]
        got, last = take(2)
        q_buf, (o_half, o_left, o_right) = take(3), take(3)
        b_sems, q_sems, deal = take(2), take(6), take(3)
        side, lines, keep, send, recv = take(5)
        me = Place(planes)
        greet(me)
        push(out_ref.at[1 - me.y], o_half, side.at[0], side.at[1], me.side).start()
        reduce_start(me, qkv_ref, q_buf[0], q_sems)
        blocks_start(me, part_ref, got, *b_sems)
        blocks_cross(me, part_ref, got, last, *b_sems)
        arrived(o_half, side.at[1], me.side)
        add_into(o_half, out_ref.at[me.y])

        @pl.when(jnp.logical_and(me.has_left, me.z <= me.rank))
        def _():
            arrived(o_left, lines.at[0], me.left)
            add_into(o_half, o_left)

        @pl.when(jnp.logical_and(me.has_right, me.z >= me.rank))
        def _():
            arrived(o_right, lines.at[1], me.right)
            add_into(o_half, o_right)

        @pl.when(me.z < me.rank)
        def _():
            push(o_half, o_left, lines.at[2], lines.at[0], me.right).start()

        @pl.when(me.z > me.rank)
        def _():
            push(o_half, o_right, lines.at[2], lines.at[1], me.left).start()

        head = o_rows // 2
        mine = o_half.at[pl.ds(pl.multiple_of(me.c * head, head), head)]
        theirs = o_half.at[pl.ds(pl.multiple_of((1 - me.c) * head, head), head)]
        owner = me.z == me.rank

        @pl.when(owner)
        def _():
            pltpu.make_async_copy(mine, out_out, keep).start()
            push(theirs, out_out, send.at[0], recv, me.core).start()
            push(mine, out_out, send.at[1], recv, me.across).start()
            push(theirs, out_out, send.at[2], recv, me.corner).start()

        for i in range(planes - 1):
            reduce_step(me, qkv_ref, *q_buf, q_sems, i)
        blocks_finish(me, part_ref, got, last, *b_sems)

        def body(strip):
            weighted = (
                part_ref[me.rank, strip, :].astype(F32)
                + got[me.s, strip, :].astype(F32)
                + last[strip, :].astype(F32)
            )
            gx_ref[strip, :] = low(norm_back(x_ref[strip, :].astype(F32), weighted, dx_ref[strip, :]))

        strips(rows, body)
        reduce_step(me, qkv_ref, *q_buf, q_sems, planes - 1)
        final = q_buf[0].at[me.z]
        deal_start(me, final, q_rows // 2, qkv_out, *deal)
        reduce_finish(me, qkv_ref, q_buf[0], q_sems)
        left_over(out_ref.at[1 - me.y], side.at[0], me.side)

        @pl.when(me.z < me.rank)
        def _():
            left_over(o_half, lines.at[2], me.right)

        @pl.when(me.z > me.rank)
        def _():
            left_over(o_half, lines.at[2], me.left)

        @pl.when(owner)
        def _():
            pltpu.make_async_copy(mine, out_out, keep).wait()
            left_over(theirs, send.at[0], me.core)
            left_over(mine, send.at[1], me.across)
            left_over(theirs, send.at[2], me.corner)

        @pl.when(jnp.logical_not(owner))
        def _():
            arrived(out_out, recv, me.core)

        deal_finish(me, final, q_rows // 2, qkv_out, *deal)

    one, two, three = pltpu.SemaphoreType.DMA, pltpu.SemaphoreType.DMA((2,)), pltpu.SemaphoreType.DMA((3,))
    return comm_call(
        kernel, 3,
        [shape((rows, width)), shape((4, q_rows // 2, q_cols)), shape((o_rows // 2, width))],
        [VMEM, ANY, ANY],
        [(VMEM, part), (VMEM, x), (VMEM, dx), (VMEM, g_qkv), (VMEM, g_out)],
        blocks_buffers(rows, width) + reduce_buffers(planes, q_rows, q_cols)
        + [pltpu.VMEM((o_rows, width), BF)] * 3
        + blocks_sems() + reduce_sems(planes) + [one, three, three] + [two, three, one, three, one],
        "reduce_attention",
    )


def shards_fast(tokens, cotangent, w_query, w_key, w_value, w_out, w_gate, w_up, w_down, gain_attn, gain_mlp):
    seqs, length, width = tokens.shape
    rows = seqs * length
    depth = w_query.shape[0]
    devices = width // depth
    planes = devices // 4
    chips = 2 * planes
    s = lax.axis_index("seq")
    kv_heads = w_key.shape[1] // HD
    groups = w_query.shape[1] // w_key.shape[1]
    hidden = w_gate.shape[1]
    block = hidden // devices // 2

    x = tokens.reshape(rows, width)
    cot = cotangent.reshape(rows, width)
    xf = x.astype(F32)
    normed = low(xf * inv_rms(xf))

    gain_one, gain_two = gain_attn.astype(F32)[:, None], gain_mlp.astype(F32)[:, None]

    def heads_of(w):
        parts = (w.astype(F32) * gain_one).reshape(depth, 2, 2, -1)
        return jnp.moveaxis(low(lax.dynamic_index_in_dim(parts, s, 1, False)), 1, 0)

    w_qkv = jnp.concatenate([heads_of(w) for w in (w_query, w_key, w_value)], -1)

    def units_of(w):
        parts = (w.astype(F32) * gain_two).reshape(depth, chips, 2, 2, block)
        return jnp.moveaxis(low(lax.dynamic_index_in_dim(parts, s, 3, False)), 2, 0)

    w_gu = jnp.stack([units_of(w_gate), units_of(w_up)], 3).reshape(2, depth, 2 * hidden // 4)
    own_down = lax.dynamic_slice_in_dim(w_down, s * block, block, 0)

    n_all, g_all, qkv_all, out_all = gather_attention(planes, normed, cot, w_qkv, w_out)
    n_all, g_all = n_all.reshape(4 * rows, width), g_all.reshape(4 * rows, width)
    qkv_all, out_all = qkv_all.reshape(width, -1), out_all.reshape(-1, width)

    total = 4 * rows
    cosine, sine = rotary(jnp.arange(length, dtype=F32), HD)
    cosine, sine = jnp.tile(cosine, (4 * seqs, 1)), jnp.tile(sine, (4 * seqs, 1))
    own_kv = kv_heads // 4
    cut_q = own_kv * groups * HD
    cut_k = cut_q + own_kv * HD
    projected = dot32(n_all, qkv_all)
    queries = low(rotate(projected[:, :cut_q].reshape(total, -1, HD), cosine, sine))
    keys = low(rotate(projected[:, cut_q:cut_k].reshape(total, -1, HD), cosine, sine))
    values = low(projected[:, cut_k:])
    queries = queries.reshape(4 * seqs, length, own_kv, groups, HD)
    keys = keys.reshape(4 * seqs, length, own_kv, HD)
    values = values.reshape(4 * seqs, length, own_kv, HD)
    probs, mixed = attend(queries, keys, values)
    mixed = mixed.reshape(total, cut_q)
    part_one = low(dot32(mixed, out_all)).reshape(4, rows, width)

    x1, n2_all, gu_all, down_all = gather_mlp(planes, part_one, x, w_gu, own_down)
    n2_all, gu_all = n2_all.reshape(total, width), gu_all.reshape(width, chips, 2, block)
    down_all = down_all.reshape(-1, width)
    units = chips * block
    full_gate, full_up = gu_all[:, :, 0].reshape(width, units), gu_all[:, :, 1].reshape(width, units)
    gate, up = dot32(n2_all, full_gate), dot32(n2_all, full_up)
    mid, grad_gate, grad_up = mlp_grads(gate, up, dot_t(g_all, down_all))
    part_out = low(dot32(mid, down_all)).reshape(4, rows, width)
    grad_gu = jnp.stack(
        [grad_gate.reshape(total, chips, block), grad_up.reshape(total, chips, block)], 2
    ).reshape(total, 2 * units)
    part_back = low(dot_t(grad_gu, gu_all.reshape(width, 2 * units))).reshape(4, rows, width)
    g_gu = low(dot_l(n2_all, grad_gu)).reshape(chips, 2 * depth, 2 * units)
    g_down = low(dot_l(mid, g_all)).reshape(chips, block, width)

    block_out, dx, dx_all, own_gu, own_dn = reduce_mlp(planes, part_back, part_out, x1, cot, g_gu, g_down)
    dx_all = dx_all.reshape(total, width)
    grad_mixed = low(dot_t(dx_all, out_all)).reshape(queries.shape)
    g_out = low(dot_l(mixed, dx_all)).reshape(2, 2 * depth, width)
    grad_q, grad_k, grad_v = attend_back(queries, keys, values, probs, grad_mixed)
    grad_q = low(rotate_back(grad_q.reshape(total, -1, HD), cosine, sine)).reshape(total, -1)
    grad_k = low(rotate_back(grad_k.reshape(total, -1, HD), cosine, sine)).reshape(total, -1)
    grad_qkv = jnp.concatenate([grad_q, grad_k, low(grad_v).reshape(total, -1)], 1)
    part_in = low(dot_t(grad_qkv, qkv_all)).reshape(4, rows, width)
    g_qkv = low(dot_l(n_all, grad_qkv)).reshape(chips, 2 * depth, -1)

    grad_tokens, own_qkv, own_out = reduce_attention(planes, part_in, x, dx, g_qkv, g_out)

    own_qkv = own_qkv.astype(F32)
    cols = lambda a, b: jnp.moveaxis(own_qkv[:, :, a:b], 0, 1).reshape(depth, -1)
    raw_q, raw_k, raw_v = cols(0, cut_q), cols(cut_q, cut_k), cols(cut_k, None)
    own_gu = own_gu.reshape(2, 2, depth, chips, 2, block).astype(F32)
    raw_gu = jnp.transpose(own_gu, (4, 2, 3, 1, 0, 5)).reshape(2, depth, hidden)
    gain_grad = lambda pairs: sum(jnp.sum(w.astype(F32) * raw, 1) for w, raw in pairs)
    return (
        block_out.reshape(tokens.shape),
        grad_tokens.reshape(tokens.shape),
        raw_q * gain_one, raw_k * gain_one, raw_v * gain_one,
        own_out.astype(F32),
        raw_gu[0] * gain_two, raw_gu[1] * gain_two,
        own_dn.reshape(-1, width).astype(F32),
        gain_grad([(w_query, raw_q), (w_key, raw_k), (w_value, raw_v)]),
        gain_grad([(w_gate, raw_gu[0]), (w_up, raw_gu[1])]),
    )


def fits(mesh):
    return mesh.shape["seq"] == 2 and mesh.shape["dp"] == 16


def solution(mesh):
    body = shards_fast if fits(mesh) else shards_plain
    return jax.shard_map(body, mesh=mesh, in_specs=IN_SPECS, out_specs=OUT_SPECS, check_vma=False)
```

```python
import jax
import jax.numpy as jnp
from jax import lax
from jax.experimental import pallas as pl
from jax.experimental.pallas import tpu as pltpu
from jax.sharding import PartitionSpec as P

HD = 96
EPS = 1e-05
THETA = 100000.0


def rotary(positions, width):
    steps_half = jnp.arange(width // 2, dtype=jnp.float32)
    frequency = jnp.power(THETA, -2.0 * steps_half / width)
    angles = positions[:, None] * frequency[None, :]
    cosine = jnp.cos(angles)
    sine = jnp.sin(angles)
    return (jnp.concatenate([cosine, cosine], -1), jnp.concatenate([sine, sine], -1))


def rotate(values, cosine, sine):
    half = values.shape[-1] // 2
    turned = jnp.concatenate([-values[..., half:], values[..., :half]], -1)
    return values * cosine[:, None, :] + turned * sine[:, None, :]


def rotate_back(grads, cosine, sine):
    half = grads.shape[-1] // 2
    sined = grads * sine[:, None, :]
    turned = jnp.concatenate([sined[..., half:], -sined[..., :half]], -1)
    return grads * cosine[:, None, :] + turned


def dot32(left, right):
    return jnp.dot(left, right, preferred_element_type=jnp.float32)


def dot_t(left, right):
    return lax.dot_general(left, right, (((1,), (1,)), ((), ())), preferred_element_type=jnp.float32)


def dot_l(left, right):
    return lax.dot_general(left, right, (((0,), (0,)), ((), ())), preferred_element_type=jnp.float32)


def inv_rms(values):
    return lax.rsqrt(jnp.mean(values * values, axis=-1, keepdims=True) + EPS)


def low(values):
    return values.astype(jnp.bfloat16)


def attend(queries, keys, values):
    rows = queries.shape[1]
    ids = jnp.arange(rows, dtype=jnp.int32)
    visible = ids[:, None] >= ids[None, :]
    scores = HD ** (-0.5) * jnp.einsum("bqkgd,bckd->bkgqc", queries, keys, preferred_element_type=jnp.float32)
    scores = jnp.where(visible, scores, -jnp.inf)
    top = jnp.max(scores, -1, keepdims=True)
    exps = jnp.exp(scores - top)
    probs = exps / jnp.sum(exps, -1, keepdims=True)
    mixed = jnp.einsum("bkgqc,bckd->bqkgd", low(probs), values, preferred_element_type=jnp.float32)
    return probs, low(mixed)


def attend_back(queries, keys, values, probs, grad_mixed):
    grad_values = jnp.einsum("bkgqc,bqkgd->bckd", low(probs), grad_mixed, preferred_element_type=jnp.float32)
    grad_probs = jnp.einsum("bqkgd,bckd->bkgqc", grad_mixed, values, preferred_element_type=jnp.float32)
    grad_scores = low(probs * (grad_probs - jnp.sum(probs * grad_probs, -1, keepdims=True)))
    scale = HD ** (-0.5)
    grad_queries = scale * jnp.einsum("bkgqc,bckd->bqkgd", grad_scores, keys, preferred_element_type=jnp.float32)
    grad_keys = scale * jnp.einsum("bkgqc,bqkgd->bckd", grad_scores, queries, preferred_element_type=jnp.float32)
    return grad_queries, grad_keys, grad_values


def mlp_grads(gate, up, grad_hidden):
    sigma = jax.nn.sigmoid(gate)
    silu = gate * sigma
    hidden = low(silu * up)
    grad_gate = low(grad_hidden * up * sigma * (1.0 + gate * (1.0 - sigma)))
    grad_up = low(grad_hidden * silu)
    return hidden, grad_gate, grad_up


def shards_plain(tokens, cotangent, w_query, w_key, w_value, w_out, w_gate, w_up, w_down, gain_attn, gain_mlp):
    seqs, length, width = tokens.shape
    rows = seqs * length
    kv_heads = w_key.shape[1] // HD
    groups = w_query.shape[1] // w_key.shape[1]
    gather = lambda w: lax.all_gather(w, "dp", axis=0, tiled=True)
    full_query, full_key, full_value, full_out = map(gather, (w_query, w_key, w_value, w_out))
    gains = gather(jnp.stack([gain_attn, gain_mlp], 1)).astype(jnp.float32)
    gain_one, gain_two = gains[:, 0], gains[:, 1]
    full_gate, full_up, full_down = map(gather, (w_gate, w_up, w_down))
    cosine, sine = rotary(jnp.arange(length, dtype=jnp.float32), HD)
    cosine, sine = jnp.tile(cosine, (seqs, 1)), jnp.tile(sine, (seqs, 1))

    inputs = tokens.reshape(rows, width).astype(jnp.float32)
    grad_in = cotangent.reshape(rows, width)
    scale_one = inv_rms(inputs)
    normed = low(inputs * scale_one * gain_one)
    queries = low(rotate(dot32(normed, full_query).reshape(rows, -1, HD), cosine, sine))
    keys = low(rotate(dot32(normed, full_key).reshape(rows, -1, HD), cosine, sine))
    values = low(dot32(normed, full_value))
    queries = queries.reshape(seqs, length, kv_heads, groups, HD)
    keys = keys.reshape(seqs, length, kv_heads, HD)
    values = values.reshape(seqs, length, kv_heads, HD)
    probs, mixed = attend(queries, keys, values)
    mixed = mixed.reshape(rows, -1)
    hidden_one = inputs + dot32(mixed, full_out)
    scale_two = inv_rms(hidden_one)
    normed_two = low(hidden_one * scale_two * gain_two)
    gate, up = dot32(normed_two, full_gate), dot32(normed_two, full_up)
    hidden, grad_gate, grad_up = mlp_grads(gate, up, dot_t(grad_in, full_down))
    block_out = low(hidden_one + dot32(hidden, full_down))

    acc_down = dot_l(hidden, grad_in)
    acc_gate = dot_l(normed_two, grad_gate)
    acc_up = dot_l(normed_two, grad_up)
    grad_normed_two = dot_t(grad_gate, full_gate) + dot_t(grad_up, full_up)
    acc_gain_two = jnp.sum(grad_normed_two * hidden_one * scale_two, 0)
    weighted = grad_normed_two * gain_two
    grad_one = grad_in.astype(jnp.float32) + scale_two * (
        weighted - hidden_one * scale_two * scale_two * jnp.mean(weighted * hidden_one, -1, keepdims=True)
    )
    grad_branch = low(grad_one)
    acc_out = dot_l(mixed, grad_branch)
    grad_mixed = low(dot_t(grad_branch, full_out)).reshape(queries.shape)
    grad_queries, grad_keys, grad_values = attend_back(queries, keys, values, probs, grad_mixed)
    grad_queries = low(rotate_back(grad_queries.reshape(rows, -1, HD), cosine, sine)).reshape(rows, -1)
    grad_keys = low(rotate_back(grad_keys.reshape(rows, -1, HD), cosine, sine)).reshape(rows, -1)
    grad_values = low(grad_values).reshape(rows, -1)
    acc_query = dot_l(normed, grad_queries)
    acc_key = dot_l(normed, grad_keys)
    acc_value = dot_l(normed, grad_values)
    grad_normed = dot_t(grad_queries, full_query) + dot_t(grad_keys, full_key) + dot_t(grad_values, full_value)
    acc_gain_one = jnp.sum(grad_normed * inputs * scale_one, 0)
    weighted = grad_normed * gain_one
    grad_tokens = grad_one + scale_one * (
        weighted - inputs * scale_one * scale_one * jnp.mean(weighted * inputs, -1, keepdims=True)
    )

    def share(acc):
        owned = lax.psum_scatter(low(acc), "dp", scatter_dimension=0, tiled=True)
        return lax.psum(owned, "seq").astype(jnp.float32)

    grads = [share(a) for a in (acc_down, acc_gate, acc_up, acc_out, acc_query, acc_key, acc_value)]
    gain_grads = lax.psum(
        lax.psum_scatter(jnp.stack([acc_gain_one, acc_gain_two], 1), "dp", scatter_dimension=0, tiled=True), "seq"
    )
    down, gate, up, out, query, key, value = grads
    return (
        block_out.reshape(tokens.shape),
        low(grad_tokens).reshape(tokens.shape),
        query, key, value, out, gate, up, down,
        gain_grads[:, 0], gain_grads[:, 1],
    )


ROWS = P(("dp", "seq"), None, None)
SPLIT = P("dp", None)
IN_SPECS = (ROWS, ROWS) + (SPLIT,) * 7 + (P("dp"), P("dp"))
OUT_SPECS = (ROWS, ROWS) + (SPLIT,) * 7 + (P("dp"), P("dp"))


MESH = pl.DeviceIdType.MESH
VMEM = pl.BlockSpec(memory_space=pltpu.VMEM)
ANY = pl.BlockSpec(memory_space=pl.ANY)
BF = jnp.bfloat16
F32 = jnp.float32
STRIP = 16


class Place:
    def __init__(self, planes):
        self.planes = planes
        d = lax.axis_index("dp")
        self.d, self.s = d, lax.axis_index("seq")
        self.c, self.y, self.z = d % 2, (d // 2) % 2, d // 4
        self.p = d // 2
        self.rank = 2 * self.s + self.c
        self.core = (d + 1 - 2 * self.c, self.s)
        self.across = (d, 1 - self.s)
        self.corner = (d + 1 - 2 * self.c, 1 - self.s)
        self.side = (d + 2 - 4 * self.y, self.s)
        self.right = (lax.rem(d + 4, 4 * planes), self.s)
        self.left = (lax.rem(d + 4 * planes - 4, 4 * planes), self.s)
        self.has_right, self.has_left = self.z < planes - 1, self.z > 0


def greet(me):
    barrier = pltpu.get_barrier_semaphore()
    for peer in (me.core, me.across, me.corner, me.side, me.right, me.left):
        pl.semaphore_signal(barrier, inc=1, device_id=peer, device_id_type=MESH)
    pl.semaphore_wait(barrier, 6)


def push(src, dst, send, recv, peer):
    return pltpu.make_async_remote_copy(
        src_ref=src, dst_ref=dst, send_sem=send, recv_sem=recv, device_id=peer, device_id_type=MESH
    )


def arrived(dst, recv, peer):
    push(dst, dst, recv, recv, peer).wait_recv()


def left_over(src, send, peer):
    push(src, src, send, send, peer).wait_send()


class Slots:
    def __init__(self, ref, rows):
        self.ref, self.rows = ref, rows
        self.at = self

    def __getitem__(self, block):
        return self.ref.at[pl.ds(pl.multiple_of(block * self.rows, self.rows), self.rows)]


def group_start(me, src, dst, local, send, recv):
    keep = pltpu.make_async_copy(src, dst.at[me.rank], local)
    keep.start()
    push(src, dst.at[me.rank], send.at[0], recv.at[0], me.core).start()
    push(src, dst.at[me.rank], send.at[1], recv.at[1], me.across).start()


def group_relay(me, dst, send, recv):
    slot = dst.at[2 * (1 - me.s) + me.c]
    arrived(slot, recv.at[1], me.across)
    push(slot, slot, send.at[2], recv.at[2], me.core).start()


def group_finish(me, src, dst, local, send, recv):
    pltpu.make_async_copy(src, dst.at[me.rank], local).wait()
    arrived(dst.at[2 * me.s + 1 - me.c], recv.at[0], me.core)
    arrived(dst.at[2 * (1 - me.s) + 1 - me.c], recv.at[2], me.core)
    left_over(src, send.at[0], me.core)
    left_over(src, send.at[1], me.across)
    slot = dst.at[2 * (1 - me.s) + me.c]
    left_over(slot, send.at[2], me.core)


def group_sems():
    return [pltpu.SemaphoreType.DMA, pltpu.SemaphoreType.DMA((3,)), pltpu.SemaphoreType.DMA((3,))]


def line_start(me, dst, sems):
    to_right, to_left, line, to_side, side = sems
    slot = dst(me.p)
    push(slot, slot, to_side.at[me.z], side.at[me.z], me.side).start()

    @pl.when(me.has_right)
    def _():
        push(slot, slot, to_right.at[me.z], line.at[me.z], me.right).start()

    @pl.when(me.has_left)
    def _():
        push(slot, slot, to_left.at[me.z], line.at[me.z], me.left).start()


def line_hop(me, dst, sems, hop):
    to_right, to_left, line, to_side, side = sems

    def pass_on(item, back, forth, may, sends):
        slot = dst(2 * item + me.y)
        arrived(slot, line.at[item], back)

        @pl.when(may)
        def _():
            push(slot, slot, sends.at[item], line.at[item], forth).start()

        push(slot, slot, to_side.at[item], side.at[item], me.side).start()

    @pl.when(me.z >= hop)
    def _():
        pass_on(me.z - hop, me.left, me.right, me.has_right, to_right)

    @pl.when(me.z + hop < me.planes)
    def _():
        pass_on(me.z + hop, me.right, me.left, me.has_left, to_left)


def line_finish(me, dst, sems):
    to_right, to_left, line, to_side, side = sems
    for item in range(me.planes):
        arrived(dst(2 * item + 1 - me.y), side.at[item], me.side)
        mine = dst(2 * item + me.y)
        left_over(mine, to_side.at[item], me.side)

        @pl.when(jnp.logical_and(me.has_right, item <= me.z))
        def _():
            left_over(mine, to_right.at[item], me.right)

        @pl.when(jnp.logical_and(me.has_left, item >= me.z))
        def _():
            left_over(mine, to_left.at[item], me.left)


def line_sems(planes):
    return [pltpu.SemaphoreType.DMA((planes,))] * 5


def pick(table, index):
    value = jnp.int32(table[0])
    for i in range(1, len(table)):
        value = jnp.where(index == i, table[i], value)
    return value


def far_first(planes):
    return [sorted(range(planes), key=lambda i, z=z: (-abs(i - z), i)) for z in range(planes)]


def add_into(dst, *others):
    rows = dst.shape[0]

    def body(i, carry):
        strip = pl.ds(pl.multiple_of(i * STRIP, STRIP), STRIP)
        total = dst[strip, :].astype(F32)
        for other in others:
            total = total + other[strip, :].astype(F32)
        dst[strip, :] = total.astype(dst.dtype)
        return carry

    lax.fori_loop(0, rows // STRIP, body, 0)


def reduce_start(me, own, half, sems):
    to_side, side = sems[0], sems[1]
    orders = far_first(me.planes)
    for i in range(me.planes):
        item = pick([o[i] for o in orders], me.z)
        push(own(2 * item + 1 - me.y), half.at[item], to_side.at[item], side.at[item], me.side).start()


def reduce_step(me, own, half, lines, sems, i):
    to_side, side, to_right, to_left, left, right = sems
    item = pick([o[i] for o in far_first(me.planes)], me.z)
    mine = half.at[item]
    arrived(mine, side.at[item], me.side)
    add_into(mine, own(2 * item + me.y))

    @pl.when(jnp.logical_and(me.has_left, item >= me.z))
    def _():
        arrived(lines.at[item], left.at[item], me.left)
        add_into(mine, lines.at[item])

    spot = jnp.where(item == me.z, me.planes, item)

    @pl.when(jnp.logical_and(me.has_right, item <= me.z))
    def _():
        arrived(lines.at[spot], right.at[item], me.right)
        add_into(mine, lines.at[spot])

    @pl.when(item > me.z)
    def _():
        push(mine, lines.at[item], to_right.at[item], left.at[item], me.right).start()

    @pl.when(item < me.z)
    def _():
        there = jnp.where(item == me.z - 1, me.planes, item)
        push(mine, lines.at[there], to_left.at[item], right.at[item], me.left).start()


def reduce_finish(me, own, half, sems):
    to_side, side, to_right, to_left, left, right = sems
    for item in range(me.planes):
        left_over(own(2 * item + 1 - me.y), to_side.at[item], me.side)

        @pl.when(item > me.z)
        def _():
            left_over(half.at[item], to_right.at[item], me.right)

        @pl.when(item < me.z)
        def _():
            left_over(half.at[item], to_left.at[item], me.left)


def reduce_sems(planes):
    return [pltpu.SemaphoreType.DMA((planes,))] * 6


def reduce_buffers(planes, rows, columns):
    return [pltpu.VMEM((planes, rows, columns), BF), pltpu.VMEM((planes + 1, rows, columns), BF)]


def by_chip(ref, rows=None):
    if rows is None:
        return lambda chip: ref.at[chip]
    return lambda chip: ref.at[pl.ds(pl.multiple_of(chip * rows, STRIP), rows)]


def deal_start(me, final, rows, out, local, send, recv):
    mine = out.at[me.rank]
    part = lambda core: final.at[pl.ds(pl.multiple_of(core * rows, rows), rows)]
    pltpu.make_async_copy(part(me.c), mine, local).start()
    push(part(1 - me.c), mine, send.at[0], recv.at[0], me.core).start()
    push(part(me.c), mine, send.at[1], recv.at[1], me.across).start()
    push(part(1 - me.c), mine, send.at[2], recv.at[2], me.corner).start()


def deal_finish(me, final, rows, out, local, send, recv):
    part = lambda core: final.at[pl.ds(pl.multiple_of(core * rows, rows), rows)]
    pltpu.make_async_copy(part(me.c), out.at[me.rank], local).wait()
    left_over(part(1 - me.c), send.at[0], me.core)
    left_over(part(me.c), send.at[1], me.across)
    left_over(part(1 - me.c), send.at[2], me.corner)
    arrived(out.at[2 * me.s + 1 - me.c], recv.at[0], me.core)
    arrived(out.at[2 * (1 - me.s) + me.c], recv.at[1], me.across)
    arrived(out.at[2 * (1 - me.s) + 1 - me.c], recv.at[2], me.corner)


def blocks_start(me, part, got, send, recv):
    for i, seq in enumerate((1 - me.s, me.s)):
        push(part.at[2 * seq + 1 - me.c], got.at[seq], send.at[i], recv.at[i], me.core).start()


def blocks_cross(me, part, got, last, send, recv):
    away = 1 - me.s
    arrived(got.at[away], recv.at[0], me.core)
    add_into(got.at[away], part.at[2 * away + me.c])
    push(got.at[away], last, send.at[2], recv.at[2], me.across).start()


def blocks_finish(me, part, got, last, send, recv):
    arrived(got.at[me.s], recv.at[1], me.core)
    arrived(last, recv.at[2], me.across)
    for i, seq in enumerate((1 - me.s, me.s)):
        left_over(part.at[2 * seq + 1 - me.c], send.at[i], me.core)
    left_over(got.at[1 - me.s], send.at[2], me.across)


def blocks_sems():
    return [pltpu.SemaphoreType.DMA((3,))] * 2


def blocks_buffers(rows, width):
    return [pltpu.VMEM((2, rows, width), BF), pltpu.VMEM((rows, width), BF)]


def strips(rows, body):
    def step(i, carry):
        body(pl.ds(pl.multiple_of(i * STRIP, STRIP), STRIP))
        return carry

    lax.fori_loop(0, rows // STRIP, step, 0)


def comm_call(kernel, ident, outs, out_specs, ins, scratch, name):
    return pl.pallas_call(
        kernel,
        out_shape=outs,
        in_specs=[spec for spec, _ in ins],
        out_specs=out_specs,
        scratch_shapes=scratch,
        name=name,
        compiler_params=pltpu.CompilerParams(
            collective_id=ident, has_side_effects=True, vmem_limit_bytes=60 * 1024 * 1024
        ),
    )(*[value for _, value in ins])


def shape(dims, dtype=BF):
    return jax.ShapeDtypeStruct(dims, dtype)


def split_start(me, parts, dst, keep, send, recv):
    pltpu.make_async_copy(parts.at[me.c], dst(me.c), keep).start()
    push(parts.at[1 - me.c], dst(me.c), send, recv, me.core).start()


def split_finish(me, parts, dst, keep, send, recv):
    pltpu.make_async_copy(parts.at[me.c], dst(me.c), keep).wait()
    arrived(dst(1 - me.c), recv, me.core)
    left_over(parts.at[1 - me.c], send, me.core)


def gather_attention(planes, normed, cot, w_qkv, w_out):
    rows, width = normed.shape
    head = w_out.shape[0]

    def kernel(n_ref, g_ref, qkv_ref, out_ref, n_all, g_all, qkv_all, out_all, *scr):
        it = iter(scr)
        take = lambda k: [next(it) for _ in range(k)]
        n_sems, g_sems, split, line, edge = take(3), take(3), take(3), take(5), take(6)
        me = Place(planes)
        greet(me)
        split_start(me, qkv_ref, lambda core: qkv_all.at[me.p, core], *split)
        group_start(me, n_ref, n_all, *n_sems)
        group_start(me, g_ref, g_all, *g_sems)
        keep, send, recv, to_right, to_left, sides = edge
        here = me.s == me.z // 2
        owner = me.z == me.rank
        spot = out_all.at[me.y, pl.ds(pl.multiple_of(me.c * head, head), head)]
        other = out_all.at[me.y, pl.ds(pl.multiple_of((1 - me.c) * head, head), head)]
        mine = out_all.at[me.y]

        @pl.when(owner)
        def _():
            pltpu.make_async_copy(out_ref, spot, keep).start()

        @pl.when(jnp.logical_and(here, jnp.logical_not(owner)))
        def _():
            push(out_ref, spot, send, recv.at[0], me.core).start()

        split_finish(me, qkv_ref, lambda core: qkv_all.at[me.p, core], *split)
        line_start(me, by_chip(qkv_all), line)

        @pl.when(owner)
        def _():
            pltpu.make_async_copy(out_ref, spot, keep).wait()
            arrived(other, recv.at[0], me.core)

        @pl.when(jnp.logical_and(here, jnp.logical_not(owner)))
        def _():
            left_over(out_ref, send, me.core)

        @pl.when(me.z > me.rank)
        def _():
            arrived(mine, recv.at[1], me.left)

        @pl.when(me.z < me.rank)
        def _():
            arrived(mine, recv.at[1], me.right)

        go_right = jnp.logical_and(me.z >= me.rank, me.has_right)
        go_left = jnp.logical_and(me.z <= me.rank, me.has_left)

        @pl.when(go_right)
        def _():
            push(mine, mine, to_right, recv.at[1], me.right).start()

        @pl.when(go_left)
        def _():
            push(mine, mine, to_left, recv.at[1], me.left).start()

        push(mine, mine, sides.at[0], sides.at[1], me.side).start()
        group_relay(me, n_all, *n_sems[1:])
        for hop in range(1, planes):
            line_hop(me, by_chip(qkv_all), line, hop)
        group_relay(me, g_all, *g_sems[1:])
        line_finish(me, by_chip(qkv_all), line)
        arrived(out_all.at[1 - me.y], sides.at[1], me.side)
        left_over(mine, sides.at[0], me.side)

        @pl.when(go_right)
        def _():
            left_over(mine, to_right, me.right)

        @pl.when(go_left)
        def _():
            left_over(mine, to_left, me.left)

        group_finish(me, n_ref, n_all, *n_sems)
        group_finish(me, g_ref, g_all, *g_sems)

    one, two = pltpu.SemaphoreType.DMA, pltpu.SemaphoreType.DMA((2,))
    return comm_call(
        kernel, 0,
        [shape((4, rows, width)), shape((4, rows, width)),
         shape((2 * planes, 2) + w_qkv.shape[1:]), shape((2, 2 * head, width))],
        [ANY] * 4,
        [(VMEM, normed), (VMEM, cot), (VMEM, w_qkv), (VMEM, w_out)],
        group_sems() + group_sems() + [one] * 3 + line_sems(planes) + [one, one, two, one, one, two],
        "gather_attention",
    )


def norm_back(values, weighted, base):
    scale = inv_rms(values)
    return base + scale * (
        weighted - values * scale * scale * jnp.mean(weighted * values, -1, keepdims=True)
    )


def feed_forward(planes, part, tokens, g_all, w_gu, w_down):
    rows, width = tokens.shape
    total = 4 * rows
    depth, cols = w_gu.shape[2:]
    block = w_down.shape[0]
    units = 2 * planes * block
    half_units = units // 2
    tile, chunk = 2 * rows, 256

    def kernel(part_ref, x_ref, g_ref, gu_loc, dn_loc,
               x1_ref, bo_ref, dx_ref, dx_all, gu_out, dn_out, *scr):
        it = iter(scr)
        take = lambda k: [next(it) for _ in range(k)]
        (got_b, last_b), (got_f, last_f) = take(2), take(2)
        normed, n_all, gu_all, dn_all, mid, dgu, g_gu, back_part, out_part = take(9)
        gu_buf, dn_buf = [take(2), take(2)], take(2)
        x_sems, b_sems, f_sems = take(2), take(2), take(2)
        n_sems, d_sems = take(3), take(3)
        split, line, dn_keep, dn_line = [take(3), take(3)], [take(5), take(5)], take(1)[0], take(5)
        gu_sems, dn_sems, deal, dn_deal = [take(6), take(6)], take(6), [take(3), take(3)], take(3)
        me = Place(planes)
        greet(me)
        tokens_of = lambda ref: Slots(ref, rows)
        dn_slots = by_chip(dn_all, block)
        gu_slots = [by_chip(gu_all.at[h], 2 * depth) for h in range(2)]
        core_rows = lambda h: lambda core: gu_all.at[
            h, pl.ds(pl.multiple_of((2 * me.p + core) * depth, STRIP), depth)
        ]

        for h in range(2):
            split_start(me, gu_loc.at[h], core_rows(h), *split[h])
        keep = pltpu.make_async_copy(dn_loc, dn_slots(me.p), dn_keep)
        keep.start()
        blocks_start(me, part_ref, got_f, *x_sems)
        split_finish(me, gu_loc.at[0], core_rows(0), *split[0])
        line_start(me, gu_slots[0], line[0])
        keep.wait()
        line_start(me, dn_slots, dn_line)
        split_finish(me, gu_loc.at[1], core_rows(1), *split[1])

        blocks_cross(me, part_ref, got_f, last_f, *x_sems)
        line_hop(me, gu_slots[0], line[0], 1)
        line_hop(me, dn_slots, dn_line, 1)
        line_start(me, gu_slots[1], line[1])
        blocks_finish(me, part_ref, got_f, last_f, *x_sems)

        def body(strip):
            value = x_ref[strip, :].astype(F32) + (
                part_ref[me.rank, strip, :].astype(F32)
                + got_f[me.s, strip, :].astype(F32)
                + last_f[strip, :].astype(F32)
            )
            x1_ref[strip, :] = value
            normed[strip, :] = low(value * inv_rms(value))

        strips(rows, body)
        group_start(me, normed, tokens_of(n_all), *n_sems)
        line_hop(me, gu_slots[0], line[0], 2)
        line_hop(me, dn_slots, dn_line, 2)
        group_relay(me, tokens_of(n_all), *n_sems[1:])
        line_hop(me, gu_slots[1], line[1], 1)
        for hop in range(3, planes):
            line_hop(me, gu_slots[0], line[0], hop)
            line_hop(me, dn_slots, dn_line, hop)
        line_finish(me, gu_slots[0], line[0])
        group_finish(me, normed, tokens_of(n_all), *n_sems)
        line_finish(me, dn_slots, dn_line)

        def activations(h, j):
            first = h * half_units + j * chunk

            def step(t, carry):
                toks = pl.ds(pl.multiple_of(t * tile, tile), tile)
                n, g = n_all[toks, :], g_ref[toks, :]
                gate = dot32(n, gu_all[h, :, j * chunk:(j + 1) * chunk])
                up = dot32(n, gu_all[h, :, half_units + j * chunk:half_units + (j + 1) * chunk])
                grad = dot_t(g, dn_all[first:first + chunk, :])
                hidden, d_gate, d_up = mlp_grads(gate, up, grad)
                mid[toks, first:first + chunk] = hidden
                dgu[h, toks, j * chunk:(j + 1) * chunk] = d_gate
                dgu[h, toks, half_units + j * chunk:half_units + (j + 1) * chunk] = d_up
                return carry

            lax.fori_loop(0, total // tile, step, 0)

        def weight_grads(h, out, part):
            third = width // 3

            def step(i, carry):
                feats = pl.ds(pl.multiple_of(part * third + i * chunk, chunk), chunk)
                out[feats, :] = low(dot_l(n_all[:, feats], dgu[h]))
                return carry

            lax.fori_loop(0, third // chunk, step, 0)

        steps = half_units // chunk
        for j in range(steps):
            activations(0, j)
            if j == 0:
                line_hop(me, gu_slots[1], line[1], 2)
        for hop in range(3, planes):
            line_hop(me, gu_slots[1], line[1], hop)
        for part in range(3):
            weight_grads(0, g_gu, part)
        own_gu = [by_chip(g_gu, 2 * depth), by_chip(gu_all.at[0], 2 * depth)]
        line_finish(me, gu_slots[1], line[1])
        reduce_start(me, own_gu[0], gu_buf[0][0], gu_sems[0])
        for j in range(steps):
            activations(1, j)

        def back(i, carry):
            feats = pl.ds(pl.multiple_of(i * chunk, chunk), chunk)
            value = dot_t(dgu[0], gu_all[0, feats, :]) + dot_t(dgu[1], gu_all[1, feats, :])
            back_part[:, feats] = low(value)
            return carry

        lax.fori_loop(0, width // chunk, back, 0)
        blocks_start(me, Slots(back_part, rows), got_b, *b_sems)
        reduce_step(me, own_gu[0], *gu_buf[0], gu_sems[0], 0)

        for part in range(3):
            weight_grads(1, gu_all.at[0], part)
            if part == 0:
                blocks_cross(me, Slots(back_part, rows), got_b, last_b, *b_sems)
        reduce_step(me, own_gu[0], *gu_buf[0], gu_sems[0], 1)
        reduce_start(me, own_gu[1], gu_buf[1][0], gu_sems[1])

        def forth(i, carry):
            feats = pl.ds(pl.multiple_of(i * chunk, chunk), chunk)
            out_part[:, feats] = low(dot32(mid[...], dn_all[:, feats]))
            return carry

        lax.fori_loop(0, width // chunk, forth, 0)
        blocks_finish(me, Slots(back_part, rows), got_b, last_b, *b_sems)

        def grads(strip):
            mine = pl.ds(pl.multiple_of(me.rank * rows + strip.start, STRIP), STRIP)
            weighted = (
                back_part[mine, :].astype(F32)
                + got_b[me.s, strip, :].astype(F32)
                + last_b[strip, :].astype(F32)
            )
            grad = norm_back(x1_ref[strip, :], weighted, g_ref[mine, :].astype(F32))
            dx_ref[strip, :] = grad
            normed[strip, :] = low(grad)

        strips(rows, grads)
        group_start(me, normed, dx_all, *d_sems)
        blocks_start(me, Slots(out_part, rows), got_f, *f_sems)
        reduce_step(me, own_gu[0], *gu_buf[0], gu_sems[0], 2)

        def down(i, carry):
            these = pl.ds(pl.multiple_of(i * chunk, chunk), chunk)
            dn_all[these, :] = low(dot_l(mid[:, these], g_ref[...]))
            return carry

        lax.fori_loop(0, units // chunk, down, 0)
        reduce_start(me, dn_slots, dn_buf[0], dn_sems)
        for i in range(3, planes):
            reduce_step(me, own_gu[0], *gu_buf[0], gu_sems[0], i)
        finals = [gu_buf[h][0].at[me.z] for h in range(2)]
        deal_start(me, finals[0], depth, gu_out.at[0], *deal[0])
        group_relay(me, dx_all, *d_sems[1:])
        blocks_cross(me, Slots(out_part, rows), got_f, last_f, *f_sems)
        reduce_step(me, own_gu[1], *gu_buf[1], gu_sems[1], 0)
        reduce_step(me, own_gu[1], *gu_buf[1], gu_sems[1], 1)
        blocks_finish(me, Slots(out_part, rows), got_f, last_f, *f_sems)

        def output(strip):
            mine = pl.ds(pl.multiple_of(me.rank * rows + strip.start, STRIP), STRIP)
            value = (
                out_part[mine, :].astype(F32)
                + got_f[me.s, strip, :].astype(F32)
                + last_f[strip, :].astype(F32)
            )
            bo_ref[strip, :] = low(x1_ref[strip, :] + value)

        strips(rows, output)
        for i in range(2, planes):
            reduce_step(me, own_gu[1], *gu_buf[1], gu_sems[1], i)
        deal_start(me, finals[1], depth, gu_out.at[1], *deal[1])
        for i in range(planes):
            reduce_step(me, dn_slots, *dn_buf, dn_sems, i)
        final_dn = dn_buf[0].at[me.z]
        keep, send, recv = dn_deal
        pltpu.make_async_copy(final_dn, dn_out.at[me.s], keep).start()
        push(final_dn, dn_out.at[me.s], send, recv, me.across).start()
        for h in range(2):
            reduce_finish(me, own_gu[h], gu_buf[h][0], gu_sems[h])
        reduce_finish(me, dn_slots, dn_buf[0], dn_sems)
        group_finish(me, normed, dx_all, *d_sems)
        for h in range(2):
            deal_finish(me, finals[h], depth, gu_out.at[h], *deal[h])
        pltpu.make_async_copy(final_dn, dn_out.at[me.s], keep).wait()
        left_over(final_dn, send, me.across)
        arrived(dn_out.at[1 - me.s], recv, me.across)

    one, three = pltpu.SemaphoreType.DMA, pltpu.SemaphoreType.DMA((3,))
    vmem = lambda *dims: pltpu.VMEM(dims, BF)
    return comm_call(
        kernel, 1,
        [shape((rows, width), F32), shape((rows, width)), shape((rows, width), F32), shape((4, rows, width)),
         shape((2, 4, depth, cols)), shape((2, block, width))],
        [VMEM, VMEM, VMEM, ANY, ANY, ANY],
        [(VMEM, part), (VMEM, tokens), (VMEM, g_all), (VMEM, w_gu), (VMEM, w_down)],
        blocks_buffers(rows, width) * 2
        + [vmem(rows, width), vmem(total, width), vmem(2, width, cols), vmem(units, width),
           vmem(total, units), vmem(2, total, cols), vmem(width, cols), vmem(total, width), vmem(total, width)]
        + reduce_buffers(planes, 2 * depth, cols) * 2 + reduce_buffers(planes, block, width)
        + blocks_sems() * 3 + group_sems() * 2
        + [one] * 6 + line_sems(planes) * 2 + [one] + line_sems(planes)
        + reduce_sems(planes) * 3 + [one, three, three] * 2 + [one] * 3,
        "feed_forward",
    )


def reduce_attention(planes, part, x, dx, g_qkv, g_out):
    rows, width = dx.shape
    q_rows, q_cols = g_qkv.shape[1:]
    o_rows = g_out.shape[1]

    def kernel(part_ref, x_ref, dx_ref, qkv_ref, out_ref, gx_ref, qkv_out, out_out, *scr):
        it = iter(scr)
        take = lambda k: [next(it) for _ in range(k)]
        got, last = take(2)
        q_buf, (o_half, o_left, o_right) = take(2), take(3)
        b_sems, q_sems, deal = take(2), take(6), take(3)
        side, lines, keep, send, recv = take(5)
        me = Place(planes)
        greet(me)
        push(out_ref.at[1 - me.y], o_half, side.at[0], side.at[1], me.side).start()
        reduce_start(me, by_chip(qkv_ref), q_buf[0], q_sems)
        blocks_start(me, part_ref, got, *b_sems)
        blocks_cross(me, part_ref, got, last, *b_sems)
        arrived(o_half, side.at[1], me.side)
        add_into(o_half, out_ref.at[me.y])

        @pl.when(jnp.logical_and(me.has_left, me.z <= me.rank))
        def _():
            arrived(o_left, lines.at[0], me.left)
            add_into(o_half, o_left)

        @pl.when(jnp.logical_and(me.has_right, me.z >= me.rank))
        def _():
            arrived(o_right, lines.at[1], me.right)
            add_into(o_half, o_right)

        @pl.when(me.z < me.rank)
        def _():
            push(o_half, o_left, lines.at[2], lines.at[0], me.right).start()

        @pl.when(me.z > me.rank)
        def _():
            push(o_half, o_right, lines.at[2], lines.at[1], me.left).start()

        head = o_rows // 2
        mine = o_half.at[pl.ds(pl.multiple_of(me.c * head, head), head)]
        theirs = o_half.at[pl.ds(pl.multiple_of((1 - me.c) * head, head), head)]
        owner = me.z == me.rank

        @pl.when(owner)
        def _():
            pltpu.make_async_copy(mine, out_out, keep).start()
            push(theirs, out_out, send.at[0], recv, me.core).start()
            push(mine, out_out, send.at[1], recv, me.across).start()
            push(theirs, out_out, send.at[2], recv, me.corner).start()

        for i in range(planes - 1):
            reduce_step(me, by_chip(qkv_ref), *q_buf, q_sems, i)
        blocks_finish(me, part_ref, got, last, *b_sems)

        def body(strip):
            weighted = (
                part_ref[me.rank, strip, :].astype(F32)
                + got[me.s, strip, :].astype(F32)
                + last[strip, :].astype(F32)
            )
            gx_ref[strip, :] = low(norm_back(x_ref[strip, :].astype(F32), weighted, dx_ref[strip, :]))

        strips(rows, body)
        reduce_step(me, by_chip(qkv_ref), *q_buf, q_sems, planes - 1)
        final = q_buf[0].at[me.z]
        deal_start(me, final, q_rows // 2, qkv_out, *deal)
        reduce_finish(me, by_chip(qkv_ref), q_buf[0], q_sems)
        left_over(out_ref.at[1 - me.y], side.at[0], me.side)

        @pl.when(me.z < me.rank)
        def _():
            left_over(o_half, lines.at[2], me.right)

        @pl.when(me.z > me.rank)
        def _():
            left_over(o_half, lines.at[2], me.left)

        @pl.when(owner)
        def _():
            pltpu.make_async_copy(mine, out_out, keep).wait()
            left_over(theirs, send.at[0], me.core)
            left_over(mine, send.at[1], me.across)
            left_over(theirs, send.at[2], me.corner)

        @pl.when(jnp.logical_not(owner))
        def _():
            arrived(out_out, recv, me.core)

        deal_finish(me, final, q_rows // 2, qkv_out, *deal)

    one, two, three = pltpu.SemaphoreType.DMA, pltpu.SemaphoreType.DMA((2,)), pltpu.SemaphoreType.DMA((3,))
    return comm_call(
        kernel, 3,
        [shape((rows, width)), shape((4, q_rows // 2, q_cols)), shape((o_rows // 2, width))],
        [VMEM, ANY, ANY],
        [(VMEM, part), (VMEM, x), (VMEM, dx), (VMEM, g_qkv), (VMEM, g_out)],
        blocks_buffers(rows, width) + reduce_buffers(planes, q_rows, q_cols)
        + [pltpu.VMEM((o_rows, width), BF)] * 3
        + blocks_sems() + reduce_sems(planes) + [one, three, three] + [two, three, one, three, one],
        "reduce_attention",
    )


def shards_fast(tokens, cotangent, w_query, w_key, w_value, w_out, w_gate, w_up, w_down, gain_attn, gain_mlp):
    seqs, length, width = tokens.shape
    rows = seqs * length
    depth = w_query.shape[0]
    devices = width // depth
    planes = devices // 4
    chips = 2 * planes
    s = lax.axis_index("seq")
    kv_heads = w_key.shape[1] // HD
    groups = w_query.shape[1] // w_key.shape[1]
    hidden = w_gate.shape[1]
    block = hidden // devices // 2

    x = tokens.reshape(rows, width)
    cot = cotangent.reshape(rows, width)
    xf = x.astype(F32)
    normed = low(xf * inv_rms(xf))

    gain_one, gain_two = gain_attn.astype(F32)[:, None], gain_mlp.astype(F32)[:, None]

    def heads_of(w):
        parts = (w.astype(F32) * gain_one).reshape(depth, 2, 2, -1)
        return jnp.moveaxis(low(lax.dynamic_index_in_dim(parts, s, 1, False)), 1, 0)

    w_qkv = jnp.concatenate([heads_of(w) for w in (w_query, w_key, w_value)], -1)

    def units_of(w):
        parts = (w.astype(F32) * gain_two).reshape(depth, 2, planes, 2, 2, block)
        parts = low(lax.dynamic_index_in_dim(parts, s, 4, False))
        return jnp.transpose(parts, (1, 3, 0, 2, 4)).reshape(2, 2, depth, planes * block)

    w_gu = jnp.concatenate([units_of(w_gate), units_of(w_up)], -1)
    own_down = lax.dynamic_slice_in_dim(w_down, s * block, block, 0)

    n_all, g_all, qkv_all, out_all = gather_attention(planes, normed, cot, w_qkv, w_out)
    n_all, g_all = n_all.reshape(4 * rows, width), g_all.reshape(4 * rows, width)
    qkv_all, out_all = qkv_all.reshape(width, -1), out_all.reshape(-1, width)

    total = 4 * rows
    cosine, sine = rotary(jnp.arange(length, dtype=F32), HD)
    cosine, sine = jnp.tile(cosine, (4 * seqs, 1)), jnp.tile(sine, (4 * seqs, 1))
    own_kv = kv_heads // 4
    cut_q = own_kv * groups * HD
    cut_k = cut_q + own_kv * HD
    projected = dot32(n_all, qkv_all)
    queries = low(rotate(projected[:, :cut_q].reshape(total, -1, HD), cosine, sine))
    keys = low(rotate(projected[:, cut_q:cut_k].reshape(total, -1, HD), cosine, sine))
    values = low(projected[:, cut_k:])
    queries = queries.reshape(4 * seqs, length, own_kv, groups, HD)
    keys = keys.reshape(4 * seqs, length, own_kv, HD)
    values = values.reshape(4 * seqs, length, own_kv, HD)
    probs, mixed = attend(queries, keys, values)
    mixed = mixed.reshape(total, cut_q)
    part_one = low(dot32(mixed, out_all)).reshape(4, rows, width)

    x1, block_out, dx, dx_all, own_gu, own_dn = feed_forward(planes, part_one, x, g_all, w_gu, own_down)
    dx_all = dx_all.reshape(total, width)
    grad_mixed = low(dot_t(dx_all, out_all)).reshape(queries.shape)
    g_out = low(dot_l(mixed, dx_all)).reshape(2, 2 * depth, width)
    grad_q, grad_k, grad_v = attend_back(queries, keys, values, probs, grad_mixed)
    grad_q = low(rotate_back(grad_q.reshape(total, -1, HD), cosine, sine)).reshape(total, -1)
    grad_k = low(rotate_back(grad_k.reshape(total, -1, HD), cosine, sine)).reshape(total, -1)
    grad_qkv = jnp.concatenate([grad_q, grad_k, low(grad_v).reshape(total, -1)], 1)
    part_in = low(dot_t(grad_qkv, qkv_all)).reshape(4, rows, width)
    g_qkv = low(dot_l(n_all, grad_qkv)).reshape(chips, 2 * depth, -1)

    grad_tokens, own_qkv, own_out = reduce_attention(planes, part_in, x, dx, g_qkv, g_out)

    own_qkv = own_qkv.astype(F32)
    cols = lambda a, b: jnp.moveaxis(own_qkv[:, :, a:b], 0, 1).reshape(depth, -1)
    raw_q, raw_k, raw_v = cols(0, cut_q), cols(cut_q, cut_k), cols(cut_k, None)
    own_gu = own_gu.reshape(2, 2, 2, depth, 2, planes, block).astype(F32)
    raw_gu = jnp.transpose(own_gu, (4, 3, 0, 5, 2, 1, 6)).reshape(2, depth, hidden)
    gain_grad = lambda pairs: sum(jnp.sum(w.astype(F32) * raw, 1) for w, raw in pairs)
    return (
        block_out.reshape(tokens.shape),
        grad_tokens.reshape(tokens.shape),
        raw_q * gain_one, raw_k * gain_one, raw_v * gain_one,
        own_out.astype(F32),
        raw_gu[0] * gain_two, raw_gu[1] * gain_two,
        own_dn.reshape(-1, width).astype(F32),
        gain_grad([(w_query, raw_q), (w_key, raw_k), (w_value, raw_v)]),
        gain_grad([(w_gate, raw_gu[0]), (w_up, raw_gu[1])]),
    )


def fits(mesh):
    return mesh.shape["seq"] == 2 and mesh.shape["dp"] == 16


def solution(mesh):
    body = shards_fast if fits(mesh) else shards_plain
    return jax.shard_map(body, mesh=mesh, in_specs=IN_SPECS, out_specs=OUT_SPECS, check_vma=False)
```

```python
import jax
import jax.numpy as jnp
from jax import lax
from jax.experimental import pallas as pl
from jax.experimental.pallas import tpu as pltpu
from jax.sharding import PartitionSpec as P

HD = 96
EPS = 1e-05
THETA = 100000.0


def rotary(positions, width):
    steps_half = jnp.arange(width // 2, dtype=jnp.float32)
    frequency = jnp.power(THETA, -2.0 * steps_half / width)
    angles = positions[:, None] * frequency[None, :]
    cosine = jnp.cos(angles)
    sine = jnp.sin(angles)
    return (jnp.concatenate([cosine, cosine], -1), jnp.concatenate([sine, sine], -1))


def rotate(values, cosine, sine):
    half = values.shape[-1] // 2
    turned = jnp.concatenate([-values[..., half:], values[..., :half]], -1)
    return values * cosine[:, None, :] + turned * sine[:, None, :]


def rotate_back(grads, cosine, sine):
    half = grads.shape[-1] // 2
    sined = grads * sine[:, None, :]
    turned = jnp.concatenate([sined[..., half:], -sined[..., :half]], -1)
    return grads * cosine[:, None, :] + turned


def dot32(left, right):
    return jnp.dot(left, right, preferred_element_type=jnp.float32)


def dot_t(left, right):
    return lax.dot_general(left, right, (((1,), (1,)), ((), ())), preferred_element_type=jnp.float32)


def dot_l(left, right):
    return lax.dot_general(left, right, (((0,), (0,)), ((), ())), preferred_element_type=jnp.float32)


def inv_rms(values):
    return lax.rsqrt(jnp.mean(values * values, axis=-1, keepdims=True) + EPS)


def low(values):
    return values.astype(jnp.bfloat16)


def attend(queries, keys, values):
    rows = queries.shape[1]
    ids = jnp.arange(rows, dtype=jnp.int32)
    visible = ids[:, None] >= ids[None, :]
    scores = HD ** (-0.5) * jnp.einsum("bqkgd,bckd->bkgqc", queries, keys, preferred_element_type=jnp.float32)
    scores = jnp.where(visible, scores, -jnp.inf)
    top = jnp.max(scores, -1, keepdims=True)
    exps = jnp.exp(scores - top)
    probs = exps / jnp.sum(exps, -1, keepdims=True)
    mixed = jnp.einsum("bkgqc,bckd->bqkgd", low(probs), values, preferred_element_type=jnp.float32)
    return probs, low(mixed)


def attend_back(queries, keys, values, probs, grad_mixed):
    grad_values = jnp.einsum("bkgqc,bqkgd->bckd", low(probs), grad_mixed, preferred_element_type=jnp.float32)
    grad_probs = jnp.einsum("bqkgd,bckd->bkgqc", grad_mixed, values, preferred_element_type=jnp.float32)
    grad_scores = low(probs * (grad_probs - jnp.sum(probs * grad_probs, -1, keepdims=True)))
    scale = HD ** (-0.5)
    grad_queries = scale * jnp.einsum("bkgqc,bckd->bqkgd", grad_scores, keys, preferred_element_type=jnp.float32)
    grad_keys = scale * jnp.einsum("bkgqc,bqkgd->bckd", grad_scores, queries, preferred_element_type=jnp.float32)
    return grad_queries, grad_keys, grad_values


def mlp_grads(gate, up, grad_hidden):
    sigma = jax.nn.sigmoid(gate)
    silu = gate * sigma
    hidden = low(silu * up)
    grad_gate = low(grad_hidden * up * sigma * (1.0 + gate * (1.0 - sigma)))
    grad_up = low(grad_hidden * silu)
    return hidden, grad_gate, grad_up


def shards_plain(tokens, cotangent, w_query, w_key, w_value, w_out, w_gate, w_up, w_down, gain_attn, gain_mlp):
    seqs, length, width = tokens.shape
    rows = seqs * length
    kv_heads = w_key.shape[1] // HD
    groups = w_query.shape[1] // w_key.shape[1]
    gather = lambda w: lax.all_gather(w, "dp", axis=0, tiled=True)
    full_query, full_key, full_value, full_out = map(gather, (w_query, w_key, w_value, w_out))
    gains = gather(jnp.stack([gain_attn, gain_mlp], 1)).astype(jnp.float32)
    gain_one, gain_two = gains[:, 0], gains[:, 1]
    full_gate, full_up, full_down = map(gather, (w_gate, w_up, w_down))
    cosine, sine = rotary(jnp.arange(length, dtype=jnp.float32), HD)
    cosine, sine = jnp.tile(cosine, (seqs, 1)), jnp.tile(sine, (seqs, 1))

    inputs = tokens.reshape(rows, width).astype(jnp.float32)
    grad_in = cotangent.reshape(rows, width)
    scale_one = inv_rms(inputs)
    normed = low(inputs * scale_one * gain_one)
    queries = low(rotate(dot32(normed, full_query).reshape(rows, -1, HD), cosine, sine))
    keys = low(rotate(dot32(normed, full_key).reshape(rows, -1, HD), cosine, sine))
    values = low(dot32(normed, full_value))
    queries = queries.reshape(seqs, length, kv_heads, groups, HD)
    keys = keys.reshape(seqs, length, kv_heads, HD)
    values = values.reshape(seqs, length, kv_heads, HD)
    probs, mixed = attend(queries, keys, values)
    mixed = mixed.reshape(rows, -1)
    hidden_one = inputs + dot32(mixed, full_out)
    scale_two = inv_rms(hidden_one)
    normed_two = low(hidden_one * scale_two * gain_two)
    gate, up = dot32(normed_two, full_gate), dot32(normed_two, full_up)
    hidden, grad_gate, grad_up = mlp_grads(gate, up, dot_t(grad_in, full_down))
    block_out = low(hidden_one + dot32(hidden, full_down))

    acc_down = dot_l(hidden, grad_in)
    acc_gate = dot_l(normed_two, grad_gate)
    acc_up = dot_l(normed_two, grad_up)
    grad_normed_two = dot_t(grad_gate, full_gate) + dot_t(grad_up, full_up)
    acc_gain_two = jnp.sum(grad_normed_two * hidden_one * scale_two, 0)
    weighted = grad_normed_two * gain_two
    grad_one = grad_in.astype(jnp.float32) + scale_two * (
        weighted - hidden_one * scale_two * scale_two * jnp.mean(weighted * hidden_one, -1, keepdims=True)
    )
    grad_branch = low(grad_one)
    acc_out = dot_l(mixed, grad_branch)
    grad_mixed = low(dot_t(grad_branch, full_out)).reshape(queries.shape)
    grad_queries, grad_keys, grad_values = attend_back(queries, keys, values, probs, grad_mixed)
    grad_queries = low(rotate_back(grad_queries.reshape(rows, -1, HD), cosine, sine)).reshape(rows, -1)
    grad_keys = low(rotate_back(grad_keys.reshape(rows, -1, HD), cosine, sine)).reshape(rows, -1)
    grad_values = low(grad_values).reshape(rows, -1)
    acc_query = dot_l(normed, grad_queries)
    acc_key = dot_l(normed, grad_keys)
    acc_value = dot_l(normed, grad_values)
    grad_normed = dot_t(grad_queries, full_query) + dot_t(grad_keys, full_key) + dot_t(grad_values, full_value)
    acc_gain_one = jnp.sum(grad_normed * inputs * scale_one, 0)
    weighted = grad_normed * gain_one
    grad_tokens = grad_one + scale_one * (
        weighted - inputs * scale_one * scale_one * jnp.mean(weighted * inputs, -1, keepdims=True)
    )

    def share(acc):
        owned = lax.psum_scatter(low(acc), "dp", scatter_dimension=0, tiled=True)
        return lax.psum(owned, "seq").astype(jnp.float32)

    grads = [share(a) for a in (acc_down, acc_gate, acc_up, acc_out, acc_query, acc_key, acc_value)]
    gain_grads = lax.psum(
        lax.psum_scatter(jnp.stack([acc_gain_one, acc_gain_two], 1), "dp", scatter_dimension=0, tiled=True), "seq"
    )
    down, gate, up, out, query, key, value = grads
    return (
        block_out.reshape(tokens.shape),
        low(grad_tokens).reshape(tokens.shape),
        query, key, value, out, gate, up, down,
        gain_grads[:, 0], gain_grads[:, 1],
    )


ROWS = P(("dp", "seq"), None, None)
SPLIT = P("dp", None)
IN_SPECS = (ROWS, ROWS) + (SPLIT,) * 7 + (P("dp"), P("dp"))
OUT_SPECS = (ROWS, ROWS) + (SPLIT,) * 7 + (P("dp"), P("dp"))


MESH = pl.DeviceIdType.MESH
VMEM = pl.BlockSpec(memory_space=pltpu.VMEM)
ANY = pl.BlockSpec(memory_space=pl.ANY)
BF = jnp.bfloat16
F32 = jnp.float32
STRIP = 16
PIECES = 4
VMEM_BYTES = 66_000_000


class Place:
    def __init__(self, planes):
        self.planes = planes
        d = lax.axis_index("dp")
        self.d, self.s = d, lax.axis_index("seq")
        self.c, self.y, self.z = d % 2, (d // 2) % 2, d // 4
        self.p = d // 2
        self.rank = 2 * self.s + self.c
        self.core = (d + 1 - 2 * self.c, self.s)
        self.across = (d, 1 - self.s)
        self.corner = (d + 1 - 2 * self.c, 1 - self.s)
        self.side = (d + 2 - 4 * self.y, self.s)
        self.right = (lax.rem(d + 4, 4 * planes), self.s)
        self.left = (lax.rem(d + 4 * planes - 4, 4 * planes), self.s)
        self.has_right, self.has_left = self.z < planes - 1, self.z > 0


def greet(me):
    barrier = pltpu.get_barrier_semaphore()
    for peer in (me.core, me.across, me.corner, me.side, me.right, me.left):
        pl.semaphore_signal(barrier, inc=1, device_id=peer, device_id_type=MESH)
    pl.semaphore_wait(barrier, 6)


def push(src, dst, send, recv, peer):
    return pltpu.make_async_remote_copy(
        src_ref=src, dst_ref=dst, send_sem=send, recv_sem=recv, device_id=peer, device_id_type=MESH
    )


def arrived(dst, recv, peer):
    push(dst, dst, recv, recv, peer).wait_recv()


def left_over(src, send, peer):
    push(src, src, send, send, peer).wait_send()


class Slots:
    def __init__(self, ref, rows):
        self.ref, self.rows = ref, rows
        self.at = self

    def __getitem__(self, block):
        return self.ref.at[pl.ds(pl.multiple_of(block * self.rows, self.rows), self.rows)]


def group_start(me, src, dst, send, recv):
    push(src, dst.at[me.rank], send.at[0], recv.at[0], me.core).start()
    push(src, dst.at[me.rank], send.at[1], recv.at[1], me.across).start()


def group_relay(me, dst, send, recv):
    slot = dst.at[2 * (1 - me.s) + me.c]
    arrived(slot, recv.at[1], me.across)
    push(slot, slot, send.at[2], recv.at[2], me.core).start()


def group_finish(me, src, dst, send, recv):
    arrived(dst.at[2 * me.s + 1 - me.c], recv.at[0], me.core)
    arrived(dst.at[2 * (1 - me.s) + 1 - me.c], recv.at[2], me.core)
    left_over(src, send.at[0], me.core)
    left_over(src, send.at[1], me.across)
    slot = dst.at[2 * (1 - me.s) + me.c]
    left_over(slot, send.at[2], me.core)


def group_sems():
    return [pltpu.SemaphoreType.DMA((3,)), pltpu.SemaphoreType.DMA((3,))]


def line_start(me, dst, sems):
    to_right, to_left, line, to_side, side = sems
    slot = dst(me.p)
    push(slot, slot, to_side.at[me.z], side.at[me.z], me.side).start()

    @pl.when(me.has_right)
    def _():
        push(slot, slot, to_right.at[me.z], line.at[me.z], me.right).start()

    @pl.when(me.has_left)
    def _():
        push(slot, slot, to_left.at[me.z], line.at[me.z], me.left).start()


def line_hop(me, dst, sems, hop):
    to_right, to_left, line, to_side, side = sems

    def pass_on(item, back, forth, may, sends):
        slot = dst(2 * item + me.y)
        arrived(slot, line.at[item], back)

        @pl.when(may)
        def _():
            push(slot, slot, sends.at[item], line.at[item], forth).start()

        push(slot, slot, to_side.at[item], side.at[item], me.side).start()

    @pl.when(me.z >= hop)
    def _():
        pass_on(me.z - hop, me.left, me.right, me.has_right, to_right)

    @pl.when(me.z + hop < me.planes)
    def _():
        pass_on(me.z + hop, me.right, me.left, me.has_left, to_left)


def line_finish(me, dst, sems):
    to_right, to_left, line, to_side, side = sems
    for item in range(me.planes):
        arrived(dst(2 * item + 1 - me.y), side.at[item], me.side)
        mine = dst(2 * item + me.y)
        left_over(mine, to_side.at[item], me.side)

        @pl.when(jnp.logical_and(me.has_right, item <= me.z))
        def _():
            left_over(mine, to_right.at[item], me.right)

        @pl.when(jnp.logical_and(me.has_left, item >= me.z))
        def _():
            left_over(mine, to_left.at[item], me.left)


def line_sems(planes):
    return [pltpu.SemaphoreType.DMA((planes,))] * 5


def pick(table, index):
    value = jnp.int32(table[0])
    for i in range(1, len(table)):
        value = jnp.where(index == i, table[i], value)
    return value


def far_first(planes):
    return [sorted(range(planes), key=lambda i, z=z: (-abs(i - z), i)) for z in range(planes)]


def add_into(dst, *others):
    rows = dst.shape[0]

    def body(i, carry):
        strip = pl.ds(pl.multiple_of(i * STRIP, STRIP), STRIP)
        total = dst[strip, :].astype(F32)
        for other in others:
            total = total + other[strip, :].astype(F32)
        dst[strip, :] = total.astype(dst.dtype)
        return carry

    lax.fori_loop(0, rows // STRIP, body, 0)


def reduce_start(me, own, half, sems):
    to_side, side = sems[0], sems[1]
    orders = far_first(me.planes)
    for i in range(me.planes):
        item = pick([o[i] for o in orders], me.z)
        push(own(2 * item + 1 - me.y), half.at[item], to_side.at[item], side.at[item], me.side).start()


def reduce_step(me, own, half, lines, sems, i):
    to_side, side, to_right, to_left, left, right = sems
    item = pick([o[i] for o in far_first(me.planes)], me.z)
    mine = half.at[item]
    arrived(mine, side.at[item], me.side)
    add_into(mine, own(2 * item + me.y))

    @pl.when(jnp.logical_and(me.has_left, item >= me.z))
    def _():
        arrived(lines.at[item], left.at[item], me.left)
        add_into(mine, lines.at[item])

    spot = jnp.where(item == me.z, me.planes, item)

    @pl.when(jnp.logical_and(me.has_right, item <= me.z))
    def _():
        arrived(lines.at[spot], right.at[item], me.right)
        add_into(mine, lines.at[spot])

    @pl.when(item > me.z)
    def _():
        push(mine, lines.at[item], to_right.at[item], left.at[item], me.right).start()

    @pl.when(item < me.z)
    def _():
        there = jnp.where(item == me.z - 1, me.planes, item)
        push(mine, lines.at[there], to_left.at[item], right.at[item], me.left).start()


def reduce_finish(me, own, half, sems):
    to_side, side, to_right, to_left, left, right = sems
    for item in range(me.planes):
        left_over(own(2 * item + 1 - me.y), to_side.at[item], me.side)

        @pl.when(item > me.z)
        def _():
            left_over(half.at[item], to_right.at[item], me.right)

        @pl.when(item < me.z)
        def _():
            left_over(half.at[item], to_left.at[item], me.left)


def reduce_sems(planes):
    return [pltpu.SemaphoreType.DMA((planes,))] * 6


def reduce_buffers(planes, rows, columns):
    return [pltpu.VMEM((planes, rows, columns), BF), pltpu.VMEM((planes + 1, rows, columns), BF)]


def by_chip(ref, rows=None):
    if rows is None:
        return lambda chip: ref.at[chip]
    return lambda chip: ref.at[pl.ds(pl.multiple_of(chip * rows, STRIP), rows)]


def deal_start(me, final, rows, out, local, send, recv):
    mine = out.at[me.rank]
    part = lambda core: final.at[pl.ds(pl.multiple_of(core * rows, rows), rows)]
    pltpu.make_async_copy(part(me.c), mine, local).start()
    push(part(1 - me.c), mine, send.at[0], recv.at[0], me.core).start()
    push(part(me.c), mine, send.at[1], recv.at[1], me.across).start()
    push(part(1 - me.c), mine, send.at[2], recv.at[2], me.corner).start()


def deal_finish(me, final, rows, out, local, send, recv):
    part = lambda core: final.at[pl.ds(pl.multiple_of(core * rows, rows), rows)]
    pltpu.make_async_copy(part(me.c), out.at[me.rank], local).wait()
    left_over(part(1 - me.c), send.at[0], me.core)
    left_over(part(me.c), send.at[1], me.across)
    left_over(part(1 - me.c), send.at[2], me.corner)
    arrived(out.at[2 * me.s + 1 - me.c], recv.at[0], me.core)
    arrived(out.at[2 * (1 - me.s) + me.c], recv.at[1], me.across)
    arrived(out.at[2 * (1 - me.s) + 1 - me.c], recv.at[2], me.corner)


def blocks_start(me, part, got, send, recv, i):
    seq = (1 - me.s, me.s)[i]
    push(part.at[2 * seq + 1 - me.c], got.at[seq], send.at[i], recv.at[i], me.core).start()


def blocks_cross(me, part, got, last, send, recv):
    away = 1 - me.s
    arrived(got.at[away], recv.at[0], me.core)
    add_into(got.at[away], part.at[2 * away + me.c])
    push(got.at[away], last, send.at[2], recv.at[2], me.across).start()


def blocks_finish(me, part, got, last, send, recv):
    arrived(got.at[me.s], recv.at[1], me.core)
    arrived(last, recv.at[2], me.across)
    for i, seq in enumerate((1 - me.s, me.s)):
        left_over(part.at[2 * seq + 1 - me.c], send.at[i], me.core)
    left_over(got.at[1 - me.s], send.at[2], me.across)


def blocks_sems():
    return [pltpu.SemaphoreType.DMA((3,))] * 2


def blocks_buffers(rows, width):
    return [pltpu.VMEM((2, rows, width), BF), pltpu.VMEM((rows, width), BF)]


def strips(rows, body):
    def step(i, carry):
        body(pl.ds(pl.multiple_of(i * STRIP, STRIP), STRIP))
        return carry

    lax.fori_loop(0, rows // STRIP, step, 0)


def comm_call(kernel, ident, outs, out_specs, ins, scratch, name):
    return pl.pallas_call(
        kernel,
        out_shape=outs,
        in_specs=[spec for spec, _ in ins],
        out_specs=out_specs,
        scratch_shapes=scratch,
        name=name,
        compiler_params=pltpu.CompilerParams(
            collective_id=ident, has_side_effects=True, vmem_limit_bytes=VMEM_BYTES
        ),
    )(*[value for _, value in ins])


def shape(dims, dtype=BF):
    return jax.ShapeDtypeStruct(dims, dtype)


def split_start(me, parts, dst, keep, send, recv):
    pltpu.make_async_copy(parts.at[me.c], dst(me.c), keep).start()
    push(parts.at[1 - me.c], dst(me.c), send, recv, me.core).start()


def split_finish(me, parts, dst, keep, send, recv):
    pltpu.make_async_copy(parts.at[me.c], dst(me.c), keep).wait()
    arrived(dst(1 - me.c), recv, me.core)
    left_over(parts.at[1 - me.c], send, me.core)


def norm_back(values, weighted, base):
    scale = inv_rms(values)
    return base + scale * (
        weighted - values * scale * scale * jnp.mean(weighted * values, -1, keepdims=True)
    )


LANES = 128


def head_tables(length):
    cosine, sine = rotary(jnp.arange(length, dtype=F32), HD)
    pad = ((0, 0), (0, LANES - HD))
    low_half = jnp.arange(HD) < HD // 2
    tables = [cosine, jnp.where(low_half, 0.0, sine), jnp.where(low_half, -sine, 0.0)]
    row, col = jnp.arange(4 * HD)[:, None], jnp.arange(4 * LANES)[None, :]
    spread = (row // HD == col // LANES) & (row % HD == col % LANES)
    return jnp.stack([jnp.pad(t, pad) for t in tables]), spread.astype(BF)


def turn(values, tables, sign):
    other = pltpu.roll(values, HD // 2, 1) * tables[1] + pltpu.roll(values, LANES - HD // 2, 1) * tables[2]
    return values * tables[0] + sign * other


def block_step(planes, length, tokens, n_own, g_own, w_qkv, w_out, w_gu, w_down):
    rows, width = tokens.shape
    total = 4 * rows
    head = w_out.shape[0]
    q_cols = w_qkv.shape[2]
    depth, cols = w_gu.shape[2:]
    block = w_down.shape[0]
    units = 2 * planes * block
    half_units = units // 2
    tile, chunk = 2 * rows, 256
    heads4 = 4 * head
    piece = 2 * head // PIECES
    tables, spread = head_tables(length)

    def kernel(x_ref, n_loc, g_loc, qkv_loc, out_loc, gu_loc, dn_loc, tab_ref, sel_ref,
               bo_ref, gx_ref, qkv_out, out_out, gu_out, dn_out, stash, *scr):
        it = iter(scr)
        take = lambda k: [next(it) for _ in range(k)]
        n_buf, g_all, qkv_all, out_all, gu_all, dn_all, heads, mixed = take(8)
        part, out_part, x1, mid, dgu, g_gu, dx_all = take(7)
        (got, last), (got_f, last_f) = take(2), take(2)
        gu_buf, dn_buf, q_buf, o_buf = [take(2), take(2)], take(2), take(2), take(3)
        n_sems, g_sems, m_sems, d_sems = take(2), take(2), take(2), take(2)
        x_sems, b_sems, f_sems, h_sems = take(2), take(2), take(2), take(2)
        q_split, gu_split = take(3), [take(3), take(3)]
        q_line, gu_line, dn_line = take(5), [take(5), take(5)], take(5)
        gu_sems, dn_sems, q_sems = [take(6), take(6)], take(6), take(6)
        gu_deal, dn_deal, q_deal, o_deal = [take(3), take(3)], take(3), take(3), take(3)
        local, edge, o_fan, o_red = take(4)
        me = Place(planes)
        greet(me)
        tok = lambda ref: Slots(ref, rows)
        q_slots, dn_slots = by_chip(qkv_all, 2 * depth), by_chip(dn_all, block)
        gu_slots = [by_chip(gu_all.at[h], 2 * depth) for h in range(2)]

        def core_rows(ref):
            return lambda core: ref.at[pl.ds(pl.multiple_of((2 * me.p + core) * depth, STRIP), depth)]

        split_start(me, qkv_loc, core_rows(qkv_all), *q_split)
        keep_n = pltpu.make_async_copy(n_loc, tok(n_buf).at[me.rank], local.at[0])
        keep_n.start()
        group_start(me, n_loc, tok(n_buf), *n_sems)
        here = me.s == me.z // 2
        owner = me.z == me.rank
        lender = jnp.logical_and(here, jnp.logical_not(owner))
        half = lambda y: out_all.at[pl.ds(pl.multiple_of(y * 2 * head, STRIP), 2 * head)]
        head_rows = lambda core: out_all.at[pl.ds(pl.multiple_of((2 * me.y + core) * head, STRIP), head)]
        keep_o = pltpu.make_async_copy(out_loc, head_rows(me.c), local.at[1])

        @pl.when(owner)
        def _():
            keep_o.start()

        @pl.when(lender)
        def _():
            push(out_loc, head_rows(me.c), edge.at[0], edge.at[1], me.core).start()

        for h in range(2):
            split_start(me, gu_loc.at[h], core_rows(gu_all.at[h]), *gu_split[h])
        keep_d = pltpu.make_async_copy(dn_loc, dn_slots(me.p), local.at[2])
        keep_d.start()
        keep_g = pltpu.make_async_copy(g_loc, tok(g_all).at[me.rank], local.at[3])
        keep_g.start()
        fetch_x = pltpu.make_async_copy(x_ref, last_f, local.at[4])
        fetch_x.start()
        split_finish(me, qkv_loc, core_rows(qkv_all), *q_split)
        line_start(me, q_slots, q_line)
        group_start(me, g_loc, tok(g_all), *g_sems)

        fan_in, fan_right, fan_left, fan_side, fan_other = [o_fan.at[k] for k in range(5)]
        bit = lambda y, q: out_all.at[pl.ds(pl.multiple_of(y * 2 * head + q * piece, STRIP), piece)]
        go_right = jnp.logical_and(me.z >= me.rank, me.has_right)
        go_left = jnp.logical_and(me.z <= me.rank, me.has_left)

        def fan(q):
            mine = bit(me.y, q)

            @pl.when(me.z > me.rank)
            def _():
                arrived(mine, fan_in.at[q], me.left)

            @pl.when(me.z < me.rank)
            def _():
                arrived(mine, fan_in.at[q], me.right)

            @pl.when(go_right)
            def _():
                push(mine, mine, fan_right.at[q], fan_in.at[q], me.right).start()

            @pl.when(go_left)
            def _():
                push(mine, mine, fan_left.at[q], fan_in.at[q], me.left).start()

            push(mine, mine, fan_side.at[q], fan_other.at[q], me.side).start()

        @pl.when(owner)
        def _():
            keep_o.wait()
            arrived(head_rows(1 - me.c), edge.at[1], me.core)

        @pl.when(lender)
        def _():
            left_over(out_loc, edge.at[0], me.core)

        line_hop(me, q_slots, q_line, 1)
        fan(0)
        line_hop(me, q_slots, q_line, 2)
        group_relay(me, tok(n_buf), *n_sems)
        fan(1)
        for hop in range(3, planes):
            line_hop(me, q_slots, q_line, hop)
        fan(2)
        fan(3)
        split_finish(me, gu_loc.at[0], core_rows(gu_all.at[0]), *gu_split[0])
        line_start(me, gu_slots[0], gu_line[0])
        keep_d.wait()
        line_start(me, dn_slots, dn_line)
        split_finish(me, gu_loc.at[1], core_rows(gu_all.at[1]), *gu_split[1])
        keep_n.wait()
        group_finish(me, n_loc, tok(n_buf), *n_sems)
        saved = pltpu.make_async_copy(n_buf, stash, local.at[0])
        saved.start()
        line_finish(me, q_slots, q_line)

        def widen(i, carry):
            feats = pl.ds(pl.multiple_of(i * tile, tile), tile)
            for k in range(2):
                g_gu[feats, k * 4 * LANES:(k + 1) * 4 * LANES] = low(
                    dot32(qkv_all[feats, k * heads4:(k + 1) * heads4], sel_ref[...])
                )
            return carry

        lax.fori_loop(0, width // tile, widen, 0)

        def project(i, carry):
            toks = pl.ds(pl.multiple_of(i * length, length), length)
            n = n_buf[toks, :]
            tabs = [tab_ref[k] for k in range(3)]
            for k in range(8):
                value = dot32(n, g_gu[:, k * LANES:(k + 1) * LANES])
                heads[toks, k * LANES:(k + 1) * LANES] = low(turn(value, tabs, 1.0) if k < 6 else value)
            return carry

        lax.fori_loop(0, total // length, project, 0)
        line_hop(me, gu_slots[0], gu_line[0], 1)
        group_relay(me, tok(g_all), *g_sems)
        line_hop(me, dn_slots, dn_line, 1)
        saved.wait()
        for q in range(PIECES):
            arrived(bit(1 - me.y, q), fan_other.at[q], me.side)

        def pair(toks, j, ref, start):
            first = start + 2 * j * LANES
            return jnp.concatenate(
                [ref[toks, first:first + LANES], ref[toks, first + LANES:first + 2 * LANES]], 0
            )

        def probabilities(toks, j):
            q = pair(toks, j, heads, 0)
            k = heads[toks, (4 + j) * LANES:(5 + j) * LANES]
            scores = HD ** (-0.5) * dot_t(q, k)
            row = lax.rem(lax.broadcasted_iota(jnp.int32, scores.shape, 0), length)
            col = lax.broadcasted_iota(jnp.int32, scores.shape, 1)
            scores = jnp.where(row >= col, scores, -jnp.inf)
            exps = jnp.exp(scores - jnp.max(scores, 1, keepdims=True))
            return q, k, exps / jnp.sum(exps, 1, keepdims=True)

        def attend_rows(first):
            def one(i, carry):
                toks = pl.ds(pl.multiple_of(first + i * length, length), length)
                outs = []
                for j in range(2):
                    _, _, p = probabilities(toks, j)
                    o = low(dot32(low(p), heads[toks, (6 + j) * LANES:(7 + j) * LANES]))
                    outs += [o[:length], o[length:]]
                mixed[toks, :] = low(dot_t(jnp.concatenate(outs, 1), sel_ref[...]))
                return carry

            lax.fori_loop(0, rows // length, one, 0)
            toks = pl.ds(pl.multiple_of(first, rows), rows)
            part[toks, :] = low(dot32(mixed[toks, :], out_all[...]))

        away, home = 1 - me.s, me.s
        attend_rows((2 * away + 1 - me.c) * rows)
        blocks_start(me, tok(part), got, *x_sems, 0)
        line_hop(me, gu_slots[0], gu_line[0], 2)
        attend_rows((2 * away + me.c) * rows)
        blocks_cross(me, tok(part), got, last, *x_sems)
        line_hop(me, dn_slots, dn_line, 2)
        attend_rows((2 * home + 1 - me.c) * rows)
        blocks_start(me, tok(part), got, *x_sems, 1)
        line_start(me, gu_slots[1], gu_line[1])
        attend_rows((2 * home + me.c) * rows)
        for hop in range(3, planes):
            line_hop(me, gu_slots[0], gu_line[0], hop)
        blocks_finish(me, tok(part), got, last, *x_sems)

        def mine(strip):
            return pl.ds(pl.multiple_of(me.rank * rows + strip.start, STRIP), STRIP)

        def summed(strip, whole, some, rest):
            return (
                whole[mine(strip), :].astype(F32)
                + some[me.s, strip, :].astype(F32)
                + rest[strip, :].astype(F32)
            )

        fetch_x.wait()

        def middle(strip):
            value = last_f[strip, :].astype(F32) + summed(strip, part, got, last)
            x1[strip, :] = value
            n_buf[mine(strip), :] = low(value * inv_rms(value))

        strips(rows, middle)
        group_start(me, tok(n_buf).at[me.rank], tok(n_buf), *m_sems)
        for hop in range(3, planes):
            line_hop(me, dn_slots, dn_line, hop)
        line_hop(me, gu_slots[1], gu_line[1], 1)
        keep_g.wait()
        group_finish(me, g_loc, tok(g_all), *g_sems)
        for q in range(PIECES):
            left_over(bit(me.y, q), fan_side.at[q], me.side)

            @pl.when(go_right)
            def _():
                left_over(bit(me.y, q), fan_right.at[q], me.right)

            @pl.when(go_left)
            def _():
                left_over(bit(me.y, q), fan_left.at[q], me.left)

        group_relay(me, tok(n_buf), *m_sems)
        group_finish(me, tok(n_buf).at[me.rank], tok(n_buf), *m_sems)
        line_finish(me, gu_slots[0], gu_line[0])
        line_finish(me, dn_slots, dn_line)

        def activations(h, j):
            first = h * half_units + j * chunk

            def step(t, carry):
                toks = pl.ds(pl.multiple_of(t * tile, tile), tile)
                n, g = n_buf[toks, :], g_all[toks, :]
                gate = dot32(n, gu_all[h, :, j * chunk:(j + 1) * chunk])
                up = dot32(n, gu_all[h, :, half_units + j * chunk:half_units + (j + 1) * chunk])
                grad = dot_t(g, dn_all[first:first + chunk, :])
                hidden, d_gate, d_up = mlp_grads(gate, up, grad)
                mid[toks, first:first + chunk] = hidden
                dgu[h, toks, j * chunk:(j + 1) * chunk] = d_gate
                dgu[h, toks, half_units + j * chunk:half_units + (j + 1) * chunk] = d_up
                return carry

            lax.fori_loop(0, total // tile, step, 0)

        def weight_grads(h, out, third):
            def step(i, carry):
                feats = pl.ds(pl.multiple_of(third * (width // 3) + i * chunk, chunk), chunk)
                out[feats, :] = low(dot_l(n_buf[:, feats], dgu[h]))
                return carry

            lax.fori_loop(0, width // 3 // chunk, step, 0)

        steps = half_units // chunk
        for j in range(steps):
            activations(0, j)
            if j == 0:
                line_hop(me, gu_slots[1], gu_line[1], 2)
        for hop in range(3, planes):
            line_hop(me, gu_slots[1], gu_line[1], hop)
        for third in range(3):
            weight_grads(0, g_gu, third)
        own_gu = [by_chip(g_gu, 2 * depth), gu_slots[0]]
        line_finish(me, gu_slots[1], gu_line[1])
        reduce_start(me, own_gu[0], gu_buf[0][0], gu_sems[0])
        for j in range(steps):
            activations(1, j)

        def back(seq):
            toks = pl.ds(pl.multiple_of(seq * tile, tile), tile)

            def step(i, carry):
                feats = pl.ds(pl.multiple_of(i * chunk, chunk), chunk)
                value = dot_t(dgu[0, toks, :], gu_all[0, feats, :]) + dot_t(dgu[1, toks, :], gu_all[1, feats, :])
                part[toks, feats] = low(value)
                return carry

            lax.fori_loop(0, width // chunk, step, 0)

        back(away)
        blocks_start(me, tok(part), got, *b_sems, 0)
        back(home)
        blocks_start(me, tok(part), got, *b_sems, 1)
        blocks_cross(me, tok(part), got, last, *b_sems)
        reduce_step(me, own_gu[0], *gu_buf[0], gu_sems[0], 0)

        for third in range(3):
            weight_grads(1, gu_all.at[0], third)
        fetch_n = pltpu.make_async_copy(stash, n_buf, local.at[0])
        fetch_n.start()
        reduce_step(me, own_gu[0], *gu_buf[0], gu_sems[0], 1)
        reduce_start(me, own_gu[1], gu_buf[1][0], gu_sems[1])
        blocks_finish(me, tok(part), got, last, *b_sems)

        def branch(strip):
            grad = norm_back(x1[strip, :], summed(strip, part, got, last), g_all[mine(strip), :].astype(F32))
            dx_all[mine(strip), :] = low(grad)

        strips(rows, branch)
        group_start(me, tok(dx_all).at[me.rank], tok(dx_all), *d_sems)

        def forth(i, carry):
            feats = pl.ds(pl.multiple_of(i * chunk, chunk), chunk)
            out_part[:, feats] = low(dot32(mid[...], dn_all[:, feats]))
            return carry

        lax.fori_loop(0, width // chunk, forth, 0)
        for i in range(2):
            blocks_start(me, tok(out_part), got_f, *f_sems, i)
        reduce_step(me, own_gu[0], *gu_buf[0], gu_sems[0], 2)

        def down(i, carry):
            these = pl.ds(pl.multiple_of(i * chunk, chunk), chunk)
            dn_all[these, :] = low(dot_l(mid[:, these], g_all[...]))
            return carry

        lax.fori_loop(0, units // chunk, down, 0)
        reduce_start(me, dn_slots, dn_buf[0], dn_sems)
        group_relay(me, tok(dx_all), *d_sems)
        for i in range(3, planes):
            reduce_step(me, own_gu[0], *gu_buf[0], gu_sems[0], i)
        finals = [gu_buf[h][0].at[me.z] for h in range(2)]
        deal_start(me, finals[0], depth, gu_out.at[0], *gu_deal[0])
        blocks_cross(me, tok(out_part), got_f, last_f, *f_sems)
        group_finish(me, tok(dx_all).at[me.rank], tok(dx_all), *d_sems)

        def spread_out(t, carry):
            toks = pl.ds(pl.multiple_of(t * rows, rows), rows)
            grad = low(dot_t(dx_all[toks, :], out_all[...]))
            mid[toks, 0:4 * LANES] = low(dot32(grad, sel_ref[...]))
            return carry

        lax.fori_loop(0, 4, spread_out, 0)
        out_all[...] = low(dot_l(mixed[...], dx_all[...]))
        for q in range(PIECES):
            push(bit(1 - me.y, q), o_buf[0].at[pl.ds(q * piece, piece)], o_red.at[0, q], o_red.at[1, q], me.side).start()
        reduce_step(me, own_gu[1], *gu_buf[1], gu_sems[1], 0)

        def attend_rows_back(first):
            def one(i, carry):
                toks = pl.ds(pl.multiple_of(first + i * length, length), length)
                tabs = [tab_ref[k] for k in range(3)]
                for j in range(2):
                    q, k, p = probabilities(toks, j)
                    v = heads[toks, (6 + j) * LANES:(7 + j) * LANES]
                    grad = pair(toks, j, mid, 0)
                    d_v = dot_l(low(p), grad)
                    d_p = dot_t(grad, v)
                    d_s = low(p * (d_p - jnp.sum(p * d_p, 1, keepdims=True)))
                    d_q = HD ** (-0.5) * dot32(d_s, k)
                    d_k = HD ** (-0.5) * dot_l(d_s, q)
                    for g in range(2):
                        spot = (2 * j + g) * LANES
                        dgu[0, toks, spot:spot + LANES] = low(turn(d_q[g * length:(g + 1) * length], tabs, -1.0))
                    dgu[0, toks, (4 + j) * LANES:(5 + j) * LANES] = low(turn(d_k, tabs, -1.0))
                    dgu[0, toks, (6 + j) * LANES:(7 + j) * LANES] = low(d_v)
                return carry

            lax.fori_loop(0, rows // length, one, 0)
            toks = pl.ds(pl.multiple_of(first, rows), rows)
            for k in range(2):
                dgu[1, toks, k * heads4:(k + 1) * heads4] = low(
                    dot_t(dgu[0, toks, k * 4 * LANES:(k + 1) * 4 * LANES], sel_ref[...])
                )
            part[toks, :] = low(dot_t(dgu[1, toks, 0:q_cols], qkv_all[...]))

        attend_rows_back((2 * away + 1 - me.c) * rows)
        blocks_start(me, tok(part), got, *h_sems, 0)
        reduce_step(me, own_gu[1], *gu_buf[1], gu_sems[1], 1)
        attend_rows_back((2 * away + me.c) * rows)
        reduce_step(me, own_gu[1], *gu_buf[1], gu_sems[1], 2)
        attend_rows_back((2 * home + 1 - me.c) * rows)
        blocks_start(me, tok(part), got, *h_sems, 1)
        attend_rows_back((2 * home + me.c) * rows)
        fetch_n.wait()

        def q_grads(i, carry):
            feats = pl.ds(pl.multiple_of(i * chunk, chunk), chunk)
            qkv_all[feats, :] = low(dot_l(n_buf[:, feats], dgu[1, :, 0:q_cols]))
            return carry

        lax.fori_loop(0, width // chunk, q_grads, 0)
        reduce_start(me, q_slots, q_buf[0], q_sems)
        blocks_cross(me, tok(part), got, last, *h_sems)
        for i in range(3, planes):
            reduce_step(me, own_gu[1], *gu_buf[1], gu_sems[1], i)
        deal_start(me, finals[1], depth, gu_out.at[1], *gu_deal[1])

        blocks_finish(me, tok(out_part), got_f, last_f, *f_sems)

        def output(strip):
            got_f[me.s, strip, :] = low(x1[strip, :] + summed(strip, out_part, got_f, last_f))

        strips(rows, output)
        keep_bo = pltpu.make_async_copy(got_f.at[me.s], bo_ref, local.at[1])
        keep_bo.start()
        fetch_x.start()
        for i in range(planes):
            reduce_step(me, dn_slots, *dn_buf, dn_sems, i)
        final_dn = dn_buf[0].at[me.z]
        dn_keep, dn_send, dn_recv = dn_deal
        keep_dn = pltpu.make_async_copy(final_dn, dn_out.at[me.s], dn_keep)
        keep_dn.start()
        push(final_dn, dn_out.at[me.s], dn_send, dn_recv, me.across).start()

        blocks_finish(me, tok(part), got, last, *h_sems)
        fetch_x.wait()

        def inner(strip):
            got[me.s, strip, :] = low(norm_back(
                last_f[strip, :].astype(F32), summed(strip, part, got, last), dx_all[mine(strip), :].astype(F32)
            ))

        strips(rows, inner)
        keep_gx = pltpu.make_async_copy(got.at[me.s], gx_ref, local.at[2])
        keep_gx.start()

        for q in range(PIECES):
            here_q = pl.ds(q * piece, piece)
            sum_q = o_buf[0].at[here_q]
            arrived(sum_q, o_red.at[1, q], me.side)
            add_into(sum_q, bit(me.y, q))

            @pl.when(jnp.logical_and(me.has_left, me.z <= me.rank))
            def _():
                arrived(o_buf[1].at[here_q], o_red.at[2, q], me.left)
                add_into(sum_q, o_buf[1].at[here_q])

            @pl.when(jnp.logical_and(me.has_right, me.z >= me.rank))
            def _():
                arrived(o_buf[2].at[here_q], o_red.at[3, q], me.right)
                add_into(sum_q, o_buf[2].at[here_q])

            @pl.when(me.z < me.rank)
            def _():
                push(sum_q, o_buf[1].at[here_q], o_red.at[4, q], o_red.at[2, q], me.right).start()

            @pl.when(me.z > me.rank)
            def _():
                push(sum_q, o_buf[2].at[here_q], o_red.at[4, q], o_red.at[3, q], me.left).start()

        own_half = o_buf[0].at[pl.ds(pl.multiple_of(me.c * head, STRIP), head)]
        other_half = o_buf[0].at[pl.ds(pl.multiple_of((1 - me.c) * head, STRIP), head)]
        o_keep, o_send, o_recv = o_deal
        keep_oo = pltpu.make_async_copy(own_half, out_out, o_keep)

        @pl.when(owner)
        def _():
            keep_oo.start()
            push(other_half, out_out, o_send.at[0], o_recv.at[0], me.core).start()
            push(own_half, out_out, o_send.at[1], o_recv.at[0], me.across).start()
            push(other_half, out_out, o_send.at[2], o_recv.at[0], me.corner).start()

        for i in range(planes):
            reduce_step(me, q_slots, *q_buf, q_sems, i)
        final_q = q_buf[0].at[me.z]
        deal_start(me, final_q, depth, qkv_out, *q_deal)

        for h in range(2):
            reduce_finish(me, own_gu[h], gu_buf[h][0], gu_sems[h])
            deal_finish(me, finals[h], depth, gu_out.at[h], *gu_deal[h])
        reduce_finish(me, dn_slots, dn_buf[0], dn_sems)
        reduce_finish(me, q_slots, q_buf[0], q_sems)
        for q in range(PIECES):
            sum_q = o_buf[0].at[pl.ds(q * piece, piece)]
            left_over(bit(1 - me.y, q), o_red.at[0, q], me.side)

            @pl.when(me.z < me.rank)
            def _():
                left_over(sum_q, o_red.at[4, q], me.right)

            @pl.when(me.z > me.rank)
            def _():
                left_over(sum_q, o_red.at[4, q], me.left)

        @pl.when(owner)
        def _():
            keep_oo.wait()
            left_over(other_half, o_send.at[0], me.core)
            left_over(own_half, o_send.at[1], me.across)
            left_over(other_half, o_send.at[2], me.corner)

        @pl.when(jnp.logical_not(owner))
        def _():
            arrived(out_out, o_recv.at[0], me.core)

        keep_dn.wait()
        left_over(final_dn, dn_send, me.across)
        arrived(dn_out.at[1 - me.s], dn_recv, me.across)
        keep_bo.wait()
        keep_gx.wait()
        deal_finish(me, final_q, depth, qkv_out, *q_deal)

    sems = lambda *dims: pltpu.SemaphoreType.DMA(dims)
    one, three = pltpu.SemaphoreType.DMA, sems(3)
    vmem = lambda *dims: pltpu.VMEM(dims, BF)
    deal = [one, three, three]
    outs = comm_call(
        kernel, 0,
        [shape((rows, width)), shape((rows, width)), shape((4, depth, q_cols)), shape((head, width)),
         shape((2, 4, depth, cols)), shape((2, block, width)), shape((total, width))],
        [ANY] * 7,
        [(ANY, tokens), (ANY, n_own), (ANY, g_own), (ANY, w_qkv), (ANY, w_out), (ANY, w_gu), (ANY, w_down),
         (VMEM, tables), (VMEM, spread)],
        [vmem(total, width), vmem(total, width), vmem(width, q_cols), vmem(heads4, width), vmem(2, width, cols),
         vmem(units, width), vmem(total, 8 * LANES), vmem(total, heads4)]
        + [vmem(total, width), vmem(total, width), pltpu.VMEM((rows, width), F32), vmem(total, units),
           vmem(2, total, cols), vmem(width, cols), vmem(total, width)]
        + blocks_buffers(rows, width) * 2
        + reduce_buffers(planes, 2 * depth, cols) * 2 + reduce_buffers(planes, block, width)
        + reduce_buffers(planes, 2 * depth, q_cols) + [vmem(2 * head, width)] * 3
        + group_sems() * 4 + blocks_sems() * 4 + [one] * 9
        + line_sems(planes) * 4 + reduce_sems(planes) * 4 + deal * 2 + [one] * 3 + deal * 2
        + [sems(5), sems(2), sems(5, PIECES), sems(5, PIECES)],
        "block_step",
    )
    return outs[:6]


def shards_fast(tokens, cotangent, w_query, w_key, w_value, w_out, w_gate, w_up, w_down, gain_attn, gain_mlp):
    seqs, length, width = tokens.shape
    rows = seqs * length
    depth = w_query.shape[0]
    devices = width // depth
    planes = devices // 4
    chips = 2 * planes
    s = lax.axis_index("seq")
    kv_heads = w_key.shape[1] // HD
    groups = w_query.shape[1] // w_key.shape[1]
    hidden = w_gate.shape[1]
    block = hidden // devices // 2

    x = tokens.reshape(rows, width)
    cot = cotangent.reshape(rows, width)
    xf = x.astype(F32)
    normed = low(xf * inv_rms(xf))

    gain_one, gain_two = gain_attn.astype(F32)[:, None], gain_mlp.astype(F32)[:, None]

    def heads_of(w):
        parts = (w.astype(F32) * gain_one).reshape(depth, 2, 2, -1)
        return jnp.moveaxis(low(lax.dynamic_index_in_dim(parts, s, 1, False)), 1, 0)

    w_qkv = jnp.concatenate([heads_of(w) for w in (w_query, w_key, w_value)], -1)

    def units_of(w):
        parts = (w.astype(F32) * gain_two).reshape(depth, 2, planes, 2, 2, block)
        parts = low(lax.dynamic_index_in_dim(parts, s, 4, False))
        return jnp.transpose(parts, (1, 3, 0, 2, 4)).reshape(2, 2, depth, planes * block)

    w_gu = jnp.concatenate([units_of(w_gate), units_of(w_up)], -1)
    own_down = lax.dynamic_slice_in_dim(w_down, s * block, block, 0)

    cut_q = kv_heads // 4 * groups * HD
    cut_k = cut_q + kv_heads // 4 * HD
    block_out, grad_tokens, own_qkv, own_out, own_gu, own_dn = block_step(
        planes, length, x, normed, cot, w_qkv, w_out, w_gu, own_down
    )
    own_qkv = own_qkv.astype(F32)
    cols = lambda a, b: jnp.moveaxis(own_qkv[:, :, a:b], 0, 1).reshape(depth, -1)
    raw_q, raw_k, raw_v = cols(0, cut_q), cols(cut_q, cut_k), cols(cut_k, None)
    own_gu = own_gu.reshape(2, 2, 2, depth, 2, planes, block).astype(F32)
    raw_gu = jnp.transpose(own_gu, (4, 3, 0, 5, 2, 1, 6)).reshape(2, depth, hidden)
    gain_grad = lambda pairs: sum(jnp.sum(w.astype(F32) * raw, 1) for w, raw in pairs)
    return (
        block_out.reshape(tokens.shape),
        grad_tokens.reshape(tokens.shape),
        raw_q * gain_one, raw_k * gain_one, raw_v * gain_one,
        own_out.astype(F32),
        raw_gu[0] * gain_two, raw_gu[1] * gain_two,
        own_dn.reshape(-1, width).astype(F32),
        gain_grad([(w_query, raw_q), (w_key, raw_k), (w_value, raw_v)]),
        gain_grad([(w_gate, raw_gu[0]), (w_up, raw_gu[1])]),
    )


def fits(mesh):
    return mesh.shape["seq"] == 2 and mesh.shape["dp"] == 16


def solution(mesh):
    body = shards_fast if fits(mesh) else shards_plain
    return jax.shard_map(body, mesh=mesh, in_specs=IN_SPECS, out_specs=OUT_SPECS, check_vma=False)
```

```python
import jax
import jax.numpy as jnp
from jax import lax
from jax.experimental import pallas as pl
from jax.experimental.pallas import tpu as pltpu
from jax.sharding import PartitionSpec as P

HD = 96
EPS = 1e-05
THETA = 100000.0


def rotary(positions, width):
    steps_half = jnp.arange(width // 2, dtype=jnp.float32)
    frequency = jnp.power(THETA, -2.0 * steps_half / width)
    angles = positions[:, None] * frequency[None, :]
    cosine = jnp.cos(angles)
    sine = jnp.sin(angles)
    return (jnp.concatenate([cosine, cosine], -1), jnp.concatenate([sine, sine], -1))


def rotate(values, cosine, sine):
    half = values.shape[-1] // 2
    turned = jnp.concatenate([-values[..., half:], values[..., :half]], -1)
    return values * cosine[:, None, :] + turned * sine[:, None, :]


def rotate_back(grads, cosine, sine):
    half = grads.shape[-1] // 2
    sined = grads * sine[:, None, :]
    turned = jnp.concatenate([sined[..., half:], -sined[..., :half]], -1)
    return grads * cosine[:, None, :] + turned


def dot32(left, right):
    return jnp.dot(left, right, preferred_element_type=jnp.float32)


def dot_t(left, right):
    return lax.dot_general(left, right, (((1,), (1,)), ((), ())), preferred_element_type=jnp.float32)


def dot_l(left, right):
    return lax.dot_general(left, right, (((0,), (0,)), ((), ())), preferred_element_type=jnp.float32)


def inv_rms(values):
    return lax.rsqrt(jnp.mean(values * values, axis=-1, keepdims=True) + EPS)


def low(values):
    return values.astype(jnp.bfloat16)


def attend(queries, keys, values):
    rows = queries.shape[1]
    ids = jnp.arange(rows, dtype=jnp.int32)
    visible = ids[:, None] >= ids[None, :]
    scores = HD ** (-0.5) * jnp.einsum("bqkgd,bckd->bkgqc", queries, keys, preferred_element_type=jnp.float32)
    scores = jnp.where(visible, scores, -jnp.inf)
    top = jnp.max(scores, -1, keepdims=True)
    exps = jnp.exp(scores - top)
    probs = exps / jnp.sum(exps, -1, keepdims=True)
    mixed = jnp.einsum("bkgqc,bckd->bqkgd", low(probs), values, preferred_element_type=jnp.float32)
    return probs, low(mixed)


def attend_back(queries, keys, values, probs, grad_mixed):
    grad_values = jnp.einsum("bkgqc,bqkgd->bckd", low(probs), grad_mixed, preferred_element_type=jnp.float32)
    grad_probs = jnp.einsum("bqkgd,bckd->bkgqc", grad_mixed, values, preferred_element_type=jnp.float32)
    grad_scores = low(probs * (grad_probs - jnp.sum(probs * grad_probs, -1, keepdims=True)))
    scale = HD ** (-0.5)
    grad_queries = scale * jnp.einsum("bkgqc,bckd->bqkgd", grad_scores, keys, preferred_element_type=jnp.float32)
    grad_keys = scale * jnp.einsum("bkgqc,bqkgd->bckd", grad_scores, queries, preferred_element_type=jnp.float32)
    return grad_queries, grad_keys, grad_values


def mlp_grads(gate, up, grad_hidden):
    sigma = jax.nn.sigmoid(gate)
    silu = gate * sigma
    hidden = low(silu * up)
    grad_gate = low(grad_hidden * up * sigma * (1.0 + gate * (1.0 - sigma)))
    grad_up = low(grad_hidden * silu)
    return hidden, grad_gate, grad_up


def shards_plain(tokens, cotangent, w_query, w_key, w_value, w_out, w_gate, w_up, w_down, gain_attn, gain_mlp):
    seqs, length, width = tokens.shape
    rows = seqs * length
    kv_heads = w_key.shape[1] // HD
    groups = w_query.shape[1] // w_key.shape[1]
    gather = lambda w: lax.all_gather(w, "dp", axis=0, tiled=True)
    full_query, full_key, full_value, full_out = map(gather, (w_query, w_key, w_value, w_out))
    gains = gather(jnp.stack([gain_attn, gain_mlp], 1)).astype(jnp.float32)
    gain_one, gain_two = gains[:, 0], gains[:, 1]
    full_gate, full_up, full_down = map(gather, (w_gate, w_up, w_down))
    cosine, sine = rotary(jnp.arange(length, dtype=jnp.float32), HD)
    cosine, sine = jnp.tile(cosine, (seqs, 1)), jnp.tile(sine, (seqs, 1))

    inputs = tokens.reshape(rows, width).astype(jnp.float32)
    grad_in = cotangent.reshape(rows, width)
    scale_one = inv_rms(inputs)
    normed = low(inputs * scale_one * gain_one)
    queries = low(rotate(dot32(normed, full_query).reshape(rows, -1, HD), cosine, sine))
    keys = low(rotate(dot32(normed, full_key).reshape(rows, -1, HD), cosine, sine))
    values = low(dot32(normed, full_value))
    queries = queries.reshape(seqs, length, kv_heads, groups, HD)
    keys = keys.reshape(seqs, length, kv_heads, HD)
    values = values.reshape(seqs, length, kv_heads, HD)
    probs, mixed = attend(queries, keys, values)
    mixed = mixed.reshape(rows, -1)
    hidden_one = inputs + dot32(mixed, full_out)
    scale_two = inv_rms(hidden_one)
    normed_two = low(hidden_one * scale_two * gain_two)
    gate, up = dot32(normed_two, full_gate), dot32(normed_two, full_up)
    hidden, grad_gate, grad_up = mlp_grads(gate, up, dot_t(grad_in, full_down))
    block_out = low(hidden_one + dot32(hidden, full_down))

    acc_down = dot_l(hidden, grad_in)
    acc_gate = dot_l(normed_two, grad_gate)
    acc_up = dot_l(normed_two, grad_up)
    grad_normed_two = dot_t(grad_gate, full_gate) + dot_t(grad_up, full_up)
    acc_gain_two = jnp.sum(grad_normed_two * hidden_one * scale_two, 0)
    weighted = grad_normed_two * gain_two
    grad_one = grad_in.astype(jnp.float32) + scale_two * (
        weighted - hidden_one * scale_two * scale_two * jnp.mean(weighted * hidden_one, -1, keepdims=True)
    )
    grad_branch = low(grad_one)
    acc_out = dot_l(mixed, grad_branch)
    grad_mixed = low(dot_t(grad_branch, full_out)).reshape(queries.shape)
    grad_queries, grad_keys, grad_values = attend_back(queries, keys, values, probs, grad_mixed)
    grad_queries = low(rotate_back(grad_queries.reshape(rows, -1, HD), cosine, sine)).reshape(rows, -1)
    grad_keys = low(rotate_back(grad_keys.reshape(rows, -1, HD), cosine, sine)).reshape(rows, -1)
    grad_values = low(grad_values).reshape(rows, -1)
    acc_query = dot_l(normed, grad_queries)
    acc_key = dot_l(normed, grad_keys)
    acc_value = dot_l(normed, grad_values)
    grad_normed = dot_t(grad_queries, full_query) + dot_t(grad_keys, full_key) + dot_t(grad_values, full_value)
    acc_gain_one = jnp.sum(grad_normed * inputs * scale_one, 0)
    weighted = grad_normed * gain_one
    grad_tokens = grad_one + scale_one * (
        weighted - inputs * scale_one * scale_one * jnp.mean(weighted * inputs, -1, keepdims=True)
    )

    def share(acc):
        owned = lax.psum_scatter(low(acc), "dp", scatter_dimension=0, tiled=True)
        return lax.psum(owned, "seq").astype(jnp.float32)

    grads = [share(a) for a in (acc_down, acc_gate, acc_up, acc_out, acc_query, acc_key, acc_value)]
    gain_grads = lax.psum(
        lax.psum_scatter(jnp.stack([acc_gain_one, acc_gain_two], 1), "dp", scatter_dimension=0, tiled=True), "seq"
    )
    down, gate, up, out, query, key, value = grads
    return (
        block_out.reshape(tokens.shape),
        low(grad_tokens).reshape(tokens.shape),
        query, key, value, out, gate, up, down,
        gain_grads[:, 0], gain_grads[:, 1],
    )


ROWS = P(("dp", "seq"), None, None)
SPLIT = P("dp", None)
IN_SPECS = (ROWS, ROWS) + (SPLIT,) * 7 + (P("dp"), P("dp"))
OUT_SPECS = (ROWS, ROWS) + (SPLIT,) * 7 + (P("dp"), P("dp"))


MESH = pl.DeviceIdType.MESH
VMEM = pl.BlockSpec(memory_space=pltpu.VMEM)
ANY = pl.BlockSpec(memory_space=pl.ANY)
BF = jnp.bfloat16
F32 = jnp.float32
STRIP = 16
PIECES = 4
VMEM_BYTES = 66_000_000


class Place:
    def __init__(self, planes):
        self.planes = planes
        d = lax.axis_index("dp")
        self.d, self.s = d, lax.axis_index("seq")
        self.c, self.y, self.z = d % 2, (d // 2) % 2, d // 4
        self.p = d // 2
        self.rank = 2 * self.s + self.c
        self.core = (d + 1 - 2 * self.c, self.s)
        self.across = (d, 1 - self.s)
        self.corner = (d + 1 - 2 * self.c, 1 - self.s)
        self.side = (d + 2 - 4 * self.y, self.s)
        self.right = (lax.rem(d + 4, 4 * planes), self.s)
        self.left = (lax.rem(d + 4 * planes - 4, 4 * planes), self.s)
        self.has_right, self.has_left = self.z < planes - 1, self.z > 0
        odd = self.z % 2
        self.twin = self.z + 1 - 2 * odd
        self.buddy = (d + 4 - 8 * odd, self.s)


def greet(me):
    barrier = pltpu.get_barrier_semaphore()
    for peer in (me.core, me.across, me.corner, me.side, me.right, me.left):
        pl.semaphore_signal(barrier, inc=1, device_id=peer, device_id_type=MESH)
    pl.semaphore_wait(barrier, 6)


def push(src, dst, send, recv, peer):
    return pltpu.make_async_remote_copy(
        src_ref=src, dst_ref=dst, send_sem=send, recv_sem=recv, device_id=peer, device_id_type=MESH
    )


def arrived(dst, recv, peer):
    push(dst, dst, recv, recv, peer).wait_recv()


def left_over(src, send, peer):
    push(src, src, send, send, peer).wait_send()


class Slots:
    def __init__(self, ref, rows):
        self.ref, self.rows = ref, rows
        self.at = self

    def __getitem__(self, block):
        return self.ref.at[pl.ds(pl.multiple_of(block * self.rows, self.rows), self.rows)]


def group_start(me, src, dst, send, recv):
    push(src, dst.at[me.rank], send.at[0], recv.at[0], me.core).start()
    push(src, dst.at[me.rank], send.at[1], recv.at[1], me.across).start()


def group_relay(me, dst, send, recv):
    slot = dst.at[2 * (1 - me.s) + me.c]
    arrived(slot, recv.at[1], me.across)
    push(slot, slot, send.at[2], recv.at[2], me.core).start()


def group_finish(me, src, dst, send, recv):
    arrived(dst.at[2 * me.s + 1 - me.c], recv.at[0], me.core)
    arrived(dst.at[2 * (1 - me.s) + 1 - me.c], recv.at[2], me.core)
    left_over(src, send.at[0], me.core)
    left_over(src, send.at[1], me.across)
    slot = dst.at[2 * (1 - me.s) + me.c]
    left_over(slot, send.at[2], me.core)


def group_sems():
    return [pltpu.SemaphoreType.DMA((3,)), pltpu.SemaphoreType.DMA((3,))]


def upper(slot):
    return slot.at[pl.ds(0, slot.shape[0] // 2)]


def lower(slot):
    return slot.at[pl.ds(slot.shape[0] // 2, slot.shape[0] // 2)]


def line_start(me, dst, sems):
    line_side(me, dst, sems)
    line_ends(me, dst, sems)


def line_side(me, dst, sems):
    to_right, to_left, line, to_side, side, twin = sems
    slot = dst(me.p)
    push(slot, slot, to_side.at[me.z], side.at[me.z], me.side).start()


def line_ends(me, dst, sems):
    to_right, to_left, line, to_side, side, twin = sems
    slot = dst(me.p)

    @pl.when(me.has_right)
    def _():
        push(slot, slot, to_right.at[me.z], line.at[me.z], me.right).start()

    @pl.when(me.has_left)
    def _():
        push(slot, slot, to_left.at[me.z], line.at[me.z], me.left).start()


def line_hop(me, dst, sems, hop):
    to_right, to_left, line, to_side, side, twin = sems

    def pass_on(item, back, forth, may, sends):
        slot = dst(2 * item + me.y)
        arrived(slot, line.at[item], back)

        @pl.when(may)
        def _():
            push(slot, slot, sends.at[item], line.at[item], forth).start()

        if hop > 1:
            push(slot, slot, to_side.at[item], side.at[item], me.side).start()
        else:

            @pl.when(item != me.twin)
            def _():
                push(slot, slot, to_side.at[item], side.at[item], me.side).start()

            @pl.when(item == me.twin)
            def _():
                half = upper(slot)
                push(half, half, to_side.at[item], side.at[item], me.side).start()

    @pl.when(me.z >= hop)
    def _():
        pass_on(me.z - hop, me.left, me.right, me.has_right, to_right)

    @pl.when(me.z + hop < me.planes)
    def _():
        pass_on(me.z + hop, me.right, me.left, me.has_left, to_left)


def line_twin(me, dst, sems):
    to_right, to_left, line, to_side, side, twin = sems
    slot = dst(2 * me.z + 1 - me.y)
    arrived(slot, side.at[me.z], me.side)
    half = lower(slot)
    push(half, half, twin.at[0], twin.at[1], me.buddy).start()


def line_finish(me, dst, sems):
    to_right, to_left, line, to_side, side, twin = sems
    for item in range(me.planes):
        slot, mine = dst(2 * item + 1 - me.y), dst(2 * item + me.y)

        @pl.when(item == me.twin)
        def _():
            arrived(upper(slot), side.at[item], me.side)
            arrived(lower(slot), twin.at[1], me.buddy)
            left_over(upper(mine), to_side.at[item], me.side)

        @pl.when(jnp.logical_and(item != me.twin, item != me.z))
        def _():
            arrived(slot, side.at[item], me.side)

        @pl.when(item != me.twin)
        def _():
            left_over(mine, to_side.at[item], me.side)

        @pl.when(item == me.z)
        def _():
            left_over(lower(slot), twin.at[0], me.buddy)

        @pl.when(jnp.logical_and(me.has_right, item <= me.z))
        def _():
            left_over(mine, to_right.at[item], me.right)

        @pl.when(jnp.logical_and(me.has_left, item >= me.z))
        def _():
            left_over(mine, to_left.at[item], me.left)


def line_sems(planes):
    return [pltpu.SemaphoreType.DMA((planes,))] * 5 + [pltpu.SemaphoreType.DMA((2,))]


def pick(table, index):
    value = jnp.int32(table[0])
    for i in range(1, len(table)):
        value = jnp.where(index == i, table[i], value)
    return value


def far_first(planes):
    return [sorted(range(planes), key=lambda i, z=z: (-abs(i - z), i)) for z in range(planes)]


def add_into(dst, *others):
    rows = dst.shape[0]

    def body(i, carry):
        strip = pl.ds(pl.multiple_of(i * STRIP, STRIP), STRIP)
        total = dst[strip, :].astype(F32)
        for other in others:
            total = total + other[strip, :].astype(F32)
        dst[strip, :] = total.astype(dst.dtype)
        return carry

    lax.fori_loop(0, rows // STRIP, body, 0)


def reduce_start(me, own, half, sems):
    to_side, side, twin = sems[0], sems[1], sems[6]
    orders = far_first(me.planes)
    away = lower(own(2 * me.twin + 1 - me.y))
    push(away, lower(half.at[me.z]), twin.at[0], twin.at[1], me.buddy).start()
    for i in range(me.planes):
        item = pick([o[i] for o in orders], me.z)
        src, dst = own(2 * item + 1 - me.y), half.at[item]

        @pl.when(item == me.twin)
        def _():
            push(upper(src), upper(dst), to_side.at[item], side.at[item], me.side).start()

        @pl.when(jnp.logical_and(item != me.twin, item != me.z))
        def _():
            push(src, dst, to_side.at[item], side.at[item], me.side).start()


def reduce_mix(me, own, half, sems):
    to_side, side, twin = sems[0], sems[1], sems[6]
    mixed, got = own(2 * me.z + 1 - me.y), lower(half.at[me.twin])
    arrived(got, twin.at[1], me.buddy)
    add_into(lower(mixed), got)
    push(mixed, half.at[me.z], to_side.at[me.z], side.at[me.z], me.side).start()


def reduce_y(me, own, half, lines, sems, i):
    to_side, side, to_right, to_left, left, right, twin = sems
    item = pick([o[i] for o in far_first(me.planes)], me.z)
    mine, ours = half.at[item], own(2 * item + me.y)

    @pl.when(item == me.twin)
    def _():
        arrived(upper(mine), side.at[item], me.side)
        add_into(upper(mine), upper(ours))
        copy_into(lower(mine), lower(ours))

    @pl.when(item != me.twin)
    def _():
        arrived(mine, side.at[item], me.side)
        add_into(mine, ours)

    @pl.when(jnp.logical_and(item > me.z, jnp.logical_not(me.has_left)))
    def _():
        push(mine, lines.at[item], to_right.at[item], left.at[item], me.right).start()

    @pl.when(jnp.logical_and(item < me.z, jnp.logical_not(me.has_right)))
    def _():
        there = jnp.where(item == me.z - 1, me.planes, item)
        push(mine, lines.at[there], to_left.at[item], right.at[item], me.left).start()


def reduce_z(me, half, lines, sems, i):
    to_side, side, to_right, to_left, left, right, twin = sems
    item = pick([o[i] for o in far_first(me.planes)], me.z)
    mine = half.at[item]
    spot = jnp.where(item == me.z, me.planes, item)

    @pl.when(jnp.logical_and(me.has_left, item >= me.z))
    def _():
        arrived(lines.at[item], left.at[item], me.left)
        add_into(mine, lines.at[item])

        @pl.when(item > me.z)
        def _():
            push(mine, lines.at[item], to_right.at[item], left.at[item], me.right).start()

    @pl.when(jnp.logical_and(me.has_right, item <= me.z))
    def _():
        arrived(lines.at[spot], right.at[item], me.right)
        add_into(mine, lines.at[spot])

        @pl.when(item < me.z)
        def _():
            there = jnp.where(item == me.z - 1, me.planes, item)
            push(mine, lines.at[there], to_left.at[item], right.at[item], me.left).start()


def reduce_finish(me, own, half, sems):
    to_side, side, to_right, to_left, left, right, twin = sems
    left_over(lower(own(2 * me.twin + 1 - me.y)), twin.at[0], me.buddy)
    for item in range(me.planes):
        sent = own(2 * item + 1 - me.y)

        @pl.when(item == me.twin)
        def _():
            left_over(upper(sent), to_side.at[item], me.side)

        @pl.when(item != me.twin)
        def _():
            left_over(sent, to_side.at[item], me.side)

        @pl.when(item > me.z)
        def _():
            left_over(half.at[item], to_right.at[item], me.right)

        @pl.when(item < me.z)
        def _():
            left_over(half.at[item], to_left.at[item], me.left)


def reduce_sems(planes):
    return [pltpu.SemaphoreType.DMA((planes,))] * 6 + [pltpu.SemaphoreType.DMA((2,))]


def copy_into(dst, src):
    def body(i, carry):
        strip = pl.ds(pl.multiple_of(i * STRIP, STRIP), STRIP)
        dst[strip, :] = src[strip, :]
        return carry

    lax.fori_loop(0, dst.shape[0] // STRIP, body, 0)


def reduce_buffers(planes, rows, columns):
    return [pltpu.VMEM((planes, rows, columns), BF), pltpu.VMEM((planes + 1, rows, columns), BF)]


def by_chip(ref, rows=None):
    if rows is None:
        return lambda chip: ref.at[chip]
    return lambda chip: ref.at[pl.ds(pl.multiple_of(chip * rows, STRIP), rows)]


def deal_start(me, final, rows, out, local, send, recv):
    mine = out.at[me.rank]
    part = lambda core: final.at[pl.ds(pl.multiple_of(core * rows, rows), rows)]
    pltpu.make_async_copy(part(me.c), mine, local).start()
    push(part(1 - me.c), mine, send.at[0], recv.at[0], me.core).start()
    push(part(me.c), mine, send.at[1], recv.at[1], me.across).start()
    push(part(1 - me.c), mine, send.at[2], recv.at[2], me.corner).start()


def deal_finish(me, final, rows, out, local, send, recv):
    part = lambda core: final.at[pl.ds(pl.multiple_of(core * rows, rows), rows)]
    pltpu.make_async_copy(part(me.c), out.at[me.rank], local).wait()
    left_over(part(1 - me.c), send.at[0], me.core)
    left_over(part(me.c), send.at[1], me.across)
    left_over(part(1 - me.c), send.at[2], me.corner)
    arrived(out.at[2 * me.s + 1 - me.c], recv.at[0], me.core)
    arrived(out.at[2 * (1 - me.s) + me.c], recv.at[1], me.across)
    arrived(out.at[2 * (1 - me.s) + 1 - me.c], recv.at[2], me.corner)


def blocks_start(me, part, got, send, recv, i):
    seq = (1 - me.s, me.s)[i]
    push(part.at[2 * seq + 1 - me.c], got.at[seq], send.at[i], recv.at[i], me.core).start()


def blocks_cross(me, part, got, last, send, recv):
    away = 1 - me.s
    arrived(got.at[away], recv.at[0], me.core)
    add_into(got.at[away], part.at[2 * away + me.c])
    push(got.at[away], last, send.at[2], recv.at[2], me.across).start()


def blocks_finish(me, part, got, last, send, recv):
    arrived(got.at[me.s], recv.at[1], me.core)
    arrived(last, recv.at[2], me.across)
    for i, seq in enumerate((1 - me.s, me.s)):
        left_over(part.at[2 * seq + 1 - me.c], send.at[i], me.core)
    left_over(got.at[1 - me.s], send.at[2], me.across)


def blocks_sems():
    return [pltpu.SemaphoreType.DMA((3,))] * 2


def blocks_buffers(rows, width):
    return [pltpu.VMEM((2, rows, width), BF), pltpu.VMEM((rows, width), BF)]


def strips(rows, body):
    def step(i, carry):
        body(pl.ds(pl.multiple_of(i * STRIP, STRIP), STRIP))
        return carry

    lax.fori_loop(0, rows // STRIP, step, 0)


def comm_call(kernel, ident, outs, out_specs, ins, scratch, name):
    return pl.pallas_call(
        kernel,
        out_shape=outs,
        in_specs=[spec for spec, _ in ins],
        out_specs=out_specs,
        scratch_shapes=scratch,
        name=name,
        compiler_params=pltpu.CompilerParams(
            collective_id=ident, has_side_effects=True, vmem_limit_bytes=VMEM_BYTES
        ),
    )(*[value for _, value in ins])


def shape(dims, dtype=BF):
    return jax.ShapeDtypeStruct(dims, dtype)


def split_start(me, parts, dst, keep, send, recv):
    pltpu.make_async_copy(parts.at[me.c], dst(me.c), keep).start()
    push(parts.at[1 - me.c], dst(me.c), send, recv, me.core).start()


def split_finish(me, parts, dst, keep, send, recv):
    pltpu.make_async_copy(parts.at[me.c], dst(me.c), keep).wait()
    arrived(dst(1 - me.c), recv, me.core)
    left_over(parts.at[1 - me.c], send, me.core)


def norm_back(values, weighted, base):
    scale = inv_rms(values)
    return base + scale * (
        weighted - values * scale * scale * jnp.mean(weighted * values, -1, keepdims=True)
    )


LANES = 128


def head_tables(length):
    cosine, sine = rotary(jnp.arange(length, dtype=F32), HD)
    pad = ((0, 0), (0, LANES - HD))
    low_half = jnp.arange(HD) < HD // 2
    tables = [cosine, jnp.where(low_half, 0.0, sine), jnp.where(low_half, -sine, 0.0)]
    row, col = jnp.arange(4 * HD)[:, None], jnp.arange(4 * LANES)[None, :]
    spread = (row // HD == col // LANES) & (row % HD == col % LANES)
    return jnp.stack([jnp.pad(t, pad) for t in tables]), spread.astype(BF)


def turn(values, tables, sign):
    other = pltpu.roll(values, HD // 2, 1) * tables[1] + pltpu.roll(values, LANES - HD // 2, 1) * tables[2]
    return values * tables[0] + sign * other


def block_step(planes, length, tokens, n_own, g_own, w_qkv, w_out, w_gu, w_down):
    rows, width = tokens.shape
    total = 4 * rows
    head = w_out.shape[0]
    q_cols = w_qkv.shape[2]
    depth, cols = w_gu.shape[2:]
    block = w_down.shape[0]
    units = 2 * planes * block
    half_units = units // 2
    tile, chunk = 2 * rows, 256
    heads4 = 4 * head
    piece = 2 * head // PIECES
    tables, spread = head_tables(length)

    def kernel(x_ref, n_loc, g_loc, qkv_loc, out_loc, gu_loc, dn_loc, tab_ref, sel_ref,
               bo_ref, gx_ref, qkv_out, out_out, gu_out, dn_out, stash, *scr):
        it = iter(scr)
        take = lambda k: [next(it) for _ in range(k)]
        n_buf, g_all, qkv_all, out_all, gu_all, dn_all, heads, mixed = take(8)
        part, out_part, x1, mid, dgu, g_gu, dx_all = take(7)
        (got, last), (got_f, last_f) = take(2), take(2)
        gu_buf, dn_buf, q_buf, o_buf = [take(2), take(2)], take(2), take(2), take(3)
        n_sems, g_sems, m_sems, d_sems = take(2), take(2), take(2), take(2)
        x_sems, b_sems, f_sems, h_sems = take(2), take(2), take(2), take(2)
        q_split, gu_split = take(3), [take(3), take(3)]
        q_line, gu_line, dn_line = take(6), [take(6), take(6)], take(6)
        gu_sems, dn_sems, q_sems = [take(7), take(7)], take(7), take(7)
        gu_deal, dn_deal, q_deal, o_deal = [take(3), take(3)], take(3), take(3), take(3)
        local, edge, o_fan, o_red = take(4)
        me = Place(planes)
        greet(me)
        tok = lambda ref: Slots(ref, rows)
        q_slots, dn_slots = by_chip(qkv_all, 2 * depth), by_chip(dn_all, block)
        gu_slots = [by_chip(gu_all.at[h], 2 * depth) for h in range(2)]

        def core_rows(ref):
            return lambda core: ref.at[pl.ds(pl.multiple_of((2 * me.p + core) * depth, STRIP), depth)]

        split_start(me, qkv_loc, core_rows(qkv_all), *q_split)
        keep_n = pltpu.make_async_copy(n_loc, tok(n_buf).at[me.rank], local.at[0])
        keep_n.start()
        group_start(me, n_loc, tok(n_buf), *n_sems)
        here = me.s == me.z // 2
        owner = me.z == me.rank
        lender = jnp.logical_and(here, jnp.logical_not(owner))
        half = lambda y: out_all.at[pl.ds(pl.multiple_of(y * 2 * head, STRIP), 2 * head)]
        head_rows = lambda core: out_all.at[pl.ds(pl.multiple_of((2 * me.y + core) * head, STRIP), head)]
        keep_o = pltpu.make_async_copy(out_loc, head_rows(me.c), local.at[1])

        @pl.when(owner)
        def _():
            keep_o.start()

        @pl.when(lender)
        def _():
            push(out_loc, head_rows(me.c), edge.at[0], edge.at[1], me.core).start()

        for h in range(2):
            split_start(me, gu_loc.at[h], core_rows(gu_all.at[h]), *gu_split[h])
        keep_d = pltpu.make_async_copy(dn_loc, dn_slots(me.p), local.at[2])
        keep_d.start()
        keep_g = pltpu.make_async_copy(g_loc, tok(g_all).at[me.rank], local.at[3])
        keep_g.start()
        fetch_x = pltpu.make_async_copy(x_ref, last_f, local.at[4])
        fetch_x.start()
        split_finish(me, qkv_loc, core_rows(qkv_all), *q_split)
        line_start(me, q_slots, q_line)
        group_start(me, g_loc, tok(g_all), *g_sems)

        fan_in, fan_right, fan_left, fan_side, fan_other = [o_fan.at[k] for k in range(5)]
        bit = lambda y, q: out_all.at[pl.ds(pl.multiple_of(y * 2 * head + q * piece, STRIP), piece)]
        go_right = jnp.logical_and(me.z >= me.rank, me.has_right)
        go_left = jnp.logical_and(me.z <= me.rank, me.has_left)

        def fan(q):
            mine = bit(me.y, q)

            @pl.when(me.z > me.rank)
            def _():
                arrived(mine, fan_in.at[q], me.left)

            @pl.when(me.z < me.rank)
            def _():
                arrived(mine, fan_in.at[q], me.right)

            @pl.when(go_right)
            def _():
                push(mine, mine, fan_right.at[q], fan_in.at[q], me.right).start()

            @pl.when(go_left)
            def _():
                push(mine, mine, fan_left.at[q], fan_in.at[q], me.left).start()

            push(mine, mine, fan_side.at[q], fan_other.at[q], me.side).start()

        @pl.when(owner)
        def _():
            keep_o.wait()
            arrived(head_rows(1 - me.c), edge.at[1], me.core)

        @pl.when(lender)
        def _():
            left_over(out_loc, edge.at[0], me.core)

        line_hop(me, q_slots, q_line, 1)
        line_twin(me, q_slots, q_line)
        fan(0)
        line_hop(me, q_slots, q_line, 2)
        group_relay(me, tok(n_buf), *n_sems)
        fan(1)
        for hop in range(3, planes):
            line_hop(me, q_slots, q_line, hop)
        fan(2)
        fan(3)
        split_finish(me, gu_loc.at[0], core_rows(gu_all.at[0]), *gu_split[0])
        line_start(me, gu_slots[0], gu_line[0])
        keep_d.wait()
        line_start(me, dn_slots, dn_line)
        split_finish(me, gu_loc.at[1], core_rows(gu_all.at[1]), *gu_split[1])
        keep_n.wait()
        group_finish(me, n_loc, tok(n_buf), *n_sems)
        saved = pltpu.make_async_copy(n_buf, stash, local.at[0])
        saved.start()
        line_finish(me, q_slots, q_line)

        def widen(i, carry):
            feats = pl.ds(pl.multiple_of(i * tile, tile), tile)
            for k in range(2):
                g_gu[feats, k * 4 * LANES:(k + 1) * 4 * LANES] = low(
                    dot32(qkv_all[feats, k * heads4:(k + 1) * heads4], sel_ref[...])
                )
            return carry

        lax.fori_loop(0, width // tile, widen, 0)

        def project(i, carry):
            toks = pl.ds(pl.multiple_of(i * length, length), length)
            n = n_buf[toks, :]
            tabs = [tab_ref[k] for k in range(3)]
            for k in range(8):
                value = dot32(n, g_gu[:, k * LANES:(k + 1) * LANES])
                heads[toks, k * LANES:(k + 1) * LANES] = low(turn(value, tabs, 1.0) if k < 6 else value)
            return carry

        lax.fori_loop(0, total // length, project, 0)
        line_hop(me, gu_slots[0], gu_line[0], 1)
        group_relay(me, tok(g_all), *g_sems)
        line_hop(me, dn_slots, dn_line, 1)
        line_twin(me, gu_slots[0], gu_line[0])
        line_twin(me, dn_slots, dn_line)
        saved.wait()
        for q in range(PIECES):
            arrived(bit(1 - me.y, q), fan_other.at[q], me.side)

        def pair(toks, j, ref, start):
            first = start + 2 * j * LANES
            return jnp.concatenate(
                [ref[toks, first:first + LANES], ref[toks, first + LANES:first + 2 * LANES]], 0
            )

        def probabilities(toks, j):
            q = pair(toks, j, heads, 0)
            k = heads[toks, (4 + j) * LANES:(5 + j) * LANES]
            scores = HD ** (-0.5) * dot_t(q, k)
            row = lax.rem(lax.broadcasted_iota(jnp.int32, scores.shape, 0), length)
            col = lax.broadcasted_iota(jnp.int32, scores.shape, 1)
            scores = jnp.where(row >= col, scores, -jnp.inf)
            exps = jnp.exp(scores - jnp.max(scores, 1, keepdims=True))
            return q, k, exps / jnp.sum(exps, 1, keepdims=True)

        def attend_rows(first):
            def one(i, carry):
                toks = pl.ds(pl.multiple_of(first + i * length, length), length)
                outs = []
                for j in range(2):
                    _, _, p = probabilities(toks, j)
                    o = low(dot32(low(p), heads[toks, (6 + j) * LANES:(7 + j) * LANES]))
                    outs += [o[:length], o[length:]]
                mixed[toks, :] = low(dot_t(jnp.concatenate(outs, 1), sel_ref[...]))
                return carry

            lax.fori_loop(0, rows // length, one, 0)
            toks = pl.ds(pl.multiple_of(first, rows), rows)
            part[toks, :] = low(dot32(mixed[toks, :], out_all[...]))

        away, home = 1 - me.s, me.s
        attend_rows((2 * away + 1 - me.c) * rows)
        blocks_start(me, tok(part), got, *x_sems, 0)
        line_hop(me, gu_slots[0], gu_line[0], 2)
        line_ends(me, gu_slots[1], gu_line[1])
        attend_rows((2 * away + me.c) * rows)
        blocks_cross(me, tok(part), got, last, *x_sems)
        line_hop(me, dn_slots, dn_line, 2)
        attend_rows((2 * home + 1 - me.c) * rows)
        blocks_start(me, tok(part), got, *x_sems, 1)
        line_side(me, gu_slots[1], gu_line[1])
        attend_rows((2 * home + me.c) * rows)
        for hop in range(3, planes):
            line_hop(me, gu_slots[0], gu_line[0], hop)
        line_hop(me, gu_slots[1], gu_line[1], 1)
        blocks_finish(me, tok(part), got, last, *x_sems)

        def mine(strip):
            return pl.ds(pl.multiple_of(me.rank * rows + strip.start, STRIP), STRIP)

        def summed(strip, whole, some, rest):
            return (
                whole[mine(strip), :].astype(F32)
                + some[me.s, strip, :].astype(F32)
                + rest[strip, :].astype(F32)
            )

        fetch_x.wait()

        def middle(strip):
            value = last_f[strip, :].astype(F32) + summed(strip, part, got, last)
            x1[strip, :] = value
            n_buf[mine(strip), :] = low(value * inv_rms(value))

        strips(rows, middle)
        group_start(me, tok(n_buf).at[me.rank], tok(n_buf), *m_sems)
        for hop in range(3, planes):
            line_hop(me, dn_slots, dn_line, hop)
        line_hop(me, gu_slots[1], gu_line[1], 2)
        line_twin(me, gu_slots[1], gu_line[1])
        keep_g.wait()
        group_finish(me, g_loc, tok(g_all), *g_sems)
        for q in range(PIECES):
            left_over(bit(me.y, q), fan_side.at[q], me.side)

            @pl.when(go_right)
            def _():
                left_over(bit(me.y, q), fan_right.at[q], me.right)

            @pl.when(go_left)
            def _():
                left_over(bit(me.y, q), fan_left.at[q], me.left)

        group_relay(me, tok(n_buf), *m_sems)
        group_finish(me, tok(n_buf).at[me.rank], tok(n_buf), *m_sems)
        line_finish(me, gu_slots[0], gu_line[0])
        line_finish(me, dn_slots, dn_line)

        def activations(h, j):
            first = h * half_units + j * chunk

            def step(t, carry):
                toks = pl.ds(pl.multiple_of(t * tile, tile), tile)
                n, g = n_buf[toks, :], g_all[toks, :]
                gate = dot32(n, gu_all[h, :, j * chunk:(j + 1) * chunk])
                up = dot32(n, gu_all[h, :, half_units + j * chunk:half_units + (j + 1) * chunk])
                grad = dot_t(g, dn_all[first:first + chunk, :])
                hidden, d_gate, d_up = mlp_grads(gate, up, grad)
                mid[toks, first:first + chunk] = hidden
                dgu[h, toks, j * chunk:(j + 1) * chunk] = d_gate
                dgu[h, toks, half_units + j * chunk:half_units + (j + 1) * chunk] = d_up
                return carry

            lax.fori_loop(0, total // tile, step, 0)

        def weight_grads(h, out, third):
            def step(i, carry):
                feats = pl.ds(pl.multiple_of(third * (width // 3) + i * chunk, chunk), chunk)
                out[feats, :] = low(dot_l(n_buf[:, feats], dgu[h]))
                return carry

            lax.fori_loop(0, width // 3 // chunk, step, 0)

        steps = half_units // chunk
        for j in range(steps):
            activations(0, j)
        for hop in range(3, planes):
            line_hop(me, gu_slots[1], gu_line[1], hop)
        for third in range(3):
            weight_grads(0, g_gu, third)
        own_gu = [by_chip(g_gu, 2 * depth), gu_slots[0]]
        reduce_start(me, own_gu[0], gu_buf[0][0], gu_sems[0])
        line_finish(me, gu_slots[1], gu_line[1])
        for j in range(steps):
            activations(1, j)
        finals = [gu_buf[h][0].at[me.z] for h in range(2)]
        gu_y = lambda h, i: reduce_y(me, own_gu[h], *gu_buf[h], gu_sems[h], i)
        gu_z = lambda h, i: reduce_z(me, *gu_buf[h], gu_sems[h], i)
        gu_mix = lambda h: reduce_mix(me, own_gu[h], gu_buf[h][0], gu_sems[h])
        dn_y = lambda i: reduce_y(me, dn_slots, *dn_buf, dn_sems, i)
        dn_z = lambda i: reduce_z(me, *dn_buf, dn_sems, i)
        q_y = lambda i: reduce_y(me, q_slots, *q_buf, q_sems, i)
        q_z = lambda i: reduce_z(me, *q_buf, q_sems, i)
        gu_mix(0)

        def back(seq):
            toks = pl.ds(pl.multiple_of(seq * tile, tile), tile)

            def step(i, carry):
                feats = pl.ds(pl.multiple_of(i * chunk, chunk), chunk)
                value = dot_t(dgu[0, toks, :], gu_all[0, feats, :]) + dot_t(dgu[1, toks, :], gu_all[1, feats, :])
                part[toks, feats] = low(value)
                return carry

            lax.fori_loop(0, width // chunk, step, 0)

        back(away)
        blocks_start(me, tok(part), got, *b_sems, 0)
        gu_y(0, 0)
        back(home)
        blocks_start(me, tok(part), got, *b_sems, 1)
        blocks_cross(me, tok(part), got, last, *b_sems)

        for third in range(3):
            weight_grads(1, gu_all.at[0], third)
        fetch_n = pltpu.make_async_copy(stash, n_buf, local.at[0])
        fetch_n.start()
        reduce_start(me, own_gu[1], gu_buf[1][0], gu_sems[1])
        gu_y(0, 1)
        gu_z(0, 0)
        gu_y(0, 2)

        def forth(i, carry):
            feats = pl.ds(pl.multiple_of(i * chunk, chunk), chunk)
            out_part[:, feats] = low(dot32(mid[...], dn_all[:, feats]))
            return carry

        lax.fori_loop(0, width // chunk, forth, 0)
        for i in range(2):
            blocks_start(me, tok(out_part), got_f, *f_sems, i)
        gu_z(0, 1)
        gu_z(0, 2)
        gu_y(0, 3)
        blocks_finish(me, tok(part), got, last, *b_sems)

        def branch(strip):
            grad = norm_back(x1[strip, :], summed(strip, part, got, last), g_all[mine(strip), :].astype(F32))
            dx_all[mine(strip), :] = low(grad)

        strips(rows, branch)
        group_start(me, tok(dx_all).at[me.rank], tok(dx_all), *d_sems)
        gu_mix(1)

        def down(i, carry):
            these = pl.ds(pl.multiple_of(i * chunk, chunk), chunk)
            dn_all[these, :] = low(dot_l(mid[:, these], g_all[...]))
            return carry

        lax.fori_loop(0, units // chunk, down, 0)
        reduce_start(me, dn_slots, dn_buf[0], dn_sems)
        gu_z(0, 3)
        gu_y(1, 0)
        gu_y(1, 1)
        gu_z(1, 0)
        gu_y(1, 2)
        reduce_mix(me, dn_slots, dn_buf[0], dn_sems)
        group_relay(me, tok(dx_all), *d_sems)
        deal_start(me, finals[0], depth, gu_out.at[0], *gu_deal[0])
        blocks_cross(me, tok(out_part), got_f, last_f, *f_sems)
        gu_z(1, 1)
        gu_z(1, 2)
        group_finish(me, tok(dx_all).at[me.rank], tok(dx_all), *d_sems)

        def spread_out(t, carry):
            toks = pl.ds(pl.multiple_of(t * rows, rows), rows)
            grad = low(dot_t(dx_all[toks, :], out_all[...]))
            mid[toks, 0:4 * LANES] = low(dot32(grad, sel_ref[...]))
            return carry

        lax.fori_loop(0, 4, spread_out, 0)
        out_all[...] = low(dot_l(mixed[...], dx_all[...]))
        for q in range(PIECES):
            push(bit(1 - me.y, q), o_buf[0].at[pl.ds(q * piece, piece)], o_red.at[0, q], o_red.at[1, q], me.side).start()
        gu_y(1, 3)

        def attend_rows_back(first):
            def one(i, carry):
                toks = pl.ds(pl.multiple_of(first + i * length, length), length)
                tabs = [tab_ref[k] for k in range(3)]
                for j in range(2):
                    q, k, p = probabilities(toks, j)
                    v = heads[toks, (6 + j) * LANES:(7 + j) * LANES]
                    grad = pair(toks, j, mid, 0)
                    d_v = dot_l(low(p), grad)
                    d_p = dot_t(grad, v)
                    d_s = low(p * (d_p - jnp.sum(p * d_p, 1, keepdims=True)))
                    d_q = HD ** (-0.5) * dot32(d_s, k)
                    d_k = HD ** (-0.5) * dot_l(d_s, q)
                    for g in range(2):
                        spot = (2 * j + g) * LANES
                        dgu[0, toks, spot:spot + LANES] = low(turn(d_q[g * length:(g + 1) * length], tabs, -1.0))
                    dgu[0, toks, (4 + j) * LANES:(5 + j) * LANES] = low(turn(d_k, tabs, -1.0))
                    dgu[0, toks, (6 + j) * LANES:(7 + j) * LANES] = low(d_v)
                return carry

            lax.fori_loop(0, rows // length, one, 0)
            toks = pl.ds(pl.multiple_of(first, rows), rows)
            for k in range(2):
                dgu[1, toks, k * heads4:(k + 1) * heads4] = low(
                    dot_t(dgu[0, toks, k * 4 * LANES:(k + 1) * 4 * LANES], sel_ref[...])
                )
            part[toks, :] = low(dot_t(dgu[1, toks, 0:q_cols], qkv_all[...]))

        attend_rows_back((2 * away + 1 - me.c) * rows)
        blocks_start(me, tok(part), got, *h_sems, 0)
        attend_rows_back((2 * away + me.c) * rows)
        blocks_cross(me, tok(part), got, last, *h_sems)
        gu_z(1, 3)
        deal_start(me, finals[1], depth, gu_out.at[1], *gu_deal[1])
        dn_y(0)
        attend_rows_back((2 * home + 1 - me.c) * rows)
        blocks_start(me, tok(part), got, *h_sems, 1)
        attend_rows_back((2 * home + me.c) * rows)
        dn_y(1)
        fetch_n.wait()

        def q_grads(i, carry):
            feats = pl.ds(pl.multiple_of(i * chunk, chunk), chunk)
            qkv_all[feats, :] = low(dot_l(n_buf[:, feats], dgu[1, :, 0:q_cols]))
            return carry

        lax.fori_loop(0, width // chunk, q_grads, 0)
        reduce_start(me, q_slots, q_buf[0], q_sems)
        dn_z(0)
        dn_y(2)

        blocks_finish(me, tok(out_part), got_f, last_f, *f_sems)

        def output(strip):
            got_f[me.s, strip, :] = low(x1[strip, :] + summed(strip, out_part, got_f, last_f))

        strips(rows, output)
        keep_bo = pltpu.make_async_copy(got_f.at[me.s], bo_ref, local.at[1])
        keep_bo.start()
        fetch_x.start()
        dn_z(1)
        dn_z(2)
        dn_y(3)
        reduce_mix(me, q_slots, q_buf[0], q_sems)

        o_sum = lambda q: o_buf[0].at[pl.ds(q * piece, piece)]
        o_left = lambda q: o_buf[1].at[pl.ds(q * piece, piece)]
        o_right = lambda q: o_buf[2].at[pl.ds(q * piece, piece)]

        def o_on(q):
            @pl.when(me.z < me.rank)
            def _():
                push(o_sum(q), o_left(q), o_red.at[4, q], o_red.at[2, q], me.right).start()

            @pl.when(me.z > me.rank)
            def _():
                push(o_sum(q), o_right(q), o_red.at[4, q], o_red.at[3, q], me.left).start()

        from_left = jnp.logical_and(me.has_left, me.z <= me.rank)
        from_right = jnp.logical_and(me.has_right, me.z >= me.rank)
        no_more = jnp.logical_not(jnp.logical_or(from_left, from_right))

        def o_y(q):
            arrived(o_sum(q), o_red.at[1, q], me.side)
            add_into(o_sum(q), bit(me.y, q))

            @pl.when(no_more)
            def _():
                o_on(q)

        def o_z(q):
            @pl.when(from_left)
            def _():
                arrived(o_left(q), o_red.at[2, q], me.left)
                add_into(o_sum(q), o_left(q))

            @pl.when(from_right)
            def _():
                arrived(o_right(q), o_red.at[3, q], me.right)
                add_into(o_sum(q), o_right(q))

            @pl.when(jnp.logical_not(no_more))
            def _():
                o_on(q)

        for q in range(PIECES):
            o_y(q)
        dn_z(3)
        final_dn = dn_buf[0].at[me.z]
        dn_keep, dn_send, dn_recv = dn_deal
        keep_dn = pltpu.make_async_copy(final_dn, dn_out.at[me.s], dn_keep)
        keep_dn.start()
        push(final_dn, dn_out.at[me.s], dn_send, dn_recv, me.across).start()
        o_z(0)
        o_z(1)
        q_y(0)
        o_z(2)
        o_z(3)
        own_half = o_buf[0].at[pl.ds(pl.multiple_of(me.c * head, STRIP), head)]
        other_half = o_buf[0].at[pl.ds(pl.multiple_of((1 - me.c) * head, STRIP), head)]
        o_keep, o_send, o_recv = o_deal
        keep_oo = pltpu.make_async_copy(own_half, out_out, o_keep)

        @pl.when(owner)
        def _():
            keep_oo.start()
            push(other_half, out_out, o_send.at[0], o_recv.at[0], me.core).start()
            push(own_half, out_out, o_send.at[1], o_recv.at[0], me.across).start()
            push(other_half, out_out, o_send.at[2], o_recv.at[0], me.corner).start()

        q_y(1)
        q_z(0)
        q_y(2)

        blocks_finish(me, tok(part), got, last, *h_sems)
        fetch_x.wait()

        def inner(strip):
            got[me.s, strip, :] = low(norm_back(
                last_f[strip, :].astype(F32), summed(strip, part, got, last), dx_all[mine(strip), :].astype(F32)
            ))

        strips(rows, inner)
        keep_gx = pltpu.make_async_copy(got.at[me.s], gx_ref, local.at[2])
        keep_gx.start()
        q_z(1)
        q_z(2)
        q_y(3)
        q_z(3)
        final_q = q_buf[0].at[me.z]
        deal_start(me, final_q, depth, qkv_out, *q_deal)

        for h in range(2):
            reduce_finish(me, own_gu[h], gu_buf[h][0], gu_sems[h])
            deal_finish(me, finals[h], depth, gu_out.at[h], *gu_deal[h])
        reduce_finish(me, dn_slots, dn_buf[0], dn_sems)
        reduce_finish(me, q_slots, q_buf[0], q_sems)
        for q in range(PIECES):
            sum_q = o_sum(q)
            left_over(bit(1 - me.y, q), o_red.at[0, q], me.side)

            @pl.when(me.z < me.rank)
            def _():
                left_over(sum_q, o_red.at[4, q], me.right)

            @pl.when(me.z > me.rank)
            def _():
                left_over(sum_q, o_red.at[4, q], me.left)

        @pl.when(owner)
        def _():
            keep_oo.wait()
            left_over(other_half, o_send.at[0], me.core)
            left_over(own_half, o_send.at[1], me.across)
            left_over(other_half, o_send.at[2], me.corner)

        @pl.when(jnp.logical_not(owner))
        def _():
            arrived(out_out, o_recv.at[0], me.core)

        keep_dn.wait()
        left_over(final_dn, dn_send, me.across)
        arrived(dn_out.at[1 - me.s], dn_recv, me.across)
        keep_bo.wait()
        keep_gx.wait()
        deal_finish(me, final_q, depth, qkv_out, *q_deal)

    sems = lambda *dims: pltpu.SemaphoreType.DMA(dims)
    one, three = pltpu.SemaphoreType.DMA, sems(3)
    vmem = lambda *dims: pltpu.VMEM(dims, BF)
    deal = [one, three, three]
    outs = comm_call(
        kernel, 0,
        [shape((rows, width)), shape((rows, width)), shape((4, depth, q_cols)), shape((head, width)),
         shape((2, 4, depth, cols)), shape((2, block, width)), shape((total, width))],
        [ANY] * 7,
        [(ANY, tokens), (ANY, n_own), (ANY, g_own), (ANY, w_qkv), (ANY, w_out), (ANY, w_gu), (ANY, w_down),
         (VMEM, tables), (VMEM, spread)],
        [vmem(total, width), vmem(total, width), vmem(width, q_cols), vmem(heads4, width), vmem(2, width, cols),
         vmem(units, width), vmem(total, 8 * LANES), vmem(total, heads4)]
        + [vmem(total, width), vmem(total, width), pltpu.VMEM((rows, width), F32), vmem(total, units),
           vmem(2, total, cols), vmem(width, cols), vmem(total, width)]
        + blocks_buffers(rows, width) * 2
        + reduce_buffers(planes, 2 * depth, cols) * 2 + reduce_buffers(planes, block, width)
        + reduce_buffers(planes, 2 * depth, q_cols) + [vmem(2 * head, width)] * 3
        + group_sems() * 4 + blocks_sems() * 4 + [one] * 9
        + line_sems(planes) * 4 + reduce_sems(planes) * 4 + deal * 2 + [one] * 3 + deal * 2
        + [sems(5), sems(2), sems(5, PIECES), sems(5, PIECES)],
        "block_step",
    )
    return outs[:6]


def shards_fast(tokens, cotangent, w_query, w_key, w_value, w_out, w_gate, w_up, w_down, gain_attn, gain_mlp):
    seqs, length, width = tokens.shape
    rows = seqs * length
    depth = w_query.shape[0]
    devices = width // depth
    planes = devices // 4
    chips = 2 * planes
    s = lax.axis_index("seq")
    kv_heads = w_key.shape[1] // HD
    groups = w_query.shape[1] // w_key.shape[1]
    hidden = w_gate.shape[1]
    block = hidden // devices // 2

    x = tokens.reshape(rows, width)
    cot = cotangent.reshape(rows, width)
    xf = x.astype(F32)
    normed = low(xf * inv_rms(xf))

    gain_one, gain_two = gain_attn.astype(F32)[:, None], gain_mlp.astype(F32)[:, None]

    def heads_of(w):
        parts = (w.astype(F32) * gain_one).reshape(depth, 2, 2, -1)
        return jnp.moveaxis(low(lax.dynamic_index_in_dim(parts, s, 1, False)), 1, 0)

    w_qkv = jnp.concatenate([heads_of(w) for w in (w_query, w_key, w_value)], -1)

    def units_of(w):
        parts = (w.astype(F32) * gain_two).reshape(depth, 2, planes, 2, 2, block)
        parts = low(lax.dynamic_index_in_dim(parts, s, 4, False))
        return jnp.transpose(parts, (1, 3, 0, 2, 4)).reshape(2, 2, depth, planes * block)

    w_gu = jnp.concatenate([units_of(w_gate), units_of(w_up)], -1)
    own_down = lax.dynamic_slice_in_dim(w_down, s * block, block, 0)

    cut_q = kv_heads // 4 * groups * HD
    cut_k = cut_q + kv_heads // 4 * HD
    block_out, grad_tokens, own_qkv, own_out, own_gu, own_dn = block_step(
        planes, length, x, normed, cot, w_qkv, w_out, w_gu, own_down
    )
    own_qkv = own_qkv.astype(F32)
    cols = lambda a, b: jnp.moveaxis(own_qkv[:, :, a:b], 0, 1).reshape(depth, -1)
    raw_q, raw_k, raw_v = cols(0, cut_q), cols(cut_q, cut_k), cols(cut_k, None)
    own_gu = own_gu.reshape(2, 2, 2, depth, 2, planes, block).astype(F32)
    raw_gu = jnp.transpose(own_gu, (4, 3, 0, 5, 2, 1, 6)).reshape(2, depth, hidden)
    gain_grad = lambda pairs: sum(jnp.sum(w.astype(F32) * raw, 1) for w, raw in pairs)
    return (
        block_out.reshape(tokens.shape),
        grad_tokens.reshape(tokens.shape),
        raw_q * gain_one, raw_k * gain_one, raw_v * gain_one,
        own_out.astype(F32),
        raw_gu[0] * gain_two, raw_gu[1] * gain_two,
        own_dn.reshape(-1, width).astype(F32),
        gain_grad([(w_query, raw_q), (w_key, raw_k), (w_value, raw_v)]),
        gain_grad([(w_gate, raw_gu[0]), (w_up, raw_gu[1])]),
    )


def fits(mesh):
    return mesh.shape["seq"] == 2 and mesh.shape["dp"] == 16


def solution(mesh):
    body = shards_fast if fits(mesh) else shards_plain
    return jax.shard_map(body, mesh=mesh, in_specs=IN_SPECS, out_specs=OUT_SPECS, check_vma=False)
```

```python
import jax
import jax.numpy as jnp
import numpy as np
from jax import lax
from jax.experimental import pallas as pl
from jax.experimental.pallas import tpu as pltpu
from jax.sharding import PartitionSpec as P

HD = 96
EPS = 1e-05
THETA = 100000.0


def rotary(positions, width):
    steps_half = jnp.arange(width // 2, dtype=jnp.float32)
    frequency = jnp.power(THETA, -2.0 * steps_half / width)
    angles = positions[:, None] * frequency[None, :]
    cosine = jnp.cos(angles)
    sine = jnp.sin(angles)
    return (jnp.concatenate([cosine, cosine], -1), jnp.concatenate([sine, sine], -1))


def rotate(values, cosine, sine):
    half = values.shape[-1] // 2
    turned = jnp.concatenate([-values[..., half:], values[..., :half]], -1)
    return values * cosine[:, None, :] + turned * sine[:, None, :]


def rotate_back(grads, cosine, sine):
    half = grads.shape[-1] // 2
    sined = grads * sine[:, None, :]
    turned = jnp.concatenate([sined[..., half:], -sined[..., :half]], -1)
    return grads * cosine[:, None, :] + turned


def dot32(left, right):
    return jnp.dot(left, right, preferred_element_type=jnp.float32)


def dot_t(left, right):
    return lax.dot_general(left, right, (((1,), (1,)), ((), ())), preferred_element_type=jnp.float32)


def dot_l(left, right):
    return lax.dot_general(left, right, (((0,), (0,)), ((), ())), preferred_element_type=jnp.float32)


def inv_rms(values):
    return lax.rsqrt(jnp.mean(values * values, axis=-1, keepdims=True) + EPS)


def low(values):
    return values.astype(jnp.bfloat16)


def attend(queries, keys, values):
    rows = queries.shape[1]
    ids = jnp.arange(rows, dtype=jnp.int32)
    visible = ids[:, None] >= ids[None, :]
    scores = HD ** (-0.5) * jnp.einsum("bqkgd,bckd->bkgqc", queries, keys, preferred_element_type=jnp.float32)
    scores = jnp.where(visible, scores, -jnp.inf)
    top = jnp.max(scores, -1, keepdims=True)
    exps = jnp.exp(scores - top)
    probs = exps / jnp.sum(exps, -1, keepdims=True)
    mixed = jnp.einsum("bkgqc,bckd->bqkgd", low(probs), values, preferred_element_type=jnp.float32)
    return probs, low(mixed)


def attend_back(queries, keys, values, probs, grad_mixed):
    grad_values = jnp.einsum("bkgqc,bqkgd->bckd", low(probs), grad_mixed, preferred_element_type=jnp.float32)
    grad_probs = jnp.einsum("bqkgd,bckd->bkgqc", grad_mixed, values, preferred_element_type=jnp.float32)
    grad_scores = low(probs * (grad_probs - jnp.sum(probs * grad_probs, -1, keepdims=True)))
    scale = HD ** (-0.5)
    grad_queries = scale * jnp.einsum("bkgqc,bckd->bqkgd", grad_scores, keys, preferred_element_type=jnp.float32)
    grad_keys = scale * jnp.einsum("bkgqc,bqkgd->bckd", grad_scores, queries, preferred_element_type=jnp.float32)
    return grad_queries, grad_keys, grad_values


def mlp_grads(gate, up, grad_hidden):
    sigma = jax.nn.sigmoid(gate)
    silu = gate * sigma
    hidden = low(silu * up)
    grad_gate = low(grad_hidden * up * sigma * (1.0 + gate * (1.0 - sigma)))
    grad_up = low(grad_hidden * silu)
    return hidden, grad_gate, grad_up


def shards_plain(tokens, cotangent, w_query, w_key, w_value, w_out, w_gate, w_up, w_down, gain_attn, gain_mlp):
    seqs, length, width = tokens.shape
    rows = seqs * length
    kv_heads = w_key.shape[1] // HD
    groups = w_query.shape[1] // w_key.shape[1]
    gather = lambda w: lax.all_gather(w, "dp", axis=0, tiled=True)
    full_query, full_key, full_value, full_out = map(gather, (w_query, w_key, w_value, w_out))
    gains = gather(jnp.stack([gain_attn, gain_mlp], 1)).astype(jnp.float32)
    gain_one, gain_two = gains[:, 0], gains[:, 1]
    full_gate, full_up, full_down = map(gather, (w_gate, w_up, w_down))
    cosine, sine = rotary(jnp.arange(length, dtype=jnp.float32), HD)
    cosine, sine = jnp.tile(cosine, (seqs, 1)), jnp.tile(sine, (seqs, 1))

    inputs = tokens.reshape(rows, width).astype(jnp.float32)
    grad_in = cotangent.reshape(rows, width)
    scale_one = inv_rms(inputs)
    normed = low(inputs * scale_one * gain_one)
    queries = low(rotate(dot32(normed, full_query).reshape(rows, -1, HD), cosine, sine))
    keys = low(rotate(dot32(normed, full_key).reshape(rows, -1, HD), cosine, sine))
    values = low(dot32(normed, full_value))
    queries = queries.reshape(seqs, length, kv_heads, groups, HD)
    keys = keys.reshape(seqs, length, kv_heads, HD)
    values = values.reshape(seqs, length, kv_heads, HD)
    probs, mixed = attend(queries, keys, values)
    mixed = mixed.reshape(rows, -1)
    hidden_one = inputs + dot32(mixed, full_out)
    scale_two = inv_rms(hidden_one)
    normed_two = low(hidden_one * scale_two * gain_two)
    gate, up = dot32(normed_two, full_gate), dot32(normed_two, full_up)
    hidden, grad_gate, grad_up = mlp_grads(gate, up, dot_t(grad_in, full_down))
    block_out = low(hidden_one + dot32(hidden, full_down))

    acc_down = dot_l(hidden, grad_in)
    acc_gate = dot_l(normed_two, grad_gate)
    acc_up = dot_l(normed_two, grad_up)
    grad_normed_two = dot_t(grad_gate, full_gate) + dot_t(grad_up, full_up)
    acc_gain_two = jnp.sum(grad_normed_two * hidden_one * scale_two, 0)
    weighted = grad_normed_two * gain_two
    grad_one = grad_in.astype(jnp.float32) + scale_two * (
        weighted - hidden_one * scale_two * scale_two * jnp.mean(weighted * hidden_one, -1, keepdims=True)
    )
    grad_branch = low(grad_one)
    acc_out = dot_l(mixed, grad_branch)
    grad_mixed = low(dot_t(grad_branch, full_out)).reshape(queries.shape)
    grad_queries, grad_keys, grad_values = attend_back(queries, keys, values, probs, grad_mixed)
    grad_queries = low(rotate_back(grad_queries.reshape(rows, -1, HD), cosine, sine)).reshape(rows, -1)
    grad_keys = low(rotate_back(grad_keys.reshape(rows, -1, HD), cosine, sine)).reshape(rows, -1)
    grad_values = low(grad_values).reshape(rows, -1)
    acc_query = dot_l(normed, grad_queries)
    acc_key = dot_l(normed, grad_keys)
    acc_value = dot_l(normed, grad_values)
    grad_normed = dot_t(grad_queries, full_query) + dot_t(grad_keys, full_key) + dot_t(grad_values, full_value)
    acc_gain_one = jnp.sum(grad_normed * inputs * scale_one, 0)
    weighted = grad_normed * gain_one
    grad_tokens = grad_one + scale_one * (
        weighted - inputs * scale_one * scale_one * jnp.mean(weighted * inputs, -1, keepdims=True)
    )

    def share(acc):
        owned = lax.psum_scatter(low(acc), "dp", scatter_dimension=0, tiled=True)
        return lax.psum(owned, "seq").astype(jnp.float32)

    grads = [share(a) for a in (acc_down, acc_gate, acc_up, acc_out, acc_query, acc_key, acc_value)]
    gain_grads = lax.psum(
        lax.psum_scatter(jnp.stack([acc_gain_one, acc_gain_two], 1), "dp", scatter_dimension=0, tiled=True), "seq"
    )
    down, gate, up, out, query, key, value = grads
    return (
        block_out.reshape(tokens.shape),
        low(grad_tokens).reshape(tokens.shape),
        query, key, value, out, gate, up, down,
        gain_grads[:, 0], gain_grads[:, 1],
    )


ROWS = P(("dp", "seq"), None, None)
SPLIT = P("dp", None)
IN_SPECS = (ROWS, ROWS) + (SPLIT,) * 7 + (P("dp"), P("dp"))
OUT_SPECS = (ROWS, ROWS) + (SPLIT,) * 7 + (P("dp"), P("dp"))


MESH = pl.DeviceIdType.MESH
VMEM = pl.BlockSpec(memory_space=pltpu.VMEM)
ANY = pl.BlockSpec(memory_space=pl.ANY)
BF = jnp.bfloat16
F32 = jnp.float32
STRIP = 16
PIECES = 4
VMEM_BYTES = 66_000_000


class Place:
    def __init__(self, planes):
        self.planes = planes
        d = lax.axis_index("dp")
        self.d, self.s = d, lax.axis_index("seq")
        self.c, self.y, self.z = d % 2, (d // 2) % 2, d // 4
        self.p = d // 2
        self.rank = 2 * self.s + self.c
        self.core = (d + 1 - 2 * self.c, self.s)
        self.across = (d, 1 - self.s)
        self.corner = (d + 1 - 2 * self.c, 1 - self.s)
        self.side = (d + 2 - 4 * self.y, self.s)
        self.right = (lax.rem(d + 4, 4 * planes), self.s)
        self.left = (lax.rem(d + 4 * planes - 4, 4 * planes), self.s)
        self.has_right, self.has_left = self.z < planes - 1, self.z > 0
        odd = self.z % 2
        self.twin = self.z + 1 - 2 * odd
        self.buddy = (d + 4 - 8 * odd, self.s)


def greet(me):
    barrier = pltpu.get_barrier_semaphore()
    for peer in (me.core, me.across, me.corner, me.side, me.right, me.left):
        pl.semaphore_signal(barrier, inc=1, device_id=peer, device_id_type=MESH)
    pl.semaphore_wait(barrier, 6)


def push(src, dst, send, recv, peer):
    return pltpu.make_async_remote_copy(
        src_ref=src, dst_ref=dst, send_sem=send, recv_sem=recv, device_id=peer, device_id_type=MESH
    )


def arrived(dst, recv, peer):
    push(dst, dst, recv, recv, peer).wait_recv()


def left_over(src, send, peer):
    push(src, src, send, send, peer).wait_send()


class Slots:
    def __init__(self, ref, rows):
        self.ref, self.rows = ref, rows
        self.at = self

    def __getitem__(self, block):
        return self.ref.at[pl.ds(pl.multiple_of(block * self.rows, self.rows), self.rows)]


def group_start(me, src, dst, send, recv):
    push(src, dst.at[me.rank], send.at[0], recv.at[0], me.core).start()
    push(src, dst.at[me.rank], send.at[1], recv.at[1], me.across).start()


def group_relay(me, dst, send, recv):
    slot = dst.at[2 * (1 - me.s) + me.c]
    arrived(slot, recv.at[1], me.across)
    push(slot, slot, send.at[2], recv.at[2], me.core).start()


def group_finish(me, src, dst, send, recv):
    arrived(dst.at[2 * me.s + 1 - me.c], recv.at[0], me.core)
    arrived(dst.at[2 * (1 - me.s) + 1 - me.c], recv.at[2], me.core)
    left_over(src, send.at[0], me.core)
    left_over(src, send.at[1], me.across)
    slot = dst.at[2 * (1 - me.s) + me.c]
    left_over(slot, send.at[2], me.core)


def group_sems():
    return [pltpu.SemaphoreType.DMA((3,)), pltpu.SemaphoreType.DMA((3,))]


def upper(slot):
    return slot.at[pl.ds(0, slot.shape[0] // 2)]


def lower(slot):
    return slot.at[pl.ds(slot.shape[0] // 2, slot.shape[0] // 2)]


def line_start(me, dst, sems):
    line_side(me, dst, sems)
    line_ends(me, dst, sems)


def line_side(me, dst, sems):
    to_right, to_left, line, to_side, side, twin = sems
    slot = dst(me.p)
    push(slot, slot, to_side.at[me.z], side.at[me.z], me.side).start()


def line_ends(me, dst, sems):
    to_right, to_left, line, to_side, side, twin = sems
    slot = dst(me.p)

    @pl.when(me.has_right)
    def _():
        push(slot, slot, to_right.at[me.z], line.at[me.z], me.right).start()

    @pl.when(me.has_left)
    def _():
        push(slot, slot, to_left.at[me.z], line.at[me.z], me.left).start()


def line_hop(me, dst, sems, hop):
    to_right, to_left, line, to_side, side, twin = sems

    def pass_on(item, back, forth, may, sends):
        slot = dst(2 * item + me.y)
        arrived(slot, line.at[item], back)

        @pl.when(may)
        def _():
            push(slot, slot, sends.at[item], line.at[item], forth).start()

        if hop > 1:
            push(slot, slot, to_side.at[item], side.at[item], me.side).start()
        else:

            @pl.when(item != me.twin)
            def _():
                push(slot, slot, to_side.at[item], side.at[item], me.side).start()

            @pl.when(item == me.twin)
            def _():
                half = upper(slot)
                push(half, half, to_side.at[item], side.at[item], me.side).start()

    @pl.when(me.z >= hop)
    def _():
        pass_on(me.z - hop, me.left, me.right, me.has_right, to_right)

    @pl.when(me.z + hop < me.planes)
    def _():
        pass_on(me.z + hop, me.right, me.left, me.has_left, to_left)


def line_twin(me, dst, sems):
    to_right, to_left, line, to_side, side, twin = sems
    slot = dst(2 * me.z + 1 - me.y)
    arrived(slot, side.at[me.z], me.side)
    half = lower(slot)
    push(half, half, twin.at[0], twin.at[1], me.buddy).start()


def line_finish(me, dst, sems):
    to_right, to_left, line, to_side, side, twin = sems
    for item in range(me.planes):
        slot, mine = dst(2 * item + 1 - me.y), dst(2 * item + me.y)

        @pl.when(item == me.twin)
        def _():
            arrived(upper(slot), side.at[item], me.side)
            arrived(lower(slot), twin.at[1], me.buddy)
            left_over(upper(mine), to_side.at[item], me.side)

        @pl.when(jnp.logical_and(item != me.twin, item != me.z))
        def _():
            arrived(slot, side.at[item], me.side)

        @pl.when(item != me.twin)
        def _():
            left_over(mine, to_side.at[item], me.side)

        @pl.when(item == me.z)
        def _():
            left_over(lower(slot), twin.at[0], me.buddy)

        @pl.when(jnp.logical_and(me.has_right, item <= me.z))
        def _():
            left_over(mine, to_right.at[item], me.right)

        @pl.when(jnp.logical_and(me.has_left, item >= me.z))
        def _():
            left_over(mine, to_left.at[item], me.left)


def line_sems(planes):
    return [pltpu.SemaphoreType.DMA((planes,))] * 5 + [pltpu.SemaphoreType.DMA((2,))]


def pick(table, index):
    value = jnp.int32(table[0])
    for i in range(1, len(table)):
        value = jnp.where(index == i, table[i], value)
    return value


def far_first(planes):
    return [sorted(range(planes), key=lambda i, z=z: (-abs(i - z), i)) for z in range(planes)]


def add_into(dst, *others):
    rows = dst.shape[0]

    def body(i, carry):
        strip = pl.ds(pl.multiple_of(i * STRIP, STRIP), STRIP)
        total = dst[strip, :].astype(F32)
        for other in others:
            total = total + other[strip, :].astype(F32)
        dst[strip, :] = total.astype(dst.dtype)
        return carry

    lax.fori_loop(0, rows // STRIP, body, 0)


def reduce_start(me, own, half, sems):
    to_side, side, twin = sems[0], sems[1], sems[6]
    orders = far_first(me.planes)
    away = lower(own(2 * me.twin + 1 - me.y))
    push(away, lower(half.at[me.z]), twin.at[0], twin.at[1], me.buddy).start()
    for i in range(me.planes):
        item = pick([o[i] for o in orders], me.z)
        src, dst = own(2 * item + 1 - me.y), half.at[item]

        @pl.when(item == me.twin)
        def _():
            push(upper(src), upper(dst), to_side.at[item], side.at[item], me.side).start()

        @pl.when(jnp.logical_and(item != me.twin, item != me.z))
        def _():
            push(src, dst, to_side.at[item], side.at[item], me.side).start()


def reduce_mix(me, own, half, sems):
    to_side, side, twin = sems[0], sems[1], sems[6]
    mixed, got = own(2 * me.z + 1 - me.y), lower(half.at[me.twin])
    arrived(got, twin.at[1], me.buddy)
    add_into(lower(mixed), got)
    push(mixed, half.at[me.z], to_side.at[me.z], side.at[me.z], me.side).start()


def reduce_y(me, own, half, lines, sems, i):
    to_side, side, to_right, to_left, left, right, twin = sems
    item = pick([o[i] for o in far_first(me.planes)], me.z)
    mine, ours = half.at[item], own(2 * item + me.y)

    @pl.when(item == me.twin)
    def _():
        arrived(upper(mine), side.at[item], me.side)
        add_into(upper(mine), upper(ours))
        copy_into(lower(mine), lower(ours))

    @pl.when(item != me.twin)
    def _():
        arrived(mine, side.at[item], me.side)
        add_into(mine, ours)

    @pl.when(jnp.logical_and(item > me.z, jnp.logical_not(me.has_left)))
    def _():
        push(mine, lines.at[item], to_right.at[item], left.at[item], me.right).start()

    @pl.when(jnp.logical_and(item < me.z, jnp.logical_not(me.has_right)))
    def _():
        there = jnp.where(item == me.z - 1, me.planes, item)
        push(mine, lines.at[there], to_left.at[item], right.at[item], me.left).start()


def reduce_z(me, half, lines, sems, i):
    to_side, side, to_right, to_left, left, right, twin = sems
    item = pick([o[i] for o in far_first(me.planes)], me.z)
    mine = half.at[item]
    spot = jnp.where(item == me.z, me.planes, item)

    @pl.when(jnp.logical_and(me.has_left, item >= me.z))
    def _():
        arrived(lines.at[item], left.at[item], me.left)
        add_into(mine, lines.at[item])

        @pl.when(item > me.z)
        def _():
            push(mine, lines.at[item], to_right.at[item], left.at[item], me.right).start()

    @pl.when(jnp.logical_and(me.has_right, item <= me.z))
    def _():
        arrived(lines.at[spot], right.at[item], me.right)
        add_into(mine, lines.at[spot])

        @pl.when(item < me.z)
        def _():
            there = jnp.where(item == me.z - 1, me.planes, item)
            push(mine, lines.at[there], to_left.at[item], right.at[item], me.left).start()


def reduce_finish(me, own, half, sems):
    to_side, side, to_right, to_left, left, right, twin = sems
    left_over(lower(own(2 * me.twin + 1 - me.y)), twin.at[0], me.buddy)
    for item in range(me.planes):
        sent = own(2 * item + 1 - me.y)

        @pl.when(item == me.twin)
        def _():
            left_over(upper(sent), to_side.at[item], me.side)

        @pl.when(item != me.twin)
        def _():
            left_over(sent, to_side.at[item], me.side)

        @pl.when(item > me.z)
        def _():
            left_over(half.at[item], to_right.at[item], me.right)

        @pl.when(item < me.z)
        def _():
            left_over(half.at[item], to_left.at[item], me.left)


def reduce_sems(planes):
    return [pltpu.SemaphoreType.DMA((planes,))] * 6 + [pltpu.SemaphoreType.DMA((2,))]


def copy_into(dst, src):
    def body(i, carry):
        strip = pl.ds(pl.multiple_of(i * STRIP, STRIP), STRIP)
        dst[strip, :] = src[strip, :]
        return carry

    lax.fori_loop(0, dst.shape[0] // STRIP, body, 0)


def reduce_buffers(planes, rows, columns):
    return [pltpu.VMEM((planes, rows, columns), BF), pltpu.VMEM((planes + 1, rows, columns), BF)]


def by_chip(ref, rows=None):
    if rows is None:
        return lambda chip: ref.at[chip]
    return lambda chip: ref.at[pl.ds(pl.multiple_of(chip * rows, STRIP), rows)]


def deal_start(me, final, rows, out, local, send, recv):
    mine = out.at[me.rank]
    part = lambda core: final.at[pl.ds(pl.multiple_of(core * rows, rows), rows)]
    pltpu.make_async_copy(part(me.c), mine, local).start()
    push(part(1 - me.c), mine, send.at[0], recv.at[0], me.core).start()
    push(part(me.c), mine, send.at[1], recv.at[1], me.across).start()
    push(part(1 - me.c), mine, send.at[2], recv.at[2], me.corner).start()


def deal_finish(me, final, rows, out, local, send, recv):
    part = lambda core: final.at[pl.ds(pl.multiple_of(core * rows, rows), rows)]
    pltpu.make_async_copy(part(me.c), out.at[me.rank], local).wait()
    left_over(part(1 - me.c), send.at[0], me.core)
    left_over(part(me.c), send.at[1], me.across)
    left_over(part(1 - me.c), send.at[2], me.corner)
    arrived(out.at[2 * me.s + 1 - me.c], recv.at[0], me.core)
    arrived(out.at[2 * (1 - me.s) + me.c], recv.at[1], me.across)
    arrived(out.at[2 * (1 - me.s) + 1 - me.c], recv.at[2], me.corner)


def blocks_start(me, part, got, send, recv, i):
    seq = (1 - me.s, me.s)[i]
    push(part.at[2 * seq + 1 - me.c], got.at[seq], send.at[i], recv.at[i], me.core).start()


def blocks_cross(me, part, got, last, send, recv):
    away = 1 - me.s
    arrived(got.at[away], recv.at[0], me.core)
    add_into(got.at[away], part.at[2 * away + me.c])
    push(got.at[away], last, send.at[2], recv.at[2], me.across).start()


def blocks_finish(me, part, got, last, send, recv):
    arrived(got.at[me.s], recv.at[1], me.core)
    arrived(last, recv.at[2], me.across)
    for i, seq in enumerate((1 - me.s, me.s)):
        left_over(part.at[2 * seq + 1 - me.c], send.at[i], me.core)
    left_over(got.at[1 - me.s], send.at[2], me.across)


def blocks_sems():
    return [pltpu.SemaphoreType.DMA((3,))] * 2


def blocks_buffers(rows, width):
    return [pltpu.VMEM((2, rows, width), BF), pltpu.VMEM((rows, width), BF)]


def strips(rows, body):
    def step(i, carry):
        body(pl.ds(pl.multiple_of(i * STRIP, STRIP), STRIP))
        return carry

    lax.fori_loop(0, rows // STRIP, step, 0)


def comm_call(kernel, ident, outs, out_specs, ins, scratch, name):
    return pl.pallas_call(
        kernel,
        out_shape=outs,
        in_specs=[spec for spec, _ in ins],
        out_specs=out_specs,
        scratch_shapes=scratch,
        name=name,
        compiler_params=pltpu.CompilerParams(
            collective_id=ident, has_side_effects=True, vmem_limit_bytes=VMEM_BYTES
        ),
    )(*[value for _, value in ins])


def shape(dims, dtype=BF):
    return jax.ShapeDtypeStruct(dims, dtype)


def split_start(me, parts, dst, keep, send, recv):
    pltpu.make_async_copy(parts.at[me.c], dst(me.c), keep).start()
    push(parts.at[1 - me.c], dst(me.c), send, recv, me.core).start()


def split_finish(me, parts, dst, keep, send, recv):
    pltpu.make_async_copy(parts.at[me.c], dst(me.c), keep).wait()
    arrived(dst(1 - me.c), recv, me.core)
    left_over(parts.at[1 - me.c], send, me.core)


def norm_back(values, weighted, base):
    scale = inv_rms(values)
    return base + scale * (
        weighted - values * scale * scale * jnp.mean(weighted * values, -1, keepdims=True)
    )


LANES = 128


def head_tables(length):
    steps = np.arange(HD // 2, dtype=np.float64)
    angles = np.arange(length, dtype=np.float64)[:, None] * np.power(THETA, -2.0 * steps / HD)[None, :]
    cosine, sine, none = np.cos(angles), np.sin(angles), np.zeros_like(angles)
    tables = [(cosine, cosine), (none, sine), (-sine, none)]
    pad = ((0, 0), (0, LANES - HD))
    return np.stack([np.pad(np.concatenate(t, 1), pad) for t in tables]).astype(np.float32)


def turn(values, tables, sign):
    other = pltpu.roll(values, HD // 2, 1) * tables[1] + pltpu.roll(values, LANES - HD // 2, 1) * tables[2]
    return values * tables[0] + sign * other


def block_step(planes, length, tokens, cot, w_query, w_key, w_value, w_out, w_gate, w_up, w_down, gain_attn, gain_mlp):
    rows, width = tokens.shape
    total = 4 * rows
    depth = w_query.shape[0]
    head = w_out.shape[0]
    q_own, k_own = w_query.shape[1] // 4, w_key.shape[1] // 4
    q_cols = q_own + 2 * k_own
    block = w_down.shape[0] // 2
    units = 2 * planes * block
    half_units = units // 2
    cols = 2 * half_units
    tile, chunk = 2 * rows, 256
    heads4 = 4 * head
    piece = 2 * head // PIECES

    def kernel(x_ref, g_loc, wq_ref, wk_ref, wv_ref, out_loc, gate_ref, up_ref, down_ref, ga_ref, gm_ref, tab_ref,
               bo_ref, gx_ref, qkv_out, out_out, gu_out, dn_out, stash, *scr):
        it = iter(scr)
        take = lambda k: [next(it) for _ in range(k)]
        n_buf, g_all, qkv_all, out_all, gu_all, dn_all, heads, mixed = take(8)
        part, out_part, x1, mid, dgu, g_gu, dx_all = take(7)
        (got, last), (got_f, last_f) = take(2), take(2)
        gu_buf, dn_buf, q_buf, o_buf = [take(2), take(2)], take(2), take(2), take(3)
        n_sems, g_sems, m_sems, d_sems = take(2), take(2), take(2), take(2)
        x_sems, b_sems, f_sems, h_sems = take(2), take(2), take(2), take(2)
        q_split, gu_split = take(3), [take(3), take(3)]
        q_line, gu_line, dn_line = take(6), [take(6), take(6)], take(6)
        gu_sems, dn_sems, q_sems = [take(7), take(7)], take(7), take(7)
        gu_deal, dn_deal, q_deal, o_deal = [take(3), take(3)], take(3), take(3), take(3)
        local, edge, o_fan, o_red, fetch, sel_ref, gains = take(7)
        me = Place(planes)
        greet(me)
        tok = lambda ref: Slots(ref, rows)
        q_slots, dn_slots = by_chip(qkv_all, 2 * depth), by_chip(dn_all, block)
        gu_slots = [by_chip(gu_all.at[h], 2 * depth) for h in range(2)]

        def core_rows(ref):
            return lambda core: ref.at[pl.ds(pl.multiple_of((2 * me.p + core) * depth, STRIP), depth)]

        fetch_x = pltpu.make_async_copy(x_ref, last_f, local.at[4])
        fetch_x.start()
        stage = out_part.at[pl.ds(0, depth)]
        heads_in = []
        for i, (ref, spot, size) in enumerate(
            ((wq_ref, 0, 2 * q_own), (wk_ref, 2 * q_own, 2 * k_own), (wv_ref, 2 * q_own + 2 * k_own, 2 * k_own))
        ):
            src = ref.at[:, pl.ds(pl.multiple_of(me.s * size, LANES), size)]
            heads_in.append(pltpu.make_async_copy(src, stage.at[:, pl.ds(spot, size)], fetch.at[i]))
            heads_in[-1].start()

        q_share = q_buf[0].at[0, pl.ds(0, depth)]
        gu_share = [mid.at[pl.ds(h * depth, depth)] for h in range(2)]
        units_in = []
        for other in range(2):
            core = (me.c, 1 - me.c)[other]
            for h in range(2):
                dst = (core_rows(gu_all.at[h])(me.c), gu_share[h])[other]
                for k in range(2 * planes):
                    ref = (gate_ref, up_ref)[k // planes]
                    chip = h * planes + k % planes
                    first = (2 * chip + core) * 2 * block + me.s * block
                    copy = pltpu.make_async_copy(
                        ref.at[:, pl.ds(pl.multiple_of(first, LANES), block)],
                        dst.at[:, pl.ds(k * block, block)],
                        fetch.at[3 + (other * 2 + h) * 2 * planes + k],
                    )
                    copy.start()
                    units_in.append(copy)
        own_down = down_ref.at[pl.ds(pl.multiple_of(me.s * block, STRIP), block)]
        keep_d = pltpu.make_async_copy(own_down, dn_slots(me.p), local.at[2])
        keep_d.start()
        keep_g = pltpu.make_async_copy(g_loc, tok(g_all).at[me.rank], local.at[3])
        keep_g.start()

        same = lax.broadcasted_iota(jnp.int32, (depth, depth), 0) == lax.broadcasted_iota(jnp.int32, (depth, depth), 1)
        for k, ref in enumerate((ga_ref, gm_ref)):
            column = jnp.sum(jnp.where(same, ref[...].astype(F32), 0.0), 1, keepdims=True)
            gains[k] = jnp.broadcast_to(column, (depth, LANES))
        row = lax.broadcasted_iota(jnp.int32, (heads4, 4 * LANES), 0)
        lane = lax.broadcasted_iota(jnp.int32, (heads4, 4 * LANES), 1)
        shift = sum(jnp.where(row >= k * HD, LANES - HD, 0) for k in range(1, 4))
        sel_ref[...] = jnp.where(lane == row + shift, 1.0, 0.0).astype(BF)

        for copy in heads_in:
            copy.wait()
        gain = gains[0][:, 0:1]
        tiles = lambda first, count: [
            stage[:, first + k * LANES:first + (k + 1) * LANES].astype(F32) * gain for k in range(count)
        ]
        queries = tiles(0, 6)
        k0, k1, k2 = tiles(2 * q_own, 3)
        v0, v1, v2 = tiles(2 * q_own + 2 * k_own, 3)
        rolled = lambda value: pltpu.roll(value, LANES // 2, 1)
        in_low = lax.broadcasted_iota(jnp.int32, (depth, LANES), 1) < LANES // 2
        join = lambda first, second: jnp.where(in_low, first, second)
        shares = (
            queries[:3] + [k0, join(k1, rolled(v0)), join(rolled(v0), rolled(v1))],
            queries[3:] + [join(rolled(k1), rolled(k2)), join(rolled(k2), v1), v2],
        )
        for core in range(2):
            value = low(jnp.concatenate(shares[core], 1))

            @pl.when(me.c == core)
            def _():
                core_rows(qkv_all)(me.c)[...] = value

            @pl.when(me.c != core)
            def _():
                q_share[...] = value

        push(q_share, core_rows(qkv_all)(me.c), q_split[1], q_split[2], me.core).start()
        here = me.s == me.z // 2
        owner = me.z == me.rank
        lender = jnp.logical_and(here, jnp.logical_not(owner))
        half = lambda y: out_all.at[pl.ds(pl.multiple_of(y * 2 * head, STRIP), 2 * head)]
        head_rows = lambda core: out_all.at[pl.ds(pl.multiple_of((2 * me.y + core) * head, STRIP), head)]
        keep_o = pltpu.make_async_copy(out_loc, head_rows(me.c), local.at[1])

        @pl.when(owner)
        def _():
            keep_o.start()

        @pl.when(lender)
        def _():
            push(out_loc, head_rows(me.c), edge.at[0], edge.at[1], me.core).start()

        fetch_x.wait()

        def first_norm(strip):
            value = last_f[strip, :].astype(F32)
            n_buf[pl.ds(pl.multiple_of(me.rank * rows + strip.start, STRIP), STRIP), :] = low(value * inv_rms(value))

        strips(rows, first_norm)
        group_start(me, tok(n_buf).at[me.rank], tok(n_buf), *n_sems)
        arrived(core_rows(qkv_all)(1 - me.c), q_split[2], me.core)
        line_start(me, q_slots, q_line)

        for copy in units_in:
            copy.wait()

        def weigh(i, carry):
            strip = pl.ds(pl.multiple_of(i * STRIP, STRIP), STRIP)
            gain = gains[1, strip, 0:1]
            for h in range(2):
                for ref in (core_rows(gu_all.at[h])(me.c), gu_share[h]):
                    ref[strip, :] = low(ref[strip, :].astype(F32) * gain)
            return carry

        lax.fori_loop(0, depth // STRIP, weigh, 0)
        for h in range(2):
            push(gu_share[h], core_rows(gu_all.at[h])(me.c), gu_split[h][1], gu_split[h][2], me.core).start()
        group_start(me, g_loc, tok(g_all), *g_sems)

        fan_in, fan_right, fan_left, fan_side, fan_other = [o_fan.at[k] for k in range(5)]
        bit = lambda y, q: out_all.at[pl.ds(pl.multiple_of(y * 2 * head + q * piece, STRIP), piece)]
        go_right = jnp.logical_and(me.z >= me.rank, me.has_right)
        go_left = jnp.logical_and(me.z <= me.rank, me.has_left)

        def fan(q):
            mine = bit(me.y, q)

            @pl.when(me.z > me.rank)
            def _():
                arrived(mine, fan_in.at[q], me.left)

            @pl.when(me.z < me.rank)
            def _():
                arrived(mine, fan_in.at[q], me.right)

            @pl.when(go_right)
            def _():
                push(mine, mine, fan_right.at[q], fan_in.at[q], me.right).start()

            @pl.when(go_left)
            def _():
                push(mine, mine, fan_left.at[q], fan_in.at[q], me.left).start()

            push(mine, mine, fan_side.at[q], fan_other.at[q], me.side).start()

        @pl.when(owner)
        def _():
            keep_o.wait()
            arrived(head_rows(1 - me.c), edge.at[1], me.core)

        @pl.when(lender)
        def _():
            left_over(out_loc, edge.at[0], me.core)

        line_hop(me, q_slots, q_line, 1)
        line_twin(me, q_slots, q_line)
        fan(0)
        line_hop(me, q_slots, q_line, 2)
        group_relay(me, tok(n_buf), *n_sems)
        fan(1)
        for hop in range(3, planes):
            line_hop(me, q_slots, q_line, hop)
        fan(2)
        fan(3)
        arrived(core_rows(gu_all.at[0])(1 - me.c), gu_split[0][2], me.core)
        line_start(me, gu_slots[0], gu_line[0])
        keep_d.wait()
        line_start(me, dn_slots, dn_line)
        arrived(core_rows(gu_all.at[1])(1 - me.c), gu_split[1][2], me.core)
        group_finish(me, tok(n_buf).at[me.rank], tok(n_buf), *n_sems)
        left_over(q_share, q_split[1], me.core)
        for h in range(2):
            left_over(gu_share[h], gu_split[h][1], me.core)
        saved = pltpu.make_async_copy(n_buf, stash, local.at[0])
        saved.start()
        line_finish(me, q_slots, q_line)

        def widen(i, carry):
            feats = pl.ds(pl.multiple_of(i * tile, tile), tile)
            for k in range(2):
                g_gu[feats, k * 4 * LANES:(k + 1) * 4 * LANES] = low(
                    dot32(qkv_all[feats, k * heads4:(k + 1) * heads4], sel_ref[...])
                )
            return carry

        lax.fori_loop(0, width // tile, widen, 0)

        def project(i, carry):
            toks = pl.ds(pl.multiple_of(i * length, length), length)
            n = n_buf[toks, :]
            tabs = [tab_ref[k] for k in range(3)]
            for k in range(8):
                value = dot32(n, g_gu[:, k * LANES:(k + 1) * LANES])
                heads[toks, k * LANES:(k + 1) * LANES] = low(turn(value, tabs, 1.0) if k < 6 else value)
            return carry

        lax.fori_loop(0, total // length, project, 0)
        line_hop(me, gu_slots[0], gu_line[0], 1)
        group_relay(me, tok(g_all), *g_sems)
        line_hop(me, dn_slots, dn_line, 1)
        line_twin(me, gu_slots[0], gu_line[0])
        line_twin(me, dn_slots, dn_line)
        saved.wait()
        for q in range(PIECES):
            arrived(bit(1 - me.y, q), fan_other.at[q], me.side)

        def pair(toks, j, ref, start):
            first = start + 2 * j * LANES
            return jnp.concatenate(
                [ref[toks, first:first + LANES], ref[toks, first + LANES:first + 2 * LANES]], 0
            )

        def probabilities(toks, j):
            q = pair(toks, j, heads, 0)
            k = heads[toks, (4 + j) * LANES:(5 + j) * LANES]
            scores = HD ** (-0.5) * dot_t(q, k)
            row = lax.rem(lax.broadcasted_iota(jnp.int32, scores.shape, 0), length)
            col = lax.broadcasted_iota(jnp.int32, scores.shape, 1)
            scores = jnp.where(row >= col, scores, -jnp.inf)
            exps = jnp.exp(scores - jnp.max(scores, 1, keepdims=True))
            return q, k, exps / jnp.sum(exps, 1, keepdims=True)

        def attend_rows(first):
            def one(i, carry):
                toks = pl.ds(pl.multiple_of(first + i * length, length), length)
                outs = []
                for j in range(2):
                    _, _, p = probabilities(toks, j)
                    o = low(dot32(low(p), heads[toks, (6 + j) * LANES:(7 + j) * LANES]))
                    outs += [o[:length], o[length:]]
                mixed[toks, :] = low(dot_t(jnp.concatenate(outs, 1), sel_ref[...]))
                return carry

            lax.fori_loop(0, rows // length, one, 0)
            toks = pl.ds(pl.multiple_of(first, rows), rows)
            part[toks, :] = low(dot32(mixed[toks, :], out_all[...]))

        away, home = 1 - me.s, me.s
        attend_rows((2 * away + 1 - me.c) * rows)
        blocks_start(me, tok(part), got, *x_sems, 0)
        line_hop(me, gu_slots[0], gu_line[0], 2)
        line_ends(me, gu_slots[1], gu_line[1])
        attend_rows((2 * away + me.c) * rows)
        blocks_cross(me, tok(part), got, last, *x_sems)
        line_hop(me, dn_slots, dn_line, 2)
        attend_rows((2 * home + 1 - me.c) * rows)
        blocks_start(me, tok(part), got, *x_sems, 1)
        line_side(me, gu_slots[1], gu_line[1])
        attend_rows((2 * home + me.c) * rows)
        for hop in range(3, planes):
            line_hop(me, gu_slots[0], gu_line[0], hop)
        line_hop(me, gu_slots[1], gu_line[1], 1)
        blocks_finish(me, tok(part), got, last, *x_sems)

        def mine(strip):
            return pl.ds(pl.multiple_of(me.rank * rows + strip.start, STRIP), STRIP)

        def summed(strip, whole, some, rest):
            return (
                whole[mine(strip), :].astype(F32)
                + some[me.s, strip, :].astype(F32)
                + rest[strip, :].astype(F32)
            )

        def middle(strip):
            value = last_f[strip, :].astype(F32) + summed(strip, part, got, last)
            x1[strip, :] = value
            n_buf[mine(strip), :] = low(value * inv_rms(value))

        strips(rows, middle)
        group_start(me, tok(n_buf).at[me.rank], tok(n_buf), *m_sems)
        for hop in range(3, planes):
            line_hop(me, dn_slots, dn_line, hop)
        line_hop(me, gu_slots[1], gu_line[1], 2)
        line_twin(me, gu_slots[1], gu_line[1])
        keep_g.wait()
        group_finish(me, g_loc, tok(g_all), *g_sems)
        for q in range(PIECES):
            left_over(bit(me.y, q), fan_side.at[q], me.side)

            @pl.when(go_right)
            def _():
                left_over(bit(me.y, q), fan_right.at[q], me.right)

            @pl.when(go_left)
            def _():
                left_over(bit(me.y, q), fan_left.at[q], me.left)

        group_relay(me, tok(n_buf), *m_sems)
        group_finish(me, tok(n_buf).at[me.rank], tok(n_buf), *m_sems)
        line_finish(me, gu_slots[0], gu_line[0])
        line_finish(me, dn_slots, dn_line)

        def activations(h, j):
            first = h * half_units + j * chunk

            def step(t, carry):
                toks = pl.ds(pl.multiple_of(t * tile, tile), tile)
                n, g = n_buf[toks, :], g_all[toks, :]
                gate = dot32(n, gu_all[h, :, j * chunk:(j + 1) * chunk])
                up = dot32(n, gu_all[h, :, half_units + j * chunk:half_units + (j + 1) * chunk])
                grad = dot_t(g, dn_all[first:first + chunk, :])
                hidden, d_gate, d_up = mlp_grads(gate, up, grad)
                mid[toks, first:first + chunk] = hidden
                dgu[h, toks, j * chunk:(j + 1) * chunk] = d_gate
                dgu[h, toks, half_units + j * chunk:half_units + (j + 1) * chunk] = d_up
                return carry

            lax.fori_loop(0, total // tile, step, 0)

        def weight_grads(h, out):
            def step(i, carry):
                feats = pl.ds(pl.multiple_of(i * chunk, chunk), chunk)
                out[feats, :] = low(dot_l(n_buf[:, feats], dgu[h]))
                return carry

            lax.fori_loop(0, width // chunk, step, 0)

        steps = half_units // chunk
        for j in range(steps):
            activations(0, j)
        for hop in range(3, planes):
            line_hop(me, gu_slots[1], gu_line[1], hop)
        weight_grads(0, g_gu)
        own_gu = [by_chip(g_gu, 2 * depth), gu_slots[0]]
        reduce_start(me, own_gu[0], gu_buf[0][0], gu_sems[0])
        line_finish(me, gu_slots[1], gu_line[1])
        for j in range(steps):
            activations(1, j)
        finals = [gu_buf[h][0].at[me.z] for h in range(2)]
        gu_y = lambda h, i: reduce_y(me, own_gu[h], *gu_buf[h], gu_sems[h], i)
        gu_z = lambda h, i: reduce_z(me, *gu_buf[h], gu_sems[h], i)
        gu_mix = lambda h: reduce_mix(me, own_gu[h], gu_buf[h][0], gu_sems[h])
        dn_y = lambda i: reduce_y(me, dn_slots, *dn_buf, dn_sems, i)
        dn_z = lambda i: reduce_z(me, *dn_buf, dn_sems, i)
        q_y = lambda i: reduce_y(me, q_slots, *q_buf, q_sems, i)
        q_z = lambda i: reduce_z(me, *q_buf, q_sems, i)
        gu_mix(0)

        def back(seq):
            toks = pl.ds(pl.multiple_of(seq * tile, tile), tile)

            def step(i, carry):
                feats = pl.ds(pl.multiple_of(i * chunk, chunk), chunk)
                value = dot_t(dgu[0, toks, :], gu_all[0, feats, :]) + dot_t(dgu[1, toks, :], gu_all[1, feats, :])
                part[toks, feats] = low(value)
                return carry

            lax.fori_loop(0, width // chunk, step, 0)

        back(away)
        blocks_start(me, tok(part), got, *b_sems, 0)
        gu_y(0, 0)
        back(home)
        blocks_start(me, tok(part), got, *b_sems, 1)
        blocks_cross(me, tok(part), got, last, *b_sems)

        weight_grads(1, gu_all.at[0])
        fetch_n = pltpu.make_async_copy(stash, n_buf, local.at[0])
        fetch_n.start()
        reduce_start(me, own_gu[1], gu_buf[1][0], gu_sems[1])
        gu_y(0, 1)
        gu_z(0, 0)
        gu_y(0, 2)

        def forth(i, carry):
            feats = pl.ds(pl.multiple_of(i * chunk, chunk), chunk)
            out_part[:, feats] = low(dot32(mid[...], dn_all[:, feats]))
            return carry

        lax.fori_loop(0, width // chunk, forth, 0)
        for i in range(2):
            blocks_start(me, tok(out_part), got_f, *f_sems, i)
        gu_z(0, 1)
        gu_z(0, 2)
        gu_y(0, 3)
        blocks_finish(me, tok(part), got, last, *b_sems)

        def branch(strip):
            grad = norm_back(x1[strip, :], summed(strip, part, got, last), g_all[mine(strip), :].astype(F32))
            dx_all[mine(strip), :] = low(grad)

        strips(rows, branch)
        group_start(me, tok(dx_all).at[me.rank], tok(dx_all), *d_sems)
        gu_mix(1)

        def down(i, carry):
            these = pl.ds(pl.multiple_of(i * chunk, chunk), chunk)
            dn_all[these, :] = low(dot_l(mid[:, these], g_all[...]))
            return carry

        lax.fori_loop(0, units // chunk, down, 0)
        reduce_start(me, dn_slots, dn_buf[0], dn_sems)
        gu_z(0, 3)
        gu_y(1, 0)
        gu_y(1, 1)
        gu_z(1, 0)
        gu_y(1, 2)
        reduce_mix(me, dn_slots, dn_buf[0], dn_sems)
        group_relay(me, tok(dx_all), *d_sems)
        deal_start(me, finals[0], depth, gu_out.at[0], *gu_deal[0])
        blocks_cross(me, tok(out_part), got_f, last_f, *f_sems)
        gu_z(1, 1)
        gu_z(1, 2)
        group_finish(me, tok(dx_all).at[me.rank], tok(dx_all), *d_sems)

        def spread_out(t, carry):
            toks = pl.ds(pl.multiple_of(t * rows, rows), rows)
            grad = low(dot_t(dx_all[toks, :], out_all[...]))
            mid[toks, 0:4 * LANES] = low(dot32(grad, sel_ref[...]))
            return carry

        lax.fori_loop(0, 4, spread_out, 0)
        out_all[...] = low(dot_l(mixed[...], dx_all[...]))
        for q in range(PIECES):
            push(bit(1 - me.y, q), o_buf[0].at[pl.ds(q * piece, piece)], o_red.at[0, q], o_red.at[1, q], me.side).start()
        gu_y(1, 3)

        def attend_rows_back(first):
            def one(i, carry):
                toks = pl.ds(pl.multiple_of(first + i * length, length), length)
                tabs = [tab_ref[k] for k in range(3)]
                for j in range(2):
                    q, k, p = probabilities(toks, j)
                    v = heads[toks, (6 + j) * LANES:(7 + j) * LANES]
                    grad = pair(toks, j, mid, 0)
                    d_v = dot_l(low(p), grad)
                    d_p = dot_t(grad, v)
                    d_s = low(p * (d_p - jnp.sum(p * d_p, 1, keepdims=True)))
                    d_q = HD ** (-0.5) * dot32(d_s, k)
                    d_k = HD ** (-0.5) * dot_l(d_s, q)
                    for g in range(2):
                        spot = (2 * j + g) * LANES
                        dgu[0, toks, spot:spot + LANES] = low(turn(d_q[g * length:(g + 1) * length], tabs, -1.0))
                    dgu[0, toks, (4 + j) * LANES:(5 + j) * LANES] = low(turn(d_k, tabs, -1.0))
                    dgu[0, toks, (6 + j) * LANES:(7 + j) * LANES] = low(d_v)
                return carry

            lax.fori_loop(0, rows // length, one, 0)
            toks = pl.ds(pl.multiple_of(first, rows), rows)
            for k in range(2):
                dgu[1, toks, k * heads4:(k + 1) * heads4] = low(
                    dot_t(dgu[0, toks, k * 4 * LANES:(k + 1) * 4 * LANES], sel_ref[...])
                )
            part[toks, :] = low(dot_t(dgu[1, toks, 0:q_cols], qkv_all[...]))

        attend_rows_back((2 * away + 1 - me.c) * rows)
        blocks_start(me, tok(part), got, *h_sems, 0)
        attend_rows_back((2 * away + me.c) * rows)
        blocks_cross(me, tok(part), got, last, *h_sems)
        gu_z(1, 3)
        deal_start(me, finals[1], depth, gu_out.at[1], *gu_deal[1])
        dn_y(0)
        attend_rows_back((2 * home + 1 - me.c) * rows)
        blocks_start(me, tok(part), got, *h_sems, 1)
        attend_rows_back((2 * home + me.c) * rows)
        dn_y(1)
        fetch_n.wait()

        def q_grads(i, carry):
            feats = pl.ds(pl.multiple_of(i * chunk, chunk), chunk)
            qkv_all[feats, :] = low(dot_l(n_buf[:, feats], dgu[1, :, 0:q_cols]))
            return carry

        lax.fori_loop(0, width // chunk, q_grads, 0)
        reduce_start(me, q_slots, q_buf[0], q_sems)
        dn_z(0)
        dn_y(2)

        blocks_finish(me, tok(out_part), got_f, last_f, *f_sems)

        def output(strip):
            got_f[me.s, strip, :] = low(x1[strip, :] + summed(strip, out_part, got_f, last_f))

        strips(rows, output)
        keep_bo = pltpu.make_async_copy(got_f.at[me.s], bo_ref, local.at[1])
        keep_bo.start()
        fetch_x.start()
        dn_z(1)
        dn_z(2)
        dn_y(3)
        reduce_mix(me, q_slots, q_buf[0], q_sems)

        o_sum = lambda q: o_buf[0].at[pl.ds(q * piece, piece)]
        o_left = lambda q: o_buf[1].at[pl.ds(q * piece, piece)]
        o_right = lambda q: o_buf[2].at[pl.ds(q * piece, piece)]

        def o_on(q):
            @pl.when(me.z < me.rank)
            def _():
                push(o_sum(q), o_left(q), o_red.at[4, q], o_red.at[2, q], me.right).start()

            @pl.when(me.z > me.rank)
            def _():
                push(o_sum(q), o_right(q), o_red.at[4, q], o_red.at[3, q], me.left).start()

        from_left = jnp.logical_and(me.has_left, me.z <= me.rank)
        from_right = jnp.logical_and(me.has_right, me.z >= me.rank)
        no_more = jnp.logical_not(jnp.logical_or(from_left, from_right))

        def o_y(q):
            arrived(o_sum(q), o_red.at[1, q], me.side)
            add_into(o_sum(q), bit(me.y, q))

            @pl.when(no_more)
            def _():
                o_on(q)

        def o_z(q):
            @pl.when(from_left)
            def _():
                arrived(o_left(q), o_red.at[2, q], me.left)
                add_into(o_sum(q), o_left(q))

            @pl.when(from_right)
            def _():
                arrived(o_right(q), o_red.at[3, q], me.right)
                add_into(o_sum(q), o_right(q))

            @pl.when(jnp.logical_not(no_more))
            def _():
                o_on(q)

        for q in range(PIECES):
            o_y(q)
        dn_z(3)
        final_dn = dn_buf[0].at[me.z]
        dn_keep, dn_send, dn_recv = dn_deal
        keep_dn = pltpu.make_async_copy(final_dn, dn_out.at[me.s], dn_keep)
        keep_dn.start()
        push(final_dn, dn_out.at[me.s], dn_send, dn_recv, me.across).start()
        o_z(0)
        o_z(1)
        q_y(0)
        o_z(2)
        o_z(3)
        own_half = o_buf[0].at[pl.ds(pl.multiple_of(me.c * head, STRIP), head)]
        other_half = o_buf[0].at[pl.ds(pl.multiple_of((1 - me.c) * head, STRIP), head)]
        o_keep, o_send, o_recv = o_deal
        keep_oo = pltpu.make_async_copy(own_half, out_out, o_keep)

        @pl.when(owner)
        def _():
            keep_oo.start()
            push(other_half, out_out, o_send.at[0], o_recv.at[0], me.core).start()
            push(own_half, out_out, o_send.at[1], o_recv.at[0], me.across).start()
            push(other_half, out_out, o_send.at[2], o_recv.at[0], me.corner).start()

        q_y(1)
        q_z(0)
        q_y(2)

        blocks_finish(me, tok(part), got, last, *h_sems)
        fetch_x.wait()

        def inner(strip):
            got[me.s, strip, :] = low(norm_back(
                last_f[strip, :].astype(F32), summed(strip, part, got, last), dx_all[mine(strip), :].astype(F32)
            ))

        strips(rows, inner)
        keep_gx = pltpu.make_async_copy(got.at[me.s], gx_ref, local.at[2])
        keep_gx.start()
        q_z(1)
        q_z(2)
        q_y(3)
        q_z(3)
        final_q = q_buf[0].at[me.z]
        deal_start(me, final_q, depth, qkv_out, *q_deal)

        for h in range(2):
            reduce_finish(me, own_gu[h], gu_buf[h][0], gu_sems[h])
            deal_finish(me, finals[h], depth, gu_out.at[h], *gu_deal[h])
        reduce_finish(me, dn_slots, dn_buf[0], dn_sems)
        reduce_finish(me, q_slots, q_buf[0], q_sems)
        for q in range(PIECES):
            sum_q = o_sum(q)
            left_over(bit(1 - me.y, q), o_red.at[0, q], me.side)

            @pl.when(me.z < me.rank)
            def _():
                left_over(sum_q, o_red.at[4, q], me.right)

            @pl.when(me.z > me.rank)
            def _():
                left_over(sum_q, o_red.at[4, q], me.left)

        @pl.when(owner)
        def _():
            keep_oo.wait()
            left_over(other_half, o_send.at[0], me.core)
            left_over(own_half, o_send.at[1], me.across)
            left_over(other_half, o_send.at[2], me.corner)

        @pl.when(jnp.logical_not(owner))
        def _():
            arrived(out_out, o_recv.at[0], me.core)

        keep_dn.wait()
        left_over(final_dn, dn_send, me.across)
        arrived(dn_out.at[1 - me.s], dn_recv, me.across)
        keep_bo.wait()
        keep_gx.wait()
        deal_finish(me, final_q, depth, qkv_out, *q_deal)

    sems = lambda *dims: pltpu.SemaphoreType.DMA(dims)
    one, three = pltpu.SemaphoreType.DMA, sems(3)
    vmem = lambda *dims: pltpu.VMEM(dims, BF)
    deal = [one, three, three]
    outs = comm_call(
        kernel, 0,
        [shape((rows, width)), shape((rows, width)), shape((4, depth, q_cols)), shape((head, width)),
         shape((2, 4, depth, cols)), shape((2, block, width)), shape((total, width))],
        [ANY] * 7,
        [(ANY, ref) for ref in (tokens, cot, w_query, w_key, w_value, w_out, w_gate, w_up, w_down)]
        + [(VMEM, gain_attn), (VMEM, gain_mlp), (VMEM, head_tables(length))],
        [vmem(total, width), vmem(total, width), vmem(width, q_cols), vmem(heads4, width), vmem(2, width, cols),
         vmem(units, width), vmem(total, 8 * LANES), vmem(total, heads4)]
        + [vmem(total, width), vmem(total, width), pltpu.VMEM((rows, width), F32), vmem(total, units),
           vmem(2, total, cols), vmem(width, cols), vmem(total, width)]
        + blocks_buffers(rows, width) * 2
        + reduce_buffers(planes, 2 * depth, cols) * 2 + reduce_buffers(planes, block, width)
        + reduce_buffers(planes, 2 * depth, q_cols) + [vmem(2 * head, width)] * 3
        + group_sems() * 4 + blocks_sems() * 4 + [one] * 9
        + line_sems(planes) * 4 + reduce_sems(planes) * 4 + deal * 2 + [one] * 3 + deal * 2
        + [sems(5), sems(2), sems(5, PIECES), sems(5, PIECES), sems(3 + 8 * planes), vmem(heads4, 4 * LANES),
           pltpu.VMEM((2, depth, LANES), F32)],
        "block_step",
    )
    return outs[:6]


def finish(planes, parts, weights, gains):
    block_out, grad_tokens, own_qkv, own_out, own_gu, own_dn = parts
    w_query, w_key, w_value, w_gate, w_up = weights
    rows, width = block_out.shape
    depth, hidden = w_gate.shape
    q_own, k_own = w_query.shape[1] // 4, w_key.shape[1] // 4
    block = own_dn.shape[1]
    steps = 2 * planes
    wide = hidden // steps
    own_dn = own_dn.reshape(2 * block, width)

    def kernel(bo_ref, gx_ref, qkv_ref, out_ref, gate_ref, up_ref, dn_ref, wq_ref, wk_ref, wv_ref, wg_ref, wu_ref,
               ga_ref, gm_ref, bo_out, gx_out, q_out, k_out, v_out, o_out, gate_out, up_out, dn_out, ga_out, gm_out,
               columns, total):
        step = pl.program_id(0)
        same = lax.broadcasted_iota(jnp.int32, (depth, depth), 0) == lax.broadcasted_iota(jnp.int32, (depth, depth), 1)

        def as_row(value):
            return jnp.sum(jnp.where(same, jnp.sum(value, 1, keepdims=True), 0.0), 0, keepdims=True)

        @pl.when(step == 0)
        def _():
            for k, ref in enumerate((ga_ref, gm_ref)):
                column = jnp.sum(jnp.where(same, ref[...].astype(F32), 0.0), 1, keepdims=True)
                columns[k] = jnp.broadcast_to(column, (depth, LANES))
            total[...] = jnp.zeros_like(total)
            o_out[...] = out_ref[...].astype(F32)
            gain = columns[0]
            gathered = jnp.zeros((depth, LANES), F32)

            def put(out, weight, tile, value):
                lanes = slice(tile * LANES, (tile + 1) * LANES)
                out[:, lanes] = value * gain
                return value * weight[:, lanes].astype(F32)

            rolled = lambda value: pltpu.roll(value, LANES // 2, 1)
            in_low = lax.broadcasted_iota(jnp.int32, (depth, LANES), 1) < LANES // 2
            join = lambda first, second: jnp.where(in_low, first, second)
            for rank in range(4):
                for k in range(q_own // LANES):
                    value = qkv_ref[rank, :, k * LANES:(k + 1) * LANES].astype(F32)
                    gathered += put(q_out, wq_ref, rank * q_own // LANES + k, value)
            for seq in range(2):
                (a0, a1, a2), (b0, b1, b2) = [
                    [qkv_ref[2 * seq + core, :, q_own + k * LANES:q_own + (k + 1) * LANES].astype(F32) for k in range(3)]
                    for core in range(2)
                ]
                keys = [a0, join(a1, rolled(b0)), join(rolled(b0), rolled(b1))]
                values = [join(rolled(a1), rolled(a2)), join(rolled(a2), b1), b2]
                for k in range(3):
                    gathered += put(k_out, wk_ref, 3 * seq + k, keys[k])
                    gathered += put(v_out, wv_ref, 3 * seq + k, values[k])
            ga_out[...] = as_row(gathered)

        bo_out[...] = bo_ref[...]
        gx_out[...] = gx_ref[...]
        dn_out[...] = dn_ref[...].astype(F32)
        gain = columns[1]
        gathered = jnp.zeros((depth, LANES), F32)
        for ref, out, weight in ((gate_ref, gate_out, wg_ref), (up_ref, up_out, wu_ref)):
            for core in range(2):
                for seq in range(2):
                    lanes = slice((2 * core + seq) * block, (2 * core + seq + 1) * block)
                    value = ref[0, 2 * seq + core].astype(F32)
                    out[:, lanes] = value * gain
                    gathered += value * weight[:, lanes].astype(F32)
        total[...] += gathered

        @pl.when(step == steps - 1)
        def _():
            gm_out[...] = as_row(total[...])

    whole = lambda ref: pl.BlockSpec(ref.shape, lambda p: (0,) * len(ref.shape))
    strip = lambda ref: pl.BlockSpec((ref.shape[0] // steps, ref.shape[1]), lambda p: (p, 0))
    part = lambda first: pl.BlockSpec((1, 4, depth, block), lambda p: (p // planes, 0, 0, first + p % planes))
    slab = pl.BlockSpec((depth, wide), lambda p: (0, p))
    outs = [shape(block_out.shape), shape(grad_tokens.shape), shape(w_query.shape, F32), shape(w_key.shape, F32),
            shape(w_value.shape, F32), shape(own_out.shape, F32), shape(w_gate.shape, F32), shape(w_up.shape, F32),
            shape(own_dn.shape, F32), shape((1, depth), F32), shape((1, depth), F32)]
    return pl.pallas_call(
        kernel,
        grid=(steps,),
        out_shape=outs,
        in_specs=[strip(block_out), strip(grad_tokens), whole(own_qkv), whole(own_out), part(0), part(planes),
                  strip(own_dn), whole(w_query), whole(w_key), whole(w_value), slab, slab, whole(gains[0]), whole(gains[1])],
        out_specs=[strip(outs[0]), strip(outs[1])] + [whole(o) for o in outs[2:6]]
        + [slab, slab, strip(outs[8]), whole(outs[9]), whole(outs[10])],
        scratch_shapes=[pltpu.VMEM((2, depth, LANES), F32), pltpu.VMEM((depth, LANES), F32)],
        name="finish",
    )(block_out, grad_tokens, own_qkv, own_out, own_gu, own_gu, own_dn, w_query, w_key, w_value, w_gate, w_up, *gains)


def shards_fast(tokens, cotangent, w_query, w_key, w_value, w_out, w_gate, w_up, w_down, gain_attn, gain_mlp):
    seqs, length, width = tokens.shape
    rows = seqs * length
    depth = w_query.shape[0]
    planes = width // depth // 4
    x, cot = tokens.reshape(rows, width), cotangent.reshape(rows, width)
    gains = (gain_attn.reshape(1, depth), gain_mlp.reshape(1, depth))
    parts = block_step(planes, length, x, cot, w_query, w_key, w_value, w_out, w_gate, w_up, w_down, *gains)
    outs = finish(planes, parts, (w_query, w_key, w_value, w_gate, w_up), gains)
    return (
        outs[0].reshape(tokens.shape), outs[1].reshape(tokens.shape), *outs[2:9],
        outs[9].reshape(depth), outs[10].reshape(depth),
    )


def fits(mesh):
    return mesh.shape["seq"] == 2 and mesh.shape["dp"] == 16


def solution(mesh):
    body = shards_fast if fits(mesh) else shards_plain
    return jax.shard_map(body, mesh=mesh, in_specs=IN_SPECS, out_specs=OUT_SPECS, check_vma=False)
```

```python
import jax
import jax.numpy as jnp
import functools
import numpy as np
from jax import lax
from jax.experimental import pallas as pl
from jax.experimental.pallas import tpu as pltpu
from jax.sharding import PartitionSpec as P

HD = 96
EPS = 1e-05
THETA = 100000.0


def rotary(positions, width):
    steps_half = jnp.arange(width // 2, dtype=jnp.float32)
    frequency = jnp.power(THETA, -2.0 * steps_half / width)
    angles = positions[:, None] * frequency[None, :]
    cosine = jnp.cos(angles)
    sine = jnp.sin(angles)
    return (jnp.concatenate([cosine, cosine], -1), jnp.concatenate([sine, sine], -1))


def rotate(values, cosine, sine):
    half = values.shape[-1] // 2
    turned = jnp.concatenate([-values[..., half:], values[..., :half]], -1)
    return values * cosine[:, None, :] + turned * sine[:, None, :]


def rotate_back(grads, cosine, sine):
    half = grads.shape[-1] // 2
    sined = grads * sine[:, None, :]
    turned = jnp.concatenate([sined[..., half:], -sined[..., :half]], -1)
    return grads * cosine[:, None, :] + turned


def dot32(left, right):
    return jnp.dot(left, right, preferred_element_type=jnp.float32)


def dot_t(left, right):
    return lax.dot_general(left, right, (((1,), (1,)), ((), ())), preferred_element_type=jnp.float32)


def dot_l(left, right):
    return lax.dot_general(left, right, (((0,), (0,)), ((), ())), preferred_element_type=jnp.float32)


def inv_rms(values):
    return lax.rsqrt(jnp.mean(values * values, axis=-1, keepdims=True) + EPS)


def low(values):
    return values.astype(jnp.bfloat16)


def attend(queries, keys, values):
    rows = queries.shape[1]
    ids = jnp.arange(rows, dtype=jnp.int32)
    visible = ids[:, None] >= ids[None, :]
    scores = HD ** (-0.5) * jnp.einsum("bqkgd,bckd->bkgqc", queries, keys, preferred_element_type=jnp.float32)
    scores = jnp.where(visible, scores, -jnp.inf)
    top = jnp.max(scores, -1, keepdims=True)
    exps = jnp.exp(scores - top)
    probs = exps / jnp.sum(exps, -1, keepdims=True)
    mixed = jnp.einsum("bkgqc,bckd->bqkgd", low(probs), values, preferred_element_type=jnp.float32)
    return probs, low(mixed)


def attend_back(queries, keys, values, probs, grad_mixed):
    grad_values = jnp.einsum("bkgqc,bqkgd->bckd", low(probs), grad_mixed, preferred_element_type=jnp.float32)
    grad_probs = jnp.einsum("bqkgd,bckd->bkgqc", grad_mixed, values, preferred_element_type=jnp.float32)
    grad_scores = low(probs * (grad_probs - jnp.sum(probs * grad_probs, -1, keepdims=True)))
    scale = HD ** (-0.5)
    grad_queries = scale * jnp.einsum("bkgqc,bckd->bqkgd", grad_scores, keys, preferred_element_type=jnp.float32)
    grad_keys = scale * jnp.einsum("bkgqc,bqkgd->bckd", grad_scores, queries, preferred_element_type=jnp.float32)
    return grad_queries, grad_keys, grad_values


def mlp_grads(gate, up, grad_hidden):
    sigma = jax.nn.sigmoid(gate)
    silu = gate * sigma
    hidden = low(silu * up)
    grad_gate = low(grad_hidden * up * sigma * (1.0 + gate * (1.0 - sigma)))
    grad_up = low(grad_hidden * silu)
    return hidden, grad_gate, grad_up


def shards_plain(tokens, cotangent, w_query, w_key, w_value, w_out, w_gate, w_up, w_down, gain_attn, gain_mlp):
    seqs, length, width = tokens.shape
    rows = seqs * length
    kv_heads = w_key.shape[1] // HD
    groups = w_query.shape[1] // w_key.shape[1]
    gather = lambda w: lax.all_gather(w, "dp", axis=0, tiled=True)
    full_query, full_key, full_value, full_out = map(gather, (w_query, w_key, w_value, w_out))
    gains = gather(jnp.stack([gain_attn, gain_mlp], 1)).astype(jnp.float32)
    gain_one, gain_two = gains[:, 0], gains[:, 1]
    full_gate, full_up, full_down = map(gather, (w_gate, w_up, w_down))
    cosine, sine = rotary(jnp.arange(length, dtype=jnp.float32), HD)
    cosine, sine = jnp.tile(cosine, (seqs, 1)), jnp.tile(sine, (seqs, 1))

    inputs = tokens.reshape(rows, width).astype(jnp.float32)
    grad_in = cotangent.reshape(rows, width)
    scale_one = inv_rms(inputs)
    normed = low(inputs * scale_one * gain_one)
    queries = low(rotate(dot32(normed, full_query).reshape(rows, -1, HD), cosine, sine))
    keys = low(rotate(dot32(normed, full_key).reshape(rows, -1, HD), cosine, sine))
    values = low(dot32(normed, full_value))
    queries = queries.reshape(seqs, length, kv_heads, groups, HD)
    keys = keys.reshape(seqs, length, kv_heads, HD)
    values = values.reshape(seqs, length, kv_heads, HD)
    probs, mixed = attend(queries, keys, values)
    mixed = mixed.reshape(rows, -1)
    hidden_one = inputs + dot32(mixed, full_out)
    scale_two = inv_rms(hidden_one)
    normed_two = low(hidden_one * scale_two * gain_two)
    gate, up = dot32(normed_two, full_gate), dot32(normed_two, full_up)
    hidden, grad_gate, grad_up = mlp_grads(gate, up, dot_t(grad_in, full_down))
    block_out = low(hidden_one + dot32(hidden, full_down))

    acc_down = dot_l(hidden, grad_in)
    acc_gate = dot_l(normed_two, grad_gate)
    acc_up = dot_l(normed_two, grad_up)
    grad_normed_two = dot_t(grad_gate, full_gate) + dot_t(grad_up, full_up)
    acc_gain_two = jnp.sum(grad_normed_two * hidden_one * scale_two, 0)
    weighted = grad_normed_two * gain_two
    grad_one = grad_in.astype(jnp.float32) + scale_two * (
        weighted - hidden_one * scale_two * scale_two * jnp.mean(weighted * hidden_one, -1, keepdims=True)
    )
    grad_branch = low(grad_one)
    acc_out = dot_l(mixed, grad_branch)
    grad_mixed = low(dot_t(grad_branch, full_out)).reshape(queries.shape)
    grad_queries, grad_keys, grad_values = attend_back(queries, keys, values, probs, grad_mixed)
    grad_queries = low(rotate_back(grad_queries.reshape(rows, -1, HD), cosine, sine)).reshape(rows, -1)
    grad_keys = low(rotate_back(grad_keys.reshape(rows, -1, HD), cosine, sine)).reshape(rows, -1)
    grad_values = low(grad_values).reshape(rows, -1)
    acc_query = dot_l(normed, grad_queries)
    acc_key = dot_l(normed, grad_keys)
    acc_value = dot_l(normed, grad_values)
    grad_normed = dot_t(grad_queries, full_query) + dot_t(grad_keys, full_key) + dot_t(grad_values, full_value)
    acc_gain_one = jnp.sum(grad_normed * inputs * scale_one, 0)
    weighted = grad_normed * gain_one
    grad_tokens = grad_one + scale_one * (
        weighted - inputs * scale_one * scale_one * jnp.mean(weighted * inputs, -1, keepdims=True)
    )

    def share(acc):
        owned = lax.psum_scatter(low(acc), "dp", scatter_dimension=0, tiled=True)
        return lax.psum(owned, "seq").astype(jnp.float32)

    grads = [share(a) for a in (acc_down, acc_gate, acc_up, acc_out, acc_query, acc_key, acc_value)]
    gain_grads = lax.psum(
        lax.psum_scatter(jnp.stack([acc_gain_one, acc_gain_two], 1), "dp", scatter_dimension=0, tiled=True), "seq"
    )
    down, gate, up, out, query, key, value = grads
    return (
        block_out.reshape(tokens.shape),
        low(grad_tokens).reshape(tokens.shape),
        query, key, value, out, gate, up, down,
        gain_grads[:, 0], gain_grads[:, 1],
    )


ROWS = P(("dp", "seq"), None, None)
SPLIT = P("dp", None)
IN_SPECS = (ROWS, ROWS) + (SPLIT,) * 7 + (P("dp"), P("dp"))
OUT_SPECS = (ROWS, ROWS) + (SPLIT,) * 7 + (P("dp"), P("dp"))


MESH = pl.DeviceIdType.MESH
VMEM = pl.BlockSpec(memory_space=pltpu.VMEM)
ANY = pl.BlockSpec(memory_space=pl.ANY)
BF = jnp.bfloat16
F32 = jnp.float32
STRIP = 16
PIECES = 4
VMEM_BYTES = 67_043_328


class Place:
    def __init__(self, planes):
        self.planes = planes
        d = lax.axis_index("dp")
        self.d, self.s = d, lax.axis_index("seq")
        self.c, self.y, self.z = d % 2, (d // 2) % 2, d // 4
        self.p = d // 2
        self.rank = 2 * self.s + self.c
        self.core = (d + 1 - 2 * self.c, self.s)
        self.across = (d, 1 - self.s)
        self.corner = (d + 1 - 2 * self.c, 1 - self.s)
        self.side = (d + 2 - 4 * self.y, self.s)
        self.right = (lax.rem(d + 4, 4 * planes), self.s)
        self.left = (lax.rem(d + 4 * planes - 4, 4 * planes), self.s)
        self.has_right, self.has_left = self.z < planes - 1, self.z > 0
        odd = self.z % 2
        self.twin = self.z + 1 - 2 * odd
        self.buddy = (d + 4 - 8 * odd, self.s)


def greet(me):
    barrier = pltpu.get_barrier_semaphore()
    for peer in (me.core, me.across, me.corner, me.side, me.right, me.left):
        pl.semaphore_signal(barrier, inc=1, device_id=peer, device_id_type=MESH)
    pl.semaphore_wait(barrier, 6)


def push(src, dst, send, recv, peer):
    return pltpu.make_async_remote_copy(
        src_ref=src, dst_ref=dst, send_sem=send, recv_sem=recv, device_id=peer, device_id_type=MESH
    )


def arrived(dst, recv, peer):
    push(dst, dst, recv, recv, peer).wait_recv()


def left_over(src, send, peer):
    push(src, src, send, send, peer).wait_send()


class Slots:
    def __init__(self, ref, rows):
        self.ref, self.rows = ref, rows
        self.at = self

    def __getitem__(self, block):
        return self.ref.at[pl.ds(pl.multiple_of(block * self.rows, self.rows), self.rows)]


def group_start(me, src, dst, send, recv):
    push(src, dst.at[me.rank], send.at[0], recv.at[0], me.core).start()
    push(src, dst.at[me.rank], send.at[1], recv.at[1], me.across).start()


def group_relay(me, dst, send, recv):
    slot = dst.at[2 * (1 - me.s) + me.c]
    arrived(slot, recv.at[1], me.across)
    push(slot, slot, send.at[2], recv.at[2], me.core).start()


def group_finish(me, src, dst, send, recv):
    arrived(dst.at[2 * me.s + 1 - me.c], recv.at[0], me.core)
    arrived(dst.at[2 * (1 - me.s) + 1 - me.c], recv.at[2], me.core)
    left_over(src, send.at[0], me.core)
    left_over(src, send.at[1], me.across)
    slot = dst.at[2 * (1 - me.s) + me.c]
    left_over(slot, send.at[2], me.core)


def group_sems():
    return [pltpu.SemaphoreType.DMA((3,)), pltpu.SemaphoreType.DMA((3,))]


def upper(slot):
    return slot.at[pl.ds(0, slot.shape[0] // 2)]


def lower(slot):
    return slot.at[pl.ds(slot.shape[0] // 2, slot.shape[0] // 2)]


def line_start(me, dst, sems):
    line_side(me, dst, sems)
    line_ends(me, dst, sems)


def line_side(me, dst, sems):
    to_right, to_left, line, to_side, side, twin = sems
    slot = dst(me.p)
    push(slot, slot, to_side.at[me.z], side.at[me.z], me.side).start()


def line_ends(me, dst, sems):
    to_right, to_left, line, to_side, side, twin = sems
    slot = dst(me.p)

    @pl.when(me.has_right)
    def _():
        push(slot, slot, to_right.at[me.z], line.at[me.z], me.right).start()

    @pl.when(me.has_left)
    def _():
        push(slot, slot, to_left.at[me.z], line.at[me.z], me.left).start()


def line_hop(me, dst, sems, hop):
    to_right, to_left, line, to_side, side, twin = sems

    def pass_on(item, back, forth, may, sends):
        slot = dst(2 * item + me.y)
        arrived(slot, line.at[item], back)

        @pl.when(may)
        def _():
            push(slot, slot, sends.at[item], line.at[item], forth).start()

        if hop > 1:
            push(slot, slot, to_side.at[item], side.at[item], me.side).start()
        else:

            @pl.when(item != me.twin)
            def _():
                push(slot, slot, to_side.at[item], side.at[item], me.side).start()

            @pl.when(item == me.twin)
            def _():
                half = upper(slot)
                push(half, half, to_side.at[item], side.at[item], me.side).start()

    @pl.when(me.z >= hop)
    def _():
        pass_on(me.z - hop, me.left, me.right, me.has_right, to_right)

    @pl.when(me.z + hop < me.planes)
    def _():
        pass_on(me.z + hop, me.right, me.left, me.has_left, to_left)


def line_twin(me, dst, sems):
    to_right, to_left, line, to_side, side, twin = sems
    slot = dst(2 * me.z + 1 - me.y)
    arrived(slot, side.at[me.z], me.side)
    half = lower(slot)
    push(half, half, twin.at[0], twin.at[1], me.buddy).start()


def line_finish(me, dst, sems):
    to_right, to_left, line, to_side, side, twin = sems
    for item in range(me.planes):
        slot, mine = dst(2 * item + 1 - me.y), dst(2 * item + me.y)

        @pl.when(item == me.twin)
        def _():
            arrived(upper(slot), side.at[item], me.side)
            arrived(lower(slot), twin.at[1], me.buddy)
            left_over(upper(mine), to_side.at[item], me.side)

        @pl.when(jnp.logical_and(item != me.twin, item != me.z))
        def _():
            arrived(slot, side.at[item], me.side)

        @pl.when(item != me.twin)
        def _():
            left_over(mine, to_side.at[item], me.side)

        @pl.when(item == me.z)
        def _():
            left_over(lower(slot), twin.at[0], me.buddy)

        @pl.when(jnp.logical_and(me.has_right, item <= me.z))
        def _():
            left_over(mine, to_right.at[item], me.right)

        @pl.when(jnp.logical_and(me.has_left, item >= me.z))
        def _():
            left_over(mine, to_left.at[item], me.left)


def line_sems(planes):
    return [pltpu.SemaphoreType.DMA((planes,))] * 5 + [pltpu.SemaphoreType.DMA((2,))]


def pick(table, index):
    value = jnp.int32(table[0])
    for i in range(1, len(table)):
        value = jnp.where(index == i, table[i], value)
    return value


def far_first(planes):
    return [sorted(range(planes), key=lambda i, z=z: (-abs(i - z), i)) for z in range(planes)]


def add_into(dst, *others):
    rows = dst.shape[0]

    def body(i, carry):
        strip = pl.ds(pl.multiple_of(i * STRIP, STRIP), STRIP)
        total = dst[strip, :].astype(F32)
        for other in others:
            total = total + other[strip, :].astype(F32)
        dst[strip, :] = total.astype(dst.dtype)
        return carry

    lax.fori_loop(0, rows // STRIP, body, 0)


def reduce_start(me, own, half, sems, which):
    to_side, side, twin = sems[0], sems[1], sems[6]
    orders = far_first(me.planes)
    if 0 in which:
        away = lower(own(2 * me.twin + 1 - me.y))
        push(away, lower(half.at[me.z]), twin.at[0], twin.at[1], me.buddy).start()
    for i in which:
        item = pick([o[i] for o in orders], me.z)
        src, dst = own(2 * item + 1 - me.y), half.at[item]

        @pl.when(item == me.twin)
        def _():
            push(upper(src), upper(dst), to_side.at[item], side.at[item], me.side).start()

        @pl.when(jnp.logical_and(item != me.twin, item != me.z))
        def _():
            push(src, dst, to_side.at[item], side.at[item], me.side).start()


def reduce_mix(me, own, half, sems):
    to_side, side, twin = sems[0], sems[1], sems[6]
    mixed, got = own(2 * me.z + 1 - me.y), lower(half.at[me.twin])
    arrived(got, twin.at[1], me.buddy)
    add_into(lower(mixed), got)
    push(mixed, half.at[me.z], to_side.at[me.z], side.at[me.z], me.side).start()


def reduce_y(me, own, half, lines, sems, i):
    to_side, side, to_right, to_left, left, right, twin = sems
    item = pick([o[i] for o in far_first(me.planes)], me.z)
    mine, ours = half.at[item], own(2 * item + me.y)

    @pl.when(item == me.twin)
    def _():
        arrived(upper(mine), side.at[item], me.side)
        add_into(upper(mine), upper(ours))
        copy_into(lower(mine), lower(ours))

    @pl.when(item != me.twin)
    def _():
        arrived(mine, side.at[item], me.side)
        add_into(mine, ours)

    @pl.when(jnp.logical_and(item > me.z, jnp.logical_not(me.has_left)))
    def _():
        push(mine, lines.at[item], to_right.at[item], left.at[item], me.right).start()

    @pl.when(jnp.logical_and(item < me.z, jnp.logical_not(me.has_right)))
    def _():
        there = jnp.where(item == me.z - 1, me.planes, item)
        push(mine, lines.at[there], to_left.at[item], right.at[item], me.left).start()


def reduce_z(me, half, lines, sems, i):
    to_side, side, to_right, to_left, left, right, twin = sems
    item = pick([o[i] for o in far_first(me.planes)], me.z)
    mine = half.at[item]
    spot = jnp.where(item == me.z, me.planes, item)

    @pl.when(jnp.logical_and(me.has_left, item >= me.z))
    def _():
        arrived(lines.at[item], left.at[item], me.left)
        add_into(mine, lines.at[item])

        @pl.when(item > me.z)
        def _():
            push(mine, lines.at[item], to_right.at[item], left.at[item], me.right).start()

    @pl.when(jnp.logical_and(me.has_right, item <= me.z))
    def _():
        arrived(lines.at[spot], right.at[item], me.right)
        add_into(mine, lines.at[spot])

        @pl.when(item < me.z)
        def _():
            there = jnp.where(item == me.z - 1, me.planes, item)
            push(mine, lines.at[there], to_left.at[item], right.at[item], me.left).start()


def reduce_finish(me, own, half, sems):
    to_side, side, to_right, to_left, left, right, twin = sems
    left_over(lower(own(2 * me.twin + 1 - me.y)), twin.at[0], me.buddy)
    for item in range(me.planes):
        sent = own(2 * item + 1 - me.y)

        @pl.when(item == me.twin)
        def _():
            left_over(upper(sent), to_side.at[item], me.side)

        @pl.when(item != me.twin)
        def _():
            left_over(sent, to_side.at[item], me.side)

        @pl.when(item > me.z)
        def _():
            left_over(half.at[item], to_right.at[item], me.right)

        @pl.when(item < me.z)
        def _():
            left_over(half.at[item], to_left.at[item], me.left)


def reduce_sems(planes):
    return [pltpu.SemaphoreType.DMA((planes,))] * 6 + [pltpu.SemaphoreType.DMA((2,))]


def copy_into(dst, src):
    def body(i, carry):
        strip = pl.ds(pl.multiple_of(i * STRIP, STRIP), STRIP)
        dst[strip, :] = src[strip, :]
        return carry

    lax.fori_loop(0, dst.shape[0] // STRIP, body, 0)


def reduce_buffers(planes, rows, columns):
    return [pltpu.VMEM((planes, rows, columns), BF), pltpu.VMEM((planes + 1, rows, columns), BF)]


def by_chip(ref, rows=None):
    if rows is None:
        return lambda chip: ref.at[chip]
    return lambda chip: ref.at[pl.ds(pl.multiple_of(chip * rows, STRIP), rows)]


def deal_start(me, final, rows, out, local, send, recv):
    mine = out.at[me.rank]
    part = lambda core: final.at[pl.ds(pl.multiple_of(core * rows, rows), rows)]
    pltpu.make_async_copy(part(me.c), mine, local).start()
    push(part(1 - me.c), mine, send.at[0], recv.at[0], me.core).start()
    push(part(me.c), mine, send.at[1], recv.at[1], me.across).start()
    push(part(1 - me.c), mine, send.at[2], recv.at[2], me.corner).start()


def deal_finish(me, final, rows, out, local, send, recv):
    part = lambda core: final.at[pl.ds(pl.multiple_of(core * rows, rows), rows)]
    pltpu.make_async_copy(part(me.c), out.at[me.rank], local).wait()
    left_over(part(1 - me.c), send.at[0], me.core)
    left_over(part(me.c), send.at[1], me.across)
    left_over(part(1 - me.c), send.at[2], me.corner)
    arrived(out.at[2 * me.s + 1 - me.c], recv.at[0], me.core)
    arrived(out.at[2 * (1 - me.s) + me.c], recv.at[1], me.across)
    arrived(out.at[2 * (1 - me.s) + 1 - me.c], recv.at[2], me.corner)


def blocks_start(me, part, got, send, recv, i):
    seq = (1 - me.s, me.s)[i]
    push(part.at[2 * seq + 1 - me.c], got.at[seq], send.at[i], recv.at[i], me.core).start()


def blocks_cross(me, part, got, last, send, recv):
    away = 1 - me.s
    arrived(got.at[away], recv.at[0], me.core)
    add_into(got.at[away], part.at[2 * away + me.c])
    push(got.at[away], last, send.at[2], recv.at[2], me.across).start()


def blocks_finish(me, part, got, last, send, recv):
    arrived(got.at[me.s], recv.at[1], me.core)
    arrived(last, recv.at[2], me.across)
    for i, seq in enumerate((1 - me.s, me.s)):
        left_over(part.at[2 * seq + 1 - me.c], send.at[i], me.core)
    left_over(got.at[1 - me.s], send.at[2], me.across)


def blocks_sems():
    return [pltpu.SemaphoreType.DMA((3,))] * 2


def blocks_buffers(rows, width):
    return [pltpu.VMEM((2, rows, width), BF), pltpu.VMEM((rows, width), BF)]


def strips(rows, body):
    def step(i, carry):
        body(pl.ds(pl.multiple_of(i * STRIP, STRIP), STRIP))
        return carry

    lax.fori_loop(0, rows // STRIP, step, 0)


def comm_call(kernel, ident, outs, out_specs, ins, scratch, name):
    return pl.pallas_call(
        kernel,
        out_shape=outs,
        in_specs=[spec for spec, _ in ins],
        out_specs=out_specs,
        scratch_shapes=scratch,
        name=name,
        compiler_params=pltpu.CompilerParams(
            collective_id=ident, has_side_effects=True, vmem_limit_bytes=VMEM_BYTES
        ),
    )(*[value for _, value in ins])


def shape(dims, dtype=BF):
    return jax.ShapeDtypeStruct(dims, dtype)


def split_start(me, parts, dst, keep, send, recv):
    pltpu.make_async_copy(parts.at[me.c], dst(me.c), keep).start()
    push(parts.at[1 - me.c], dst(me.c), send, recv, me.core).start()


def split_finish(me, parts, dst, keep, send, recv):
    pltpu.make_async_copy(parts.at[me.c], dst(me.c), keep).wait()
    arrived(dst(1 - me.c), recv, me.core)
    left_over(parts.at[1 - me.c], send, me.core)


def norm_back(values, weighted, base):
    scale = inv_rms(values)
    return base + scale * (
        weighted - values * scale * scale * jnp.mean(weighted * values, -1, keepdims=True)
    )


LANES = 128


def head_tables(length):
    steps = np.arange(HD // 2, dtype=np.float64)
    angles = np.arange(length, dtype=np.float64)[:, None] * np.power(THETA, -2.0 * steps / HD)[None, :]
    cosine, sine, none = np.cos(angles), np.sin(angles), np.zeros_like(angles)
    tables = [(cosine, cosine), (none, sine), (-sine, none)]
    pad = ((0, 0), (0, LANES - HD))
    return np.stack([np.pad(np.concatenate(t, 1), pad) for t in tables]).astype(np.float32)


def turn(values, tables, sign):
    other = pltpu.roll(values, HD // 2, 1) * tables[1] + pltpu.roll(values, LANES - HD // 2, 1) * tables[2]
    return values * tables[0] + sign * other


SCHEDULE = (
    "De", "Ds", "Q1", "weigh", "Qt", "Q2", "Ae", "D1", "Q3", "rn", "As", "nf", "own", "f0", "f1", "f2", "Qf",
    "widen", "f3", "A1", "D2", "project", "Be", "oh", "t0", "x0", "Bs", "Dt", "t1", "xc", "D3", "t2", "x1",
    "A2", "At", "rg", "t3", "xs", "B1", "A3", "Df", "B2", "Bt", "rm", "mf", "Af", "gf", "u0", "B3", "u1",
    "w0", "ar0", "Bf", "ol", "v0", "v1", "ar1", "b0", "p0", "ay0", "am", "pc", "ay1", "b1", "w1", "br0",
    "ay2", "az0", "p1", "bs", "br1", "fo", "bm", "by0", "dw", "by1", "rx", "dr0", "az1", "xf", "sp", "fc",
    "by2", "bz0", "h0", "go", "h1", "dy0", "az2", "oy0", "k0", "dr1", "h2", "kc", "oy1", "bz1", "oy2", "bz2",
    "h3", "oy3", "qg", "dz0", "ay3", "az3", "by3", "qr0", "dm", "k1", "dy1", "fs", "qr1", "bz3", "be", "oz0",
    "ae", "qy0", "dy2", "oz1", "oz2", "oz3", "dz1", "oe", "qm", "qy1", "dz2", "qz0", "dy3", "qy2", "dz3",
    "de", "qy3", "qz1", "qz2", "qz3", "qe", "hs",
)


def block_step(planes, length, tokens, cot, w_query, w_key, w_value, w_out, w_gate, w_up, w_down, gain_attn, gain_mlp):
    rows, width = tokens.shape
    total = 4 * rows
    depth = w_query.shape[0]
    head = w_out.shape[0]
    q_own, k_own = w_query.shape[1] // 4, w_key.shape[1] // 4
    q_cols = q_own + 2 * k_own
    block = w_down.shape[0] // 2
    units = 2 * planes * block
    half_units = units // 2
    cols = 2 * half_units
    tile, chunk = 2 * rows, 256
    heads4 = 4 * head
    piece = 2 * head // PIECES

    def kernel(x_ref, g_loc, wq_ref, wk_ref, wv_ref, out_loc, gate_ref, up_ref, down_ref, ga_ref, gm_ref, tab_ref,
               bo_ref, gx_ref, qkv_out, out_out, gu_out, dn_out, stash, *scr):
        it = iter(scr)
        take = lambda k: [next(it) for _ in range(k)]
        n_buf, g_all, qkv_all, out_all, gu_all, dn_all, heads, mixed = take(8)
        part, out_part, x1, mid, dgu, g_gu, dx_all = take(7)
        (got, last), (got_f, last_f) = take(2), take(2)
        gu_buf, dn_buf, q_buf, o_buf = [take(2), take(2)], take(2), take(2), take(3)
        n_sems, g_sems, m_sems, d_sems = take(2), take(2), take(2), take(2)
        x_sems, b_sems, f_sems, h_sems = take(2), take(2), take(2), take(2)
        q_split, gu_split = take(3), [take(3), take(3)]
        q_line, gu_line, dn_line = take(6), [take(6), take(6)], take(6)
        gu_sems, dn_sems, q_sems = [take(7), take(7)], take(7), take(7)
        gu_deal, dn_deal, q_deal, o_deal = [take(3), take(3)], take(3), take(3), take(3)
        local, edge, o_fan, o_red, fetch, sel_ref, gains = take(7)
        me = Place(planes)
        greet(me)
        tok = lambda ref: Slots(ref, rows)
        q_slots, dn_slots = by_chip(qkv_all, 2 * depth), by_chip(dn_all, block)
        gu_slots = [by_chip(gu_all.at[h], 2 * depth) for h in range(2)]

        def core_rows(ref):
            return lambda core: ref.at[pl.ds(pl.multiple_of((2 * me.p + core) * depth, STRIP), depth)]

        fetch_x = pltpu.make_async_copy(x_ref, last_f, local.at[4])
        fetch_x.start()
        stage = out_part.at[pl.ds(0, depth)]
        heads_in = []
        for i, (ref, spot, size) in enumerate(
            ((wq_ref, 0, 2 * q_own), (wk_ref, 2 * q_own, 2 * k_own), (wv_ref, 2 * q_own + 2 * k_own, 2 * k_own))
        ):
            src = ref.at[:, pl.ds(pl.multiple_of(me.s * size, LANES), size)]
            heads_in.append(pltpu.make_async_copy(src, stage.at[:, pl.ds(spot, size)], fetch.at[i]))
            heads_in[-1].start()

        q_share = q_buf[0].at[0, pl.ds(0, depth)]
        gu_share = [mid.at[pl.ds(h * depth, depth)] for h in range(2)]
        units_in = []
        for other in range(2):
            core = (me.c, 1 - me.c)[other]
            for h in range(2):
                dst = (core_rows(gu_all.at[h])(me.c), gu_share[h])[other]
                for k in range(2 * planes):
                    ref = (gate_ref, up_ref)[k // planes]
                    chip = h * planes + k % planes
                    first = (2 * chip + core) * 2 * block + me.s * block
                    copy = pltpu.make_async_copy(
                        ref.at[:, pl.ds(pl.multiple_of(first, LANES), block)],
                        dst.at[:, pl.ds(k * block, block)],
                        fetch.at[3 + (other * 2 + h) * 2 * planes + k],
                    )
                    copy.start()
                    units_in.append(copy)
        own_down = down_ref.at[pl.ds(pl.multiple_of(me.s * block, STRIP), block)]
        keep_d = pltpu.make_async_copy(own_down, dn_slots(me.p), local.at[2])
        keep_d.start()
        keep_g = pltpu.make_async_copy(g_loc, tok(g_all).at[me.rank], local.at[3])
        keep_g.start()

        same = lax.broadcasted_iota(jnp.int32, (depth, depth), 0) == lax.broadcasted_iota(jnp.int32, (depth, depth), 1)
        for k, ref in enumerate((ga_ref, gm_ref)):
            column = jnp.sum(jnp.where(same, ref[...].astype(F32), 0.0), 1, keepdims=True)
            gains[k] = jnp.broadcast_to(column, (depth, LANES))
        row = lax.broadcasted_iota(jnp.int32, (heads4, 4 * LANES), 0)
        lane = lax.broadcasted_iota(jnp.int32, (heads4, 4 * LANES), 1)
        shift = sum(jnp.where(row >= k * HD, LANES - HD, 0) for k in range(1, 4))
        sel_ref[...] = jnp.where(lane == row + shift, 1.0, 0.0).astype(BF)

        for copy in heads_in:
            copy.wait()
        gain = gains[0][:, 0:1]
        tiles = lambda first, count: [
            stage[:, first + k * LANES:first + (k + 1) * LANES].astype(F32) * gain for k in range(count)
        ]
        queries = tiles(0, 6)
        k0, k1, k2 = tiles(2 * q_own, 3)
        v0, v1, v2 = tiles(2 * q_own + 2 * k_own, 3)
        rolled = lambda value: pltpu.roll(value, LANES // 2, 1)
        in_low = lax.broadcasted_iota(jnp.int32, (depth, LANES), 1) < LANES // 2
        join = lambda first, second: jnp.where(in_low, first, second)
        shares = (
            queries[:3] + [k0, join(k1, rolled(v0)), join(rolled(v0), rolled(v1))],
            queries[3:] + [join(rolled(k1), rolled(k2)), join(rolled(k2), v1), v2],
        )
        for core in range(2):
            value = low(jnp.concatenate(shares[core], 1))

            @pl.when(me.c == core)
            def _():
                core_rows(qkv_all)(me.c)[...] = value

            @pl.when(me.c != core)
            def _():
                q_share[...] = value

        push(q_share, core_rows(qkv_all)(me.c), q_split[1], q_split[2], me.core).start()
        here = me.s == me.z // 2
        owner = me.z == me.rank
        lender = jnp.logical_and(here, jnp.logical_not(owner))
        half = lambda y: out_all.at[pl.ds(pl.multiple_of(y * 2 * head, STRIP), 2 * head)]
        head_rows = lambda core: out_all.at[pl.ds(pl.multiple_of((2 * me.y + core) * head, STRIP), head)]
        keep_o = pltpu.make_async_copy(out_loc, head_rows(me.c), local.at[1])

        @pl.when(owner)
        def _():
            keep_o.start()

        @pl.when(lender)
        def _():
            push(out_loc, head_rows(me.c), edge.at[0], edge.at[1], me.core).start()

        fetch_x.wait()

        def first_norm(strip):
            value = last_f[strip, :].astype(F32)
            n_buf[pl.ds(pl.multiple_of(me.rank * rows + strip.start, STRIP), STRIP), :] = low(value * inv_rms(value))

        strips(rows, first_norm)
        group_start(me, tok(n_buf).at[me.rank], tok(n_buf), *n_sems)
        arrived(core_rows(qkv_all)(1 - me.c), q_split[2], me.core)
        line_start(me, q_slots, q_line)

        away, home = 1 - me.s, me.s

        def weigh_units():
            for copy in units_in:
                copy.wait()

            def weigh(i, carry):
                strip = pl.ds(pl.multiple_of(i * STRIP, STRIP), STRIP)
                gain = gains[1, strip, 0:1]
                for h in range(2):
                    for ref in (core_rows(gu_all.at[h])(me.c), gu_share[h]):
                        ref[strip, :] = low(ref[strip, :].astype(F32) * gain)
                return carry

            lax.fori_loop(0, depth // STRIP, weigh, 0)
            for h in range(2):
                push(gu_share[h], core_rows(gu_all.at[h])(me.c), gu_split[h][1], gu_split[h][2], me.core).start()
            group_start(me, g_loc, tok(g_all), *g_sems)

        fan_in, fan_right, fan_left, fan_side, fan_other = [o_fan.at[k] for k in range(5)]
        bit = lambda y, q: out_all.at[pl.ds(pl.multiple_of(y * 2 * head + q * piece, STRIP), piece)]
        go_right = jnp.logical_and(me.z >= me.rank, me.has_right)
        go_left = jnp.logical_and(me.z <= me.rank, me.has_left)

        def fan(q):
            mine = bit(me.y, q)

            @pl.when(me.z > me.rank)
            def _():
                arrived(mine, fan_in.at[q], me.left)

            @pl.when(me.z < me.rank)
            def _():
                arrived(mine, fan_in.at[q], me.right)

            @pl.when(go_right)
            def _():
                push(mine, mine, fan_right.at[q], fan_in.at[q], me.right).start()

            @pl.when(go_left)
            def _():
                push(mine, mine, fan_left.at[q], fan_in.at[q], me.left).start()

            push(mine, mine, fan_side.at[q], fan_other.at[q], me.side).start()

        def own_heads():
            @pl.when(owner)
            def _():
                keep_o.wait()
                arrived(head_rows(1 - me.c), edge.at[1], me.core)

            @pl.when(lender)
            def _():
                left_over(out_loc, edge.at[0], me.core)

        def ends(h):
            arrived(core_rows(gu_all.at[h])(1 - me.c), gu_split[h][2], me.core)
            line_ends(me, gu_slots[h], gu_line[h])

        def dn_ends():
            keep_d.wait()
            line_ends(me, dn_slots, dn_line)

        saved = pltpu.make_async_copy(n_buf, stash, local.at[0])
        fetch_n = pltpu.make_async_copy(stash, n_buf, local.at[0])

        def normed_here():
            group_finish(me, tok(n_buf).at[me.rank], tok(n_buf), *n_sems)
            left_over(q_share, q_split[1], me.core)
            for h in range(2):
                left_over(gu_share[h], gu_split[h][1], me.core)
            saved.start()

        def widen_weights():
            def widen(i, carry):
                feats = pl.ds(pl.multiple_of(i * tile, tile), tile)
                for k in range(2):
                    g_gu[feats, k * 4 * LANES:(k + 1) * 4 * LANES] = low(
                        dot32(qkv_all[feats, k * heads4:(k + 1) * heads4], sel_ref[...])
                    )
                return carry

            lax.fori_loop(0, width // tile, widen, 0)

        def project_tokens():
            def project(i, carry):
                toks = pl.ds(pl.multiple_of(i * length, length), length)
                n = n_buf[toks, :]
                tabs = [tab_ref[k] for k in range(3)]
                for k in range(8):
                    value = dot32(n, g_gu[:, k * LANES:(k + 1) * LANES])
                    heads[toks, k * LANES:(k + 1) * LANES] = low(turn(value, tabs, 1.0) if k < 6 else value)
                return carry

            lax.fori_loop(0, total // length, project, 0)

        def heads_here():
            saved.wait()
            for q in range(PIECES):
                arrived(bit(1 - me.y, q), fan_other.at[q], me.side)

        def pair(toks, j, ref, start):
            first = start + 2 * j * LANES
            return jnp.concatenate(
                [ref[toks, first:first + LANES], ref[toks, first + LANES:first + 2 * LANES]], 0
            )

        def probabilities(toks, j):
            q = pair(toks, j, heads, 0)
            k = heads[toks, (4 + j) * LANES:(5 + j) * LANES]
            scores = HD ** (-0.5) * dot_t(q, k)
            row = lax.rem(lax.broadcasted_iota(jnp.int32, scores.shape, 0), length)
            col = lax.broadcasted_iota(jnp.int32, scores.shape, 1)
            scores = jnp.where(row >= col, scores, -jnp.inf)
            exps = jnp.exp(scores - jnp.max(scores, 1, keepdims=True))
            return q, k, exps / jnp.sum(exps, 1, keepdims=True)

        def attend_rows(first):
            def one(i, carry):
                toks = pl.ds(pl.multiple_of(first + i * length, length), length)
                outs = []
                for j in range(2):
                    _, _, p = probabilities(toks, j)
                    o = low(dot32(low(p), heads[toks, (6 + j) * LANES:(7 + j) * LANES]))
                    outs += [o[:length], o[length:]]
                mixed[toks, :] = low(dot_t(jnp.concatenate(outs, 1), sel_ref[...]))
                return carry

            lax.fori_loop(0, rows // length, one, 0)
            toks = pl.ds(pl.multiple_of(first, rows), rows)
            part[toks, :] = low(dot32(mixed[toks, :], out_all[...]))

        def mine(strip):
            return pl.ds(pl.multiple_of(me.rank * rows + strip.start, STRIP), STRIP)

        def summed(strip, whole, some, rest):
            return (
                whole[mine(strip), :].astype(F32)
                + some[me.s, strip, :].astype(F32)
                + rest[strip, :].astype(F32)
            )

        def middle(strip):
            value = last_f[strip, :].astype(F32) + summed(strip, part, got, last)
            x1[strip, :] = value
            n_buf[mine(strip), :] = low(value * inv_rms(value))

        def first_sum():
            blocks_finish(me, tok(part), got, last, *x_sems)
            strips(rows, middle)
            group_start(me, tok(n_buf).at[me.rank], tok(n_buf), *m_sems)

        def cot_here():
            keep_g.wait()
            group_finish(me, g_loc, tok(g_all), *g_sems)

        def heads_left():
            for q in range(PIECES):
                left_over(bit(me.y, q), fan_side.at[q], me.side)

                @pl.when(go_right)
                def _():
                    left_over(bit(me.y, q), fan_right.at[q], me.right)

                @pl.when(go_left)
                def _():
                    left_over(bit(me.y, q), fan_left.at[q], me.left)

        def activations(h, j):
            first = h * half_units + j * chunk

            def step(t, carry):
                toks = pl.ds(pl.multiple_of(t * tile, tile), tile)
                n, g = n_buf[toks, :], g_all[toks, :]
                gate = dot32(n, gu_all[h, :, j * chunk:(j + 1) * chunk])
                up = dot32(n, gu_all[h, :, half_units + j * chunk:half_units + (j + 1) * chunk])
                grad = dot_t(g, dn_all[first:first + chunk, :])
                hidden, d_gate, d_up = mlp_grads(gate, up, grad)
                mid[toks, first:first + chunk] = hidden
                dgu[h, toks, j * chunk:(j + 1) * chunk] = d_gate
                dgu[h, toks, half_units + j * chunk:half_units + (j + 1) * chunk] = d_up
                return carry

            lax.fori_loop(0, total // tile, step, 0)

        def weight_grads(h, out):
            def step(i, carry):
                feats = pl.ds(pl.multiple_of(i * chunk, chunk), chunk)
                out[feats, :] = low(dot_l(n_buf[:, feats], dgu[h]))
                return carry

            lax.fori_loop(0, width // chunk, step, 0)

        own_gu = [by_chip(g_gu, 2 * depth), gu_slots[0]]
        finals = [gu_buf[h][0].at[me.z] for h in range(2)]

        def back(seq):
            toks = pl.ds(pl.multiple_of(seq * tile, tile), tile)

            def step(i, carry):
                feats = pl.ds(pl.multiple_of(i * chunk, chunk), chunk)
                value = dot_t(dgu[0, toks, :], gu_all[0, feats, :]) + dot_t(dgu[1, toks, :], gu_all[1, feats, :])
                part[toks, feats] = low(value)
                return carry

            lax.fori_loop(0, width // chunk, step, 0)

        def second_grads():
            weight_grads(1, gu_all.at[0])
            fetch_n.start()

        def outward():
            def forth(i, carry):
                feats = pl.ds(pl.multiple_of(i * chunk, chunk), chunk)
                out_part[:, feats] = low(dot32(mid[...], dn_all[:, feats]))
                return carry

            lax.fori_loop(0, width // chunk, forth, 0)
            for i in range(2):
                blocks_start(me, tok(out_part), got_f, *f_sems, i)

        def branch(strip):
            grad = norm_back(x1[strip, :], summed(strip, part, got, last), g_all[mine(strip), :].astype(F32))
            dx_all[mine(strip), :] = low(grad)

        def second_sum():
            blocks_finish(me, tok(part), got, last, *b_sems)
            strips(rows, branch)
            group_start(me, tok(dx_all).at[me.rank], tok(dx_all), *d_sems)

        def down_grads():
            def down(i, carry):
                these = pl.ds(pl.multiple_of(i * chunk, chunk), chunk)
                dn_all[these, :] = low(dot_l(mid[:, these], g_all[...]))
                return carry

            lax.fori_loop(0, units // chunk, down, 0)

        def spread_grads():
            def spread_out(t, carry):
                toks = pl.ds(pl.multiple_of(t * rows, rows), rows)
                grad = low(dot_t(dx_all[toks, :], out_all[...]))
                mid[toks, 0:4 * LANES] = low(dot32(grad, sel_ref[...]))
                return carry

            lax.fori_loop(0, 4, spread_out, 0)

        def out_grads():
            out_all[...] = low(dot_l(mixed[...], dx_all[...]))
            for q in range(PIECES):
                push(bit(1 - me.y, q), o_buf[0].at[pl.ds(q * piece, piece)], o_red.at[0, q], o_red.at[1, q], me.side).start()

        def attend_rows_back(first):
            def one(i, carry):
                toks = pl.ds(pl.multiple_of(first + i * length, length), length)
                tabs = [tab_ref[k] for k in range(3)]
                for j in range(2):
                    q, k, p = probabilities(toks, j)
                    v = heads[toks, (6 + j) * LANES:(7 + j) * LANES]
                    grad = pair(toks, j, mid, 0)
                    d_v = dot_l(low(p), grad)
                    d_p = dot_t(grad, v)
                    d_s = low(p * (d_p - jnp.sum(p * d_p, 1, keepdims=True)))
                    d_q = HD ** (-0.5) * dot32(d_s, k)
                    d_k = HD ** (-0.5) * dot_l(d_s, q)
                    for g in range(2):
                        spot = (2 * j + g) * LANES
                        dgu[0, toks, spot:spot + LANES] = low(turn(d_q[g * length:(g + 1) * length], tabs, -1.0))
                    dgu[0, toks, (4 + j) * LANES:(5 + j) * LANES] = low(turn(d_k, tabs, -1.0))
                    dgu[0, toks, (6 + j) * LANES:(7 + j) * LANES] = low(d_v)
                return carry

            lax.fori_loop(0, rows // length, one, 0)
            toks = pl.ds(pl.multiple_of(first, rows), rows)
            for k in range(2):
                dgu[1, toks, k * heads4:(k + 1) * heads4] = low(
                    dot_t(dgu[0, toks, k * 4 * LANES:(k + 1) * 4 * LANES], sel_ref[...])
                )
            part[toks, :] = low(dot_t(dgu[1, toks, 0:q_cols], qkv_all[...]))

        def in_grads():
            fetch_n.wait()

            def q_grads(i, carry):
                feats = pl.ds(pl.multiple_of(i * chunk, chunk), chunk)
                qkv_all[feats, :] = low(dot_l(n_buf[:, feats], dgu[1, :, 0:q_cols]))
                return carry

            lax.fori_loop(0, width // chunk, q_grads, 0)

        o_sum = lambda q: o_buf[0].at[pl.ds(q * piece, piece)]
        o_left = lambda q: o_buf[1].at[pl.ds(q * piece, piece)]
        o_right = lambda q: o_buf[2].at[pl.ds(q * piece, piece)]

        def o_on(q):
            @pl.when(me.z < me.rank)
            def _():
                push(o_sum(q), o_left(q), o_red.at[4, q], o_red.at[2, q], me.right).start()

            @pl.when(me.z > me.rank)
            def _():
                push(o_sum(q), o_right(q), o_red.at[4, q], o_red.at[3, q], me.left).start()

        from_left = jnp.logical_and(me.has_left, me.z <= me.rank)
        from_right = jnp.logical_and(me.has_right, me.z >= me.rank)
        no_more = jnp.logical_not(jnp.logical_or(from_left, from_right))

        def o_y(q):
            arrived(o_sum(q), o_red.at[1, q], me.side)
            add_into(o_sum(q), bit(me.y, q))

            @pl.when(no_more)
            def _():
                o_on(q)

        def o_z(q):
            @pl.when(from_left)
            def _():
                arrived(o_left(q), o_red.at[2, q], me.left)
                add_into(o_sum(q), o_left(q))

            @pl.when(from_right)
            def _():
                arrived(o_right(q), o_red.at[3, q], me.right)
                add_into(o_sum(q), o_right(q))

            @pl.when(jnp.logical_not(no_more))
            def _():
                o_on(q)

        own_half = o_buf[0].at[pl.ds(pl.multiple_of(me.c * head, STRIP), head)]
        other_half = o_buf[0].at[pl.ds(pl.multiple_of((1 - me.c) * head, STRIP), head)]
        o_keep, o_send, o_recv = o_deal
        keep_oo = pltpu.make_async_copy(own_half, out_out, o_keep)


        def o_end():
            @pl.when(owner)
            def _():
                keep_oo.start()
                push(other_half, out_out, o_send.at[0], o_recv.at[0], me.core).start()
                push(own_half, out_out, o_send.at[1], o_recv.at[0], me.across).start()
                push(other_half, out_out, o_send.at[2], o_recv.at[0], me.corner).start()

        def output(strip):
            got_f[me.s, strip, :] = low(x1[strip, :] + summed(strip, out_part, got_f, last_f))

        def third_sum():
            blocks_finish(me, tok(out_part), got_f, last_f, *f_sems)
            strips(rows, output)
            pltpu.make_async_copy(got_f.at[me.s], bo_ref, local.at[1]).start()
            fetch_x.start()

        def inner(strip):
            got[me.s, strip, :] = low(norm_back(
                last_f[strip, :].astype(F32), summed(strip, part, got, last), dx_all[mine(strip), :].astype(F32)
            ))

        def fourth_sum():
            blocks_finish(me, tok(part), got, last, *h_sems)
            fetch_x.wait()
            strips(rows, inner)
            pltpu.make_async_copy(got.at[me.s], gx_ref, local.at[2]).start()

        final_dn, final_q = dn_buf[0].at[me.z], q_buf[0].at[me.z]
        dn_keep, dn_send, dn_recv = dn_deal

        def dn_end():
            pltpu.make_async_copy(final_dn, dn_out.at[me.s], dn_keep).start()
            push(final_dn, dn_out.at[me.s], dn_send, dn_recv, me.across).start()

        steps = {
            "weigh": weigh_units, "own": own_heads, "rn": lambda: group_relay(me, tok(n_buf), *n_sems),
            "Ae": lambda: ends(0), "Be": lambda: ends(1), "De": dn_ends, "nf": normed_here,
            "widen": widen_weights, "project": project_tokens, "oh": heads_here,
            "rg": lambda: group_relay(me, tok(g_all), *g_sems), "gf": cot_here, "ol": heads_left,
            "xs": first_sum, "rm": lambda: group_relay(me, tok(n_buf), *m_sems),
            "mf": lambda: group_finish(me, tok(n_buf).at[me.rank], tok(n_buf), *m_sems),
            "w0": lambda: weight_grads(0, g_gu), "w1": second_grads,
            "b0": lambda: back(away), "b1": lambda: back(home), "fo": outward, "bs": second_sum, "dw": down_grads,
            "rx": lambda: group_relay(me, tok(dx_all), *d_sems),
            "xf": lambda: group_finish(me, tok(dx_all).at[me.rank], tok(dx_all), *d_sems),
            "sp": spread_grads, "go": out_grads, "qg": in_grads, "oe": o_end, "fs": third_sum, "hs": fourth_sum,
            "fc": lambda: blocks_cross(me, tok(out_part), got_f, last_f, *f_sems),
            "de": dn_end, "ae": lambda: deal_start(me, finals[0], depth, gu_out.at[0], *gu_deal[0]),
            "be": lambda: deal_start(me, finals[1], depth, gu_out.at[1], *gu_deal[1]),
            "qe": lambda: deal_start(me, final_q, depth, qkv_out, *q_deal),
        }
        for key, slots, line in (
            ("Q", q_slots, q_line), ("A", gu_slots[0], gu_line[0]), ("B", gu_slots[1], gu_line[1]), ("D", dn_slots, dn_line)
        ):
            steps[key + "s"] = functools.partial(line_side, me, slots, line)
            steps[key + "t"] = functools.partial(line_twin, me, slots, line)
            steps[key + "f"] = functools.partial(line_finish, me, slots, line)
            for hop in range(1, planes):
                steps[key + str(hop)] = functools.partial(line_hop, me, slots, line, hop)
        for key, own, buffers, sems in (
            ("a", own_gu[0], gu_buf[0], gu_sems[0]), ("b", own_gu[1], gu_buf[1], gu_sems[1]),
            ("d", dn_slots, dn_buf, dn_sems), ("q", q_slots, q_buf, q_sems),
        ):
            steps[key + "r0"] = functools.partial(reduce_start, me, own, buffers[0], sems, [0])
            steps[key + "r1"] = functools.partial(reduce_start, me, own, buffers[0], sems, range(1, planes))
            steps[key + "m"] = functools.partial(reduce_mix, me, own, buffers[0], sems)
            for i in range(planes):
                steps[key + "y" + str(i)] = functools.partial(reduce_y, me, own, *buffers, sems, i)
                steps[key + "z" + str(i)] = functools.partial(reduce_z, me, *buffers, sems, i)
        for i in range(PIECES):
            steps["f" + str(i)] = functools.partial(fan, i)
            steps["oy" + str(i)] = functools.partial(o_y, i)
            steps["oz" + str(i)] = functools.partial(o_z, i)
        for i, (seq, core) in enumerate(((away, 1 - me.c), (away, me.c), (home, 1 - me.c), (home, me.c))):
            steps["t" + str(i)] = functools.partial(attend_rows, (2 * seq + core) * rows)
            steps["h" + str(i)] = functools.partial(attend_rows_back, (2 * seq + core) * rows)
        for key, whole, some, rest, sems in (
            ("x", part, got, last, x_sems), ("p", part, got, last, b_sems), ("k", part, got, last, h_sems)
        ):
            for i in range(2):
                steps[key + str(i)] = functools.partial(blocks_start, me, tok(whole), some, *sems, i)
            steps[key + "c"] = functools.partial(blocks_cross, me, tok(whole), some, rest, *sems)
        for h in range(2):
            for j in range(half_units // chunk):
                steps["uv"[h] + str(j)] = functools.partial(activations, h, j)
        for name in SCHEDULE:
            steps[name]()

        for h in range(2):
            reduce_finish(me, own_gu[h], gu_buf[h][0], gu_sems[h])
            deal_finish(me, finals[h], depth, gu_out.at[h], *gu_deal[h])
        reduce_finish(me, dn_slots, dn_buf[0], dn_sems)
        reduce_finish(me, q_slots, q_buf[0], q_sems)
        for q in range(PIECES):
            sum_q = o_sum(q)
            left_over(bit(1 - me.y, q), o_red.at[0, q], me.side)

            @pl.when(me.z < me.rank)
            def _():
                left_over(sum_q, o_red.at[4, q], me.right)

            @pl.when(me.z > me.rank)
            def _():
                left_over(sum_q, o_red.at[4, q], me.left)

        @pl.when(owner)
        def _():
            keep_oo.wait()
            left_over(other_half, o_send.at[0], me.core)
            left_over(own_half, o_send.at[1], me.across)
            left_over(other_half, o_send.at[2], me.corner)

        @pl.when(jnp.logical_not(owner))
        def _():
            arrived(out_out, o_recv.at[0], me.core)

        pltpu.make_async_copy(final_dn, dn_out.at[me.s], dn_keep).wait()
        left_over(final_dn, dn_send, me.across)
        arrived(dn_out.at[1 - me.s], dn_recv, me.across)
        pltpu.make_async_copy(got_f.at[me.s], bo_ref, local.at[1]).wait()
        pltpu.make_async_copy(got.at[me.s], gx_ref, local.at[2]).wait()
        deal_finish(me, final_q, depth, qkv_out, *q_deal)

    sems = lambda *dims: pltpu.SemaphoreType.DMA(dims)
    one, three = pltpu.SemaphoreType.DMA, sems(3)
    vmem = lambda *dims: pltpu.VMEM(dims, BF)
    deal = [one, three, three]
    outs = comm_call(
        kernel, 0,
        [shape((rows, width)), shape((rows, width)), shape((4, depth, q_cols)), shape((head, width)),
         shape((2, 4, depth, cols)), shape((2, block, width)), shape((total, width))],
        [ANY] * 7,
        [(ANY, ref) for ref in (tokens, cot, w_query, w_key, w_value, w_out, w_gate, w_up, w_down)]
        + [(VMEM, gain_attn), (VMEM, gain_mlp), (VMEM, head_tables(length))],
        [vmem(total, width), vmem(total, width), vmem(width, q_cols), vmem(heads4, width), vmem(2, width, cols),
         vmem(units, width), vmem(total, 8 * LANES), vmem(total, heads4)]
        + [vmem(total, width), vmem(total, width), pltpu.VMEM((rows, width), F32), vmem(total, units),
           vmem(2, total, cols), vmem(width, cols), vmem(total, width)]
        + blocks_buffers(rows, width) * 2
        + reduce_buffers(planes, 2 * depth, cols) * 2 + reduce_buffers(planes, block, width)
        + reduce_buffers(planes, 2 * depth, q_cols) + [vmem(2 * head, width)] * 3
        + group_sems() * 4 + blocks_sems() * 4 + [one] * 9
        + line_sems(planes) * 4 + reduce_sems(planes) * 4 + deal * 2 + [one] * 3 + deal * 2
        + [sems(5), sems(2), sems(5, PIECES), sems(5, PIECES), sems(3 + 8 * planes), vmem(heads4, 4 * LANES),
           pltpu.VMEM((2, depth, LANES), F32)],
        "block_step",
    )
    return outs[:6]


def finish(planes, parts, weights, gains):
    block_out, grad_tokens, own_qkv, own_out, own_gu, own_dn = parts
    w_query, w_key, w_value, w_gate, w_up = weights
    rows, width = block_out.shape
    depth, hidden = w_gate.shape
    q_own, k_own = w_query.shape[1] // 4, w_key.shape[1] // 4
    block = own_dn.shape[1]
    per = 4
    steps = 2 * planes // per
    wide = hidden // steps
    own_dn = own_dn.reshape(2 * block, width)

    def kernel(bo_ref, gx_ref, qkv_ref, out_ref, gate_ref, up_ref, dn_ref, wq_ref, wk_ref, wv_ref, wg_ref, wu_ref,
               ga_ref, gm_ref, bo_out, gx_out, q_out, k_out, v_out, o_out, gate_out, up_out, dn_out, ga_out, gm_out,
               columns, total):
        step = pl.program_id(0)
        same = lax.broadcasted_iota(jnp.int32, (depth, depth), 0) == lax.broadcasted_iota(jnp.int32, (depth, depth), 1)

        def as_row(value):
            return jnp.sum(jnp.where(same, jnp.sum(value, 1, keepdims=True), 0.0), 0, keepdims=True)

        @pl.when(step == 0)
        def _():
            for k, ref in enumerate((ga_ref, gm_ref)):
                column = jnp.sum(jnp.where(same, ref[...].astype(F32), 0.0), 1, keepdims=True)
                columns[k] = jnp.broadcast_to(column, (depth, LANES))
            total[...] = jnp.zeros_like(total)
            o_out[...] = out_ref[...].astype(F32)
            gain = columns[0]
            gathered = jnp.zeros((depth, LANES), F32)

            def put(out, weight, tile, value):
                lanes = slice(tile * LANES, (tile + 1) * LANES)
                out[:, lanes] = value * gain
                return value * weight[:, lanes].astype(F32)

            rolled = lambda value: pltpu.roll(value, LANES // 2, 1)
            in_low = lax.broadcasted_iota(jnp.int32, (depth, LANES), 1) < LANES // 2
            join = lambda first, second: jnp.where(in_low, first, second)
            for rank in range(4):
                for k in range(q_own // LANES):
                    value = qkv_ref[rank, :, k * LANES:(k + 1) * LANES].astype(F32)
                    gathered += put(q_out, wq_ref, rank * q_own // LANES + k, value)
            for seq in range(2):
                (a0, a1, a2), (b0, b1, b2) = [
                    [qkv_ref[2 * seq + core, :, q_own + k * LANES:q_own + (k + 1) * LANES].astype(F32) for k in range(3)]
                    for core in range(2)
                ]
                keys = [a0, join(a1, rolled(b0)), join(rolled(b0), rolled(b1))]
                values = [join(rolled(a1), rolled(a2)), join(rolled(a2), b1), b2]
                for k in range(3):
                    gathered += put(k_out, wk_ref, 3 * seq + k, keys[k])
                    gathered += put(v_out, wv_ref, 3 * seq + k, values[k])
            ga_out[...] = as_row(gathered)

        bo_out[...] = bo_ref[...]
        gx_out[...] = gx_ref[...]
        dn_out[...] = dn_ref[...].astype(F32)
        gain = columns[1]
        gathered = jnp.zeros((depth, LANES), F32)
        for ref, out, weight in ((gate_ref, gate_out, wg_ref), (up_ref, up_out, wu_ref)):
            for k in range(4 * per):
                chip, core, seq = k // 4, k // 2 % 2, k % 2
                lanes = slice(k * block, (k + 1) * block)
                value = ref[0, 2 * seq + core, :, chip * block:(chip + 1) * block].astype(F32)
                out[:, lanes] = value * gain
                gathered += value * weight[:, lanes].astype(F32)
        total[...] += gathered

        @pl.when(step == steps - 1)
        def _():
            gm_out[...] = as_row(total[...])

    whole = lambda ref: pl.BlockSpec(ref.shape, lambda p: (0,) * len(ref.shape))
    strip = lambda ref: pl.BlockSpec((ref.shape[0] // steps, ref.shape[1]), lambda p: (p, 0))
    runs = planes // per
    part = lambda first: pl.BlockSpec((1, 4, depth, per * block), lambda p: (p // runs, 0, 0, first + p % runs))
    slab = pl.BlockSpec((depth, wide), lambda p: (0, p))
    outs = [shape(block_out.shape), shape(grad_tokens.shape), shape(w_query.shape, F32), shape(w_key.shape, F32),
            shape(w_value.shape, F32), shape(own_out.shape, F32), shape(w_gate.shape, F32), shape(w_up.shape, F32),
            shape(own_dn.shape, F32), shape((1, depth), F32), shape((1, depth), F32)]
    return pl.pallas_call(
        kernel,
        grid=(steps,),
        out_shape=outs,
        in_specs=[strip(block_out), strip(grad_tokens), whole(own_qkv), whole(own_out), part(0), part(runs),
                  strip(own_dn), whole(w_query), whole(w_key), whole(w_value), slab, slab, whole(gains[0]), whole(gains[1])],
        out_specs=[strip(outs[0]), strip(outs[1])] + [whole(o) for o in outs[2:6]]
        + [slab, slab, strip(outs[8]), whole(outs[9]), whole(outs[10])],
        scratch_shapes=[pltpu.VMEM((2, depth, LANES), F32), pltpu.VMEM((depth, LANES), F32)],
        name="finish",
    )(block_out, grad_tokens, own_qkv, own_out, own_gu, own_gu, own_dn, w_query, w_key, w_value, w_gate, w_up, *gains)


def shards_fast(tokens, cotangent, w_query, w_key, w_value, w_out, w_gate, w_up, w_down, gain_attn, gain_mlp):
    seqs, length, width = tokens.shape
    rows = seqs * length
    depth = w_query.shape[0]
    planes = width // depth // 4
    x, cot = tokens.reshape(rows, width), cotangent.reshape(rows, width)
    gains = (gain_attn.reshape(1, depth), gain_mlp.reshape(1, depth))
    parts = block_step(planes, length, x, cot, w_query, w_key, w_value, w_out, w_gate, w_up, w_down, *gains)
    outs = finish(planes, parts, (w_query, w_key, w_value, w_gate, w_up), gains)
    return (
        outs[0].reshape(tokens.shape), outs[1].reshape(tokens.shape), *outs[2:9],
        outs[9].reshape(depth), outs[10].reshape(depth),
    )


def fits(mesh):
    return mesh.shape["seq"] == 2 and mesh.shape["dp"] == 16


def solution(mesh):
    body = shards_fast if fits(mesh) else shards_plain
    return jax.shard_map(body, mesh=mesh, in_specs=IN_SPECS, out_specs=OUT_SPECS, check_vma=False)
```

```python
import jax
import jax.numpy as jnp
import functools
import numpy as np
from jax import lax
from jax.experimental import pallas as pl
from jax.experimental.pallas import tpu as pltpu
from jax.sharding import PartitionSpec as P

HD = 96
EPS = 1e-05
THETA = 100000.0


def rotary(positions, width):
    steps_half = jnp.arange(width // 2, dtype=jnp.float32)
    frequency = jnp.power(THETA, -2.0 * steps_half / width)
    angles = positions[:, None] * frequency[None, :]
    cosine = jnp.cos(angles)
    sine = jnp.sin(angles)
    return (jnp.concatenate([cosine, cosine], -1), jnp.concatenate([sine, sine], -1))


def rotate(values, cosine, sine):
    half = values.shape[-1] // 2
    turned = jnp.concatenate([-values[..., half:], values[..., :half]], -1)
    return values * cosine[:, None, :] + turned * sine[:, None, :]


def rotate_back(grads, cosine, sine):
    half = grads.shape[-1] // 2
    sined = grads * sine[:, None, :]
    turned = jnp.concatenate([sined[..., half:], -sined[..., :half]], -1)
    return grads * cosine[:, None, :] + turned


def dot32(left, right):
    return jnp.dot(left, right, preferred_element_type=jnp.float32)


def dot_t(left, right):
    return lax.dot_general(left, right, (((1,), (1,)), ((), ())), preferred_element_type=jnp.float32)


def dot_l(left, right):
    return lax.dot_general(left, right, (((0,), (0,)), ((), ())), preferred_element_type=jnp.float32)


def inv_rms(values):
    return lax.rsqrt(jnp.mean(values * values, axis=-1, keepdims=True) + EPS)


def low(values):
    return values.astype(jnp.bfloat16)


def attend(queries, keys, values):
    rows = queries.shape[1]
    ids = jnp.arange(rows, dtype=jnp.int32)
    visible = ids[:, None] >= ids[None, :]
    scores = HD ** (-0.5) * jnp.einsum("bqkgd,bckd->bkgqc", queries, keys, preferred_element_type=jnp.float32)
    scores = jnp.where(visible, scores, -jnp.inf)
    top = jnp.max(scores, -1, keepdims=True)
    exps = jnp.exp(scores - top)
    probs = exps / jnp.sum(exps, -1, keepdims=True)
    mixed = jnp.einsum("bkgqc,bckd->bqkgd", low(probs), values, preferred_element_type=jnp.float32)
    return probs, low(mixed)


def attend_back(queries, keys, values, probs, grad_mixed):
    grad_values = jnp.einsum("bkgqc,bqkgd->bckd", low(probs), grad_mixed, preferred_element_type=jnp.float32)
    grad_probs = jnp.einsum("bqkgd,bckd->bkgqc", grad_mixed, values, preferred_element_type=jnp.float32)
    grad_scores = low(probs * (grad_probs - jnp.sum(probs * grad_probs, -1, keepdims=True)))
    scale = HD ** (-0.5)
    grad_queries = scale * jnp.einsum("bkgqc,bckd->bqkgd", grad_scores, keys, preferred_element_type=jnp.float32)
    grad_keys = scale * jnp.einsum("bkgqc,bqkgd->bckd", grad_scores, queries, preferred_element_type=jnp.float32)
    return grad_queries, grad_keys, grad_values


def mlp_grads(gate, up, grad_hidden):
    sigma = jax.nn.sigmoid(gate)
    silu = gate * sigma
    hidden = low(silu * up)
    grad_gate = low(grad_hidden * up * sigma * (1.0 + gate * (1.0 - sigma)))
    grad_up = low(grad_hidden * silu)
    return hidden, grad_gate, grad_up


def shards_plain(tokens, cotangent, w_query, w_key, w_value, w_out, w_gate, w_up, w_down, gain_attn, gain_mlp):
    seqs, length, width = tokens.shape
    rows = seqs * length
    kv_heads = w_key.shape[1] // HD
    groups = w_query.shape[1] // w_key.shape[1]
    gather = lambda w: lax.all_gather(w, "dp", axis=0, tiled=True)
    full_query, full_key, full_value, full_out = map(gather, (w_query, w_key, w_value, w_out))
    gains = gather(jnp.stack([gain_attn, gain_mlp], 1)).astype(jnp.float32)
    gain_one, gain_two = gains[:, 0], gains[:, 1]
    full_gate, full_up, full_down = map(gather, (w_gate, w_up, w_down))
    cosine, sine = rotary(jnp.arange(length, dtype=jnp.float32), HD)
    cosine, sine = jnp.tile(cosine, (seqs, 1)), jnp.tile(sine, (seqs, 1))

    inputs = tokens.reshape(rows, width).astype(jnp.float32)
    grad_in = cotangent.reshape(rows, width)
    scale_one = inv_rms(inputs)
    normed = low(inputs * scale_one * gain_one)
    queries = low(rotate(dot32(normed, full_query).reshape(rows, -1, HD), cosine, sine))
    keys = low(rotate(dot32(normed, full_key).reshape(rows, -1, HD), cosine, sine))
    values = low(dot32(normed, full_value))
    queries = queries.reshape(seqs, length, kv_heads, groups, HD)
    keys = keys.reshape(seqs, length, kv_heads, HD)
    values = values.reshape(seqs, length, kv_heads, HD)
    probs, mixed = attend(queries, keys, values)
    mixed = mixed.reshape(rows, -1)
    hidden_one = inputs + dot32(mixed, full_out)
    scale_two = inv_rms(hidden_one)
    normed_two = low(hidden_one * scale_two * gain_two)
    gate, up = dot32(normed_two, full_gate), dot32(normed_two, full_up)
    hidden, grad_gate, grad_up = mlp_grads(gate, up, dot_t(grad_in, full_down))
    block_out = low(hidden_one + dot32(hidden, full_down))

    acc_down = dot_l(hidden, grad_in)
    acc_gate = dot_l(normed_two, grad_gate)
    acc_up = dot_l(normed_two, grad_up)
    grad_normed_two = dot_t(grad_gate, full_gate) + dot_t(grad_up, full_up)
    acc_gain_two = jnp.sum(grad_normed_two * hidden_one * scale_two, 0)
    weighted = grad_normed_two * gain_two
    grad_one = grad_in.astype(jnp.float32) + scale_two * (
        weighted - hidden_one * scale_two * scale_two * jnp.mean(weighted * hidden_one, -1, keepdims=True)
    )
    grad_branch = low(grad_one)
    acc_out = dot_l(mixed, grad_branch)
    grad_mixed = low(dot_t(grad_branch, full_out)).reshape(queries.shape)
    grad_queries, grad_keys, grad_values = attend_back(queries, keys, values, probs, grad_mixed)
    grad_queries = low(rotate_back(grad_queries.reshape(rows, -1, HD), cosine, sine)).reshape(rows, -1)
    grad_keys = low(rotate_back(grad_keys.reshape(rows, -1, HD), cosine, sine)).reshape(rows, -1)
    grad_values = low(grad_values).reshape(rows, -1)
    acc_query = dot_l(normed, grad_queries)
    acc_key = dot_l(normed, grad_keys)
    acc_value = dot_l(normed, grad_values)
    grad_normed = dot_t(grad_queries, full_query) + dot_t(grad_keys, full_key) + dot_t(grad_values, full_value)
    acc_gain_one = jnp.sum(grad_normed * inputs * scale_one, 0)
    weighted = grad_normed * gain_one
    grad_tokens = grad_one + scale_one * (
        weighted - inputs * scale_one * scale_one * jnp.mean(weighted * inputs, -1, keepdims=True)
    )

    def share(acc):
        owned = lax.psum_scatter(low(acc), "dp", scatter_dimension=0, tiled=True)
        return lax.psum(owned, "seq").astype(jnp.float32)

    grads = [share(a) for a in (acc_down, acc_gate, acc_up, acc_out, acc_query, acc_key, acc_value)]
    gain_grads = lax.psum(
        lax.psum_scatter(jnp.stack([acc_gain_one, acc_gain_two], 1), "dp", scatter_dimension=0, tiled=True), "seq"
    )
    down, gate, up, out, query, key, value = grads
    return (
        block_out.reshape(tokens.shape),
        low(grad_tokens).reshape(tokens.shape),
        query, key, value, out, gate, up, down,
        gain_grads[:, 0], gain_grads[:, 1],
    )


ROWS = P(("dp", "seq"), None, None)
SPLIT = P("dp", None)
IN_SPECS = (ROWS, ROWS) + (SPLIT,) * 7 + (P("dp"), P("dp"))
OUT_SPECS = (ROWS, ROWS) + (SPLIT,) * 7 + (P("dp"), P("dp"))


MESH = pl.DeviceIdType.MESH
VMEM = pl.BlockSpec(memory_space=pltpu.VMEM)
ANY = pl.BlockSpec(memory_space=pl.ANY)
BF = jnp.bfloat16
F32 = jnp.float32
STRIP = 16
PIECES = 4
VMEM_BYTES = 67_043_328


class Place:
    def __init__(self, planes):
        self.planes = planes
        d = lax.axis_index("dp")
        self.d, self.s = d, lax.axis_index("seq")
        self.c, self.y, self.z = d % 2, (d // 2) % 2, d // 4
        self.p = d // 2
        self.rank = 2 * self.s + self.c
        self.core = (d + 1 - 2 * self.c, self.s)
        self.across = (d, 1 - self.s)
        self.corner = (d + 1 - 2 * self.c, 1 - self.s)
        self.side = (d + 2 - 4 * self.y, self.s)
        self.right = (lax.rem(d + 4, 4 * planes), self.s)
        self.left = (lax.rem(d + 4 * planes - 4, 4 * planes), self.s)
        self.has_right, self.has_left = self.z < planes - 1, self.z > 0
        odd = self.z % 2
        self.twin = self.z + 1 - 2 * odd
        self.buddy = (d + 4 - 8 * odd, self.s)


def greet(me):
    barrier = pltpu.get_barrier_semaphore()
    for peer in (me.core, me.across, me.corner, me.side, me.right, me.left):
        pl.semaphore_signal(barrier, inc=1, device_id=peer, device_id_type=MESH)


def met():
    pl.semaphore_wait(pltpu.get_barrier_semaphore(), 6)


def push(src, dst, send, recv, peer):
    return pltpu.make_async_remote_copy(
        src_ref=src, dst_ref=dst, send_sem=send, recv_sem=recv, device_id=peer, device_id_type=MESH
    )


def arrived(dst, recv, peer):
    push(dst, dst, recv, recv, peer).wait_recv()


def left_over(src, send, peer):
    push(src, src, send, send, peer).wait_send()


class Slots:
    def __init__(self, ref, rows):
        self.ref, self.rows = ref, rows
        self.at = self

    def __getitem__(self, block):
        return self.ref.at[pl.ds(pl.multiple_of(block * self.rows, self.rows), self.rows)]


def group_start(me, src, dst, send, recv):
    push(src, dst.at[me.rank], send.at[0], recv.at[0], me.core).start()
    push(src, dst.at[me.rank], send.at[1], recv.at[1], me.across).start()


def group_relay(me, dst, send, recv):
    slot = dst.at[2 * (1 - me.s) + me.c]
    arrived(slot, recv.at[1], me.across)
    push(slot, slot, send.at[2], recv.at[2], me.core).start()


def group_finish(me, src, dst, send, recv):
    arrived(dst.at[2 * me.s + 1 - me.c], recv.at[0], me.core)
    arrived(dst.at[2 * (1 - me.s) + 1 - me.c], recv.at[2], me.core)
    left_over(src, send.at[0], me.core)
    left_over(src, send.at[1], me.across)
    slot = dst.at[2 * (1 - me.s) + me.c]
    left_over(slot, send.at[2], me.core)


def group_sems():
    return [pltpu.SemaphoreType.DMA((3,)), pltpu.SemaphoreType.DMA((3,))]


def upper(slot):
    return slot.at[pl.ds(0, slot.shape[0] // 2)]


def lower(slot):
    return slot.at[pl.ds(slot.shape[0] // 2, slot.shape[0] // 2)]


def line_start(me, dst, sems):
    line_side(me, dst, sems)
    line_ends(me, dst, sems)


def line_side(me, dst, sems):
    to_right, to_left, line, to_side, side, twin = sems
    slot = dst(me.p)
    push(slot, slot, to_side.at[me.z], side.at[me.z], me.side).start()


def line_ends(me, dst, sems):
    to_right, to_left, line, to_side, side, twin = sems
    slot = dst(me.p)

    @pl.when(me.has_right)
    def _():
        push(slot, slot, to_right.at[me.z], line.at[me.z], me.right).start()

    @pl.when(me.has_left)
    def _():
        push(slot, slot, to_left.at[me.z], line.at[me.z], me.left).start()


def line_hop(me, dst, sems, hop):
    to_right, to_left, line, to_side, side, twin = sems

    def pass_on(item, back, forth, may, sends):
        slot = dst(2 * item + me.y)
        arrived(slot, line.at[item], back)

        @pl.when(may)
        def _():
            push(slot, slot, sends.at[item], line.at[item], forth).start()

        if hop > 1:
            push(slot, slot, to_side.at[item], side.at[item], me.side).start()
        else:

            @pl.when(item != me.twin)
            def _():
                push(slot, slot, to_side.at[item], side.at[item], me.side).start()

            @pl.when(item == me.twin)
            def _():
                half = upper(slot)
                push(half, half, to_side.at[item], side.at[item], me.side).start()

    @pl.when(me.z >= hop)
    def _():
        pass_on(me.z - hop, me.left, me.right, me.has_right, to_right)

    @pl.when(me.z + hop < me.planes)
    def _():
        pass_on(me.z + hop, me.right, me.left, me.has_left, to_left)


def line_twin(me, dst, sems):
    to_right, to_left, line, to_side, side, twin = sems
    slot = dst(2 * me.z + 1 - me.y)
    arrived(slot, side.at[me.z], me.side)
    half = lower(slot)
    push(half, half, twin.at[0], twin.at[1], me.buddy).start()


def line_finish(me, dst, sems):
    to_right, to_left, line, to_side, side, twin = sems
    for item in range(me.planes):
        slot, mine = dst(2 * item + 1 - me.y), dst(2 * item + me.y)

        @pl.when(item == me.twin)
        def _():
            arrived(upper(slot), side.at[item], me.side)
            arrived(lower(slot), twin.at[1], me.buddy)
            left_over(upper(mine), to_side.at[item], me.side)

        @pl.when(jnp.logical_and(item != me.twin, item != me.z))
        def _():
            arrived(slot, side.at[item], me.side)

        @pl.when(item != me.twin)
        def _():
            left_over(mine, to_side.at[item], me.side)

        @pl.when(item == me.z)
        def _():
            left_over(lower(slot), twin.at[0], me.buddy)

        @pl.when(jnp.logical_and(me.has_right, item <= me.z))
        def _():
            left_over(mine, to_right.at[item], me.right)

        @pl.when(jnp.logical_and(me.has_left, item >= me.z))
        def _():
            left_over(mine, to_left.at[item], me.left)


def line_sems(planes):
    return [pltpu.SemaphoreType.DMA((planes,))] * 5 + [pltpu.SemaphoreType.DMA((2,))]


def pick(table, index):
    value = jnp.int32(table[0])
    for i in range(1, len(table)):
        value = jnp.where(index == i, table[i], value)
    return value


def far_first(planes):
    return [sorted(range(planes), key=lambda i, z=z: (-abs(i - z), i)) for z in range(planes)]


def add_into(dst, *others):
    rows = dst.shape[0]

    def body(i, carry):
        strip = pl.ds(pl.multiple_of(i * STRIP, STRIP), STRIP)
        total = dst[strip, :].astype(F32)
        for other in others:
            total = total + other[strip, :].astype(F32)
        dst[strip, :] = total.astype(dst.dtype)
        return carry

    lax.fori_loop(0, rows // STRIP, body, 0)


def reduce_start(me, own, half, sems, which):
    to_side, side, twin = sems[0], sems[1], sems[6]
    orders = far_first(me.planes)
    if 0 in which:
        away = lower(own(2 * me.twin + 1 - me.y))
        push(away, lower(half.at[me.z]), twin.at[0], twin.at[1], me.buddy).start()
    for i in which:
        item = pick([o[i] for o in orders], me.z)
        src, dst = own(2 * item + 1 - me.y), half.at[item]

        @pl.when(item == me.twin)
        def _():
            push(upper(src), upper(dst), to_side.at[item], side.at[item], me.side).start()

        @pl.when(jnp.logical_and(item != me.twin, item != me.z))
        def _():
            push(src, dst, to_side.at[item], side.at[item], me.side).start()


def reduce_mix(me, own, half, sems):
    to_side, side, twin = sems[0], sems[1], sems[6]
    mixed, got = own(2 * me.z + 1 - me.y), lower(half.at[me.twin])
    arrived(got, twin.at[1], me.buddy)
    add_into(lower(mixed), got)
    push(mixed, half.at[me.z], to_side.at[me.z], side.at[me.z], me.side).start()


def reduce_y(me, own, half, lines, sems, i):
    to_side, side, to_right, to_left, left, right, twin = sems
    item = pick([o[i] for o in far_first(me.planes)], me.z)
    mine, ours = half.at[item], own(2 * item + me.y)

    @pl.when(item == me.twin)
    def _():
        arrived(upper(mine), side.at[item], me.side)
        add_into(upper(mine), upper(ours))
        copy_into(lower(mine), lower(ours))

    @pl.when(item != me.twin)
    def _():
        arrived(mine, side.at[item], me.side)
        add_into(mine, ours)

    @pl.when(jnp.logical_and(item > me.z, jnp.logical_not(me.has_left)))
    def _():
        push(mine, lines.at[item], to_right.at[item], left.at[item], me.right).start()

    @pl.when(jnp.logical_and(item < me.z, jnp.logical_not(me.has_right)))
    def _():
        there = jnp.where(item == me.z - 1, me.planes, item)
        push(mine, lines.at[there], to_left.at[item], right.at[item], me.left).start()


def reduce_z(me, half, lines, sems, i):
    to_side, side, to_right, to_left, left, right, twin = sems
    item = pick([o[i] for o in far_first(me.planes)], me.z)
    mine = half.at[item]
    spot = jnp.where(item == me.z, me.planes, item)

    @pl.when(jnp.logical_and(me.has_left, item >= me.z))
    def _():
        arrived(lines.at[item], left.at[item], me.left)
        add_into(mine, lines.at[item])

        @pl.when(item > me.z)
        def _():
            push(mine, lines.at[item], to_right.at[item], left.at[item], me.right).start()

    @pl.when(jnp.logical_and(me.has_right, item <= me.z))
    def _():
        arrived(lines.at[spot], right.at[item], me.right)
        add_into(mine, lines.at[spot])

        @pl.when(item < me.z)
        def _():
            there = jnp.where(item == me.z - 1, me.planes, item)
            push(mine, lines.at[there], to_left.at[item], right.at[item], me.left).start()


def reduce_finish(me, own, half, sems):
    to_side, side, to_right, to_left, left, right, twin = sems
    left_over(lower(own(2 * me.twin + 1 - me.y)), twin.at[0], me.buddy)
    for item in range(me.planes):
        sent = own(2 * item + 1 - me.y)

        @pl.when(item == me.twin)
        def _():
            left_over(upper(sent), to_side.at[item], me.side)

        @pl.when(item != me.twin)
        def _():
            left_over(sent, to_side.at[item], me.side)

        @pl.when(item > me.z)
        def _():
            left_over(half.at[item], to_right.at[item], me.right)

        @pl.when(item < me.z)
        def _():
            left_over(half.at[item], to_left.at[item], me.left)


def reduce_sems(planes):
    return [pltpu.SemaphoreType.DMA((planes,))] * 6 + [pltpu.SemaphoreType.DMA((2,))]


def copy_into(dst, src):
    def body(i, carry):
        strip = pl.ds(pl.multiple_of(i * STRIP, STRIP), STRIP)
        dst[strip, :] = src[strip, :]
        return carry

    lax.fori_loop(0, dst.shape[0] // STRIP, body, 0)


def reduce_buffers(planes, rows, columns):
    return [pltpu.VMEM((planes, rows, columns), BF), pltpu.VMEM((planes + 1, rows, columns), BF)]


def by_chip(ref, rows=None):
    if rows is None:
        return lambda chip: ref.at[chip]
    return lambda chip: ref.at[pl.ds(pl.multiple_of(chip * rows, STRIP), rows)]


def deal_start(me, final, rows, out, local, send, recv):
    mine = out.at[me.rank]
    part = lambda core: final.at[pl.ds(pl.multiple_of(core * rows, rows), rows)]
    pltpu.make_async_copy(part(me.c), mine, local).start()
    push(part(1 - me.c), mine, send.at[0], recv.at[0], me.core).start()
    push(part(me.c), mine, send.at[1], recv.at[1], me.across).start()
    push(part(1 - me.c), mine, send.at[2], recv.at[2], me.corner).start()


def deal_finish(me, final, rows, out, local, send, recv):
    part = lambda core: final.at[pl.ds(pl.multiple_of(core * rows, rows), rows)]
    pltpu.make_async_copy(part(me.c), out.at[me.rank], local).wait()
    left_over(part(1 - me.c), send.at[0], me.core)
    left_over(part(me.c), send.at[1], me.across)
    left_over(part(1 - me.c), send.at[2], me.corner)
    arrived(out.at[2 * me.s + 1 - me.c], recv.at[0], me.core)
    arrived(out.at[2 * (1 - me.s) + me.c], recv.at[1], me.across)
    arrived(out.at[2 * (1 - me.s) + 1 - me.c], recv.at[2], me.corner)


def blocks_start(me, part, got, send, recv, i):
    seq = (1 - me.s, me.s)[i]
    push(part.at[2 * seq + 1 - me.c], got.at[seq], send.at[i], recv.at[i], me.core).start()


def blocks_cross(me, part, got, last, send, recv):
    away = 1 - me.s
    arrived(got.at[away], recv.at[0], me.core)
    add_into(got.at[away], part.at[2 * away + me.c])
    push(got.at[away], last, send.at[2], recv.at[2], me.across).start()


def blocks_finish(me, part, got, last, send, recv):
    arrived(got.at[me.s], recv.at[1], me.core)
    arrived(last, recv.at[2], me.across)
    for i, seq in enumerate((1 - me.s, me.s)):
        left_over(part.at[2 * seq + 1 - me.c], send.at[i], me.core)
    left_over(got.at[1 - me.s], send.at[2], me.across)


def blocks_sems():
    return [pltpu.SemaphoreType.DMA((3,))] * 2


def blocks_buffers(rows, width):
    return [pltpu.VMEM((2, rows, width), BF), pltpu.VMEM((rows, width), BF)]


def strips(rows, body):
    def step(i, carry):
        body(pl.ds(pl.multiple_of(i * STRIP, STRIP), STRIP))
        return carry

    lax.fori_loop(0, rows // STRIP, step, 0)


def comm_call(kernel, ident, outs, out_specs, ins, scratch, name):
    return pl.pallas_call(
        kernel,
        out_shape=outs,
        in_specs=[spec for spec, _ in ins],
        out_specs=out_specs,
        scratch_shapes=scratch,
        name=name,
        compiler_params=pltpu.CompilerParams(
            collective_id=ident, has_side_effects=True, vmem_limit_bytes=VMEM_BYTES
        ),
    )(*[value for _, value in ins])


def shape(dims, dtype=BF):
    return jax.ShapeDtypeStruct(dims, dtype)


def split_start(me, parts, dst, keep, send, recv):
    pltpu.make_async_copy(parts.at[me.c], dst(me.c), keep).start()
    push(parts.at[1 - me.c], dst(me.c), send, recv, me.core).start()


def split_finish(me, parts, dst, keep, send, recv):
    pltpu.make_async_copy(parts.at[me.c], dst(me.c), keep).wait()
    arrived(dst(1 - me.c), recv, me.core)
    left_over(parts.at[1 - me.c], send, me.core)


def norm_back(values, weighted, base):
    scale = inv_rms(values)
    return base + scale * (
        weighted - values * scale * scale * jnp.mean(weighted * values, -1, keepdims=True)
    )


LANES = 128


def head_tables(length):
    steps = np.arange(HD // 2, dtype=np.float64)
    angles = np.arange(length, dtype=np.float64)[:, None] * np.power(THETA, -2.0 * steps / HD)[None, :]
    cosine, sine, none = np.cos(angles), np.sin(angles), np.zeros_like(angles)
    tables = [(cosine, cosine), (none, sine), (-sine, none)]
    pad = ((0, 0), (0, LANES - HD))
    return np.stack([np.pad(np.concatenate(t, 1), pad) for t in tables]).astype(np.float32)


def turn(values, tables, sign):
    other = pltpu.roll(values, HD // 2, 1) * tables[1] + pltpu.roll(values, LANES - HD // 2, 1) * tables[2]
    return values * tables[0] + sign * other


SCHEDULE = (
    "weigh", "Q1", "De", "Q2", "Ae", "Qt", "As", "Q3", "own", "Ds", "f0", "f1", "f2", "f3", "D1", "Qf", "Be",
    "rn", "Bs", "widen", "nf", "project", "oh", "D2", "A1", "t0", "x0", "t1", "xc", "rg", "t2", "x1", "ol",
    "t3", "gf", "At", "D3", "A2", "xs", "A3", "B1", "Dt", "B2", "rm", "Af", "mf", "Bt", "Df", "u0", "B3",
    "u1", "w0", "ar0", "ar1", "Bf", "v0", "v1", "b0", "p0", "ay0", "am", "pc", "b1", "ay1", "p1", "w1", "ay2",
    "br0", "fo", "br1", "az0", "bs", "dw", "by0", "az1", "az2", "bm", "ay3", "by1", "by2", "rx", "az3", "xf",
    "fc", "dr0", "ae", "sp", "go", "bz0", "h0", "h1", "dr1", "k0", "dy0", "bz1", "h2", "oy0", "k1", "oy1",
    "bz2", "kc", "by3", "oy2", "h3", "oy3", "qg", "qr0", "qr1", "jr0", "oz0", "dm", "dy1", "oz1", "bz3", "be",
    "jr1", "oz2", "qy0", "oz3", "oe", "dz0", "qm", "dy2", "dy3", "dz1", "dz2", "jy0", "jm", "qy1", "qz0",
    "fs", "jy1", "qy2", "dz3", "jz0", "de", "jy2", "qz1", "qz2", "qy3", "jz1", "jz2", "qz3", "qe", "jy3",
    "jz3", "je", "hs",
)


def block_step(planes, length, tokens, cot, w_query, w_key, w_value, w_out, w_gate, w_up, w_down, gain_attn, gain_mlp):
    rows, width = tokens.shape
    total = 4 * rows
    depth = w_query.shape[0]
    head = w_out.shape[0]
    q_own, k_own = w_query.shape[1] // 4, w_key.shape[1] // 4
    q_cols = q_own + 2 * k_own
    block = w_down.shape[0] // 2
    units = 2 * planes * block
    half_units = units // 2
    cols = 2 * half_units
    tile, chunk = 2 * rows, 256
    heads4 = 4 * head
    piece = 2 * head // PIECES

    def kernel(x_ref, g_loc, wq_ref, wk_ref, wv_ref, out_loc, gate_ref, up_ref, down_ref, ga_ref, gm_ref, tab_ref,
               bo_ref, gx_ref, qkv_out, out_out, gu_out, dn_out, stash, *scr):
        it = iter(scr)
        take = lambda k: [next(it) for _ in range(k)]
        n_buf, g_all, qkv_all, out_all, gu_all, dn_all, heads, mixed = take(8)
        part, out_part, x1, mid, dgu, g_gu, dx_all = take(7)
        (got, last), (got_f, last_f) = take(2), take(2)
        gu_buf, dn_buf, q_buf, o_buf = [take(2), take(2)], take(2), [take(2), take(2)], take(3)
        n_sems, g_sems, m_sems, d_sems = take(2), take(2), take(2), take(2)
        x_sems, b_sems, f_sems, h_sems = take(2), take(2), take(2), take(2)
        q_split, gu_split = take(3), [take(3), take(3)]
        q_line, gu_line, dn_line = take(6), [take(6), take(6)], take(6)
        gu_sems, dn_sems, q_sems = [take(7), take(7)], take(7), [take(7), take(7)]
        gu_deal, dn_deal, q_deal, o_deal = [take(3), take(3)], take(3), take(3), take(3)
        local, edge, o_fan, o_red, fetch, sel_ref, gains = take(7)
        me = Place(planes)
        greet(me)
        tok = lambda ref: Slots(ref, rows)
        q_slots, dn_slots = by_chip(qkv_all, 2 * depth), by_chip(dn_all, block)
        gu_slots = [by_chip(gu_all.at[h], 2 * depth) for h in range(2)]

        def core_rows(ref):
            return lambda core: ref.at[pl.ds(pl.multiple_of((2 * me.p + core) * depth, STRIP), depth)]

        fetch_x = pltpu.make_async_copy(x_ref, last_f, local.at[4])
        fetch_x.start()
        stage = out_part.at[pl.ds(0, depth)]
        heads_in = []
        for i, (ref, spot, size) in enumerate(
            ((wq_ref, 0, 2 * q_own), (wk_ref, 2 * q_own, 2 * k_own), (wv_ref, 2 * q_own + 2 * k_own, 2 * k_own))
        ):
            src = ref.at[:, pl.ds(pl.multiple_of(me.s * size, LANES), size)]
            heads_in.append(pltpu.make_async_copy(src, stage.at[:, pl.ds(spot, size)], fetch.at[i]))
            heads_in[-1].start()

        q_share = q_buf[0][0].at[0]
        gu_share = [mid.at[pl.ds(h * depth, depth)] for h in range(2)]
        units_in = []
        for other in range(2):
            core = (me.c, 1 - me.c)[other]
            for h in range(2):
                dst = (core_rows(gu_all.at[h])(me.c), gu_share[h])[other]
                for k in range(2 * planes):
                    ref = (gate_ref, up_ref)[k // planes]
                    chip = h * planes + k % planes
                    first = (2 * chip + core) * 2 * block + me.s * block
                    copy = pltpu.make_async_copy(
                        ref.at[:, pl.ds(pl.multiple_of(first, LANES), block)],
                        dst.at[:, pl.ds(k * block, block)],
                        fetch.at[3 + (other * 2 + h) * 2 * planes + k],
                    )
                    copy.start()
                    units_in.append(copy)
        own_down = down_ref.at[pl.ds(pl.multiple_of(me.s * block, STRIP), block)]
        keep_d = pltpu.make_async_copy(own_down, dn_slots(me.p), local.at[2])
        keep_d.start()
        keep_g = pltpu.make_async_copy(g_loc, tok(g_all).at[me.rank], local.at[3])
        keep_g.start()

        same = lax.broadcasted_iota(jnp.int32, (depth, depth), 0) == lax.broadcasted_iota(jnp.int32, (depth, depth), 1)
        for k, ref in enumerate((ga_ref, gm_ref)):
            column = jnp.sum(jnp.where(same, ref[...].astype(F32), 0.0), 1, keepdims=True)
            gains[k] = jnp.broadcast_to(column, (depth, LANES))
        row = lax.broadcasted_iota(jnp.int32, (heads4, 4 * LANES), 0)
        lane = lax.broadcasted_iota(jnp.int32, (heads4, 4 * LANES), 1)
        shift = sum(jnp.where(row >= k * HD, LANES - HD, 0) for k in range(1, 4))
        sel_ref[...] = jnp.where(lane == row + shift, 1.0, 0.0).astype(BF)

        for copy in heads_in:
            copy.wait()
        gain = gains[0][:, 0:1]
        tiles = lambda first, count: [
            stage[:, first + k * LANES:first + (k + 1) * LANES].astype(F32) * gain for k in range(count)
        ]
        queries = tiles(0, 6)
        k0, k1, k2 = tiles(2 * q_own, 3)
        v0, v1, v2 = tiles(2 * q_own + 2 * k_own, 3)
        rolled = lambda value: pltpu.roll(value, LANES // 2, 1)
        in_low = lax.broadcasted_iota(jnp.int32, (depth, LANES), 1) < LANES // 2
        join = lambda first, second: jnp.where(in_low, first, second)
        shares = (
            queries[:3] + [k0, join(k1, rolled(v0)), join(rolled(v0), rolled(v1))],
            queries[3:] + [join(rolled(k1), rolled(k2)), join(rolled(k2), v1), v2],
        )
        for core in range(2):
            value = low(jnp.concatenate(shares[core], 1))

            @pl.when(me.c == core)
            def _():
                core_rows(qkv_all)(me.c)[...] = value

            @pl.when(me.c != core)
            def _():
                q_share[...] = value

        met()
        push(q_share, core_rows(qkv_all)(me.c), q_split[1], q_split[2], me.core).start()
        here = me.s == me.z // 2
        owner = me.z == me.rank
        lender = jnp.logical_and(here, jnp.logical_not(owner))
        half = lambda y: out_all.at[pl.ds(pl.multiple_of(y * 2 * head, STRIP), 2 * head)]
        head_rows = lambda core: out_all.at[pl.ds(pl.multiple_of((2 * me.y + core) * head, STRIP), head)]
        keep_o = pltpu.make_async_copy(out_loc, head_rows(me.c), local.at[1])

        @pl.when(owner)
        def _():
            keep_o.start()

        @pl.when(lender)
        def _():
            push(out_loc, head_rows(me.c), edge.at[0], edge.at[1], me.core).start()

        fetch_x.wait()

        def first_norm(strip):
            value = last_f[strip, :].astype(F32)
            n_buf[pl.ds(pl.multiple_of(me.rank * rows + strip.start, STRIP), STRIP), :] = low(value * inv_rms(value))

        strips(rows, first_norm)
        group_start(me, tok(n_buf).at[me.rank], tok(n_buf), *n_sems)
        arrived(core_rows(qkv_all)(1 - me.c), q_split[2], me.core)
        line_start(me, q_slots, q_line)

        away, home = 1 - me.s, me.s

        def weigh_units():
            for copy in units_in:
                copy.wait()

            def weigh(i, carry):
                strip = pl.ds(pl.multiple_of(i * STRIP, STRIP), STRIP)
                gain = gains[1, strip, 0:1]
                for h in range(2):
                    for ref in (core_rows(gu_all.at[h])(me.c), gu_share[h]):
                        ref[strip, :] = low(ref[strip, :].astype(F32) * gain)
                return carry

            lax.fori_loop(0, depth // STRIP, weigh, 0)
            for h in range(2):
                push(gu_share[h], core_rows(gu_all.at[h])(me.c), gu_split[h][1], gu_split[h][2], me.core).start()
            group_start(me, g_loc, tok(g_all), *g_sems)

        fan_in, fan_right, fan_left, fan_side, fan_other = [o_fan.at[k] for k in range(5)]
        bit = lambda y, q: out_all.at[pl.ds(pl.multiple_of(y * 2 * head + q * piece, STRIP), piece)]
        go_right = jnp.logical_and(me.z >= me.rank, me.has_right)
        go_left = jnp.logical_and(me.z <= me.rank, me.has_left)

        def fan(q):
            mine = bit(me.y, q)

            @pl.when(me.z > me.rank)
            def _():
                arrived(mine, fan_in.at[q], me.left)

            @pl.when(me.z < me.rank)
            def _():
                arrived(mine, fan_in.at[q], me.right)

            @pl.when(go_right)
            def _():
                push(mine, mine, fan_right.at[q], fan_in.at[q], me.right).start()

            @pl.when(go_left)
            def _():
                push(mine, mine, fan_left.at[q], fan_in.at[q], me.left).start()

            push(mine, mine, fan_side.at[q], fan_other.at[q], me.side).start()

        def own_heads():
            @pl.when(owner)
            def _():
                keep_o.wait()
                arrived(head_rows(1 - me.c), edge.at[1], me.core)

            @pl.when(lender)
            def _():
                left_over(out_loc, edge.at[0], me.core)

        def ends(h):
            arrived(core_rows(gu_all.at[h])(1 - me.c), gu_split[h][2], me.core)
            line_ends(me, gu_slots[h], gu_line[h])

        def dn_ends():
            keep_d.wait()
            line_ends(me, dn_slots, dn_line)

        saved = pltpu.make_async_copy(n_buf, stash, local.at[0])
        fetch_n = pltpu.make_async_copy(stash, n_buf, local.at[0])

        def normed_here():
            group_finish(me, tok(n_buf).at[me.rank], tok(n_buf), *n_sems)
            left_over(q_share, q_split[1], me.core)
            for h in range(2):
                left_over(gu_share[h], gu_split[h][1], me.core)
            saved.start()

        def widen_weights():
            def widen(i, carry):
                feats = pl.ds(pl.multiple_of(i * tile, tile), tile)
                for k in range(2):
                    g_gu[feats, k * 4 * LANES:(k + 1) * 4 * LANES] = low(
                        dot32(qkv_all[feats, k * heads4:(k + 1) * heads4], sel_ref[...])
                    )
                return carry

            lax.fori_loop(0, width // tile, widen, 0)

        def project_tokens():
            def project(i, carry):
                toks = pl.ds(pl.multiple_of(i * length, length), length)
                n = n_buf[toks, :]
                tabs = [tab_ref[k] for k in range(3)]
                for k in range(8):
                    value = dot32(n, g_gu[:, k * LANES:(k + 1) * LANES])
                    heads[toks, k * LANES:(k + 1) * LANES] = low(turn(value, tabs, 1.0) if k < 6 else value)
                return carry

            lax.fori_loop(0, total // length, project, 0)

        def heads_here():
            saved.wait()
            for q in range(PIECES):
                arrived(bit(1 - me.y, q), fan_other.at[q], me.side)

        def pair(toks, j, ref, start):
            first = start + 2 * j * LANES
            return jnp.concatenate(
                [ref[toks, first:first + LANES], ref[toks, first + LANES:first + 2 * LANES]], 0
            )

        def probabilities(toks, j):
            q = pair(toks, j, heads, 0)
            k = heads[toks, (4 + j) * LANES:(5 + j) * LANES]
            scores = HD ** (-0.5) * dot_t(q, k)
            row = lax.rem(lax.broadcasted_iota(jnp.int32, scores.shape, 0), length)
            col = lax.broadcasted_iota(jnp.int32, scores.shape, 1)
            scores = jnp.where(row >= col, scores, -jnp.inf)
            exps = jnp.exp(scores - jnp.max(scores, 1, keepdims=True))
            return q, k, exps / jnp.sum(exps, 1, keepdims=True)

        def attend_rows(first):
            def one(i, carry):
                toks = pl.ds(pl.multiple_of(first + i * length, length), length)
                outs = []
                for j in range(2):
                    _, _, p = probabilities(toks, j)
                    o = low(dot32(low(p), heads[toks, (6 + j) * LANES:(7 + j) * LANES]))
                    outs += [o[:length], o[length:]]
                mixed[toks, :] = low(dot_t(jnp.concatenate(outs, 1), sel_ref[...]))
                return carry

            lax.fori_loop(0, rows // length, one, 0)
            toks = pl.ds(pl.multiple_of(first, rows), rows)
            part[toks, :] = low(dot32(mixed[toks, :], out_all[...]))

        def mine(strip):
            return pl.ds(pl.multiple_of(me.rank * rows + strip.start, STRIP), STRIP)

        def summed(strip, whole, some, rest):
            return (
                whole[mine(strip), :].astype(F32)
                + some[me.s, strip, :].astype(F32)
                + rest[strip, :].astype(F32)
            )

        def middle(strip):
            value = last_f[strip, :].astype(F32) + summed(strip, part, got, last)
            x1[strip, :] = value
            n_buf[mine(strip), :] = low(value * inv_rms(value))

        def first_sum():
            blocks_finish(me, tok(part), got, last, *x_sems)
            strips(rows, middle)
            group_start(me, tok(n_buf).at[me.rank], tok(n_buf), *m_sems)

        def cot_here():
            keep_g.wait()
            group_finish(me, g_loc, tok(g_all), *g_sems)

        def heads_left():
            for q in range(PIECES):
                left_over(bit(me.y, q), fan_side.at[q], me.side)

                @pl.when(go_right)
                def _():
                    left_over(bit(me.y, q), fan_right.at[q], me.right)

                @pl.when(go_left)
                def _():
                    left_over(bit(me.y, q), fan_left.at[q], me.left)

        def activations(h, j):
            first = h * half_units + j * chunk

            def step(t, carry):
                toks = pl.ds(pl.multiple_of(t * tile, tile), tile)
                n, g = n_buf[toks, :], g_all[toks, :]
                gate = dot32(n, gu_all[h, :, j * chunk:(j + 1) * chunk])
                up = dot32(n, gu_all[h, :, half_units + j * chunk:half_units + (j + 1) * chunk])
                grad = dot_t(g, dn_all[first:first + chunk, :])
                hidden, d_gate, d_up = mlp_grads(gate, up, grad)
                mid[toks, first:first + chunk] = hidden
                dgu[h, toks, j * chunk:(j + 1) * chunk] = d_gate
                dgu[h, toks, half_units + j * chunk:half_units + (j + 1) * chunk] = d_up
                return carry

            lax.fori_loop(0, total // tile, step, 0)

        def weight_grads(h, out):
            def step(i, carry):
                feats = pl.ds(pl.multiple_of(i * chunk, chunk), chunk)
                out[feats, :] = low(dot_l(n_buf[:, feats], dgu[h]))
                return carry

            lax.fori_loop(0, width // chunk, step, 0)

        own_gu = [by_chip(g_gu, 2 * depth), gu_slots[0]]
        finals = [gu_buf[h][0].at[me.z] for h in range(2)]

        def back(seq):
            toks = pl.ds(pl.multiple_of(seq * tile, tile), tile)

            def step(i, carry):
                feats = pl.ds(pl.multiple_of(i * chunk, chunk), chunk)
                value = dot_t(dgu[0, toks, :], gu_all[0, feats, :]) + dot_t(dgu[1, toks, :], gu_all[1, feats, :])
                part[toks, feats] = low(value)
                return carry

            lax.fori_loop(0, width // chunk, step, 0)

        def second_grads():
            weight_grads(1, gu_all.at[0])
            fetch_n.start()

        def outward():
            def forth(i, carry):
                feats = pl.ds(pl.multiple_of(i * chunk, chunk), chunk)
                out_part[:, feats] = low(dot32(mid[...], dn_all[:, feats]))
                return carry

            lax.fori_loop(0, width // chunk, forth, 0)
            for i in range(2):
                blocks_start(me, tok(out_part), got_f, *f_sems, i)

        def branch(strip):
            grad = norm_back(x1[strip, :], summed(strip, part, got, last), g_all[mine(strip), :].astype(F32))
            dx_all[mine(strip), :] = low(grad)

        def second_sum():
            blocks_finish(me, tok(part), got, last, *b_sems)
            strips(rows, branch)
            group_start(me, tok(dx_all).at[me.rank], tok(dx_all), *d_sems)

        def down_grads():
            def down(i, carry):
                these = pl.ds(pl.multiple_of(i * chunk, chunk), chunk)
                dn_all[these, :] = low(dot_l(mid[:, these], g_all[...]))
                return carry

            lax.fori_loop(0, units // chunk, down, 0)

        def spread_grads():
            def spread_out(t, carry):
                toks = pl.ds(pl.multiple_of(t * rows, rows), rows)
                grad = low(dot_t(dx_all[toks, :], out_all[...]))
                mid[toks, 0:4 * LANES] = low(dot32(grad, sel_ref[...]))
                return carry

            lax.fori_loop(0, 4, spread_out, 0)

        def out_grads():
            out_all[...] = low(dot_l(mixed[...], dx_all[...]))
            for q in range(PIECES):
                push(bit(1 - me.y, q), o_buf[0].at[pl.ds(q * piece, piece)], o_red.at[0, q], o_red.at[1, q], me.side).start()

        def attend_rows_back(first):
            def one(i, carry):
                toks = pl.ds(pl.multiple_of(first + i * length, length), length)
                tabs = [tab_ref[k] for k in range(3)]
                for j in range(2):
                    q, k, p = probabilities(toks, j)
                    v = heads[toks, (6 + j) * LANES:(7 + j) * LANES]
                    grad = pair(toks, j, mid, 0)
                    d_v = dot_l(low(p), grad)
                    d_p = dot_t(grad, v)
                    d_s = low(p * (d_p - jnp.sum(p * d_p, 1, keepdims=True)))
                    d_q = HD ** (-0.5) * dot32(d_s, k)
                    d_k = HD ** (-0.5) * dot_l(d_s, q)
                    for g in range(2):
                        spot = (2 * j + g) * LANES
                        dgu[0, toks, spot:spot + LANES] = low(turn(d_q[g * length:(g + 1) * length], tabs, -1.0))
                    dgu[0, toks, (4 + j) * LANES:(5 + j) * LANES] = low(turn(d_k, tabs, -1.0))
                    dgu[0, toks, (6 + j) * LANES:(7 + j) * LANES] = low(d_v)
                return carry

            lax.fori_loop(0, rows // length, one, 0)
            toks = pl.ds(pl.multiple_of(first, rows), rows)
            for k in range(2):
                dgu[1, toks, k * heads4:(k + 1) * heads4] = low(
                    dot_t(dgu[0, toks, k * 4 * LANES:(k + 1) * 4 * LANES], sel_ref[...])
                )
            part[toks, :] = low(dot_t(dgu[1, toks, 0:q_cols], qkv_all[...]))

        def in_grads():
            fetch_n.wait()

            def q_grads(i, carry):
                feats = pl.ds(pl.multiple_of(i * chunk, chunk), chunk)
                qkv_all[feats, :] = low(dot_l(n_buf[:, feats], dgu[1, :, 0:q_cols]))
                return carry

            lax.fori_loop(0, width // chunk, q_grads, 0)

        o_sum = lambda q: o_buf[0].at[pl.ds(q * piece, piece)]
        o_left = lambda q: o_buf[1].at[pl.ds(q * piece, piece)]
        o_right = lambda q: o_buf[2].at[pl.ds(q * piece, piece)]

        def o_on(q):
            @pl.when(me.z < me.rank)
            def _():
                push(o_sum(q), o_left(q), o_red.at[4, q], o_red.at[2, q], me.right).start()

            @pl.when(me.z > me.rank)
            def _():
                push(o_sum(q), o_right(q), o_red.at[4, q], o_red.at[3, q], me.left).start()

        from_left = jnp.logical_and(me.has_left, me.z <= me.rank)
        from_right = jnp.logical_and(me.has_right, me.z >= me.rank)
        no_more = jnp.logical_not(jnp.logical_or(from_left, from_right))

        def o_y(q):
            arrived(o_sum(q), o_red.at[1, q], me.side)
            add_into(o_sum(q), bit(me.y, q))

            @pl.when(no_more)
            def _():
                o_on(q)

        def o_z(q):
            @pl.when(from_left)
            def _():
                arrived(o_left(q), o_red.at[2, q], me.left)
                add_into(o_sum(q), o_left(q))

            @pl.when(from_right)
            def _():
                arrived(o_right(q), o_red.at[3, q], me.right)
                add_into(o_sum(q), o_right(q))

            @pl.when(jnp.logical_not(no_more))
            def _():
                o_on(q)

        own_half = o_buf[0].at[pl.ds(pl.multiple_of(me.c * head, STRIP), head)]
        other_half = o_buf[0].at[pl.ds(pl.multiple_of((1 - me.c) * head, STRIP), head)]
        o_keep, o_send, o_recv = o_deal
        keep_oo = pltpu.make_async_copy(own_half, out_out, o_keep)


        def o_end():
            @pl.when(owner)
            def _():
                keep_oo.start()
                push(other_half, out_out, o_send.at[0], o_recv.at[0], me.core).start()
                push(own_half, out_out, o_send.at[1], o_recv.at[0], me.across).start()
                push(other_half, out_out, o_send.at[2], o_recv.at[0], me.corner).start()

        def output(strip):
            got_f[me.s, strip, :] = low(x1[strip, :] + summed(strip, out_part, got_f, last_f))

        def third_sum():
            blocks_finish(me, tok(out_part), got_f, last_f, *f_sems)
            strips(rows, output)
            pltpu.make_async_copy(got_f.at[me.s], bo_ref, local.at[1]).start()
            fetch_x.start()

        def inner(strip):
            got[me.s, strip, :] = low(norm_back(
                last_f[strip, :].astype(F32), summed(strip, part, got, last), dx_all[mine(strip), :].astype(F32)
            ))

        def fourth_sum():
            blocks_finish(me, tok(part), got, last, *h_sems)
            fetch_x.wait()
            strips(rows, inner)
            pltpu.make_async_copy(got.at[me.s], gx_ref, local.at[2]).start()

        final_dn = dn_buf[0].at[me.z]
        final_q = [q_buf[k][0].at[me.z] for k in range(2)]
        own_q = [functools.partial(lambda k, chip: core_rows_of(chip, k), k) for k in range(2)]
        q_keep, q_send, q_recv = q_deal

        def core_rows_of(chip, core):
            return qkv_all.at[pl.ds(pl.multiple_of((2 * chip + core) * depth, STRIP), depth)]

        def q_end(core):
            @pl.when(me.c == core)
            def _():
                pltpu.make_async_copy(final_q[core], qkv_out.at[me.rank], q_keep).start()
                push(final_q[core], qkv_out.at[me.rank], q_send.at[0], q_recv.at[0], me.across).start()

            @pl.when(me.c != core)
            def _():
                push(final_q[core], qkv_out.at[me.rank], q_send.at[1], q_recv.at[1], me.core).start()
                push(final_q[core], qkv_out.at[me.rank], q_send.at[2], q_recv.at[2], me.corner).start()
        dn_keep, dn_send, dn_recv = dn_deal

        def dn_end():
            pltpu.make_async_copy(final_dn, dn_out.at[me.s], dn_keep).start()
            push(final_dn, dn_out.at[me.s], dn_send, dn_recv, me.across).start()

        steps = {
            "weigh": weigh_units, "own": own_heads, "rn": lambda: group_relay(me, tok(n_buf), *n_sems),
            "Ae": lambda: ends(0), "Be": lambda: ends(1), "De": dn_ends, "nf": normed_here,
            "widen": widen_weights, "project": project_tokens, "oh": heads_here,
            "rg": lambda: group_relay(me, tok(g_all), *g_sems), "gf": cot_here, "ol": heads_left,
            "xs": first_sum, "rm": lambda: group_relay(me, tok(n_buf), *m_sems),
            "mf": lambda: group_finish(me, tok(n_buf).at[me.rank], tok(n_buf), *m_sems),
            "w0": lambda: weight_grads(0, g_gu), "w1": second_grads,
            "b0": lambda: back(away), "b1": lambda: back(home), "fo": outward, "bs": second_sum, "dw": down_grads,
            "rx": lambda: group_relay(me, tok(dx_all), *d_sems),
            "xf": lambda: group_finish(me, tok(dx_all).at[me.rank], tok(dx_all), *d_sems),
            "sp": spread_grads, "go": out_grads, "qg": in_grads, "oe": o_end, "fs": third_sum, "hs": fourth_sum,
            "fc": lambda: blocks_cross(me, tok(out_part), got_f, last_f, *f_sems),
            "de": dn_end, "ae": lambda: deal_start(me, finals[0], depth, gu_out.at[0], *gu_deal[0]),
            "be": lambda: deal_start(me, finals[1], depth, gu_out.at[1], *gu_deal[1]),
            "qe": lambda: q_end(0), "je": lambda: q_end(1),
        }
        for key, slots, line in (
            ("Q", q_slots, q_line), ("A", gu_slots[0], gu_line[0]), ("B", gu_slots[1], gu_line[1]), ("D", dn_slots, dn_line)
        ):
            steps[key + "s"] = functools.partial(line_side, me, slots, line)
            steps[key + "t"] = functools.partial(line_twin, me, slots, line)
            steps[key + "f"] = functools.partial(line_finish, me, slots, line)
            for hop in range(1, planes):
                steps[key + str(hop)] = functools.partial(line_hop, me, slots, line, hop)
        for key, own, buffers, sems in (
            ("a", own_gu[0], gu_buf[0], gu_sems[0]), ("b", own_gu[1], gu_buf[1], gu_sems[1]),
            ("d", dn_slots, dn_buf, dn_sems), ("q", own_q[0], q_buf[0], q_sems[0]), ("j", own_q[1], q_buf[1], q_sems[1]),
        ):
            steps[key + "r0"] = functools.partial(reduce_start, me, own, buffers[0], sems, [0])
            steps[key + "r1"] = functools.partial(reduce_start, me, own, buffers[0], sems, range(1, planes))
            steps[key + "m"] = functools.partial(reduce_mix, me, own, buffers[0], sems)
            for i in range(planes):
                steps[key + "y" + str(i)] = functools.partial(reduce_y, me, own, *buffers, sems, i)
                steps[key + "z" + str(i)] = functools.partial(reduce_z, me, *buffers, sems, i)
        for i in range(PIECES):
            steps["f" + str(i)] = functools.partial(fan, i)
            steps["oy" + str(i)] = functools.partial(o_y, i)
            steps["oz" + str(i)] = functools.partial(o_z, i)
        for i, (seq, core) in enumerate(((away, 1 - me.c), (away, me.c), (home, 1 - me.c), (home, me.c))):
            steps["t" + str(i)] = functools.partial(attend_rows, (2 * seq + core) * rows)
            steps["h" + str(i)] = functools.partial(attend_rows_back, (2 * seq + core) * rows)
        for key, whole, some, rest, sems in (
            ("x", part, got, last, x_sems), ("p", part, got, last, b_sems), ("k", part, got, last, h_sems)
        ):
            for i in range(2):
                steps[key + str(i)] = functools.partial(blocks_start, me, tok(whole), some, *sems, i)
            steps[key + "c"] = functools.partial(blocks_cross, me, tok(whole), some, rest, *sems)
        for h in range(2):
            for j in range(half_units // chunk):
                steps["uv"[h] + str(j)] = functools.partial(activations, h, j)
        for name in SCHEDULE:
            steps[name]()

        for h in range(2):
            reduce_finish(me, own_gu[h], gu_buf[h][0], gu_sems[h])
            deal_finish(me, finals[h], depth, gu_out.at[h], *gu_deal[h])
        reduce_finish(me, dn_slots, dn_buf[0], dn_sems)
        for k in range(2):
            reduce_finish(me, own_q[k], q_buf[k][0], q_sems[k])
        for q in range(PIECES):
            sum_q = o_sum(q)
            left_over(bit(1 - me.y, q), o_red.at[0, q], me.side)

            @pl.when(me.z < me.rank)
            def _():
                left_over(sum_q, o_red.at[4, q], me.right)

            @pl.when(me.z > me.rank)
            def _():
                left_over(sum_q, o_red.at[4, q], me.left)

        @pl.when(owner)
        def _():
            keep_oo.wait()
            left_over(other_half, o_send.at[0], me.core)
            left_over(own_half, o_send.at[1], me.across)
            left_over(other_half, o_send.at[2], me.corner)

        @pl.when(jnp.logical_not(owner))
        def _():
            arrived(out_out, o_recv.at[0], me.core)

        pltpu.make_async_copy(final_dn, dn_out.at[me.s], dn_keep).wait()
        left_over(final_dn, dn_send, me.across)
        arrived(dn_out.at[1 - me.s], dn_recv, me.across)
        pltpu.make_async_copy(got_f.at[me.s], bo_ref, local.at[1]).wait()
        pltpu.make_async_copy(got.at[me.s], gx_ref, local.at[2]).wait()

        for core in range(2):

            @pl.when(me.c == core)
            def _():
                pltpu.make_async_copy(final_q[core], qkv_out.at[me.rank], q_keep).wait()
                left_over(final_q[core], q_send.at[0], me.across)

            @pl.when(me.c != core)
            def _():
                left_over(final_q[core], q_send.at[1], me.core)
                left_over(final_q[core], q_send.at[2], me.corner)

        arrived(qkv_out.at[2 * (1 - me.s) + me.c], q_recv.at[0], me.across)
        arrived(qkv_out.at[2 * me.s + 1 - me.c], q_recv.at[1], me.core)
        arrived(qkv_out.at[2 * (1 - me.s) + 1 - me.c], q_recv.at[2], me.corner)

    sems = lambda *dims: pltpu.SemaphoreType.DMA(dims)
    one, three = pltpu.SemaphoreType.DMA, sems(3)
    vmem = lambda *dims: pltpu.VMEM(dims, BF)
    deal = [one, three, three]
    outs = comm_call(
        kernel, 0,
        [shape((rows, width)), shape((rows, width)), shape((4, depth, q_cols)), shape((head, width)),
         shape((2, 4, depth, cols)), shape((2, block, width)), shape((total, width))],
        [ANY] * 7,
        [(ANY, ref) for ref in (tokens, cot, w_query, w_key, w_value, w_out, w_gate, w_up, w_down)]
        + [(VMEM, gain_attn), (VMEM, gain_mlp), (VMEM, head_tables(length))],
        [vmem(total, width), vmem(total, width), vmem(width, q_cols), vmem(heads4, width), vmem(2, width, cols),
         vmem(units, width), vmem(total, 8 * LANES), vmem(total, heads4)]
        + [vmem(total, width), vmem(total, width), pltpu.VMEM((rows, width), F32), vmem(total, units),
           vmem(2, total, cols), vmem(width, cols), vmem(total, width)]
        + blocks_buffers(rows, width) * 2
        + reduce_buffers(planes, 2 * depth, cols) * 2 + reduce_buffers(planes, block, width)
        + reduce_buffers(planes, depth, q_cols) * 2 + [vmem(2 * head, width)] * 3
        + group_sems() * 4 + blocks_sems() * 4 + [one] * 9
        + line_sems(planes) * 4 + reduce_sems(planes) * 5 + deal * 2 + [one] * 3 + deal * 2
        + [sems(5), sems(2), sems(5, PIECES), sems(5, PIECES), sems(3 + 8 * planes), vmem(heads4, 4 * LANES),
           pltpu.VMEM((2, depth, LANES), F32)],
        "block_step",
    )
    return outs[:6]


def finish(planes, parts, weights, gains):
    block_out, grad_tokens, own_qkv, own_out, own_gu, own_dn = parts
    w_query, w_key, w_value, w_gate, w_up = weights
    rows, width = block_out.shape
    depth, hidden = w_gate.shape
    q_own, k_own = w_query.shape[1] // 4, w_key.shape[1] // 4
    block = own_dn.shape[1]
    per = 4
    steps = 2 * planes // per
    wide = hidden // steps
    own_dn = own_dn.reshape(2 * block, width)

    def kernel(bo_ref, gx_ref, qkv_ref, out_ref, gate_ref, up_ref, dn_ref, wq_ref, wk_ref, wv_ref, wg_ref, wu_ref,
               ga_ref, gm_ref, bo_out, gx_out, q_out, k_out, v_out, o_out, gate_out, up_out, dn_out, ga_out, gm_out,
               columns, total):
        step = pl.program_id(0)
        same = lax.broadcasted_iota(jnp.int32, (depth, depth), 0) == lax.broadcasted_iota(jnp.int32, (depth, depth), 1)

        def as_row(value):
            return jnp.sum(jnp.where(same, jnp.sum(value, 1, keepdims=True), 0.0), 0, keepdims=True)

        @pl.when(step == 0)
        def _():
            for k, ref in enumerate((ga_ref, gm_ref)):
                column = jnp.sum(jnp.where(same, ref[...].astype(F32), 0.0), 1, keepdims=True)
                columns[k] = jnp.broadcast_to(column, (depth, LANES))
            total[...] = jnp.zeros_like(total)
            o_out[...] = out_ref[...].astype(F32)
            gain = columns[0]
            gathered = jnp.zeros((depth, LANES), F32)

            def put(out, weight, tile, value):
                lanes = slice(tile * LANES, (tile + 1) * LANES)
                out[:, lanes] = value * gain
                return value * weight[:, lanes].astype(F32)

            rolled = lambda value: pltpu.roll(value, LANES // 2, 1)
            in_low = lax.broadcasted_iota(jnp.int32, (depth, LANES), 1) < LANES // 2
            join = lambda first, second: jnp.where(in_low, first, second)
            for rank in range(4):
                for k in range(q_own // LANES):
                    value = qkv_ref[rank, :, k * LANES:(k + 1) * LANES].astype(F32)
                    gathered += put(q_out, wq_ref, rank * q_own // LANES + k, value)
            for seq in range(2):
                (a0, a1, a2), (b0, b1, b2) = [
                    [qkv_ref[2 * seq + core, :, q_own + k * LANES:q_own + (k + 1) * LANES].astype(F32) for k in range(3)]
                    for core in range(2)
                ]
                keys = [a0, join(a1, rolled(b0)), join(rolled(b0), rolled(b1))]
                values = [join(rolled(a1), rolled(a2)), join(rolled(a2), b1), b2]
                for k in range(3):
                    gathered += put(k_out, wk_ref, 3 * seq + k, keys[k])
                    gathered += put(v_out, wv_ref, 3 * seq + k, values[k])
            ga_out[...] = as_row(gathered)

        bo_out[...] = bo_ref[...]
        gx_out[...] = gx_ref[...]
        dn_out[...] = dn_ref[...].astype(F32)
        gain = columns[1]
        gathered = jnp.zeros((depth, LANES), F32)
        for ref, out, weight in ((gate_ref, gate_out, wg_ref), (up_ref, up_out, wu_ref)):
            for k in range(4 * per):
                chip, core, seq = k // 4, k // 2 % 2, k % 2
                lanes = slice(k * block, (k + 1) * block)
                value = ref[0, 2 * seq + core, :, chip * block:(chip + 1) * block].astype(F32)
                out[:, lanes] = value * gain
                gathered += value * weight[:, lanes].astype(F32)
        total[...] += gathered

        @pl.when(step == steps - 1)
        def _():
            gm_out[...] = as_row(total[...])

    whole = lambda ref: pl.BlockSpec(ref.shape, lambda p: (0,) * len(ref.shape))
    strip = lambda ref: pl.BlockSpec((ref.shape[0] // steps, ref.shape[1]), lambda p: (p, 0))
    runs = planes // per
    part = lambda first: pl.BlockSpec((1, 4, depth, per * block), lambda p: (p // runs, 0, 0, first + p % runs))
    slab = pl.BlockSpec((depth, wide), lambda p: (0, p))
    outs = [shape(block_out.shape), shape(grad_tokens.shape), shape(w_query.shape, F32), shape(w_key.shape, F32),
            shape(w_value.shape, F32), shape(own_out.shape, F32), shape(w_gate.shape, F32), shape(w_up.shape, F32),
            shape(own_dn.shape, F32), shape((1, depth), F32), shape((1, depth), F32)]
    return pl.pallas_call(
        kernel,
        grid=(steps,),
        out_shape=outs,
        in_specs=[strip(block_out), strip(grad_tokens), whole(own_qkv), whole(own_out), part(0), part(runs),
                  strip(own_dn), whole(w_query), whole(w_key), whole(w_value), slab, slab, whole(gains[0]), whole(gains[1])],
        out_specs=[strip(outs[0]), strip(outs[1])] + [whole(o) for o in outs[2:6]]
        + [slab, slab, strip(outs[8]), whole(outs[9]), whole(outs[10])],
        scratch_shapes=[pltpu.VMEM((2, depth, LANES), F32), pltpu.VMEM((depth, LANES), F32)],
        name="finish",
    )(block_out, grad_tokens, own_qkv, own_out, own_gu, own_gu, own_dn, w_query, w_key, w_value, w_gate, w_up, *gains)


def shards_fast(tokens, cotangent, w_query, w_key, w_value, w_out, w_gate, w_up, w_down, gain_attn, gain_mlp):
    seqs, length, width = tokens.shape
    rows = seqs * length
    depth = w_query.shape[0]
    planes = width // depth // 4
    x, cot = tokens.reshape(rows, width), cotangent.reshape(rows, width)
    gains = (gain_attn.reshape(1, depth), gain_mlp.reshape(1, depth))
    parts = block_step(planes, length, x, cot, w_query, w_key, w_value, w_out, w_gate, w_up, w_down, *gains)
    outs = finish(planes, parts, (w_query, w_key, w_value, w_gate, w_up), gains)
    return (
        outs[0].reshape(tokens.shape), outs[1].reshape(tokens.shape), *outs[2:9],
        outs[9].reshape(depth), outs[10].reshape(depth),
    )


def fits(mesh):
    return mesh.shape["seq"] == 2 and mesh.shape["dp"] == 16


def solution(mesh):
    body = shards_fast if fits(mesh) else shards_plain
    return jax.shard_map(body, mesh=mesh, in_specs=IN_SPECS, out_specs=OUT_SPECS, check_vma=False)
```

```python
import jax
import jax.numpy as jnp
import functools
import numpy as np
from jax import lax
from jax.experimental import pallas as pl
from jax.experimental.pallas import tpu as pltpu
from jax.sharding import PartitionSpec as P

HD = 96
EPS = 1e-05
THETA = 100000.0


def rotary(positions, width):
    steps_half = jnp.arange(width // 2, dtype=jnp.float32)
    frequency = jnp.power(THETA, -2.0 * steps_half / width)
    angles = positions[:, None] * frequency[None, :]
    cosine = jnp.cos(angles)
    sine = jnp.sin(angles)
    return (jnp.concatenate([cosine, cosine], -1), jnp.concatenate([sine, sine], -1))


def rotate(values, cosine, sine):
    half = values.shape[-1] // 2
    turned = jnp.concatenate([-values[..., half:], values[..., :half]], -1)
    return values * cosine[:, None, :] + turned * sine[:, None, :]


def rotate_back(grads, cosine, sine):
    half = grads.shape[-1] // 2
    sined = grads * sine[:, None, :]
    turned = jnp.concatenate([sined[..., half:], -sined[..., :half]], -1)
    return grads * cosine[:, None, :] + turned


def dot32(left, right):
    return jnp.dot(left, right, preferred_element_type=jnp.float32)


def dot_t(left, right):
    return lax.dot_general(left, right, (((1,), (1,)), ((), ())), preferred_element_type=jnp.float32)


def dot_l(left, right):
    return lax.dot_general(left, right, (((0,), (0,)), ((), ())), preferred_element_type=jnp.float32)


def inv_rms(values):
    return lax.rsqrt(jnp.mean(values * values, axis=-1, keepdims=True) + EPS)


def low(values):
    return values.astype(jnp.bfloat16)


def attend(queries, keys, values):
    rows = queries.shape[1]
    ids = jnp.arange(rows, dtype=jnp.int32)
    visible = ids[:, None] >= ids[None, :]
    scores = HD ** (-0.5) * jnp.einsum("bqkgd,bckd->bkgqc", queries, keys, preferred_element_type=jnp.float32)
    scores = jnp.where(visible, scores, -jnp.inf)
    top = jnp.max(scores, -1, keepdims=True)
    exps = jnp.exp(scores - top)
    probs = exps / jnp.sum(exps, -1, keepdims=True)
    mixed = jnp.einsum("bkgqc,bckd->bqkgd", low(probs), values, preferred_element_type=jnp.float32)
    return probs, low(mixed)


def attend_back(queries, keys, values, probs, grad_mixed):
    grad_values = jnp.einsum("bkgqc,bqkgd->bckd", low(probs), grad_mixed, preferred_element_type=jnp.float32)
    grad_probs = jnp.einsum("bqkgd,bckd->bkgqc", grad_mixed, values, preferred_element_type=jnp.float32)
    grad_scores = low(probs * (grad_probs - jnp.sum(probs * grad_probs, -1, keepdims=True)))
    scale = HD ** (-0.5)
    grad_queries = scale * jnp.einsum("bkgqc,bckd->bqkgd", grad_scores, keys, preferred_element_type=jnp.float32)
    grad_keys = scale * jnp.einsum("bkgqc,bqkgd->bckd", grad_scores, queries, preferred_element_type=jnp.float32)
    return grad_queries, grad_keys, grad_values


def mlp_grads(gate, up, grad_hidden):
    sigma = jax.nn.sigmoid(gate)
    silu = gate * sigma
    hidden = low(silu * up)
    grad_gate = low(grad_hidden * up * sigma * (1.0 + gate * (1.0 - sigma)))
    grad_up = low(grad_hidden * silu)
    return hidden, grad_gate, grad_up


def shards_plain(tokens, cotangent, w_query, w_key, w_value, w_out, w_gate, w_up, w_down, gain_attn, gain_mlp):
    seqs, length, width = tokens.shape
    rows = seqs * length
    kv_heads = w_key.shape[1] // HD
    groups = w_query.shape[1] // w_key.shape[1]
    gather = lambda w: lax.all_gather(w, "dp", axis=0, tiled=True)
    full_query, full_key, full_value, full_out = map(gather, (w_query, w_key, w_value, w_out))
    gains = gather(jnp.stack([gain_attn, gain_mlp], 1)).astype(jnp.float32)
    gain_one, gain_two = gains[:, 0], gains[:, 1]
    full_gate, full_up, full_down = map(gather, (w_gate, w_up, w_down))
    cosine, sine = rotary(jnp.arange(length, dtype=jnp.float32), HD)
    cosine, sine = jnp.tile(cosine, (seqs, 1)), jnp.tile(sine, (seqs, 1))

    inputs = tokens.reshape(rows, width).astype(jnp.float32)
    grad_in = cotangent.reshape(rows, width)
    scale_one = inv_rms(inputs)
    normed = low(inputs * scale_one * gain_one)
    queries = low(rotate(dot32(normed, full_query).reshape(rows, -1, HD), cosine, sine))
    keys = low(rotate(dot32(normed, full_key).reshape(rows, -1, HD), cosine, sine))
    values = low(dot32(normed, full_value))
    queries = queries.reshape(seqs, length, kv_heads, groups, HD)
    keys = keys.reshape(seqs, length, kv_heads, HD)
    values = values.reshape(seqs, length, kv_heads, HD)
    probs, mixed = attend(queries, keys, values)
    mixed = mixed.reshape(rows, -1)
    hidden_one = inputs + dot32(mixed, full_out)
    scale_two = inv_rms(hidden_one)
    normed_two = low(hidden_one * scale_two * gain_two)
    gate, up = dot32(normed_two, full_gate), dot32(normed_two, full_up)
    hidden, grad_gate, grad_up = mlp_grads(gate, up, dot_t(grad_in, full_down))
    block_out = low(hidden_one + dot32(hidden, full_down))

    acc_down = dot_l(hidden, grad_in)
    acc_gate = dot_l(normed_two, grad_gate)
    acc_up = dot_l(normed_two, grad_up)
    grad_normed_two = dot_t(grad_gate, full_gate) + dot_t(grad_up, full_up)
    acc_gain_two = jnp.sum(grad_normed_two * hidden_one * scale_two, 0)
    weighted = grad_normed_two * gain_two
    grad_one = grad_in.astype(jnp.float32) + scale_two * (
        weighted - hidden_one * scale_two * scale_two * jnp.mean(weighted * hidden_one, -1, keepdims=True)
    )
    grad_branch = low(grad_one)
    acc_out = dot_l(mixed, grad_branch)
    grad_mixed = low(dot_t(grad_branch, full_out)).reshape(queries.shape)
    grad_queries, grad_keys, grad_values = attend_back(queries, keys, values, probs, grad_mixed)
    grad_queries = low(rotate_back(grad_queries.reshape(rows, -1, HD), cosine, sine)).reshape(rows, -1)
    grad_keys = low(rotate_back(grad_keys.reshape(rows, -1, HD), cosine, sine)).reshape(rows, -1)
    grad_values = low(grad_values).reshape(rows, -1)
    acc_query = dot_l(normed, grad_queries)
    acc_key = dot_l(normed, grad_keys)
    acc_value = dot_l(normed, grad_values)
    grad_normed = dot_t(grad_queries, full_query) + dot_t(grad_keys, full_key) + dot_t(grad_values, full_value)
    acc_gain_one = jnp.sum(grad_normed * inputs * scale_one, 0)
    weighted = grad_normed * gain_one
    grad_tokens = grad_one + scale_one * (
        weighted - inputs * scale_one * scale_one * jnp.mean(weighted * inputs, -1, keepdims=True)
    )

    def share(acc):
        owned = lax.psum_scatter(low(acc), "dp", scatter_dimension=0, tiled=True)
        return lax.psum(owned, "seq").astype(jnp.float32)

    grads = [share(a) for a in (acc_down, acc_gate, acc_up, acc_out, acc_query, acc_key, acc_value)]
    gain_grads = lax.psum(
        lax.psum_scatter(jnp.stack([acc_gain_one, acc_gain_two], 1), "dp", scatter_dimension=0, tiled=True), "seq"
    )
    down, gate, up, out, query, key, value = grads
    return (
        block_out.reshape(tokens.shape),
        low(grad_tokens).reshape(tokens.shape),
        query, key, value, out, gate, up, down,
        gain_grads[:, 0], gain_grads[:, 1],
    )


ROWS = P(("dp", "seq"), None, None)
SPLIT = P("dp", None)
IN_SPECS = (ROWS, ROWS) + (SPLIT,) * 7 + (P("dp"), P("dp"))
OUT_SPECS = (ROWS, ROWS) + (SPLIT,) * 7 + (P("dp"), P("dp"))


MESH = pl.DeviceIdType.MESH
VMEM = pl.BlockSpec(memory_space=pltpu.VMEM)
ANY = pl.BlockSpec(memory_space=pl.ANY)
BF = jnp.bfloat16
F32 = jnp.float32
STRIP = 16
PIECES = 4
VMEM_BYTES = 67_043_328


class Place:
    def __init__(self, planes):
        self.planes = planes
        d = lax.axis_index("dp")
        self.d, self.s = d, lax.axis_index("seq")
        self.c, self.y, self.z = d % 2, (d // 2) % 2, d // 4
        self.p = d // 2
        self.rank = 2 * self.s + self.c
        self.core = (d + 1 - 2 * self.c, self.s)
        self.across = (d, 1 - self.s)
        self.corner = (d + 1 - 2 * self.c, 1 - self.s)
        self.side = (d + 2 - 4 * self.y, self.s)
        self.right = (lax.rem(d + 4, 4 * planes), self.s)
        self.left = (lax.rem(d + 4 * planes - 4, 4 * planes), self.s)
        self.has_right, self.has_left = self.z < planes - 1, self.z > 0
        odd = self.z % 2
        self.twin = self.z + 1 - 2 * odd
        self.buddy = (d + 4 - 8 * odd, self.s)


def greet(me):
    barrier = pltpu.get_barrier_semaphore()
    for peer in (me.core, me.across, me.corner, me.side, me.right, me.left):
        pl.semaphore_signal(barrier, inc=1, device_id=peer, device_id_type=MESH)


def met():
    pl.semaphore_wait(pltpu.get_barrier_semaphore(), 6)


def push(src, dst, send, recv, peer):
    return pltpu.make_async_remote_copy(
        src_ref=src, dst_ref=dst, send_sem=send, recv_sem=recv, device_id=peer, device_id_type=MESH
    )


def arrived(dst, recv, peer):
    push(dst, dst, recv, recv, peer).wait_recv()


def left_over(src, send, peer):
    push(src, src, send, send, peer).wait_send()


class Slots:
    def __init__(self, ref, rows):
        self.ref, self.rows = ref, rows
        self.at = self

    def __getitem__(self, block):
        return self.ref.at[pl.ds(pl.multiple_of(block * self.rows, self.rows), self.rows)]


def group_start(me, src, dst, send, recv):
    push(src, dst.at[me.rank], send.at[0], recv.at[0], me.core).start()
    push(src, dst.at[me.rank], send.at[1], recv.at[1], me.across).start()


def group_relay(me, dst, send, recv):
    slot = dst.at[2 * (1 - me.s) + me.c]
    arrived(slot, recv.at[1], me.across)
    push(slot, slot, send.at[2], recv.at[2], me.core).start()


def group_finish(me, src, dst, send, recv):
    arrived(dst.at[2 * me.s + 1 - me.c], recv.at[0], me.core)
    arrived(dst.at[2 * (1 - me.s) + 1 - me.c], recv.at[2], me.core)
    left_over(src, send.at[0], me.core)
    left_over(src, send.at[1], me.across)
    slot = dst.at[2 * (1 - me.s) + me.c]
    left_over(slot, send.at[2], me.core)


def group_sems():
    return [pltpu.SemaphoreType.DMA((3,)), pltpu.SemaphoreType.DMA((3,))]


def upper(slot):
    return slot.at[pl.ds(0, slot.shape[0] // 2)]


def lower(slot):
    return slot.at[pl.ds(slot.shape[0] // 2, slot.shape[0] // 2)]


def line_start(me, dst, sems):
    line_side(me, dst, sems)
    line_ends(me, dst, sems)


def line_side(me, dst, sems):
    to_right, to_left, line, to_side, side, twin = sems
    slot = dst(me.p)
    push(slot, slot, to_side.at[me.z], side.at[me.z], me.side).start()


def line_ends(me, dst, sems):
    to_right, to_left, line, to_side, side, twin = sems
    slot = dst(me.p)

    @pl.when(me.has_right)
    def _():
        push(slot, slot, to_right.at[me.z], line.at[me.z], me.right).start()

    @pl.when(me.has_left)
    def _():
        push(slot, slot, to_left.at[me.z], line.at[me.z], me.left).start()


def line_hop(me, dst, sems, hop):
    to_right, to_left, line, to_side, side, twin = sems

    def pass_on(item, back, forth, may, sends):
        slot = dst(2 * item + me.y)
        arrived(slot, line.at[item], back)

        @pl.when(may)
        def _():
            push(slot, slot, sends.at[item], line.at[item], forth).start()

        if hop > 1:
            push(slot, slot, to_side.at[item], side.at[item], me.side).start()
        else:

            @pl.when(item != me.twin)
            def _():
                push(slot, slot, to_side.at[item], side.at[item], me.side).start()

            @pl.when(item == me.twin)
            def _():
                half = upper(slot)
                push(half, half, to_side.at[item], side.at[item], me.side).start()

    @pl.when(me.z >= hop)
    def _():
        pass_on(me.z - hop, me.left, me.right, me.has_right, to_right)

    @pl.when(me.z + hop < me.planes)
    def _():
        pass_on(me.z + hop, me.right, me.left, me.has_left, to_left)


def line_twin(me, dst, sems):
    to_right, to_left, line, to_side, side, twin = sems
    slot = dst(2 * me.z + 1 - me.y)
    arrived(slot, side.at[me.z], me.side)
    half = lower(slot)
    push(half, half, twin.at[0], twin.at[1], me.buddy).start()


def line_finish(me, dst, sems):
    to_right, to_left, line, to_side, side, twin = sems
    for item in range(me.planes):
        slot, mine = dst(2 * item + 1 - me.y), dst(2 * item + me.y)

        @pl.when(item == me.twin)
        def _():
            arrived(upper(slot), side.at[item], me.side)
            arrived(lower(slot), twin.at[1], me.buddy)
            left_over(upper(mine), to_side.at[item], me.side)

        @pl.when(jnp.logical_and(item != me.twin, item != me.z))
        def _():
            arrived(slot, side.at[item], me.side)

        @pl.when(item != me.twin)
        def _():
            left_over(mine, to_side.at[item], me.side)

        @pl.when(item == me.z)
        def _():
            left_over(lower(slot), twin.at[0], me.buddy)

        @pl.when(jnp.logical_and(me.has_right, item <= me.z))
        def _():
            left_over(mine, to_right.at[item], me.right)

        @pl.when(jnp.logical_and(me.has_left, item >= me.z))
        def _():
            left_over(mine, to_left.at[item], me.left)


def line_sems(planes):
    return [pltpu.SemaphoreType.DMA((planes,))] * 5 + [pltpu.SemaphoreType.DMA((2,))]


def pick(table, index):
    value = jnp.int32(table[0])
    for i in range(1, len(table)):
        value = jnp.where(index == i, table[i], value)
    return value


def far_first(planes):
    return [sorted(range(planes), key=lambda i, z=z: (-abs(i - z), i)) for z in range(planes)]


def add_into(dst, *others):
    rows = dst.shape[0]

    def body(i, carry):
        strip = pl.ds(pl.multiple_of(i * STRIP, STRIP), STRIP)
        total = dst[strip, :].astype(F32)
        for other in others:
            total = total + other[strip, :].astype(F32)
        dst[strip, :] = total.astype(dst.dtype)
        return carry

    lax.fori_loop(0, rows // STRIP, body, 0)


def reduce_start(me, own, half, sems, which):
    to_side, side, twin = sems[0], sems[1], sems[6]
    orders = far_first(me.planes)
    if 0 in which:
        away = lower(own(2 * me.twin + 1 - me.y))
        push(away, lower(half.at[me.z]), twin.at[0], twin.at[1], me.buddy).start()
    for i in which:
        item = pick([o[i] for o in orders], me.z)
        src, dst = own(2 * item + 1 - me.y), half.at[item]

        @pl.when(item == me.twin)
        def _():
            push(upper(src), upper(dst), to_side.at[item], side.at[item], me.side).start()

        @pl.when(jnp.logical_and(item != me.twin, item != me.z))
        def _():
            push(src, dst, to_side.at[item], side.at[item], me.side).start()


def reduce_mix(me, own, half, sems):
    to_side, side, twin = sems[0], sems[1], sems[6]
    mixed, got = own(2 * me.z + 1 - me.y), lower(half.at[me.twin])
    arrived(got, twin.at[1], me.buddy)
    add_into(lower(mixed), got)
    push(mixed, half.at[me.z], to_side.at[me.z], side.at[me.z], me.side).start()


def reduce_y(me, own, half, lines, sems, i):
    to_side, side, to_right, to_left, left, right, twin = sems
    item = pick([o[i] for o in far_first(me.planes)], me.z)
    mine, ours = half.at[item], own(2 * item + me.y)

    @pl.when(item == me.twin)
    def _():
        arrived(upper(mine), side.at[item], me.side)
        add_into(upper(mine), upper(ours))
        copy_into(lower(mine), lower(ours))

    @pl.when(item != me.twin)
    def _():
        arrived(mine, side.at[item], me.side)
        add_into(mine, ours)

    @pl.when(jnp.logical_and(item > me.z, jnp.logical_not(me.has_left)))
    def _():
        push(mine, lines.at[item], to_right.at[item], left.at[item], me.right).start()

    @pl.when(jnp.logical_and(item < me.z, jnp.logical_not(me.has_right)))
    def _():
        there = jnp.where(item == me.z - 1, me.planes, item)
        push(mine, lines.at[there], to_left.at[item], right.at[item], me.left).start()


def reduce_z(me, half, lines, sems, i):
    to_side, side, to_right, to_left, left, right, twin = sems
    item = pick([o[i] for o in far_first(me.planes)], me.z)
    mine = half.at[item]
    spot = jnp.where(item == me.z, me.planes, item)

    @pl.when(jnp.logical_and(me.has_left, item >= me.z))
    def _():
        arrived(lines.at[item], left.at[item], me.left)
        add_into(mine, lines.at[item])

        @pl.when(item > me.z)
        def _():
            push(mine, lines.at[item], to_right.at[item], left.at[item], me.right).start()

    @pl.when(jnp.logical_and(me.has_right, item <= me.z))
    def _():
        arrived(lines.at[spot], right.at[item], me.right)
        add_into(mine, lines.at[spot])

        @pl.when(item < me.z)
        def _():
            there = jnp.where(item == me.z - 1, me.planes, item)
            push(mine, lines.at[there], to_left.at[item], right.at[item], me.left).start()


def reduce_finish(me, own, half, sems):
    to_side, side, to_right, to_left, left, right, twin = sems
    left_over(lower(own(2 * me.twin + 1 - me.y)), twin.at[0], me.buddy)
    for item in range(me.planes):
        sent = own(2 * item + 1 - me.y)

        @pl.when(item == me.twin)
        def _():
            left_over(upper(sent), to_side.at[item], me.side)

        @pl.when(item != me.twin)
        def _():
            left_over(sent, to_side.at[item], me.side)

        @pl.when(item > me.z)
        def _():
            left_over(half.at[item], to_right.at[item], me.right)

        @pl.when(item < me.z)
        def _():
            left_over(half.at[item], to_left.at[item], me.left)


def reduce_sems(planes):
    return [pltpu.SemaphoreType.DMA((planes,))] * 6 + [pltpu.SemaphoreType.DMA((2,))]


def copy_into(dst, src):
    def body(i, carry):
        strip = pl.ds(pl.multiple_of(i * STRIP, STRIP), STRIP)
        dst[strip, :] = src[strip, :]
        return carry

    lax.fori_loop(0, dst.shape[0] // STRIP, body, 0)


def reduce_buffers(planes, rows, columns):
    return [pltpu.VMEM((planes, rows, columns), BF), pltpu.VMEM((planes + 1, rows, columns), BF)]


def by_chip(ref, rows=None):
    if rows is None:
        return lambda chip: ref.at[chip]
    return lambda chip: ref.at[pl.ds(pl.multiple_of(chip * rows, STRIP), rows)]


def deal_start(me, final, rows, out, local, send, recv):
    mine = out.at[me.rank]
    part = lambda core: final.at[pl.ds(pl.multiple_of(core * rows, rows), rows)]
    pltpu.make_async_copy(part(me.c), mine, local).start()
    push(part(1 - me.c), mine, send.at[0], recv.at[0], me.core).start()
    push(part(me.c), mine, send.at[1], recv.at[1], me.across).start()
    push(part(1 - me.c), mine, send.at[2], recv.at[2], me.corner).start()


def deal_finish(me, final, rows, out, local, send, recv):
    part = lambda core: final.at[pl.ds(pl.multiple_of(core * rows, rows), rows)]
    pltpu.make_async_copy(part(me.c), out.at[me.rank], local).wait()
    left_over(part(1 - me.c), send.at[0], me.core)
    left_over(part(me.c), send.at[1], me.across)
    left_over(part(1 - me.c), send.at[2], me.corner)
    arrived(out.at[2 * me.s + 1 - me.c], recv.at[0], me.core)
    arrived(out.at[2 * (1 - me.s) + me.c], recv.at[1], me.across)
    arrived(out.at[2 * (1 - me.s) + 1 - me.c], recv.at[2], me.corner)


def blocks_start(me, part, got, send, recv, i):
    seq = (1 - me.s, me.s)[i]
    push(part.at[2 * seq + 1 - me.c], got.at[seq], send.at[i], recv.at[i], me.core).start()


def blocks_cross(me, part, got, last, send, recv):
    away = 1 - me.s
    arrived(got.at[away], recv.at[0], me.core)
    add_into(got.at[away], part.at[2 * away + me.c])
    push(got.at[away], last, send.at[2], recv.at[2], me.across).start()


def blocks_finish(me, part, got, last, send, recv):
    arrived(got.at[me.s], recv.at[1], me.core)
    arrived(last, recv.at[2], me.across)
    for i, seq in enumerate((1 - me.s, me.s)):
        left_over(part.at[2 * seq + 1 - me.c], send.at[i], me.core)
    left_over(got.at[1 - me.s], send.at[2], me.across)


def blocks_sems():
    return [pltpu.SemaphoreType.DMA((3,))] * 2


def blocks_buffers(rows, width):
    return [pltpu.VMEM((2, rows, width), BF), pltpu.VMEM((rows, width), BF)]


def strips(rows, body):
    def step(i, carry):
        body(pl.ds(pl.multiple_of(i * STRIP, STRIP), STRIP))
        return carry

    lax.fori_loop(0, rows // STRIP, step, 0)


def comm_call(kernel, ident, outs, out_specs, ins, scratch, name):
    return pl.pallas_call(
        kernel,
        out_shape=outs,
        in_specs=[spec for spec, _ in ins],
        out_specs=out_specs,
        scratch_shapes=scratch,
        name=name,
        compiler_params=pltpu.CompilerParams(
            collective_id=ident, has_side_effects=True, vmem_limit_bytes=VMEM_BYTES
        ),
    )(*[value for _, value in ins])


def shape(dims, dtype=BF):
    return jax.ShapeDtypeStruct(dims, dtype)


def split_start(me, parts, dst, keep, send, recv):
    pltpu.make_async_copy(parts.at[me.c], dst(me.c), keep).start()
    push(parts.at[1 - me.c], dst(me.c), send, recv, me.core).start()


def split_finish(me, parts, dst, keep, send, recv):
    pltpu.make_async_copy(parts.at[me.c], dst(me.c), keep).wait()
    arrived(dst(1 - me.c), recv, me.core)
    left_over(parts.at[1 - me.c], send, me.core)


def norm_back(values, weighted, base):
    scale = inv_rms(values)
    return base + scale * (
        weighted - values * scale * scale * jnp.mean(weighted * values, -1, keepdims=True)
    )


LANES = 128


def head_tables(length):
    steps = np.arange(HD // 2, dtype=np.float64)
    angles = np.arange(length, dtype=np.float64)[:, None] * np.power(THETA, -2.0 * steps / HD)[None, :]
    cosine, sine, none = np.cos(angles), np.sin(angles), np.zeros_like(angles)
    tables = [(cosine, cosine), (none, sine), (-sine, none)]
    pad = ((0, 0), (0, LANES - HD))
    return np.stack([np.pad(np.concatenate(t, 1), pad) for t in tables]).astype(np.float32)


def turn(values, tables, sign):
    other = pltpu.roll(values, HD // 2, 1) * tables[1] + pltpu.roll(values, LANES - HD // 2, 1) * tables[2]
    return values * tables[0] + sign * other


SCHEDULE = (
    "weigh", "Q1", "Ae", "Q2", "As", "rn", "own", "f0", "f1", "f2", "Qt", "Q3", "f3", "A1", "De", "Be", "Qf",
    "Bs", "Ds", "widen", "nf", "project", "D1", "oh", "t0", "x0", "t1", "xc", "A2", "t2", "D2", "rg", "x1",
    "t3", "Dt", "A3", "At", "xs", "gf", "ol", "B1", "D3", "B2", "rm", "Af", "Df", "Bt", "mf", "u0", "B3",
    "u1", "w0", "ar0", "ar1", "Bf", "v0", "v1", "b0", "p0", "ay0", "am", "pc", "ay1", "b1", "p1", "w1", "br0",
    "az0", "ay2", "bs", "br1", "fo", "by0", "dw", "dr0", "az1", "ay3", "bm", "by1", "az2", "rx", "by2", "xf",
    "fc", "sp", "go", "bz0", "h0", "k0", "dy0", "az3", "h1", "dr1", "oy0", "kc", "bz1", "oy1", "bz2", "h2",
    "by3", "k1", "oy2", "ae", "oy3", "dm", "h3", "dz0", "dy1", "qg", "qr0", "jr0", "dy2", "oz0", "bz3", "be",
    "qr1", "oz1", "oz2", "jr1", "qy0", "oz3", "oe", "dz1", "jy0", "jm", "dy3", "dz2", "qm", "fs", "jy1",
    "qz0", "qy1", "jz0", "dz3", "jy2", "de", "qy2", "jy3", "jz1", "jz2", "qz1", "qy3", "hs", "qz2", "jz3",
    "je", "qz3", "qe",
)


def block_step(planes, length, tokens, cot, w_query, w_key, w_value, w_out, w_gate, w_up, w_down, gain_attn, gain_mlp):
    rows, width = tokens.shape
    total = 4 * rows
    depth = w_query.shape[0]
    head = w_out.shape[0]
    q_own, k_own = w_query.shape[1] // 4, w_key.shape[1] // 4
    q_cols = q_own + 2 * k_own
    block = w_down.shape[0] // 2
    units = 2 * planes * block
    half_units = units // 2
    cols = 2 * half_units
    tile, chunk = 2 * rows, 256
    heads4 = 4 * head
    piece = 2 * head // PIECES

    def kernel(x_ref, g_loc, wq_ref, wk_ref, wv_ref, out_loc, gate_ref, up_ref, down_ref, ga_ref, gm_ref, tab_ref,
               bo_ref, gx_ref, qkv_out, out_out, gu_out, dn_out, stash, *scr):
        it = iter(scr)
        take = lambda k: [next(it) for _ in range(k)]
        n_buf, g_all, qkv_all, out_all, gu_all, dn_all, heads, mixed = take(8)
        part, out_part, x1, mid, dgu, g_gu, dx_all = take(7)
        (got, last), (got_f, last_f) = take(2), take(2)
        gu_buf, dn_buf, q_buf, o_buf = [take(2), take(2)], take(2), [take(2), take(2)], take(3)
        n_sems, g_sems, m_sems, d_sems = take(2), take(2), take(2), take(2)
        x_sems, b_sems, f_sems, h_sems = take(2), take(2), take(2), take(2)
        q_split, gu_split = take(3), [take(3), take(3)]
        q_line, gu_line, dn_line = take(6), [take(6), take(6)], take(6)
        gu_sems, dn_sems, q_sems = [take(7), take(7)], take(7), [take(7), take(7)]
        gu_deal, dn_deal, q_deal, o_deal = [take(3), take(3)], take(3), take(3), take(3)
        local, edge, o_fan, o_red, fetch, sel_ref, gains = take(7)
        me = Place(planes)
        greet(me)
        tok = lambda ref: Slots(ref, rows)
        q_slots, dn_slots = by_chip(qkv_all, 2 * depth), by_chip(dn_all, block)
        gu_slots = [by_chip(gu_all.at[h], 2 * depth) for h in range(2)]

        def core_rows(ref):
            return lambda core: ref.at[pl.ds(pl.multiple_of((2 * me.p + core) * depth, STRIP), depth)]

        fetch_x = pltpu.make_async_copy(x_ref, last_f, local.at[4])
        fetch_x.start()
        stage = out_part.at[pl.ds(0, depth)]
        heads_in = []
        for i, (ref, spot, size) in enumerate(
            ((wq_ref, 0, 2 * q_own), (wk_ref, 2 * q_own, 2 * k_own), (wv_ref, 2 * q_own + 2 * k_own, 2 * k_own))
        ):
            src = ref.at[:, pl.ds(pl.multiple_of(me.s * size, LANES), size)]
            heads_in.append(pltpu.make_async_copy(src, stage.at[:, pl.ds(spot, size)], fetch.at[i]))
            heads_in[-1].start()

        q_share = q_buf[0][0].at[0]
        gu_share = [mid.at[pl.ds(h * depth, depth)] for h in range(2)]
        units_in = []
        for other in range(2):
            core = (me.c, 1 - me.c)[other]
            for h in range(2):
                dst = (core_rows(gu_all.at[h])(me.c), gu_share[h])[other]
                for k in range(2 * planes):
                    ref = (gate_ref, up_ref)[k // planes]
                    chip = h * planes + k % planes
                    first = (2 * chip + core) * 2 * block + me.s * block
                    copy = pltpu.make_async_copy(
                        ref.at[:, pl.ds(pl.multiple_of(first, LANES), block)],
                        dst.at[:, pl.ds(k * block, block)],
                        fetch.at[3 + (other * 2 + h) * 2 * planes + k],
                    )
                    copy.start()
                    units_in.append(copy)
        own_down = down_ref.at[pl.ds(pl.multiple_of(me.s * block, STRIP), block)]
        keep_d = pltpu.make_async_copy(own_down, dn_slots(me.p), local.at[2])
        keep_d.start()
        keep_g = pltpu.make_async_copy(g_loc, tok(g_all).at[me.rank], local.at[3])
        keep_g.start()

        same = lax.broadcasted_iota(jnp.int32, (depth, depth), 0) == lax.broadcasted_iota(jnp.int32, (depth, depth), 1)
        for k, ref in enumerate((ga_ref, gm_ref)):
            column = jnp.sum(jnp.where(same, ref[...].astype(F32), 0.0), 1, keepdims=True)
            gains[k] = jnp.broadcast_to(column, (depth, LANES))
        row = lax.broadcasted_iota(jnp.int32, (heads4, 4 * LANES), 0)
        lane = lax.broadcasted_iota(jnp.int32, (heads4, 4 * LANES), 1)
        shift = sum(jnp.where(row >= k * HD, LANES - HD, 0) for k in range(1, 4))
        sel_ref[...] = jnp.where(lane == row + shift, 1.0, 0.0).astype(BF)

        for copy in heads_in:
            copy.wait()
        gain = gains[0][:, 0:1]
        tiles = lambda first, count: [
            stage[:, first + k * LANES:first + (k + 1) * LANES].astype(F32) * gain for k in range(count)
        ]
        queries = tiles(0, 6)
        k0, k1, k2 = tiles(2 * q_own, 3)
        v0, v1, v2 = tiles(2 * q_own + 2 * k_own, 3)
        rolled = lambda value: pltpu.roll(value, LANES // 2, 1)
        in_low = lax.broadcasted_iota(jnp.int32, (depth, LANES), 1) < LANES // 2
        join = lambda first, second: jnp.where(in_low, first, second)
        shares = (
            queries[:3] + [k0, join(k1, rolled(v0)), join(rolled(v0), rolled(v1))],
            queries[3:] + [join(rolled(k1), rolled(k2)), join(rolled(k2), v1), v2],
        )
        for core in range(2):
            value = low(jnp.concatenate(shares[core], 1))

            @pl.when(me.c == core)
            def _():
                core_rows(qkv_all)(me.c)[...] = value

            @pl.when(me.c != core)
            def _():
                q_share[...] = value

        met()
        push(q_share, core_rows(qkv_all)(me.c), q_split[1], q_split[2], me.core).start()
        here = me.s == me.z // 2
        owner = me.z == me.rank
        lender = jnp.logical_and(here, jnp.logical_not(owner))
        half = lambda y: out_all.at[pl.ds(pl.multiple_of(y * 2 * head, STRIP), 2 * head)]
        head_rows = lambda core: out_all.at[pl.ds(pl.multiple_of((2 * me.y + core) * head, STRIP), head)]
        keep_o = pltpu.make_async_copy(out_loc, head_rows(me.c), local.at[1])

        @pl.when(owner)
        def _():
            keep_o.start()

        @pl.when(lender)
        def _():
            push(out_loc, head_rows(me.c), edge.at[0], edge.at[1], me.core).start()

        fetch_x.wait()

        def first_norm(strip):
            value = last_f[strip, :].astype(F32)
            n_buf[pl.ds(pl.multiple_of(me.rank * rows + strip.start, STRIP), STRIP), :] = low(value * inv_rms(value))

        strips(rows, first_norm)
        group_start(me, tok(n_buf).at[me.rank], tok(n_buf), *n_sems)
        arrived(core_rows(qkv_all)(1 - me.c), q_split[2], me.core)
        line_start(me, q_slots, q_line)

        away, home = 1 - me.s, me.s

        def weigh_units():
            for copy in units_in:
                copy.wait()

            def weigh(i, carry):
                strip = pl.ds(pl.multiple_of(i * STRIP, STRIP), STRIP)
                gain = gains[1, strip, 0:1]
                for h in range(2):
                    for ref in (core_rows(gu_all.at[h])(me.c), gu_share[h]):
                        ref[strip, :] = low(ref[strip, :].astype(F32) * gain)
                return carry

            lax.fori_loop(0, depth // STRIP, weigh, 0)
            for h in range(2):
                push(gu_share[h], core_rows(gu_all.at[h])(me.c), gu_split[h][1], gu_split[h][2], me.core).start()
            group_start(me, g_loc, tok(g_all), *g_sems)

        fan_in, fan_right, fan_left, fan_side, fan_other = [o_fan.at[k] for k in range(5)]
        bit = lambda y, q: out_all.at[pl.ds(pl.multiple_of(y * 2 * head + q * piece, STRIP), piece)]
        go_right = jnp.logical_and(me.z >= me.rank, me.has_right)
        go_left = jnp.logical_and(me.z <= me.rank, me.has_left)

        def fan(q):
            mine = bit(me.y, q)

            @pl.when(me.z > me.rank)
            def _():
                arrived(mine, fan_in.at[q], me.left)

            @pl.when(me.z < me.rank)
            def _():
                arrived(mine, fan_in.at[q], me.right)

            @pl.when(go_right)
            def _():
                push(mine, mine, fan_right.at[q], fan_in.at[q], me.right).start()

            @pl.when(go_left)
            def _():
                push(mine, mine, fan_left.at[q], fan_in.at[q], me.left).start()

            push(mine, mine, fan_side.at[q], fan_other.at[q], me.side).start()

        def own_heads():
            @pl.when(owner)
            def _():
                keep_o.wait()
                arrived(head_rows(1 - me.c), edge.at[1], me.core)

            @pl.when(lender)
            def _():
                left_over(out_loc, edge.at[0], me.core)

        def ends(h):
            arrived(core_rows(gu_all.at[h])(1 - me.c), gu_split[h][2], me.core)
            line_ends(me, gu_slots[h], gu_line[h])

        def dn_ends():
            keep_d.wait()
            line_ends(me, dn_slots, dn_line)

        saved = pltpu.make_async_copy(n_buf, stash, local.at[0])
        fetch_n = pltpu.make_async_copy(stash, n_buf, local.at[0])

        def normed_here():
            group_finish(me, tok(n_buf).at[me.rank], tok(n_buf), *n_sems)
            left_over(q_share, q_split[1], me.core)
            for h in range(2):
                left_over(gu_share[h], gu_split[h][1], me.core)
            saved.start()

        def widen_weights():
            def widen(i, carry):
                feats = pl.ds(pl.multiple_of(i * tile, tile), tile)
                for k in range(2):
                    g_gu[feats, k * 4 * LANES:(k + 1) * 4 * LANES] = low(
                        dot32(qkv_all[feats, k * heads4:(k + 1) * heads4], sel_ref[...])
                    )
                return carry

            lax.fori_loop(0, width // tile, widen, 0)

        def project_tokens():
            def project(i, carry):
                toks = pl.ds(pl.multiple_of(i * length, length), length)
                n = n_buf[toks, :]
                tabs = [tab_ref[k] for k in range(3)]
                for k in range(8):
                    value = dot32(n, g_gu[:, k * LANES:(k + 1) * LANES])
                    heads[toks, k * LANES:(k + 1) * LANES] = low(turn(value, tabs, 1.0) if k < 6 else value)
                return carry

            lax.fori_loop(0, total // length, project, 0)

        def heads_here():
            saved.wait()
            for q in range(PIECES):
                arrived(bit(1 - me.y, q), fan_other.at[q], me.side)

        def pair(toks, j, ref, start):
            first = start + 2 * j * LANES
            return jnp.concatenate(
                [ref[toks, first:first + LANES], ref[toks, first + LANES:first + 2 * LANES]], 0
            )

        def probabilities(toks, j):
            q = pair(toks, j, heads, 0)
            k = heads[toks, (4 + j) * LANES:(5 + j) * LANES]
            scores = HD ** (-0.5) * dot_t(q, k)
            row = lax.rem(lax.broadcasted_iota(jnp.int32, scores.shape, 0), length)
            col = lax.broadcasted_iota(jnp.int32, scores.shape, 1)
            scores = jnp.where(row >= col, scores, -jnp.inf)
            exps = jnp.exp(scores - jnp.max(scores, 1, keepdims=True))
            return q, k, exps / jnp.sum(exps, 1, keepdims=True)

        def attend_rows(first):
            def one(i, carry):
                toks = pl.ds(pl.multiple_of(first + i * length, length), length)
                outs = []
                for j in range(2):
                    _, _, p = probabilities(toks, j)
                    o = low(dot32(low(p), heads[toks, (6 + j) * LANES:(7 + j) * LANES]))
                    outs += [o[:length], o[length:]]
                mixed[toks, :] = low(dot_t(jnp.concatenate(outs, 1), sel_ref[...]))
                return carry

            lax.fori_loop(0, rows // length, one, 0)
            toks = pl.ds(pl.multiple_of(first, rows), rows)
            part[toks, :] = low(dot32(mixed[toks, :], out_all[...]))

        def mine(strip):
            return pl.ds(pl.multiple_of(me.rank * rows + strip.start, STRIP), STRIP)

        def summed(strip, whole, some, rest):
            return (
                whole[mine(strip), :].astype(F32)
                + some[me.s, strip, :].astype(F32)
                + rest[strip, :].astype(F32)
            )

        def middle(strip):
            value = last_f[strip, :].astype(F32) + summed(strip, part, got, last)
            x1[strip, :] = value
            n_buf[mine(strip), :] = low(value * inv_rms(value))

        def first_sum():
            blocks_finish(me, tok(part), got, last, *x_sems)
            strips(rows, middle)
            group_start(me, tok(n_buf).at[me.rank], tok(n_buf), *m_sems)

        def cot_here():
            keep_g.wait()
            group_finish(me, g_loc, tok(g_all), *g_sems)

        def heads_left():
            for q in range(PIECES):
                left_over(bit(me.y, q), fan_side.at[q], me.side)

                @pl.when(go_right)
                def _():
                    left_over(bit(me.y, q), fan_right.at[q], me.right)

                @pl.when(go_left)
                def _():
                    left_over(bit(me.y, q), fan_left.at[q], me.left)

        def activations(h, j):
            first = h * half_units + j * chunk

            def step(t, carry):
                toks = pl.ds(pl.multiple_of(t * tile, tile), tile)
                n, g = n_buf[toks, :], g_all[toks, :]
                gate = dot32(n, gu_all[h, :, j * chunk:(j + 1) * chunk])
                up = dot32(n, gu_all[h, :, half_units + j * chunk:half_units + (j + 1) * chunk])
                grad = dot_t(g, dn_all[first:first + chunk, :])
                hidden, d_gate, d_up = mlp_grads(gate, up, grad)
                mid[toks, first:first + chunk] = hidden
                dgu[h, toks, j * chunk:(j + 1) * chunk] = d_gate
                dgu[h, toks, half_units + j * chunk:half_units + (j + 1) * chunk] = d_up
                return carry

            lax.fori_loop(0, total // tile, step, 0)

        def weight_grads(h, out):
            def step(i, carry):
                feats = pl.ds(pl.multiple_of(i * chunk, chunk), chunk)
                out[feats, :] = low(dot_l(n_buf[:, feats], dgu[h]))
                return carry

            lax.fori_loop(0, width // chunk, step, 0)

        own_gu = [by_chip(g_gu, 2 * depth), gu_slots[0]]
        finals = [gu_buf[h][0].at[me.z] for h in range(2)]

        def back(seq):
            toks = pl.ds(pl.multiple_of(seq * tile, tile), tile)

            def step(i, carry):
                feats = pl.ds(pl.multiple_of(i * chunk, chunk), chunk)
                value = dot_t(dgu[0, toks, :], gu_all[0, feats, :]) + dot_t(dgu[1, toks, :], gu_all[1, feats, :])
                part[toks, feats] = low(value)
                return carry

            lax.fori_loop(0, width // chunk, step, 0)

        def second_grads():
            weight_grads(1, gu_all.at[0])
            fetch_n.start()

        def outward():
            def forth(i, carry):
                feats = pl.ds(pl.multiple_of(i * chunk, chunk), chunk)
                out_part[:, feats] = low(dot32(mid[...], dn_all[:, feats]))
                return carry

            lax.fori_loop(0, width // chunk, forth, 0)
            for i in range(2):
                blocks_start(me, tok(out_part), got_f, *f_sems, i)

        def branch(strip):
            grad = norm_back(x1[strip, :], summed(strip, part, got, last), g_all[mine(strip), :].astype(F32))
            dx_all[mine(strip), :] = low(grad)

        def second_sum():
            blocks_finish(me, tok(part), got, last, *b_sems)
            strips(rows, branch)
            group_start(me, tok(dx_all).at[me.rank], tok(dx_all), *d_sems)

        def down_grads():
            def down(i, carry):
                these = pl.ds(pl.multiple_of(i * chunk, chunk), chunk)
                dn_all[these, :] = low(dot_l(mid[:, these], g_all[...]))
                return carry

            lax.fori_loop(0, units // chunk, down, 0)

        def spread_grads():
            def spread_out(t, carry):
                toks = pl.ds(pl.multiple_of(t * rows, rows), rows)
                grad = low(dot_t(dx_all[toks, :], out_all[...]))
                mid[toks, 0:4 * LANES] = low(dot32(grad, sel_ref[...]))
                return carry

            lax.fori_loop(0, 4, spread_out, 0)

        def out_grads():
            out_all[...] = low(dot_l(mixed[...], dx_all[...]))
            for q in range(PIECES):
                push(bit(1 - me.y, q), o_buf[0].at[pl.ds(q * piece, piece)], o_red.at[0, q], o_red.at[1, q], me.side).start()

        def attend_rows_back(first):
            def one(i, carry):
                toks = pl.ds(pl.multiple_of(first + i * length, length), length)
                tabs = [tab_ref[k] for k in range(3)]
                for j in range(2):
                    q, k, p = probabilities(toks, j)
                    v = heads[toks, (6 + j) * LANES:(7 + j) * LANES]
                    grad = pair(toks, j, mid, 0)
                    d_v = dot_l(low(p), grad)
                    d_p = dot_t(grad, v)
                    d_s = low(p * (d_p - jnp.sum(p * d_p, 1, keepdims=True)))
                    d_q = HD ** (-0.5) * dot32(d_s, k)
                    d_k = HD ** (-0.5) * dot_l(d_s, q)
                    for g in range(2):
                        spot = (2 * j + g) * LANES
                        dgu[0, toks, spot:spot + LANES] = low(turn(d_q[g * length:(g + 1) * length], tabs, -1.0))
                    dgu[0, toks, (4 + j) * LANES:(5 + j) * LANES] = low(turn(d_k, tabs, -1.0))
                    dgu[0, toks, (6 + j) * LANES:(7 + j) * LANES] = low(d_v)
                return carry

            lax.fori_loop(0, rows // length, one, 0)
            toks = pl.ds(pl.multiple_of(first, rows), rows)
            for k in range(2):
                dgu[1, toks, k * heads4:(k + 1) * heads4] = low(
                    dot_t(dgu[0, toks, k * 4 * LANES:(k + 1) * 4 * LANES], sel_ref[...])
                )
            part[toks, :] = low(dot_t(dgu[1, toks, 0:q_cols], qkv_all[...]))

        def in_grads():
            fetch_n.wait()

            def q_grads(i, carry):
                feats = pl.ds(pl.multiple_of(i * chunk, chunk), chunk)
                qkv_all[feats, :] = low(dot_l(n_buf[:, feats], dgu[1, :, 0:q_cols]))
                return carry

            lax.fori_loop(0, width // chunk, q_grads, 0)

        o_sum = lambda q: o_buf[0].at[pl.ds(q * piece, piece)]
        o_left = lambda q: o_buf[1].at[pl.ds(q * piece, piece)]
        o_right = lambda q: o_buf[2].at[pl.ds(q * piece, piece)]

        def o_on(q):
            @pl.when(me.z < me.rank)
            def _():
                push(o_sum(q), o_left(q), o_red.at[4, q], o_red.at[2, q], me.right).start()

            @pl.when(me.z > me.rank)
            def _():
                push(o_sum(q), o_right(q), o_red.at[4, q], o_red.at[3, q], me.left).start()

        from_left = jnp.logical_and(me.has_left, me.z <= me.rank)
        from_right = jnp.logical_and(me.has_right, me.z >= me.rank)
        no_more = jnp.logical_not(jnp.logical_or(from_left, from_right))

        def o_y(q):
            arrived(o_sum(q), o_red.at[1, q], me.side)
            add_into(o_sum(q), bit(me.y, q))

            @pl.when(no_more)
            def _():
                o_on(q)

        def o_z(q):
            @pl.when(from_left)
            def _():
                arrived(o_left(q), o_red.at[2, q], me.left)
                add_into(o_sum(q), o_left(q))

            @pl.when(from_right)
            def _():
                arrived(o_right(q), o_red.at[3, q], me.right)
                add_into(o_sum(q), o_right(q))

            @pl.when(jnp.logical_not(no_more))
            def _():
                o_on(q)

        own_half = o_buf[0].at[pl.ds(pl.multiple_of(me.c * head, STRIP), head)]
        other_half = o_buf[0].at[pl.ds(pl.multiple_of((1 - me.c) * head, STRIP), head)]
        o_keep, o_send, o_recv = o_deal
        keep_oo = pltpu.make_async_copy(own_half, out_out, o_keep)


        def o_end():
            @pl.when(owner)
            def _():
                keep_oo.start()
                push(other_half, out_out, o_send.at[0], o_recv.at[0], me.core).start()
                push(own_half, out_out, o_send.at[1], o_recv.at[0], me.across).start()
                push(other_half, out_out, o_send.at[2], o_recv.at[0], me.corner).start()

        def output(strip):
            got_f[me.s, strip, :] = low(x1[strip, :] + summed(strip, out_part, got_f, last_f))

        def third_sum():
            blocks_finish(me, tok(out_part), got_f, last_f, *f_sems)
            strips(rows, output)
            pltpu.make_async_copy(got_f.at[me.s], bo_ref, local.at[1]).start()
            fetch_x.start()

        def inner(strip):
            got[me.s, strip, :] = low(norm_back(
                last_f[strip, :].astype(F32), summed(strip, part, got, last), dx_all[mine(strip), :].astype(F32)
            ))

        def fourth_sum():
            blocks_finish(me, tok(part), got, last, *h_sems)
            fetch_x.wait()
            strips(rows, inner)
            pltpu.make_async_copy(got.at[me.s], gx_ref, local.at[2]).start()

        final_dn = dn_buf[0].at[me.z]
        final_q = [q_buf[k][0].at[me.z] for k in range(2)]
        own_q = [functools.partial(lambda k, chip: core_rows_of(chip, k), k) for k in range(2)]
        q_keep, q_send, q_recv = q_deal

        def core_rows_of(chip, core):
            return qkv_all.at[pl.ds(pl.multiple_of((2 * chip + core) * depth, STRIP), depth)]

        def q_end(core):
            @pl.when(me.c == core)
            def _():
                pltpu.make_async_copy(final_q[core], qkv_out.at[me.rank], q_keep).start()
                push(final_q[core], qkv_out.at[me.rank], q_send.at[0], q_recv.at[0], me.across).start()

            @pl.when(me.c != core)
            def _():
                push(final_q[core], qkv_out.at[me.rank], q_send.at[1], q_recv.at[1], me.core).start()
                push(final_q[core], qkv_out.at[me.rank], q_send.at[2], q_recv.at[2], me.corner).start()
        dn_keep, dn_send, dn_recv = dn_deal

        def dn_end():
            pltpu.make_async_copy(final_dn, dn_out.at[me.s], dn_keep).start()
            push(final_dn, dn_out.at[me.s], dn_send, dn_recv, me.across).start()

        steps = {
            "weigh": weigh_units, "own": own_heads, "rn": lambda: group_relay(me, tok(n_buf), *n_sems),
            "Ae": lambda: ends(0), "Be": lambda: ends(1), "De": dn_ends, "nf": normed_here,
            "widen": widen_weights, "project": project_tokens, "oh": heads_here,
            "rg": lambda: group_relay(me, tok(g_all), *g_sems), "gf": cot_here, "ol": heads_left,
            "xs": first_sum, "rm": lambda: group_relay(me, tok(n_buf), *m_sems),
            "mf": lambda: group_finish(me, tok(n_buf).at[me.rank], tok(n_buf), *m_sems),
            "w0": lambda: weight_grads(0, g_gu), "w1": second_grads,
            "b0": lambda: back(away), "b1": lambda: back(home), "fo": outward, "bs": second_sum, "dw": down_grads,
            "rx": lambda: group_relay(me, tok(dx_all), *d_sems),
            "xf": lambda: group_finish(me, tok(dx_all).at[me.rank], tok(dx_all), *d_sems),
            "sp": spread_grads, "go": out_grads, "qg": in_grads, "oe": o_end, "fs": third_sum, "hs": fourth_sum,
            "fc": lambda: blocks_cross(me, tok(out_part), got_f, last_f, *f_sems),
            "de": dn_end, "ae": lambda: deal_start(me, finals[0], depth, gu_out.at[0], *gu_deal[0]),
            "be": lambda: deal_start(me, finals[1], depth, gu_out.at[1], *gu_deal[1]),
            "qe": lambda: q_end(0), "je": lambda: q_end(1),
        }
        for key, slots, line in (
            ("Q", q_slots, q_line), ("A", gu_slots[0], gu_line[0]), ("B", gu_slots[1], gu_line[1]), ("D", dn_slots, dn_line)
        ):
            steps[key + "s"] = functools.partial(line_side, me, slots, line)
            steps[key + "t"] = functools.partial(line_twin, me, slots, line)
            steps[key + "f"] = functools.partial(line_finish, me, slots, line)
            for hop in range(1, planes):
                steps[key + str(hop)] = functools.partial(line_hop, me, slots, line, hop)
        for key, own, buffers, sems in (
            ("a", own_gu[0], gu_buf[0], gu_sems[0]), ("b", own_gu[1], gu_buf[1], gu_sems[1]),
            ("d", dn_slots, dn_buf, dn_sems), ("q", own_q[0], q_buf[0], q_sems[0]), ("j", own_q[1], q_buf[1], q_sems[1]),
        ):
            steps[key + "r0"] = functools.partial(reduce_start, me, own, buffers[0], sems, [0])
            steps[key + "r1"] = functools.partial(reduce_start, me, own, buffers[0], sems, range(1, planes))
            steps[key + "m"] = functools.partial(reduce_mix, me, own, buffers[0], sems)
            for i in range(planes):
                steps[key + "y" + str(i)] = functools.partial(reduce_y, me, own, *buffers, sems, i)
                steps[key + "z" + str(i)] = functools.partial(reduce_z, me, *buffers, sems, i)
        for i in range(PIECES):
            steps["f" + str(i)] = functools.partial(fan, i)
            steps["oy" + str(i)] = functools.partial(o_y, i)
            steps["oz" + str(i)] = functools.partial(o_z, i)
        for i, (seq, core) in enumerate(((away, 1 - me.c), (away, me.c), (home, 1 - me.c), (home, me.c))):
            steps["t" + str(i)] = functools.partial(attend_rows, (2 * seq + core) * rows)
            steps["h" + str(i)] = functools.partial(attend_rows_back, (2 * seq + core) * rows)
        for key, whole, some, rest, sems in (
            ("x", part, got, last, x_sems), ("p", part, got, last, b_sems), ("k", part, got, last, h_sems)
        ):
            for i in range(2):
                steps[key + str(i)] = functools.partial(blocks_start, me, tok(whole), some, *sems, i)
            steps[key + "c"] = functools.partial(blocks_cross, me, tok(whole), some, rest, *sems)
        for h in range(2):
            for j in range(half_units // chunk):
                steps["uv"[h] + str(j)] = functools.partial(activations, h, j)
        for name in SCHEDULE:
            steps[name]()

        for h in range(2):
            reduce_finish(me, own_gu[h], gu_buf[h][0], gu_sems[h])
            deal_finish(me, finals[h], depth, gu_out.at[h], *gu_deal[h])
        reduce_finish(me, dn_slots, dn_buf[0], dn_sems)
        for k in range(2):
            reduce_finish(me, own_q[k], q_buf[k][0], q_sems[k])
        for q in range(PIECES):
            sum_q = o_sum(q)
            left_over(bit(1 - me.y, q), o_red.at[0, q], me.side)

            @pl.when(me.z < me.rank)
            def _():
                left_over(sum_q, o_red.at[4, q], me.right)

            @pl.when(me.z > me.rank)
            def _():
                left_over(sum_q, o_red.at[4, q], me.left)

        @pl.when(owner)
        def _():
            keep_oo.wait()
            left_over(other_half, o_send.at[0], me.core)
            left_over(own_half, o_send.at[1], me.across)
            left_over(other_half, o_send.at[2], me.corner)

        @pl.when(jnp.logical_not(owner))
        def _():
            arrived(out_out, o_recv.at[0], me.core)

        pltpu.make_async_copy(final_dn, dn_out.at[me.s], dn_keep).wait()
        left_over(final_dn, dn_send, me.across)
        arrived(dn_out.at[1 - me.s], dn_recv, me.across)
        pltpu.make_async_copy(got_f.at[me.s], bo_ref, local.at[1]).wait()
        pltpu.make_async_copy(got.at[me.s], gx_ref, local.at[2]).wait()

        for core in range(2):

            @pl.when(me.c == core)
            def _():
                pltpu.make_async_copy(final_q[core], qkv_out.at[me.rank], q_keep).wait()
                left_over(final_q[core], q_send.at[0], me.across)

            @pl.when(me.c != core)
            def _():
                left_over(final_q[core], q_send.at[1], me.core)
                left_over(final_q[core], q_send.at[2], me.corner)

        arrived(qkv_out.at[2 * (1 - me.s) + me.c], q_recv.at[0], me.across)
        arrived(qkv_out.at[2 * me.s + 1 - me.c], q_recv.at[1], me.core)
        arrived(qkv_out.at[2 * (1 - me.s) + 1 - me.c], q_recv.at[2], me.corner)

    sems = lambda *dims: pltpu.SemaphoreType.DMA(dims)
    one, three = pltpu.SemaphoreType.DMA, sems(3)
    vmem = lambda *dims: pltpu.VMEM(dims, BF)
    deal = [one, three, three]
    outs = comm_call(
        kernel, 0,
        [shape((rows, width)), shape((rows, width)), shape((4, depth, q_cols)), shape((head, width)),
         shape((2, 4, depth, cols)), shape((2, block, width)), shape((total, width))],
        [ANY] * 7,
        [(ANY, ref) for ref in (tokens, cot, w_query, w_key, w_value, w_out, w_gate, w_up, w_down)]
        + [(VMEM, gain_attn), (VMEM, gain_mlp), (VMEM, head_tables(length))],
        [vmem(total, width), vmem(total, width), vmem(width, q_cols), vmem(heads4, width), vmem(2, width, cols),
         vmem(units, width), vmem(total, 8 * LANES), vmem(total, heads4)]
        + [vmem(total, width), vmem(total, width), pltpu.VMEM((rows, width), F32), vmem(total, units),
           vmem(2, total, cols), vmem(width, cols), vmem(total, width)]
        + blocks_buffers(rows, width) * 2
        + reduce_buffers(planes, 2 * depth, cols) * 2 + reduce_buffers(planes, block, width)
        + reduce_buffers(planes, depth, q_cols) * 2 + [vmem(2 * head, width)] * 3
        + group_sems() * 4 + blocks_sems() * 4 + [one] * 9
        + line_sems(planes) * 4 + reduce_sems(planes) * 5 + deal * 2 + [one] * 3 + deal * 2
        + [sems(5), sems(2), sems(5, PIECES), sems(5, PIECES), sems(3 + 8 * planes), vmem(heads4, 4 * LANES),
           pltpu.VMEM((2, depth, LANES), F32)],
        "block_step",
    )
    return outs[:6]


def finish(planes, parts, weights, gains):
    block_out, grad_tokens, own_qkv, own_out, own_gu, own_dn = parts
    w_query, w_key, w_value, w_gate, w_up = weights
    rows, width = block_out.shape
    depth, hidden = w_gate.shape
    q_own, k_own = w_query.shape[1] // 4, w_key.shape[1] // 4
    block = own_dn.shape[1]
    per = 4
    steps = 2 * planes // per
    wide = hidden // steps
    own_dn = own_dn.reshape(2 * block, width)

    def kernel(bo_ref, gx_ref, qkv_ref, out_ref, gate_ref, up_ref, dn_ref, wq_ref, wk_ref, wv_ref, wg_ref, wu_ref,
               ga_ref, gm_ref, bo_out, gx_out, q_out, k_out, v_out, o_out, gate_out, up_out, dn_out, ga_out, gm_out,
               columns, total):
        step = pl.program_id(0)
        same = lax.broadcasted_iota(jnp.int32, (depth, depth), 0) == lax.broadcasted_iota(jnp.int32, (depth, depth), 1)

        def as_row(value):
            return jnp.sum(jnp.where(same, jnp.sum(value, 1, keepdims=True), 0.0), 0, keepdims=True)

        @pl.when(step == 0)
        def _():
            for k, ref in enumerate((ga_ref, gm_ref)):
                column = jnp.sum(jnp.where(same, ref[...].astype(F32), 0.0), 1, keepdims=True)
                columns[k] = jnp.broadcast_to(column, (depth, LANES))
            total[...] = jnp.zeros_like(total)
            o_out[...] = out_ref[...].astype(F32)
            gain = columns[0]
            gathered = jnp.zeros((depth, LANES), F32)

            def put(out, weight, tile, value):
                lanes = slice(tile * LANES, (tile + 1) * LANES)
                out[:, lanes] = value * gain
                return value * weight[:, lanes].astype(F32)

            rolled = lambda value: pltpu.roll(value, LANES // 2, 1)
            in_low = lax.broadcasted_iota(jnp.int32, (depth, LANES), 1) < LANES // 2
            join = lambda first, second: jnp.where(in_low, first, second)
            for rank in range(4):
                for k in range(q_own // LANES):
                    value = qkv_ref[rank, :, k * LANES:(k + 1) * LANES].astype(F32)
                    gathered += put(q_out, wq_ref, rank * q_own // LANES + k, value)
            for seq in range(2):
                (a0, a1, a2), (b0, b1, b2) = [
                    [qkv_ref[2 * seq + core, :, q_own + k * LANES:q_own + (k + 1) * LANES].astype(F32) for k in range(3)]
                    for core in range(2)
                ]
                keys = [a0, join(a1, rolled(b0)), join(rolled(b0), rolled(b1))]
                values = [join(rolled(a1), rolled(a2)), join(rolled(a2), b1), b2]
                for k in range(3):
                    gathered += put(k_out, wk_ref, 3 * seq + k, keys[k])
                    gathered += put(v_out, wv_ref, 3 * seq + k, values[k])
            ga_out[...] = as_row(gathered)

        bo_out[...] = bo_ref[...]
        gx_out[...] = gx_ref[...]
        dn_out[...] = dn_ref[...].astype(F32)
        gain = columns[1]
        gathered = jnp.zeros((depth, LANES), F32)
        for ref, out, weight in ((gate_ref, gate_out, wg_ref), (up_ref, up_out, wu_ref)):
            for k in range(4 * per):
                chip, core, seq = k // 4, k // 2 % 2, k % 2
                lanes = slice(k * block, (k + 1) * block)
                value = ref[0, 2 * seq + core, :, chip * block:(chip + 1) * block].astype(F32)
                out[:, lanes] = value * gain
                gathered += value * weight[:, lanes].astype(F32)
        total[...] += gathered

        @pl.when(step == steps - 1)
        def _():
            gm_out[...] = as_row(total[...])

    whole = lambda ref: pl.BlockSpec(ref.shape, lambda p: (0,) * len(ref.shape))
    strip = lambda ref: pl.BlockSpec((ref.shape[0] // steps, ref.shape[1]), lambda p: (p, 0))
    runs = planes // per
    part = lambda first: pl.BlockSpec((1, 4, depth, per * block), lambda p: (p // runs, 0, 0, first + p % runs))
    slab = pl.BlockSpec((depth, wide), lambda p: (0, p))
    outs = [shape(block_out.shape), shape(grad_tokens.shape), shape(w_query.shape, F32), shape(w_key.shape, F32),
            shape(w_value.shape, F32), shape(own_out.shape, F32), shape(w_gate.shape, F32), shape(w_up.shape, F32),
            shape(own_dn.shape, F32), shape((1, depth), F32), shape((1, depth), F32)]
    return pl.pallas_call(
        kernel,
        grid=(steps,),
        out_shape=outs,
        in_specs=[strip(block_out), strip(grad_tokens), whole(own_qkv), whole(own_out), part(0), part(runs),
                  strip(own_dn), whole(w_query), whole(w_key), whole(w_value), slab, slab, whole(gains[0]), whole(gains[1])],
        out_specs=[strip(outs[0]), strip(outs[1])] + [whole(o) for o in outs[2:6]]
        + [slab, slab, strip(outs[8]), whole(outs[9]), whole(outs[10])],
        scratch_shapes=[pltpu.VMEM((2, depth, LANES), F32), pltpu.VMEM((depth, LANES), F32)],
        name="finish",
    )(block_out, grad_tokens, own_qkv, own_out, own_gu, own_gu, own_dn, w_query, w_key, w_value, w_gate, w_up, *gains)


def shards_fast(tokens, cotangent, w_query, w_key, w_value, w_out, w_gate, w_up, w_down, gain_attn, gain_mlp):
    seqs, length, width = tokens.shape
    rows = seqs * length
    depth = w_query.shape[0]
    planes = width // depth // 4
    x, cot = tokens.reshape(rows, width), cotangent.reshape(rows, width)
    gains = (gain_attn.reshape(1, depth), gain_mlp.reshape(1, depth))
    parts = block_step(planes, length, x, cot, w_query, w_key, w_value, w_out, w_gate, w_up, w_down, *gains)
    outs = finish(planes, parts, (w_query, w_key, w_value, w_gate, w_up), gains)
    return (
        outs[0].reshape(tokens.shape), outs[1].reshape(tokens.shape), *outs[2:9],
        outs[9].reshape(depth), outs[10].reshape(depth),
    )


def fits(mesh):
    return mesh.shape["seq"] == 2 and mesh.shape["dp"] == 16


def solution(mesh):
    body = shards_fast if fits(mesh) else shards_plain
    return jax.shard_map(body, mesh=mesh, in_specs=IN_SPECS, out_specs=OUT_SPECS, check_vma=False)
```
